32 devices in a mesh: dev: 32 (over z, y, x, core).
Axes of the slice: x: 2, y: 2, z: 4, core: 2. Of those that a mesh axis runs over, the one named last changes fastest.
Arguments:
- tokens: bfloat16 [4608, 1536], P('dev'), may hold values from -6 to 6
- conditioning: bfloat16 [4, 1536], replicated, may hold values from -5 to 5
- text_lengths: int32 [4], replicated, may hold values from 86 to 154, as said below
- modulation_weight: bfloat16 [3072, 9216], P('dev'), may hold values from -0.15625 to 0.15625
- project_weight: bfloat16 [3072, 4608], P('dev'), may hold values from -1 to 1
- merge_weight: bfloat16 [3072, 1536], P('dev'), may hold values from -1.25 to 1.25
- up_weight: bfloat16 [3072, 6144], P('dev'), may hold values from -0.15625 to 0.15625
- down_weight: bfloat16 [12288, 1536], P('dev'), may hold values from -0.078125 to 0.078125
- cotangent: bfloat16 [4608, 1536], P('dev'), may hold values from -6 to 6
Outputs:
- layer_out: bfloat16 [4608, 1536], P('dev')
- tokens_grad: float32 [4608, 1536], P('dev')
- conditioning_grad: float32 [4, 1536], replicated
- modulation_grad: float32 [3072, 9216], P('dev')
- project_grad: float32 [3072, 4608], P('dev')
- merge_grad: float32 [3072, 1536], P('dev')
- up_grad: float32 [3072, 6144], P('dev')
- down_grad: float32 [12288, 1536], P('dev')
The draws below stay inside these ranges and needn't reach their ends.
Inputs may be any that keep to these rules, and one draw needn't show every extreme that they name: `text_lengths`: the text tokens of all sequences sum to 512, so that the sequences fill the packed rows exactly; one sequence has exactly 154 text tokens.
All inputs are finite; a program needn't handle non-finite values.
Results may differ from the reference program's by a relative error of at most 0.025.
The reference program's roundings to bfloat16 on the way count: a program that leaves them out, or rounds other values in their place, can miss the bound.
Values may be sent and summed in bfloat16 or wider, within the bound.
A program may use at most 576 MiB of HBM per device.

```python
import jax
import jax.numpy as jnp
from jax import lax

D = 1536
HEADS = 24
HDIM = 64
FF = 6144
IMG = 1024
TXT = 154
TOKENS = 4608
SEQS = 4


def draw_tokens(key, part):
    noise = jax.random.normal(jax.random.fold_in(key, 101), (TOKENS, D), jnp.float32)
    values = noise
    return jnp.clip(values, -6.0, 6.0).astype(jnp.bfloat16)


def draw_project_weight(key, part):
    base = jax.random.normal(jax.random.fold_in(key, 107), (2 * D, 3 * D), jnp.float32)
    values = jnp.clip(base, -6.0, 6.0) * D ** (-0.5)
    return values.astype(jnp.bfloat16)


def draw_text_lengths(key, part):
    remaining = TOKENS - SEQS * IMG - TXT
    others = SEQS - 1
    base_len = remaining // others
    extra_count = remaining % others
    spread_max = max(1, min(TXT - base_len - 1, base_len - 1, 48))
    key_bumps = jax.random.fold_in(key, 11)
    key_pick = jax.random.fold_in(key, 23)
    bump_vals = jax.random.randint(key_bumps, (others,), 0, spread_max)
    slot_index = jnp.arange(others, dtype=jnp.int32)
    bump_vals = jnp.where(slot_index == 0, 0, jnp.where(slot_index == 1, spread_max - 1, bump_vals)).astype(jnp.int32)
    text_vals = base_len + (slot_index >= others - extra_count).astype(jnp.int32) + bump_vals - jnp.roll(bump_vals, -1)
    pick_index = jax.random.randint(key_pick, (), 0, SEQS)
    seq_index = jnp.arange(SEQS, dtype=jnp.int32)
    from_left = text_vals[jnp.clip(seq_index, 0, others - 1)]
    from_right = text_vals[jnp.clip(seq_index - 1, 0, others - 1)]
    chosen = jnp.where(seq_index < pick_index, from_left, jnp.where(seq_index == pick_index, TXT, from_right))
    return chosen.astype(jnp.int32)


def block_levels(key, extent, cuts, smallest, high):
    loudness, own = 1.0, jax.random.fold_in(key, 6)
    for axis_at, shards_of in cuts:
        heights = jnp.exp(jax.random.uniform(jax.random.fold_in(own, axis_at), (shards_of,), jnp.float32, smallest / len(cuts), high / len(cuts)))
        loudness = loudness * jnp.repeat(heights, extent[axis_at] // shards_of).reshape([-1 if axis == axis_at else 1 for axis in range(len(extent))])
    return loudness


def normal_values(stream_key, extent, deviation, bound, cuts=(), held_as=jnp.bfloat16):
    loudness = block_levels(stream_key, extent, cuts, -0.22, 0.18) if cuts else 1.0
    drawn = jax.random.normal(stream_key, extent, jnp.float32) * deviation * loudness
    return jnp.minimum(jnp.maximum(drawn, -bound), bound).astype(held_as)


def setup_inputs(seed: int = 0) -> dict:
    key_list = jax.random.split(jax.random.key(seed), 10)
    return {
        "tokens": draw_tokens(jax.random.fold_in(key_list[9], 71), 0),
        "conditioning": normal_values(key_list[1], (SEQS, D), 1.0, 5.0),
        "text_lengths": draw_text_lengths(jax.random.fold_in(key_list[9], 71), 0),
        "modulation_weight": normal_values(key_list[3], (2 * D, 6 * D), D ** -0.5, 0.15625, ((0, 32),)),
        "project_weight": draw_project_weight(jax.random.fold_in(key_list[9], 71), 0),
        "merge_weight": normal_values(key_list[5], (2 * D, D), (D // 64) ** -0.5, 1.25, ((0, 32),)),
        "up_weight": normal_values(key_list[6], (2 * D, FF), D ** -0.5, 0.15625, ((0, 32),)),
        "down_weight": normal_values(key_list[7], (2 * FF, D), FF ** -0.5, 0.078125, ((0, 32),)),
        "cotangent": normal_values(key_list[8], (TOKENS, D), 1.0, 6.0, ((0, 32),)),
    }


HIGHEST_PRECISION = lax.Precision.HIGHEST
EPSILON = 1e-06

@jax.custom_vjp
def low(v):
    return lax.optimization_barrier(v.astype(jnp.bfloat16)).astype(jnp.float32)

@jax.custom_vjp
def low_back(v):
    return v

def low_keep(v):
    return (low(v), None)

def low_pass(kept, grad):
    return (grad,)

def back_keep(v):
    return (v, None)

def back_low(kept, grad):
    return (low(grad),)
low.defvjp(low_keep, low_pass)
low_back.defvjp(back_keep, back_low)

def layer_norm(values):
    mean = lax.optimization_barrier(jnp.mean(values, axis=-1, keepdims=True))
    centred = values - mean
    variance = lax.optimization_barrier(jnp.mean(centred * centred, axis=-1, keepdims=True))
    return centred * lax.rsqrt(variance + EPSILON)

def two_streams(rows, weight_pair):
    image_part = jnp.dot(rows[:IMG], weight_pair[0], precision=HIGHEST_PRECISION, preferred_element_type=jnp.float32)
    text_part = jnp.dot(rows[IMG:], weight_pair[1], precision=HIGHEST_PRECISION, preferred_element_type=jnp.float32)
    return jnp.concatenate([image_part, text_part], axis=0)

def sequence_layer(rows, mods, text_count, weights):
    project_pair, merge_pair, up_pair, down_pair = weights
    length = IMG + TXT
    row_index = jnp.arange(length, dtype=jnp.int32)
    is_text = (row_index >= IMG)[:, None]
    mod_rows = jnp.where(is_text, mods[1][None, :], mods[0][None, :])
    shift_a, scale_a, gate_a, shift_b, scale_b, gate_b = jnp.split(mod_rows, 6, axis=1)
    hidden_a = low(layer_norm(rows) * (1.0 + scale_a) + shift_a)
    projected = low_back(low(two_streams(hidden_a, project_pair)))
    queries, keys, values = jnp.split(projected, 3, axis=1)
    queries = queries.reshape(length, HEADS, HDIM)
    keys = keys.reshape(length, HEADS, HDIM)
    values = values.reshape(length, HEADS, HDIM)
    scores = jnp.einsum('qhd,khd->hqk', queries, keys, precision=HIGHEST_PRECISION) * HDIM ** (-0.5)
    scores = low_back(scores)
    key_valid = row_index < IMG + text_count
    masked = jnp.where(key_valid[None, None, :], scores, -jnp.inf)
    top = lax.optimization_barrier(jnp.max(masked, axis=-1, keepdims=True))
    exponent = jnp.exp(masked - top)
    probs = exponent / lax.optimization_barrier(jnp.sum(exponent, axis=-1, keepdims=True))
    attended = jnp.einsum('hqk,khd->qhd', low(probs), values, precision=HIGHEST_PRECISION).reshape(length, HEADS * HDIM)
    attended = low_back(low(attended))
    merged = low_back(two_streams(attended, merge_pair))
    middle = rows + gate_a * merged
    hidden_b = low(layer_norm(middle) * (1.0 + scale_b) + shift_b)
    upper = low_back(two_streams(hidden_b, up_pair))
    activated = low(jax.nn.gelu(upper, approximate=True))
    lowered = low_back(two_streams(activated, down_pair))
    return middle + gate_b * lowered

def reference(tokens, conditioning, text_lengths, modulation_weight, project_weight, merge_weight, up_weight, down_weight, cotangent):
    lengths = text_lengths.astype(jnp.int32)
    ends = jnp.cumsum(IMG + lengths).astype(jnp.int32)
    starts = jnp.concatenate([jnp.zeros((1,), jnp.int32), ends[:-1]])

    def forward(tokens_float, cond_float, mod_flat, project_flat, merge_flat, up_flat, down_flat):
        mod_pair = mod_flat.reshape(2, D, 6 * D)
        project_pair = project_flat.reshape(2, D, 3 * D)
        merge_pair = merge_flat.reshape(2, D, D)
        up_pair = up_flat.reshape(2, D, FF)
        down_pair = down_flat.reshape(2, FF, D)
        silu_low = low(jax.nn.silu(cond_float))
        mods = low_back(jnp.einsum('sd,jdc->sjc', silu_low, mod_pair, precision=HIGHEST_PRECISION))
        padded = jnp.concatenate([tokens_float, jnp.zeros((IMG + TXT, D), jnp.float32)], axis=0)
        layer_fn = jax.checkpoint(sequence_layer)

        def apply_one(carry, seq_index):
            start = starts[seq_index]
            rows = lax.dynamic_slice_in_dim(padded, start, IMG + TXT, 0)
            result = layer_fn(rows, mods[seq_index], lengths[seq_index], (project_pair, merge_pair, up_pair, down_pair))
            return (lax.dynamic_update_slice_in_dim(carry, result, start, 0), None)
        final, unused = lax.scan(apply_one, padded, jnp.arange(SEQS, dtype=jnp.int32))
        return final[:TOKENS]
    output, pullback = jax.vjp(forward, tokens.astype(jnp.float32), conditioning.astype(jnp.float32), modulation_weight.astype(jnp.float32), project_weight.astype(jnp.float32), merge_weight.astype(jnp.float32), up_weight.astype(jnp.float32), down_weight.astype(jnp.float32))
    grads = pullback(cotangent.astype(jnp.float32))
    return (output.astype(jnp.bfloat16), grads[0], grads[1], grads[2], grads[3], grads[4], grads[5], grads[6])
```

```python
import functools

import jax
import jax.numpy as jnp
import numpy as np
from jax import lax
from jax.experimental import pallas as pl
from jax.experimental.pallas import tpu as pltpu
from jax.sharding import PartitionSpec as P

HEADS = 24
HDIM = 64
IMG = 1024
TXT_MIN = 86
TXT_MAX = 154
EPSILON = 1e-06
F32 = jnp.float32
BF16 = jnp.bfloat16
CONTRACT_LAST = (((1,), (1,)), ((), ()))
CONTRACT_FIRST = (((0,), (0,)), ((), ()))
MASKED = -1e30


class Plan:
    def __init__(self, devices, sequences, rows_dev, width):
        self.devices, self.sequences, self.rows_dev, self.width = devices, sequences, rows_dev, width
        self.group = devices // sequences
        self.span = self.group * rows_dev
        mean = self.span - IMG
        up, down = TXT_MAX - mean, mean - TXT_MIN
        drift = 0
        for k in range(sequences + 1):
            drift = max(drift, min(up * k, down * (sequences - k)), min(down * k, up * (sequences - k)))
        self.edge = -(-drift // 64) * 64
        self.rows = self.span + 2 * self.edge
        self.piece = 2 * self.edge // self.group
        self.own = rows_dev + self.piece
        self.image_end = -(-(self.edge + drift + IMG) // 128) * 128
        self.text_start = (self.edge - drift + IMG) // 128 * 128
        self.heads = HEADS // self.group
        self.segments = self.edge_segments()
        self.chip_heads = devices == 4 * self.group

    def device_of(self, seq, rank):
        return seq * self.group + rank

    def place_of(self, device):
        return lax.div(device, self.group), lax.rem(device, self.group)

    def seq_groups(self):
        return [[self.device_of(s, r) for r in range(self.group)] for s in range(self.sequences)]

    def rank_groups(self):
        return [[self.device_of(s, r) for s in range(self.sequences)] for r in range(self.group)]

    def edge_row(self, rank):
        half = self.group // 2
        return jnp.where(rank < half, self.piece * rank, self.edge + self.span + self.piece * (rank - half))

    def main_row(self, rank):
        return self.edge + self.rows_dev * rank

    def edge_segments(self):
        found = []
        for rank in range(self.group):
            half = self.group // 2
            first = self.piece * rank - self.edge if rank < half else self.span + self.piece * (rank - half)
            row = 0
            while row < self.piece:
                owner, owner_row = (first + row) // self.rows_dev, (first + row) % self.rows_dev
                count = min(self.piece - row, self.rows_dev - owner_row)
                found.append((rank, row, count, owner // self.group, owner % self.group, owner_row))
                row += count
        return found


def layer_norm(values):
    mean = jnp.mean(values, axis=-1, keepdims=True)
    centred = values - mean
    variance = jnp.mean(centred * centred, axis=-1, keepdims=True)
    inv_std = lax.rsqrt(variance + EPSILON)
    return (centred * inv_std, inv_std)


def norm_back(grad_normed, normed, inv_std):
    mean_grad = jnp.mean(grad_normed, axis=-1, keepdims=True)
    mean_cross = jnp.mean(grad_normed * normed, axis=-1, keepdims=True)
    return inv_std * (grad_normed - mean_grad - normed * mean_cross)


def softmax_parts(query, key, bias):
    scores = lax.dot_general(query, key, CONTRACT_LAST, preferred_element_type=F32) + bias
    top = jnp.max(scores, axis=1, keepdims=True)
    exponent = jnp.exp(scores - top)
    total = jnp.sum(exponent, axis=1, keepdims=True)
    return exponent * (1.0 / total)


def attend_kernel(heads, q_ref, k_ref, v_ref, bias_ref, out_ref):
    bias = bias_ref[...]
    outs = []
    for head in range(heads):
        cols = slice(head * HDIM, (head + 1) * HDIM)
        query = q_ref[:, cols] * jnp.asarray(HDIM ** (-0.5), BF16)
        probs = softmax_parts(query, k_ref[:, cols], bias).astype(BF16)
        outs.append(jnp.dot(probs, v_ref[:, cols], preferred_element_type=F32))
    out_ref[...] = jnp.concatenate(outs, axis=1).astype(BF16)


def block_rows(rows):
    return 256 if rows % 256 == 0 else 128


def attend(plan, queries, keys, values, bias):
    rows, cols = queries.shape
    block = block_rows(rows)
    whole = pl.BlockSpec((rows, cols), lambda i: (0, 0))
    return pl.pallas_call(
        functools.partial(attend_kernel, plan.heads),
        out_shape=jax.ShapeDtypeStruct((rows, cols), BF16),
        grid=(rows // block,),
        in_specs=[
            pl.BlockSpec((block, cols), lambda i: (i, 0)),
            whole,
            whole,
            pl.BlockSpec((1, rows), lambda i: (0, 0)),
        ],
        out_specs=pl.BlockSpec((block, cols), lambda i: (i, 0)),
        compiler_params=pltpu.CompilerParams(vmem_limit_bytes=48 << 20),
        cost_estimate=pl.CostEstimate(flops=16 * rows * rows * cols, bytes_accessed=8 * rows * cols, transcendentals=0),
        name="attend",
    )(queries, keys, values, bias)


def attend_back_kernel(heads, steps, q_ref, k_ref, v_ref, g_ref, bias_ref, gq_ref, gk_ref, gv_ref, key_sum, value_sum):
    step = pl.program_id(0)
    scale = jnp.asarray(HDIM ** (-0.5), BF16)

    @pl.when(step == 0)
    def _():
        key_sum[...] = jnp.zeros_like(key_sum)
        value_sum[...] = jnp.zeros_like(value_sum)

    bias = bias_ref[...]
    grads = []
    for head in range(heads):
        cols = slice(head * HDIM, (head + 1) * HDIM)
        query = q_ref[:, cols] * scale
        key = k_ref[:, cols]
        grad_out = g_ref[:, cols]
        probs = softmax_parts(query, key, bias)
        grad_probs = lax.dot_general(grad_out, v_ref[:, cols], CONTRACT_LAST, preferred_element_type=F32)
        inner = jnp.sum(probs * grad_probs, axis=1, keepdims=True)
        grad_scores = (probs * (grad_probs - inner)).astype(BF16)
        grads.append(jnp.dot(grad_scores, key, preferred_element_type=F32) * HDIM ** (-0.5))
        key_sum[head] += lax.dot_general(query, grad_scores, CONTRACT_FIRST, preferred_element_type=F32)
        value_sum[head] += lax.dot_general(grad_out, probs.astype(BF16), CONTRACT_FIRST, preferred_element_type=F32)
    gq_ref[...] = jnp.concatenate(grads, axis=1).astype(BF16)

    @pl.when(step == steps - 1)
    def _():
        rows = gk_ref.shape[0]
        gk_ref[...] = key_sum[...].reshape(heads * HDIM, rows).T.astype(BF16)
        gv_ref[...] = value_sum[...].reshape(heads * HDIM, rows).T.astype(BF16)


def attend_back(plan, queries, keys, values, grad_out, bias):
    rows, cols = queries.shape
    block = block_rows(rows)
    whole = pl.BlockSpec((rows, cols), lambda i: (0, 0))
    part = pl.BlockSpec((block, cols), lambda i: (i, 0))
    shape = jax.ShapeDtypeStruct((rows, cols), BF16)
    return pl.pallas_call(
        functools.partial(attend_back_kernel, plan.heads, rows // block),
        out_shape=(shape, shape, shape),
        grid=(rows // block,),
        in_specs=[part, whole, whole, part, pl.BlockSpec((1, rows), lambda i: (0, 0))],
        out_specs=(part, whole, whole),
        scratch_shapes=[pltpu.VMEM((plan.heads, HDIM, rows), F32)] * 2,
        compiler_params=pltpu.CompilerParams(vmem_limit_bytes=56 << 20),
        cost_estimate=pl.CostEstimate(flops=40 * rows * rows * cols, bytes_accessed=14 * rows * cols, transcendentals=0),
        name="attend_back",
    )(queries, keys, values, grad_out, bias)


VMEM = pl.BlockSpec(memory_space=pltpu.VMEM)


def own_rows(plan, window, rank):
    main = lax.dynamic_slice_in_dim(window, plan.main_row(rank), plan.rows_dev, 0)
    edge = lax.dynamic_slice_in_dim(window, plan.edge_row(rank), plan.piece, 0)
    return jnp.concatenate([main, edge], axis=0)


def remote(source, target, send_sem, recv_sem, device):
    return pltpu.make_async_remote_copy(
        src_ref=source,
        dst_ref=target,
        send_sem=send_sem,
        recv_sem=recv_sem,
        device_id=(device,),
        device_id_type=pl.DeviceIdType.MESH,
    )


def here(plan):
    return plan.place_of(lax.axis_index("dev"))


def other(rank, step, size):
    return lax.rem(rank + step, size)


def meet(devices):
    barrier = pltpu.get_barrier_semaphore()
    for device in devices:
        pl.semaphore_signal(barrier, inc=1, device_id=(device,), device_id_type=pl.DeviceIdType.MESH)
    pl.semaphore_wait(barrier, len(devices))


def group_devices(plan, seq, rank):
    return [plan.device_of(seq, other(rank, step, plan.group)) for step in range(1, plan.group)]


def column_devices(plan, seq, rank):
    return [plan.device_of(other(seq, step, plan.sequences), rank) for step in range(1, plan.sequences)]


def every_device(plan, device):
    return [other(device, step, plan.devices) for step in range(1, plan.devices)]


def call(kernel, name, ident, out_shape, scratch, operands, in_specs=None, out_specs=None):
    outs = out_shape if isinstance(out_shape, tuple) else (out_shape,)
    return pl.pallas_call(
        kernel,
        out_shape=out_shape,
        in_specs=in_specs or [VMEM] * len(operands),
        out_specs=out_specs or (tuple([VMEM] * len(outs)) if isinstance(out_shape, tuple) else VMEM),
        scratch_shapes=scratch,
        compiler_params=pltpu.CompilerParams(
            collective_id=ident, has_side_effects=True, vmem_limit_bytes=40 << 20
        ),
        name=name,
    )(*operands)


def aligned(start):
    return pl.multiple_of(start, 16)


def block_parts(plan, ref, rank):
    return (
        ref.at[pl.ds(aligned(plan.main_row(rank)), plan.rows_dev)],
        ref.at[pl.ds(aligned(plan.edge_row(rank)), plan.piece)],
    )


def own_parts(plan, ref):
    return ref.at[pl.ds(0, plan.rows_dev)], ref.at[pl.ds(plan.rows_dev, plan.piece)]


def load_block(plan, ref, rank):
    main, edge = block_parts(plan, ref, rank)
    return jnp.concatenate([main[...], edge[...]], axis=0)


def sum_scratch(plan):
    half, own, width = plan.group // 2, plan.own, plan.width
    return [
        pltpu.VMEM((half, own, width), F32),
        pltpu.VMEM((half, own, width), BF16),
        pltpu.VMEM((half, own, width), BF16),
        pltpu.SemaphoreType.DMA((half, 2)),
        pltpu.SemaphoreType.DMA((half, 2)),
        pltpu.SemaphoreType.DMA((half,)),
        pltpu.SemaphoreType.DMA((half,)),
    ]


def scatter_sum(plan, seq, rank, part, pair, going, coming, pair_send, pair_recv, far_send, far_recv):
    half = plan.group // 2
    chip, core = lax.div(rank, 2), lax.rem(rank, 2)
    partner = plan.device_of(seq, 2 * chip + 1 - core)
    started = []
    order = list(range(1, half)) + [0]
    for step in order:
        chip_to = other(chip, step, half)
        copies = [
            remote(source, target, pair_send.at[step, i], pair_recv.at[step, i], partner)
            for i, (source, target) in enumerate(
                zip(block_parts(plan, part, 2 * chip_to + 1 - core), own_parts(plan, pair.at[step]))
            )
        ]
        for copy in copies:
            copy.start()
        started.append(copies)
    total, sends = None, []
    for step, copies in zip(order, started):
        for copy in copies:
            copy.wait_recv()
        chip_to = other(chip, step, half)
        both = load_block(plan, part, 2 * chip_to + core) + pair[step]
        if step == 0:
            total = both
        else:
            going[step] = both.astype(BF16)
            copy = remote(
                going.at[step], coming.at[step], far_send.at[step], far_recv.at[step], plan.device_of(seq, 2 * chip_to + core)
            )
            copy.start()
            sends.append(copy)
    for step, copy in zip(order, sends):
        copy.wait_recv()
        total = total + coming[step].astype(F32)
    for copies in started:
        for copy in copies:
            copy.wait_send()
    for copy in sends:
        copy.wait_send()
    return total


def share_scratch(plan):
    return [pltpu.SemaphoreType.DMA((plan.group, 2))] * 2 + [pltpu.SemaphoreType.DMA((plan.group, 2))]


def share_rows(plan, seq, rank, parts, window, send, recv, pass_send):
    half = plan.group // 2
    chip, core = lax.div(rank, 2), lax.rem(rank, 2)
    partner_rank = 2 * chip + 1 - core
    partner = plan.device_of(seq, partner_rank)

    def send_own(to_device, slot):
        copies = [
            remote(source, target, send.at[slot, i], recv.at[slot, i], to_device)
            for i, (source, target) in enumerate(zip(parts, block_parts(plan, window, rank)))
        ]
        for copy in copies:
            copy.start()
        return copies

    flying = {}
    for step in range(1, half):
        flying[step] = send_own(plan.device_of(seq, 2 * other(chip, step, half) + core), step)
    flying[0] = send_own(partner, 0)
    for source, target in zip(parts, block_parts(plan, window, rank)):
        target[...] = source[...]
    passed = []
    for step in range(1, half):
        for copy in flying[step]:
            copy.wait_recv()
        came = 2 * other(chip, half - step, half) + core
        copies = [
            remote(place, place, pass_send.at[step, i], recv.at[half + step, i], partner)
            for i, place in enumerate(block_parts(plan, window, came))
        ]
        for copy in copies:
            copy.start()
        passed.extend(copies)
    for copy in flying[0]:
        copy.wait_recv()
    for copy in passed:
        copy.wait_recv()
    for copies in flying.values():
        for copy in copies:
            copy.wait_send()
    for copy in passed:
        copy.wait_send()


def entry_kernel(plan, tokens, grads, mod_part, token_window, grad_window, mods, token_own, grad_own, plane, across,
                 chunk, edge_send, edge_recv, t_send, t_recv, t_pass, g_send, g_recv, g_pass, m_send, m_recv):
    device = lax.axis_index("dev")
    seq, rank = plan.place_of(device)
    meet(every_device(plan, device))
    hops = []
    for step in range(1, plan.group):
        to = other(rank, step, plan.group)
        copy = remote(mod_part.at[to], plane.at[step], m_send.at[0, step], m_recv.at[0, step], plan.device_of(seq, to))
        copy.start()
        hops.append(copy)
    arrays = ((tokens, token_own), (grads, grad_own))
    count = len(plan.segments)
    for which, (source, own) in enumerate(arrays):
        for index, (to_rank, row, rows, step, owner, owner_row) in enumerate(plan.segments):
            @pl.when(rank == owner)
            def _():
                remote(
                    source.at[pl.ds(owner_row, rows)],
                    own.at[pl.ds(row, rows)],
                    edge_send.at[which * count + index],
                    edge_recv.at[which * count + index],
                    plan.device_of(lax.rem(seq + plan.sequences - step, plan.sequences), to_rank),
                ).start()
    for copy in hops:
        copy.wait_recv()
    total = mod_part[rank]
    for step in range(1, plan.group):
        total = total + plane[step]
    plane[0] = total
    hops_across = []
    for step in range(1, plan.sequences):
        to = other(seq, step, plan.sequences)
        copy = remote(plane.at[0, to], across.at[seq], m_send.at[1, step], m_recv.at[1, step], plan.device_of(to, rank))
        copy.start()
        hops_across.append(copy)
    across[seq] = plane[0, seq]
    for which, (source, own) in enumerate(arrays):
        for index, (to_rank, row, rows, step, owner, owner_row) in enumerate(plan.segments):
            @pl.when(rank == to_rank)
            def _():
                remote(
                    source.at[pl.ds(owner_row, rows)],
                    own.at[pl.ds(row, rows)],
                    edge_send.at[which * count + index],
                    edge_recv.at[which * count + index],
                    plan.device_of(lax.rem(seq + plan.sequences + step, plan.sequences), owner),
                ).wait_recv()
    share_rows(plan, seq, rank, (tokens, token_own), token_window, t_send, t_recv, t_pass)
    for copy in hops_across:
        copy.wait_recv()
    half = plan.sequences // 2
    for stream in range(2):
        total = across[stream * half]
        for i in range(1, half):
            total = total + across[stream * half + i]
        chunk[stream] = total
    hops_back = []
    for step in range(1, plan.group):
        to = other(rank, step, plan.group)
        copy = remote(chunk, mods.at[rank], m_send.at[2, step], m_recv.at[2, step], plan.device_of(seq, to))
        copy.start()
        hops_back.append(copy)
    mods[rank] = chunk[...]
    share_rows(plan, seq, rank, (grads, grad_own), grad_window, g_send, g_recv, g_pass)
    for copy in hops_back:
        copy.wait_recv()
    for copy in hops + hops_across + hops_back:
        copy.wait_send()
    for which, (source, own) in enumerate(arrays):
        for index, (to_rank, row, rows, step, owner, owner_row) in enumerate(plan.segments):
            @pl.when(rank == owner)
            def _():
                remote(
                    source.at[pl.ds(owner_row, rows)],
                    own.at[pl.ds(row, rows)],
                    edge_send.at[which * count + index],
                    edge_recv.at[which * count + index],
                    plan.device_of(lax.rem(seq + plan.sequences - step, plan.sequences), to_rank),
                ).wait_send()


def entry(plan, tokens, grads, mod_part):
    lanes = mod_part.shape[1] // plan.group // 128
    pieces = mod_part.reshape(plan.sequences, plan.group, lanes, 128).transpose(1, 0, 2, 3)
    window = jax.ShapeDtypeStruct((plan.rows, plan.width), BF16)
    dma = pltpu.SemaphoreType.DMA
    most = max(plan.group, plan.sequences)
    token_window, grad_window, mods = call(
        functools.partial(entry_kernel, plan),
        "entry",
        1,
        (window, window, jax.ShapeDtypeStruct((plan.group, 2, lanes, 128), F32)),
        [
            pltpu.VMEM((plan.piece, plan.width), BF16),
            pltpu.VMEM((plan.piece, plan.width), BF16),
            pltpu.VMEM((plan.group, plan.sequences, lanes, 128), F32),
            pltpu.VMEM((plan.sequences, lanes, 128), F32),
            pltpu.VMEM((2, lanes, 128), F32),
            dma((2 * len(plan.segments),)),
            dma((2 * len(plan.segments),)),
        ]
        + share_scratch(plan)
        + share_scratch(plan)
        + [dma((3, most)), dma((3, most))],
        (tokens, grads, pieces),
    )
    return token_window, grad_window, mods.transpose(1, 0, 2, 3).reshape(2, -1)


def swap_kernel(plan, source, target, send, recv):
    seq, rank = here(plan)
    meet(group_devices(plan, seq, rank))
    copies = []
    for step in range(1, plan.group):
        to = other(rank, step, plan.group)
        copy = remote(source.at[to], target.at[rank], send.at[step], recv.at[step], plan.device_of(seq, to))
        copy.start()
        copies.append(copy)
    target[rank] = source[rank]
    for copy in copies:
        copy.wait()


def swap(plan, pieces, ident):
    dma = pltpu.SemaphoreType.DMA
    return call(
        functools.partial(swap_kernel, plan),
        "swap_%d" % ident,
        ident,
        jax.ShapeDtypeStruct(pieces.shape, pieces.dtype),
        [dma((plan.group,)), dma((plan.group,))],
        (pieces,),
    )


def pick_rows(table, text):
    return jnp.where(text > 0, table[1:2, :], table[0:1, :])


def norm_rows(values):
    mean = jnp.mean(values, axis=1, keepdims=True)
    centred = values - mean
    inv = lax.rsqrt(jnp.mean(centred * centred, axis=1, keepdims=True) + EPSILON)
    return centred * inv, inv


def middle_kernel(plan, part, tokens, gate_a, scale_b, shift_b, text, merged, window, own, *scratch):
    seq, rank = here(plan)
    meet(group_devices(plan, seq, rank))
    total = scatter_sum(plan, seq, rank, part, *scratch[:7])
    merged[...] = total
    mask = text[...]
    middle = tokens[...].astype(F32) + pick_rows(gate_a[...], mask) * total
    normed, _ = norm_rows(middle)
    own[...] = (normed * (1.0 + pick_rows(scale_b[...], mask)) + pick_rows(shift_b[...], mask)).astype(BF16)
    share_rows(plan, seq, rank, own_parts(plan, own), window, *scratch[7:])


def own_shape(plan, dtype=F32):
    return jax.ShapeDtypeStruct((plan.own, plan.width), dtype)


def window_shape(plan):
    return jax.ShapeDtypeStruct((plan.rows, plan.width), BF16)


def middle_rows(plan, part, tokens, gate_a, scale_b, shift_b, text):
    return call(
        functools.partial(middle_kernel, plan),
        "middle",
        2,
        (own_shape(plan), window_shape(plan)),
        [pltpu.VMEM((plan.own, plan.width), BF16)] + sum_scratch(plan) + share_scratch(plan),
        (part, tokens, gate_a, scale_b, shift_b, text),
    )


def back_kernel(plan, part, grad, middle, gate_a, scale_b, text, grad_hidden, grad_middle, window, own, *scratch):
    seq, rank = here(plan)
    meet(group_devices(plan, seq, rank))
    total = scatter_sum(plan, seq, rank, part, *scratch[:7])
    grad_hidden[...] = total
    mask = text[...]
    normed, inv = norm_rows(middle[...])
    inner = total * (1.0 + pick_rows(scale_b[...], mask))
    mean_grad = jnp.mean(inner, axis=1, keepdims=True)
    mean_cross = jnp.mean(inner * normed, axis=1, keepdims=True)
    result = grad[...].astype(F32) + inv * (inner - mean_grad - normed * mean_cross)
    grad_middle[...] = result
    own[...] = (pick_rows(gate_a[...], mask) * result).astype(BF16)
    share_rows(plan, seq, rank, own_parts(plan, own), window, *scratch[7:])


def back_rows(plan, part, grad, middle, gate_a, scale_b, text):
    return call(
        functools.partial(back_kernel, plan),
        "back",
        3,
        (own_shape(plan), own_shape(plan), window_shape(plan)),
        [pltpu.VMEM((plan.own, plan.width), BF16)] + sum_scratch(plan) + share_scratch(plan),
        (part, grad, middle, gate_a, scale_b, text),
    )


def sum_kernel(plan, part, out, *scratch):
    seq, rank = here(plan)
    meet(group_devices(plan, seq, rank))
    out[...] = scatter_sum(plan, seq, rank, part, *scratch)


def sum_rows(plan, part, ident):
    return call(
        functools.partial(sum_kernel, plan), "sum_%d" % ident, ident, own_shape(plan), sum_scratch(plan), (part,)
    )


def edge_kernel(plan, own, extra, send, recv):
    device = lax.axis_index("dev")
    seq, rank = plan.place_of(device)
    extra[...] = jnp.zeros_like(extra)
    meet(every_device(plan, device))

    def copy(index):
        from_rank, row, rows, step, owner, owner_row = plan.segments[index]
        return remote(
            own.at[pl.ds(plan.rows_dev + row, rows)],
            extra.at[pl.ds(owner_row, rows)],
            send.at[index],
            recv.at[index],
            plan.device_of(lax.rem(seq + plan.sequences + step, plan.sequences), owner),
        )

    for index, segment in enumerate(plan.segments):
        @pl.when(rank == segment[0])
        def _():
            copy(index).start()
    for index, segment in enumerate(plan.segments):
        @pl.when(rank == segment[4])
        def _():
            copy(index).wait_recv()

        @pl.when(rank == segment[0])
        def _():
            copy(index).wait_send()


def to_packed(plan, own, foreign, ident):
    dma = pltpu.SemaphoreType.DMA
    extra = call(
        functools.partial(edge_kernel, plan),
        "edges_%d" % ident,
        ident,
        jax.ShapeDtypeStruct((plan.rows_dev, plan.width), own.dtype),
        [dma((len(plan.segments),)), dma((len(plan.segments),))],
        (own,),
    )
    return jnp.where(foreign[:, None], extra, own[: plan.rows_dev])


def table_kernel(plan, local, table, first, second, mine, send, recv):
    device = lax.axis_index("dev")
    seq, rank = plan.place_of(device)
    stream = lax.div(2 * seq, plan.sequences)
    meet(every_device(plan, device))
    hops = []
    for step in range(1, plan.group):
        to = other(rank, step, plan.group)
        copy = remote(local.at[to], first.at[step], send.at[0, step], recv.at[0, step], plan.device_of(seq, to))
        copy.start()
        hops.append(copy)
    for copy in hops:
        copy.wait_recv()
    total = local[rank]
    for step in range(1, plan.group):
        total = total + first[step]
    first[0] = total
    across = []
    for step in range(1, plan.sequences):
        to = other(seq, step, plan.sequences)
        to_stream = lax.div(2 * to, plan.sequences)
        copy = remote(first.at[0, to_stream], second.at[seq], send.at[1, step], recv.at[1, step], plan.device_of(to, rank))
        copy.start()
        across.append(copy)
    second[seq] = first[0, stream]
    for copy in across:
        copy.wait_recv()
    mine[...] = second[...]
    last = []
    for step in range(1, plan.group):
        to = other(rank, step, plan.group)
        copy = remote(mine, table.at[rank], send.at[2, step], recv.at[2, step], plan.device_of(seq, to))
        copy.start()
        last.append(copy)
    table[rank] = mine[...]
    for copy in last:
        copy.wait_recv()
    for copy in hops + across + last:
        copy.wait_send()


def stream_table(plan, local, ident):
    lanes = local.shape[1] // plan.group // 128
    pieces = local.reshape(2, plan.group, lanes, 128).transpose(1, 0, 2, 3)
    dma = pltpu.SemaphoreType.DMA
    most = max(plan.group, plan.sequences)
    table = call(
        functools.partial(table_kernel, plan),
        "mod_table",
        ident,
        jax.ShapeDtypeStruct((plan.group, plan.sequences, lanes, 128), F32),
        [
            pltpu.VMEM((plan.group, 2, lanes, 128), F32),
            pltpu.VMEM((plan.sequences, lanes, 128), F32),
            pltpu.VMEM((plan.sequences, lanes, 128), F32),
            dma((3, most)),
            dma((3, most)),
        ],
        (pieces,),
    )
    return table.transpose(1, 0, 2, 3).reshape(plan.sequences, -1)


def spread_kernel(plan, piece, everyone, send, recv):
    device = lax.axis_index("dev")
    seq, rank = plan.place_of(device)
    meet(group_devices(plan, seq, rank) + column_devices(plan, seq, rank))
    copies = []
    everyone[seq, rank] = piece[...]
    for step in range(1, plan.group):
        to = other(rank, step, plan.group)
        copy = remote(piece, everyone.at[seq, rank], send.at[0, step], recv.at[0, step], plan.device_of(seq, to))
        copy.start()
        copies.append(copy)
    for copy in copies:
        copy.wait_recv()
    across = []
    for step in range(1, plan.sequences):
        to = other(seq, step, plan.sequences)
        copy = remote(everyone.at[seq], everyone.at[seq], send.at[1, step], recv.at[1, step], plan.device_of(to, rank))
        copy.start()
        across.append(copy)
    for copy in across:
        copy.wait_recv()
    for copy in copies + across:
        copy.wait_send()


def spread(plan, piece, ident):
    dma = pltpu.SemaphoreType.DMA
    most = max(plan.group, plan.sequences)
    return call(
        functools.partial(spread_kernel, plan),
        "spread",
        ident,
        jax.ShapeDtypeStruct((plan.sequences, plan.group) + piece.shape, piece.dtype),
        [dma((2, most)), dma((2, most))],
        (piece,),
    )


def project_slices(plan, weight):
    rows, share = weight.shape[0], plan.width // plan.group
    view = weight.reshape(rows, 3, 2, plan.group // 2, share).transpose(3, 2, 0, 1, 4)
    got = swap(plan, view.reshape(plan.group, rows, 3 * share), 4)
    got = lax.all_gather(got, "dev", axis=0, axis_index_groups=plan.rank_groups())
    return got.reshape(2, plan.width, 3 * share)


def up_slices(plan, weight):
    rows, cols = weight.shape
    planes = plan.sequences // 2
    share = cols // planes // plan.group
    view = weight.reshape(rows, planes, plan.group, share).transpose(2, 0, 1, 3)
    got = swap(plan, view.reshape(plan.group, rows, planes * share), 5)
    got = lax.all_gather(got, "dev", axis=0, axis_index_groups=plan.rank_groups())
    return got.reshape(2, plan.width, planes * share)


def sum_to_owners(plan, grad, rows, ident):
    cols = grad.shape[2]
    pieces = grad.astype(BF16).reshape(plan.sequences, plan.group, rows, cols)
    got = lax.psum_scatter(pieces, "dev", scatter_dimension=0, axis_index_groups=plan.rank_groups())
    return swap(plan, got, ident)


def project_grads(plan, grad, rows):
    share = plan.width // plan.group
    got = sum_to_owners(plan, grad, rows, 6)
    got = got.reshape(plan.group // 2, 2, rows, 3, share).transpose(2, 3, 1, 0, 4)
    return got.reshape(rows, -1).astype(F32)


def up_grads(plan, grad, rows):
    planes = plan.sequences // 2
    got = sum_to_owners(plan, grad, rows, 7)
    got = got.reshape(plan.group, rows, planes, -1).transpose(1, 2, 0, 3)
    return got.reshape(rows, -1).astype(F32)


def chip_groups(plan):
    return [
        [plan.device_of(s, 2 * q + core) for s in range(plan.sequences) for core in range(2)]
        for q in range(plan.group // 2)
    ]


def merge_slices(plan, weight, rank):
    half = plan.group // 2
    rows = weight.shape[0]
    share = plan.width // plan.group
    if plan.chip_heads:
        full = lax.all_gather(weight, "dev", axis=0, axis_index_groups=chip_groups(plan))
        full = full.reshape(2, 2, share, weight.shape[1])
        return lax.dynamic_index_in_dim(full, lax.rem(rank, 2), 1, keepdims=False)
    full = lax.all_gather(weight, "dev", axis=0, tiled=True)
    full = full.reshape(2, 2, half, share, weight.shape[1])
    full = lax.dynamic_index_in_dim(full, lax.rem(rank, 2), 1, keepdims=False)
    return lax.dynamic_index_in_dim(full, lax.div(rank, 2), 1, keepdims=False)


def merge_grads(plan, grad, rank):
    half = plan.group // 2
    _, share, cols = grad.shape
    core = lax.rem(rank, 2)
    grad = grad.astype(BF16)
    mine = [jnp.where(core == k, grad, jnp.zeros((), BF16)) for k in range(2)]
    if plan.chip_heads:
        full = jnp.stack(mine, axis=1).reshape(2 * plan.sequences, -1, cols)
        out = lax.psum_scatter(full, "dev", scatter_dimension=0, axis_index_groups=chip_groups(plan))
        return out.astype(F32)
    full = jnp.zeros((2, 2, half, share, cols), BF16)
    full = lax.dynamic_update_slice_in_dim(full, jnp.stack(mine, axis=1)[:, :, None], lax.div(rank, 2), 2)
    return lax.psum_scatter(full.reshape(-1, cols), "dev", scatter_dimension=0, tiled=True).astype(F32)


def down_slices(plan, weight):
    full = lax.all_gather(weight, "dev", axis=0, axis_index_groups=plan.rank_groups())
    return full.reshape(2, -1, weight.shape[1])


def down_grads(plan, grad):
    cols = grad.shape[2]
    pieces = grad.astype(BF16).reshape(plan.sequences, -1, cols)
    return lax.psum_scatter(pieces, "dev", scatter_dimension=0, axis_index_groups=plan.rank_groups()).astype(F32)


def by_stream(plan, image_part, text_part, is_text):
    start, end = plan.text_start, plan.image_end
    mixed = jnp.where(is_text[start:end, None], text_part[: end - start], image_part[start:])
    return jnp.concatenate([image_part[:start], mixed, text_part[end - start :]], axis=0)


def stream_dot(plan, rows, pair, is_text):
    image_part = jnp.dot(rows[: plan.image_end], pair[0], preferred_element_type=F32)
    text_part = jnp.dot(rows[plan.text_start :], pair[1], preferred_element_type=F32)
    return by_stream(plan, image_part, text_part, is_text)


def stream_dot_back(plan, grads, pair, is_text):
    image_part = lax.dot_general(grads[: plan.image_end], pair[0], CONTRACT_LAST, preferred_element_type=F32)
    text_part = lax.dot_general(grads[plan.text_start :], pair[1], CONTRACT_LAST, preferred_element_type=F32)
    return by_stream(plan, image_part, text_part, is_text)


def weight_terms(plan, rows, grads, is_text):
    zero = jnp.zeros((), grads.dtype)
    image = jnp.where(is_text[: plan.image_end, None], zero, grads[: plan.image_end])
    text = jnp.where(is_text[plan.text_start :, None], grads[plan.text_start :], zero)
    image_term = lax.dot_general(rows[: plan.image_end], image, CONTRACT_FIRST, preferred_element_type=F32)
    text_term = lax.dot_general(rows[plan.text_start :], text, CONTRACT_FIRST, preferred_element_type=F32)
    return jnp.stack([image_term, text_term])


def pick(table, text_rows):
    return jnp.where(text_rows[:, None], table[1][None, :], table[0][None, :])


def on_device(
    tokens,
    conditioning,
    text_lengths,
    modulation_weight,
    project_weight,
    merge_weight,
    up_weight,
    down_weight,
    cotangent,
):
    rows_dev, width = tokens.shape
    mod_rows = modulation_weight.shape[0]
    plan = Plan(lax.axis_size("dev"), conditioning.shape[0], rows_dev, width)
    device = lax.axis_index("dev")
    seq, rank = plan.place_of(device)
    feature_start = device * mod_rows % width

    ends = jnp.cumsum(IMG + text_lengths)
    starts = jnp.concatenate([jnp.zeros((1,), jnp.int32), ends[:-1]])
    positions = device * rows_dev + jnp.arange(rows_dev, dtype=jnp.int32)
    row_seq = jnp.sum((starts[None, :] <= positions[:, None]).astype(jnp.int32), axis=1) - 1
    offset = plan.span * seq - plan.edge + jnp.arange(plan.rows, dtype=jnp.int32) - starts[seq]
    valid = (offset >= 0) & (offset < IMG + text_lengths[seq])
    is_text = offset >= IMG
    bias = jnp.where(valid, 0.0, MASKED).astype(F32)[None, :]
    own_valid = own_rows(plan, valid[:, None], rank)[:, 0]
    own_text = own_rows(plan, is_text[:, None], rank)[:, 0]

    cond_float = conditioning.astype(F32)
    silu_low = jax.nn.silu(cond_float).astype(BF16)
    silu_part = lax.dynamic_slice_in_dim(silu_low, feature_start, mod_rows, 1)
    mod_part = jnp.dot(silu_part, modulation_weight, preferred_element_type=F32)

    merge_pair = merge_slices(plan, merge_weight, rank)
    project_pair = project_slices(plan, project_weight)
    up_pair = up_slices(plan, up_weight)
    down_pair = down_slices(plan, down_weight)

    token_window, grad_window, mods = entry(plan, tokens, cotangent, mod_part)
    shift_a, scale_a, gate_a, shift_b, scale_b, gate_b = jnp.split(mods, 6, axis=1)
    grad_window = jnp.where(valid[:, None], grad_window, jnp.zeros((), BF16))

    normed_full, _ = layer_norm(token_window.astype(F32))
    hidden_a = (normed_full * (1.0 + pick(scale_a, is_text)) + pick(shift_a, is_text)).astype(BF16)
    projected = stream_dot(plan, hidden_a, project_pair, is_text).astype(BF16)
    queries, keys, values = jnp.split(projected, 3, axis=1)
    attended = attend(plan, queries, keys, values, bias)

    own_tokens = own_rows(plan, token_window, rank)
    own_grad = own_rows(plan, grad_window, rank)
    text_mask = own_text.astype(F32)[:, None]
    merged, hidden_b = middle_rows(
        plan, stream_dot(plan, attended, merge_pair, is_text), own_tokens, gate_a, scale_b, shift_b, text_mask
    )
    middle = own_tokens.astype(F32) + pick(gate_a, own_text) * merged
    normed_b, inv_b = layer_norm(middle)

    upper = stream_dot(plan, hidden_b, up_pair, is_text)
    activated = jax.nn.gelu(upper, approximate=True).astype(BF16)
    grad_lowered = (pick(gate_b, is_text) * grad_window.astype(F32)).astype(BF16)
    down_term = weight_terms(plan, activated, grad_lowered, is_text)
    down_grad = down_grads(plan, down_term)
    grad_activated = stream_dot_back(plan, grad_lowered, down_pair, is_text)
    gelu_pull = jax.vjp(lambda value_in: jax.nn.gelu(value_in, approximate=True), upper)[1]
    grad_upper = gelu_pull(grad_activated)[0].astype(BF16)
    up_term = weight_terms(plan, hidden_b, grad_upper, is_text)
    up_grad = up_grads(plan, up_term, mod_rows)
    grad_hidden_b, grad_middle, grad_merged = back_rows(
        plan, stream_dot_back(plan, grad_upper, up_pair, is_text), own_grad, middle, gate_a, scale_b, text_mask
    )
    lowered = sum_rows(plan, stream_dot(plan, activated, down_pair, is_text), 8)
    foreign = row_seq != seq
    layer_out = to_packed(plan, (middle + pick(gate_b, own_text) * lowered).astype(BF16), foreign, 9)
    grad_gate_b = own_grad.astype(F32) * lowered
    grad_scale_b = grad_hidden_b * normed_b
    grad_gate_a = grad_middle * merged
    grad_attended = stream_dot_back(plan, grad_merged, merge_pair, is_text).astype(BF16)
    merge_grad = merge_grads(plan, weight_terms(plan, attended, grad_merged, is_text), rank)

    grad_projected = jnp.concatenate(attend_back(plan, queries, keys, values, grad_attended, bias), axis=1)
    project_grad = project_grads(plan, weight_terms(plan, hidden_a, grad_projected, is_text), mod_rows)
    grad_hidden_a = sum_rows(plan, stream_dot_back(plan, grad_projected, project_pair, is_text), 10)

    normed_a, inv_a = layer_norm(own_tokens.astype(F32))
    grad_scale_a = grad_hidden_a * normed_a
    own_back = grad_middle + norm_back(grad_hidden_a * (1.0 + pick(scale_a, own_text)), normed_a, inv_a)
    tokens_grad = to_packed(plan, own_back, foreign, 11)

    rows_of = jnp.stack([own_valid & ~own_text, own_valid & own_text]).astype(F32)
    sums = [
        jnp.stack([jnp.sum(jnp.where(own[:, None] > 0, part, 0.0), axis=0) for own in rows_of])
        for part in (grad_hidden_a, grad_scale_a, grad_gate_a, grad_hidden_b, grad_scale_b, grad_gate_b)
    ]
    local_mods = jnp.concatenate(sums, axis=1)
    own_grads = stream_table(plan, local_mods, 12).astype(BF16)
    modulation_grad = lax.dot_general(silu_part, own_grads, CONTRACT_FIRST, preferred_element_type=F32)
    grad_piece = lax.dot_general(own_grads, modulation_weight, CONTRACT_LAST, preferred_element_type=F32)
    everyone = spread(plan, grad_piece.reshape(-1, 128), 13)
    everyone = everyone.reshape(2, plan.devices // 2, plan.sequences, mod_rows)
    grad_silu = (everyone[0] + everyone[1]).transpose(1, 0, 2).reshape(plan.sequences, width)
    conditioning_grad = jax.vjp(jax.nn.silu, cond_float)[1](grad_silu)[0]
    return (
        layer_out,
        tokens_grad,
        conditioning_grad,
        modulation_grad,
        project_grad,
        merge_grad,
        up_grad,
        down_grad,
    )


def solution(mesh):
    shard, whole = P("dev", None), P()
    return jax.shard_map(
        on_device,
        mesh=mesh,
        in_specs=(shard, whole, whole, shard, shard, shard, shard, shard, shard),
        out_specs=(shard, shard, whole, shard, shard, shard, shard, shard),
        check_vma=False,
    )
```

```python
import functools

import jax
import jax.numpy as jnp
import numpy as np
from jax import lax
from jax.experimental import pallas as pl
from jax.experimental.pallas import tpu as pltpu
from jax.sharding import PartitionSpec as P

HEADS = 24
HDIM = 64
IMG = 1024
TXT_MIN = 86
TXT_MAX = 154
EPSILON = 1e-06
F32 = jnp.float32
BF16 = jnp.bfloat16
CONTRACT_LAST = (((1,), (1,)), ((), ()))
CONTRACT_FIRST = (((0,), (0,)), ((), ()))
MASKED = -1e30


class Plan:
    def __init__(self, devices, sequences, rows_dev, width):
        self.devices, self.sequences, self.rows_dev, self.width = devices, sequences, rows_dev, width
        self.group = devices // sequences
        self.span = self.group * rows_dev
        mean = self.span - IMG
        up, down = TXT_MAX - mean, mean - TXT_MIN
        drift = 0
        for k in range(sequences + 1):
            drift = max(drift, min(up * k, down * (sequences - k)), min(down * k, up * (sequences - k)))
        self.edge = -(-drift // 64) * 64
        self.rows = self.span + 2 * self.edge
        self.piece = 2 * self.edge // self.group
        self.own = rows_dev + self.piece
        self.image_end = -(-(self.edge + drift + IMG) // 128) * 128
        self.text_start = (self.edge - drift + IMG) // 128 * 128
        self.heads = HEADS // self.group
        self.segments = self.edge_segments()
        self.chip_heads = devices == 4 * self.group

    def device_of(self, seq, rank):
        return seq * self.group + rank

    def place_of(self, device):
        return lax.div(device, self.group), lax.rem(device, self.group)

    def seq_groups(self):
        return [[self.device_of(s, r) for r in range(self.group)] for s in range(self.sequences)]

    def rank_groups(self):
        return [[self.device_of(s, r) for s in range(self.sequences)] for r in range(self.group)]

    def edge_row(self, rank):
        half = self.group // 2
        return jnp.where(rank < half, self.piece * rank, self.edge + self.span + self.piece * (rank - half))

    def main_row(self, rank):
        return self.edge + self.rows_dev * rank

    def edge_segments(self):
        found = []
        for rank in range(self.group):
            half = self.group // 2
            first = self.piece * rank - self.edge if rank < half else self.span + self.piece * (rank - half)
            row = 0
            while row < self.piece:
                owner, owner_row = (first + row) // self.rows_dev, (first + row) % self.rows_dev
                count = min(self.piece - row, self.rows_dev - owner_row)
                found.append((rank, row, count, owner // self.group, owner % self.group, owner_row))
                row += count
        return found


def layer_norm(values):
    mean = jnp.mean(values, axis=-1, keepdims=True)
    centred = values - mean
    variance = jnp.mean(centred * centred, axis=-1, keepdims=True)
    inv_std = lax.rsqrt(variance + EPSILON)
    return (centred * inv_std, inv_std)


def norm_back(grad_normed, normed, inv_std):
    mean_grad = jnp.mean(grad_normed, axis=-1, keepdims=True)
    mean_cross = jnp.mean(grad_normed * normed, axis=-1, keepdims=True)
    return inv_std * (grad_normed - mean_grad - normed * mean_cross)


def softmax_parts(query, key, bias):
    scores = lax.dot_general(query, key, CONTRACT_LAST, preferred_element_type=F32) + bias
    top = jnp.max(scores, axis=1, keepdims=True)
    exponent = jnp.exp(scores - top)
    total = jnp.sum(exponent, axis=1, keepdims=True)
    return exponent * (1.0 / total)


def attend_kernel(heads, q_ref, k_ref, v_ref, bias_ref, out_ref):
    bias = bias_ref[...]
    outs = []
    for head in range(heads):
        cols = slice(head * HDIM, (head + 1) * HDIM)
        query = q_ref[:, cols] * jnp.asarray(HDIM ** (-0.5), BF16)
        probs = softmax_parts(query, k_ref[:, cols], bias).astype(BF16)
        outs.append(jnp.dot(probs, v_ref[:, cols], preferred_element_type=F32))
    out_ref[...] = jnp.concatenate(outs, axis=1).astype(BF16)


def block_rows(rows):
    return 256 if rows % 256 == 0 else 128


def attend(plan, queries, keys, values, bias):
    rows, cols = queries.shape
    block = block_rows(rows)
    whole = pl.BlockSpec((rows, cols), lambda i: (0, 0))
    return pl.pallas_call(
        functools.partial(attend_kernel, plan.heads),
        out_shape=jax.ShapeDtypeStruct((rows, cols), BF16),
        grid=(rows // block,),
        in_specs=[
            pl.BlockSpec((block, cols), lambda i: (i, 0)),
            whole,
            whole,
            pl.BlockSpec((1, rows), lambda i: (0, 0)),
        ],
        out_specs=pl.BlockSpec((block, cols), lambda i: (i, 0)),
        compiler_params=pltpu.CompilerParams(vmem_limit_bytes=48 << 20),
        cost_estimate=pl.CostEstimate(flops=16 * rows * rows * cols, bytes_accessed=8 * rows * cols, transcendentals=0),
        name="attend",
    )(queries, keys, values, bias)


def attend_back_kernel(heads, steps, q_ref, k_ref, v_ref, g_ref, bias_ref, gq_ref, gk_ref, gv_ref, key_sum, value_sum):
    step = pl.program_id(0)
    scale = jnp.asarray(HDIM ** (-0.5), BF16)

    @pl.when(step == 0)
    def _():
        key_sum[...] = jnp.zeros_like(key_sum)
        value_sum[...] = jnp.zeros_like(value_sum)

    bias = bias_ref[...]
    grads = []
    for head in range(heads):
        cols = slice(head * HDIM, (head + 1) * HDIM)
        query = q_ref[:, cols] * scale
        key = k_ref[:, cols]
        grad_out = g_ref[:, cols]
        probs = softmax_parts(query, key, bias)
        grad_probs = lax.dot_general(grad_out, v_ref[:, cols], CONTRACT_LAST, preferred_element_type=F32)
        inner = jnp.sum(probs * grad_probs, axis=1, keepdims=True)
        grad_scores = (probs * (grad_probs - inner)).astype(BF16)
        grads.append(jnp.dot(grad_scores, key, preferred_element_type=F32) * HDIM ** (-0.5))
        key_sum[head] += lax.dot_general(query, grad_scores, CONTRACT_FIRST, preferred_element_type=F32)
        value_sum[head] += lax.dot_general(grad_out, probs.astype(BF16), CONTRACT_FIRST, preferred_element_type=F32)
    gq_ref[...] = jnp.concatenate(grads, axis=1).astype(BF16)

    @pl.when(step == steps - 1)
    def _():
        rows = gk_ref.shape[0]
        gk_ref[...] = key_sum[...].reshape(heads * HDIM, rows).T.astype(BF16)
        gv_ref[...] = value_sum[...].reshape(heads * HDIM, rows).T.astype(BF16)


def attend_back(plan, queries, keys, values, grad_out, bias):
    rows, cols = queries.shape
    block = block_rows(rows)
    whole = pl.BlockSpec((rows, cols), lambda i: (0, 0))
    part = pl.BlockSpec((block, cols), lambda i: (i, 0))
    shape = jax.ShapeDtypeStruct((rows, cols), BF16)
    return pl.pallas_call(
        functools.partial(attend_back_kernel, plan.heads, rows // block),
        out_shape=(shape, shape, shape),
        grid=(rows // block,),
        in_specs=[part, whole, whole, part, pl.BlockSpec((1, rows), lambda i: (0, 0))],
        out_specs=(part, whole, whole),
        scratch_shapes=[pltpu.VMEM((plan.heads, HDIM, rows), F32)] * 2,
        compiler_params=pltpu.CompilerParams(vmem_limit_bytes=56 << 20),
        cost_estimate=pl.CostEstimate(flops=40 * rows * rows * cols, bytes_accessed=14 * rows * cols, transcendentals=0),
        name="attend_back",
    )(queries, keys, values, grad_out, bias)


VMEM = pl.BlockSpec(memory_space=pltpu.VMEM)


def own_rows(plan, window, rank):
    main = lax.dynamic_slice_in_dim(window, plan.main_row(rank), plan.rows_dev, 0)
    edge = lax.dynamic_slice_in_dim(window, plan.edge_row(rank), plan.piece, 0)
    return jnp.concatenate([main, edge], axis=0)


def remote(source, target, send_sem, recv_sem, device):
    return pltpu.make_async_remote_copy(
        src_ref=source,
        dst_ref=target,
        send_sem=send_sem,
        recv_sem=recv_sem,
        device_id=(device,),
        device_id_type=pl.DeviceIdType.MESH,
    )


def here(plan):
    return plan.place_of(lax.axis_index("dev"))


def other(rank, step, size):
    return lax.rem(rank + step, size)


def meet(devices):
    barrier = pltpu.get_barrier_semaphore()
    for device in devices:
        pl.semaphore_signal(barrier, inc=1, device_id=(device,), device_id_type=pl.DeviceIdType.MESH)
    pl.semaphore_wait(barrier, len(devices))


def group_devices(plan, seq, rank):
    return [plan.device_of(seq, other(rank, step, plan.group)) for step in range(1, plan.group)]


def column_devices(plan, seq, rank):
    return [plan.device_of(other(seq, step, plan.sequences), rank) for step in range(1, plan.sequences)]


def every_device(plan, device):
    return [other(device, step, plan.devices) for step in range(1, plan.devices)]


def call(kernel, name, ident, out_shape, scratch, operands, in_specs=None, out_specs=None):
    outs = out_shape if isinstance(out_shape, tuple) else (out_shape,)
    return pl.pallas_call(
        kernel,
        out_shape=out_shape,
        in_specs=in_specs or [VMEM] * len(operands),
        out_specs=out_specs or (tuple([VMEM] * len(outs)) if isinstance(out_shape, tuple) else VMEM),
        scratch_shapes=scratch,
        compiler_params=pltpu.CompilerParams(
            collective_id=ident, has_side_effects=True, vmem_limit_bytes=40 << 20
        ),
        name=name,
    )(*operands)


def aligned(start):
    return pl.multiple_of(start, 16)


def block_parts(plan, ref, rank):
    return (
        ref.at[pl.ds(aligned(plan.main_row(rank)), plan.rows_dev)],
        ref.at[pl.ds(aligned(plan.edge_row(rank)), plan.piece)],
    )


def own_parts(plan, ref):
    return ref.at[pl.ds(0, plan.rows_dev)], ref.at[pl.ds(plan.rows_dev, plan.piece)]


def load_block(plan, ref, rank):
    main, edge = block_parts(plan, ref, rank)
    return jnp.concatenate([main[...], edge[...]], axis=0)


def sum_scratch(plan):
    half, own, width = plan.group // 2, plan.own, plan.width
    return [
        pltpu.VMEM((half, own, width), F32),
        pltpu.VMEM((half, own, width), BF16),
        pltpu.VMEM((half, own, width), BF16),
        pltpu.SemaphoreType.DMA((half, 2)),
        pltpu.SemaphoreType.DMA((half, 2)),
        pltpu.SemaphoreType.DMA((half,)),
        pltpu.SemaphoreType.DMA((half,)),
    ]


def scatter_sum(plan, seq, rank, part, pair, going, coming, pair_send, pair_recv, far_send, far_recv):
    half = plan.group // 2
    chip, core = lax.div(rank, 2), lax.rem(rank, 2)
    partner = plan.device_of(seq, 2 * chip + 1 - core)
    started = []
    order = list(range(1, half)) + [0]
    for step in order:
        chip_to = other(chip, step, half)
        copies = [
            remote(source, target, pair_send.at[step, i], pair_recv.at[step, i], partner)
            for i, (source, target) in enumerate(
                zip(block_parts(plan, part, 2 * chip_to + 1 - core), own_parts(plan, pair.at[step]))
            )
        ]
        for copy in copies:
            copy.start()
        started.append(copies)
    total, sends = None, []
    for step, copies in zip(order, started):
        for copy in copies:
            copy.wait_recv()
        chip_to = other(chip, step, half)
        both = load_block(plan, part, 2 * chip_to + core) + pair[step]
        if step == 0:
            total = both
        else:
            going[step] = both.astype(BF16)
            copy = remote(
                going.at[step], coming.at[step], far_send.at[step], far_recv.at[step], plan.device_of(seq, 2 * chip_to + core)
            )
            copy.start()
            sends.append(copy)
    for step, copy in zip(order, sends):
        copy.wait_recv()
        total = total + coming[step].astype(F32)
    for copies in started:
        for copy in copies:
            copy.wait_send()
    for copy in sends:
        copy.wait_send()
    return total


def share_scratch(plan):
    return [pltpu.SemaphoreType.DMA((plan.group, 2))] * 2 + [pltpu.SemaphoreType.DMA((plan.group, 2))]


def share_rows(plan, seq, rank, parts, window, send, recv, pass_send):
    half = plan.group // 2
    chip, core = lax.div(rank, 2), lax.rem(rank, 2)
    partner_rank = 2 * chip + 1 - core
    partner = plan.device_of(seq, partner_rank)

    def send_own(to_device, slot):
        copies = [
            remote(source, target, send.at[slot, i], recv.at[slot, i], to_device)
            for i, (source, target) in enumerate(zip(parts, block_parts(plan, window, rank)))
        ]
        for copy in copies:
            copy.start()
        return copies

    flying = {}
    for step in range(1, half):
        flying[step] = send_own(plan.device_of(seq, 2 * other(chip, step, half) + core), step)
    flying[0] = send_own(partner, 0)
    for source, target in zip(parts, block_parts(plan, window, rank)):
        target[...] = source[...]
    passed = []
    for step in range(1, half):
        for copy in flying[step]:
            copy.wait_recv()
        came = 2 * other(chip, half - step, half) + core
        copies = [
            remote(place, place, pass_send.at[step, i], recv.at[half + step, i], partner)
            for i, place in enumerate(block_parts(plan, window, came))
        ]
        for copy in copies:
            copy.start()
        passed.extend(copies)
    for copy in flying[0]:
        copy.wait_recv()
    for copy in passed:
        copy.wait_recv()
    for copies in flying.values():
        for copy in copies:
            copy.wait_send()
    for copy in passed:
        copy.wait_send()


def entry_kernel(plan, tokens, grads, mod_part, token_window, grad_window, mods, token_own, grad_own, plane, across,
                 chunk, edge_send, edge_recv, t_send, t_recv, t_pass, g_send, g_recv, g_pass, m_send, m_recv):
    device = lax.axis_index("dev")
    seq, rank = plan.place_of(device)
    meet(every_device(plan, device))
    hops = []
    for step in range(1, plan.group):
        to = other(rank, step, plan.group)
        copy = remote(mod_part.at[to], plane.at[step], m_send.at[0, step], m_recv.at[0, step], plan.device_of(seq, to))
        copy.start()
        hops.append(copy)
    arrays = ((tokens, token_own), (grads, grad_own))
    count = len(plan.segments)
    for which, (source, own) in enumerate(arrays):
        for index, (to_rank, row, rows, step, owner, owner_row) in enumerate(plan.segments):
            @pl.when(rank == owner)
            def _():
                remote(
                    source.at[pl.ds(owner_row, rows)],
                    own.at[pl.ds(row, rows)],
                    edge_send.at[which * count + index],
                    edge_recv.at[which * count + index],
                    plan.device_of(lax.rem(seq + plan.sequences - step, plan.sequences), to_rank),
                ).start()
    for copy in hops:
        copy.wait_recv()
    total = mod_part[rank]
    for step in range(1, plan.group):
        total = total + plane[step]
    plane[0] = total
    hops_across = []
    for step in range(1, plan.sequences):
        to = other(seq, step, plan.sequences)
        copy = remote(plane.at[0, to], across.at[seq], m_send.at[1, step], m_recv.at[1, step], plan.device_of(to, rank))
        copy.start()
        hops_across.append(copy)
    across[seq] = plane[0, seq]
    for which, (source, own) in enumerate(arrays):
        for index, (to_rank, row, rows, step, owner, owner_row) in enumerate(plan.segments):
            @pl.when(rank == to_rank)
            def _():
                remote(
                    source.at[pl.ds(owner_row, rows)],
                    own.at[pl.ds(row, rows)],
                    edge_send.at[which * count + index],
                    edge_recv.at[which * count + index],
                    plan.device_of(lax.rem(seq + plan.sequences + step, plan.sequences), owner),
                ).wait_recv()
    share_rows(plan, seq, rank, (tokens, token_own), token_window, t_send, t_recv, t_pass)
    for copy in hops_across:
        copy.wait_recv()
    half = plan.sequences // 2
    for stream in range(2):
        total = across[stream * half]
        for i in range(1, half):
            total = total + across[stream * half + i]
        chunk[stream] = total
    hops_back = []
    for step in range(1, plan.group):
        to = other(rank, step, plan.group)
        copy = remote(chunk, mods.at[rank], m_send.at[2, step], m_recv.at[2, step], plan.device_of(seq, to))
        copy.start()
        hops_back.append(copy)
    mods[rank] = chunk[...]
    share_rows(plan, seq, rank, (grads, grad_own), grad_window, g_send, g_recv, g_pass)
    for copy in hops_back:
        copy.wait_recv()
    for copy in hops + hops_across + hops_back:
        copy.wait_send()
    for which, (source, own) in enumerate(arrays):
        for index, (to_rank, row, rows, step, owner, owner_row) in enumerate(plan.segments):
            @pl.when(rank == owner)
            def _():
                remote(
                    source.at[pl.ds(owner_row, rows)],
                    own.at[pl.ds(row, rows)],
                    edge_send.at[which * count + index],
                    edge_recv.at[which * count + index],
                    plan.device_of(lax.rem(seq + plan.sequences - step, plan.sequences), to_rank),
                ).wait_send()


def entry(plan, tokens, grads, mod_part):
    lanes = mod_part.shape[1] // plan.group // 128
    pieces = mod_part.reshape(plan.sequences, plan.group, lanes, 128).transpose(1, 0, 2, 3)
    window = jax.ShapeDtypeStruct((plan.rows, plan.width), BF16)
    dma = pltpu.SemaphoreType.DMA
    most = max(plan.group, plan.sequences)
    token_window, grad_window, mods = call(
        functools.partial(entry_kernel, plan),
        "entry",
        1,
        (window, window, jax.ShapeDtypeStruct((plan.group, 2, lanes, 128), F32)),
        [
            pltpu.VMEM((plan.piece, plan.width), BF16),
            pltpu.VMEM((plan.piece, plan.width), BF16),
            pltpu.VMEM((plan.group, plan.sequences, lanes, 128), F32),
            pltpu.VMEM((plan.sequences, lanes, 128), F32),
            pltpu.VMEM((2, lanes, 128), F32),
            dma((2 * len(plan.segments),)),
            dma((2 * len(plan.segments),)),
        ]
        + share_scratch(plan)
        + share_scratch(plan)
        + [dma((3, most)), dma((3, most))],
        (tokens, grads, pieces),
    )
    return token_window, grad_window, mods.transpose(1, 0, 2, 3).reshape(2, -1)


def project_columns(plan, rank):
    share = plan.width // plan.group
    first = (rank % 2) * (plan.width // 2) + (rank // 2) * share
    return [part * plan.width + first for part in range(3)], share


def up_columns(plan, rank, cols):
    planes = plan.sequences // 2
    share = cols // planes // plan.group
    return [plane * plan.group * share + rank * share for plane in range(planes)], share


def start_swap(plan, seq, rank, source, target, send, recv):
    copies = []
    for step in range(1, plan.group):
        to = other(rank, step, plan.group)
        copy = remote(source.at[to], target.at[rank], send.at[step], recv.at[step], plan.device_of(seq, to))
        copy.start()
        copies.append(copy)
    target[rank] = source[rank]
    return copies


def swap_in_kernel(plan, project, up, project_out, up_out, project_cut, up_cut, p_send, p_recv, u_send, u_recv):
    seq, rank = here(plan)
    for to in range(plan.group):
        starts, share = project_columns(plan, to)
        project_cut[to] = jnp.concatenate([project[:, c : c + share] for c in starts], axis=1)
    meet(group_devices(plan, seq, rank))
    copies = start_swap(plan, seq, rank, project_cut, project_out, p_send, p_recv)
    for to in range(plan.group):
        starts, share = up_columns(plan, to, up.shape[1])
        up_cut[to] = jnp.concatenate([up[:, c : c + share] for c in starts], axis=1)
    copies += start_swap(plan, seq, rank, up_cut, up_out, u_send, u_recv)
    for copy in copies:
        copy.wait()


def swap_in(plan, project, up):
    rows = project.shape[0]
    dma = pltpu.SemaphoreType.DMA
    shapes = [(plan.group, rows, project.shape[1] // plan.group), (plan.group, rows, up.shape[1] // plan.group)]
    return call(
        functools.partial(swap_in_kernel, plan),
        "swap_in",
        4,
        tuple(jax.ShapeDtypeStruct(shape, BF16) for shape in shapes),
        [pltpu.VMEM(shape, BF16) for shape in shapes] + [dma((plan.group,))] * 4,
        (project, up),
    )


def swap_out_kernel(plan, columns, pieces, out, got, send, recv):
    seq, rank = here(plan)
    meet(group_devices(plan, seq, rank))
    copies = start_swap(plan, seq, rank, pieces, got, send, recv)
    for copy in copies:
        copy.wait()
    for source in range(plan.group):
        starts, share = columns(plan, source)
        piece = got[source].astype(F32)
        for i, c in enumerate(starts):
            out[:, c : c + share] = piece[:, i * share : (i + 1) * share]


def swap_out(plan, pieces, columns, name, ident):
    dma = pltpu.SemaphoreType.DMA
    group, rows, cols = pieces.shape
    return call(
        functools.partial(swap_out_kernel, plan, columns),
        name,
        ident,
        jax.ShapeDtypeStruct((rows, group * cols), F32),
        [pltpu.VMEM(pieces.shape, BF16), dma((plan.group,)), dma((plan.group,))],
        (pieces,),
    )


def pick_rows(table, text):
    return jnp.where(text > 0, table[1:2, :], table[0:1, :])


def norm_rows(values):
    mean = jnp.mean(values, axis=1, keepdims=True)
    centred = values - mean
    inv = lax.rsqrt(jnp.mean(centred * centred, axis=1, keepdims=True) + EPSILON)
    return centred * inv, inv


def middle_kernel(plan, part, tokens, gate_a, scale_b, shift_b, text, merged, window, own, *scratch):
    seq, rank = here(plan)
    meet(group_devices(plan, seq, rank))
    total = scatter_sum(plan, seq, rank, part, *scratch[:7])
    merged[...] = total
    mask = text[...]
    middle = tokens[...].astype(F32) + pick_rows(gate_a[...], mask) * total
    normed, _ = norm_rows(middle)
    own[...] = (normed * (1.0 + pick_rows(scale_b[...], mask)) + pick_rows(shift_b[...], mask)).astype(BF16)
    share_rows(plan, seq, rank, own_parts(plan, own), window, *scratch[7:])


def own_shape(plan, dtype=F32):
    return jax.ShapeDtypeStruct((plan.own, plan.width), dtype)


def window_shape(plan):
    return jax.ShapeDtypeStruct((plan.rows, plan.width), BF16)


def middle_rows(plan, part, tokens, gate_a, scale_b, shift_b, text):
    return call(
        functools.partial(middle_kernel, plan),
        "middle",
        2,
        (own_shape(plan), window_shape(plan)),
        [pltpu.VMEM((plan.own, plan.width), BF16)] + sum_scratch(plan) + share_scratch(plan),
        (part, tokens, gate_a, scale_b, shift_b, text),
    )


def back_kernel(plan, part, grad, middle, gate_a, scale_b, text, grad_hidden, grad_middle, window, own, *scratch):
    seq, rank = here(plan)
    meet(group_devices(plan, seq, rank))
    total = scatter_sum(plan, seq, rank, part, *scratch[:7])
    grad_hidden[...] = total
    mask = text[...]
    normed, inv = norm_rows(middle[...])
    inner = total * (1.0 + pick_rows(scale_b[...], mask))
    mean_grad = jnp.mean(inner, axis=1, keepdims=True)
    mean_cross = jnp.mean(inner * normed, axis=1, keepdims=True)
    result = grad[...].astype(F32) + inv * (inner - mean_grad - normed * mean_cross)
    grad_middle[...] = result
    own[...] = (pick_rows(gate_a[...], mask) * result).astype(BF16)
    share_rows(plan, seq, rank, own_parts(plan, own), window, *scratch[7:])


def back_rows(plan, part, grad, middle, gate_a, scale_b, text):
    return call(
        functools.partial(back_kernel, plan),
        "back",
        3,
        (own_shape(plan), own_shape(plan), window_shape(plan)),
        [pltpu.VMEM((plan.own, plan.width), BF16)] + sum_scratch(plan) + share_scratch(plan),
        (part, grad, middle, gate_a, scale_b, text),
    )


def edge_copy(plan, seq, source, first_row, target, send, recv, index):
    from_rank, row, rows, step, owner, owner_row = plan.segments[index]
    return remote(
        source.at[pl.ds(first_row + row, rows)],
        target.at[pl.ds(owner_row, rows)],
        send.at[index],
        recv.at[index],
        plan.device_of(lax.rem(seq + plan.sequences + step, plan.sequences), owner),
    )


def start_edges(plan, seq, rank, *refs):
    for index, segment in enumerate(plan.segments):
        @pl.when(rank == segment[0])
        def _():
            edge_copy(plan, seq, *refs, index).start()


def finish_edges(plan, seq, rank, *refs):
    for index, segment in enumerate(plan.segments):
        @pl.when(rank == segment[4])
        def _():
            edge_copy(plan, seq, *refs, index).wait_recv()

        @pl.when(rank == segment[0])
        def _():
            edge_copy(plan, seq, *refs, index).wait_send()


def edge_scratch(plan):
    return [pltpu.SemaphoreType.DMA((len(plan.segments),))] * 2


def output_kernel(plan, part, middle, gate_b, text, lowered, out, extra, own, *scratch):
    device = lax.axis_index("dev")
    seq, rank = plan.place_of(device)
    extra[...] = jnp.zeros_like(extra)
    meet(every_device(plan, device))
    total = scatter_sum(plan, seq, rank, part, *scratch[:7])
    lowered[...] = total
    own[...] = (middle[...] + pick_rows(gate_b[...], text[...]) * total).astype(BF16)
    refs = (own, plan.rows_dev, extra) + scratch[7:]
    start_edges(plan, seq, rank, *refs)
    out[...] = own[pl.ds(0, plan.rows_dev)]
    finish_edges(plan, seq, rank, *refs)


def output_rows(plan, part, middle, gate_b, text):
    rows = jax.ShapeDtypeStruct((plan.rows_dev, plan.width), BF16)
    return call(
        functools.partial(output_kernel, plan),
        "output",
        8,
        (own_shape(plan), rows, rows),
        [pltpu.VMEM((plan.own, plan.width), BF16)] + sum_scratch(plan) + edge_scratch(plan),
        (part, middle, gate_b, text),
    )


def stream_sums(values, masks):
    return jnp.concatenate([jnp.sum(values * mask, axis=0, keepdims=True) for mask in masks], axis=0)


def last_kernel(plan, part, tokens, grad_middle, scale_a, text, masks, rest, out, extra, table,
                own, local, first, second, mine, t_send, t_recv, *scratch):
    device = lax.axis_index("dev")
    seq, rank = plan.place_of(device)
    stream = lax.div(2 * seq, plan.sequences)
    extra[...] = jnp.zeros_like(extra)
    meet(every_device(plan, device))
    total = scatter_sum(plan, seq, rank, part, *scratch[:7])
    normed, inv = norm_rows(tokens[...].astype(F32))
    streams = (masks[:, 0:1], masks[:, 1:2])
    local[:, : plan.width] = stream_sums(total, streams)
    local[:, plan.width : 2 * plan.width] = stream_sums(total * normed, streams)
    local[:, 2 * plan.width :] = rest[...]
    cols = 6 * plan.width // plan.group

    def chunk(index):
        return pl.ds(pl.multiple_of(index * cols, 128), cols)

    hops = []
    for step in range(1, plan.group):
        to = other(rank, step, plan.group)
        copy = remote(local.at[:, chunk(to)], first.at[step], t_send.at[0, step], t_recv.at[0, step], plan.device_of(seq, to))
        copy.start()
        hops.append(copy)
    inner = total * (1.0 + pick_rows(scale_a[...], text[...]))
    mean_grad = jnp.mean(inner, axis=1, keepdims=True)
    mean_cross = jnp.mean(inner * normed, axis=1, keepdims=True)
    own[...] = grad_middle[...] + inv * (inner - mean_grad - normed * mean_cross)
    refs = (own, plan.rows_dev, extra) + scratch[7:]
    start_edges(plan, seq, rank, *refs)
    for copy in hops:
        copy.wait_recv()
    sums = local[:, chunk(rank)]
    for step in range(1, plan.group):
        sums = sums + first[step]
    for i in range(2):
        mine[i] = sums[i : i + 1]
    across = []
    for step in range(1, plan.sequences):
        to = other(seq, step, plan.sequences)
        to_stream = lax.div(2 * to, plan.sequences)
        copy = remote(mine.at[to_stream], second.at[seq], t_send.at[1, step], t_recv.at[1, step], plan.device_of(to, rank))
        copy.start()
        across.append(copy)
    second[seq] = mine[stream]
    out[...] = own[pl.ds(0, plan.rows_dev)]
    for copy in across:
        copy.wait_recv()
    last = []
    for step in range(1, plan.group):
        to = other(rank, step, plan.group)
        copy = remote(second, table.at[rank], t_send.at[2, step], t_recv.at[2, step], plan.device_of(seq, to))
        copy.start()
        last.append(copy)
    table[rank] = second[...]
    for copy in last:
        copy.wait_recv()
    for copy in hops + across + last:
        copy.wait_send()
    finish_edges(plan, seq, rank, *refs)


def last_rows(plan, part, tokens, grad_middle, scale_a, text, masks, rest):
    rows = jax.ShapeDtypeStruct((plan.rows_dev, plan.width), F32)
    cols = 6 * plan.width // plan.group
    dma = pltpu.SemaphoreType.DMA
    most = max(plan.group, plan.sequences)
    out, extra, table = call(
        functools.partial(last_kernel, plan),
        "last",
        10,
        (rows, rows, jax.ShapeDtypeStruct((plan.group, plan.sequences, 1, cols), F32)),
        [
            pltpu.VMEM((plan.own, plan.width), F32),
            pltpu.VMEM((2, 6 * plan.width), F32),
            pltpu.VMEM((plan.group, 2, cols), F32),
            pltpu.VMEM((plan.sequences, 1, cols), F32),
            pltpu.VMEM((2, 1, cols), F32),
            dma((3, most)),
            dma((3, most)),
        ]
        + sum_scratch(plan)
        + edge_scratch(plan),
        (part, tokens, grad_middle, scale_a, text, masks, rest),
    )
    return out, extra, table[:, :, 0].transpose(1, 0, 2).reshape(plan.sequences, -1)


def spread_kernel(plan, piece, everyone, send, recv):
    device = lax.axis_index("dev")
    seq, rank = plan.place_of(device)
    meet(group_devices(plan, seq, rank) + column_devices(plan, seq, rank))
    copies = []
    everyone[seq, rank] = piece[...]
    for step in range(1, plan.group):
        to = other(rank, step, plan.group)
        copy = remote(piece, everyone.at[seq, rank], send.at[0, step], recv.at[0, step], plan.device_of(seq, to))
        copy.start()
        copies.append(copy)
    for copy in copies:
        copy.wait_recv()
    across = []
    for step in range(1, plan.sequences):
        to = other(seq, step, plan.sequences)
        copy = remote(everyone.at[seq], everyone.at[seq], send.at[1, step], recv.at[1, step], plan.device_of(to, rank))
        copy.start()
        across.append(copy)
    for copy in across:
        copy.wait_recv()
    for copy in copies + across:
        copy.wait_send()


def spread(plan, piece, ident):
    dma = pltpu.SemaphoreType.DMA
    most = max(plan.group, plan.sequences)
    return call(
        functools.partial(spread_kernel, plan),
        "spread",
        ident,
        jax.ShapeDtypeStruct((plan.sequences, plan.group) + piece.shape, piece.dtype),
        [dma((2, most)), dma((2, most))],
        (piece,),
    )


def over_sequences(plan, pieces):
    full = lax.all_gather(pieces, "dev", axis=0, axis_index_groups=plan.rank_groups())
    return full.reshape(2, plan.width, pieces.shape[2])


def terms_to_send(plan, grad, rows):
    return grad.astype(BF16).reshape(plan.sequences, plan.group, rows, grad.shape[2])


def over_sequences_sum(plan, pieces):
    return lax.psum_scatter(pieces, "dev", scatter_dimension=0, axis_index_groups=plan.rank_groups())


def chip_groups(plan):
    return [
        [plan.device_of(s, 2 * q + core) for s in range(plan.sequences) for core in range(2)]
        for q in range(plan.group // 2)
    ]


def merge_slices(plan, weight, rank):
    half = plan.group // 2
    rows = weight.shape[0]
    share = plan.width // plan.group
    if plan.chip_heads:
        full = lax.all_gather(weight, "dev", axis=0, axis_index_groups=chip_groups(plan))
        full = full.reshape(2, 2, share, weight.shape[1])
        return lax.dynamic_index_in_dim(full, lax.rem(rank, 2), 1, keepdims=False)
    full = lax.all_gather(weight, "dev", axis=0, tiled=True)
    full = full.reshape(2, 2, half, share, weight.shape[1])
    full = lax.dynamic_index_in_dim(full, lax.rem(rank, 2), 1, keepdims=False)
    return lax.dynamic_index_in_dim(full, lax.div(rank, 2), 1, keepdims=False)


def merge_grads(plan, grad, rank):
    half = plan.group // 2
    _, share, cols = grad.shape
    core = lax.rem(rank, 2)
    grad = grad.astype(BF16)
    mine = [jnp.where(core == k, grad, jnp.zeros((), BF16)) for k in range(2)]
    if plan.chip_heads:
        full = jnp.stack(mine, axis=1).reshape(2 * plan.sequences, -1, cols)
        out = lax.psum_scatter(full, "dev", scatter_dimension=0, axis_index_groups=chip_groups(plan))
        return out.astype(F32)
    full = jnp.zeros((2, 2, half, share, cols), BF16)
    full = lax.dynamic_update_slice_in_dim(full, jnp.stack(mine, axis=1)[:, :, None], lax.div(rank, 2), 2)
    return lax.psum_scatter(full.reshape(-1, cols), "dev", scatter_dimension=0, tiled=True).astype(F32)


def down_slices(plan, weight):
    full = lax.all_gather(weight, "dev", axis=0, axis_index_groups=plan.rank_groups())
    return full.reshape(2, -1, weight.shape[1])


def by_stream(plan, image_part, text_part, is_text):
    start, end = plan.text_start, plan.image_end
    mixed = jnp.where(is_text[start:end, None], text_part[: end - start], image_part[start:])
    return jnp.concatenate([image_part[:start], mixed, text_part[end - start :]], axis=0)


def stream_dot(plan, rows, pair, is_text):
    image_part = jnp.dot(rows[: plan.image_end], pair[0], preferred_element_type=F32)
    text_part = jnp.dot(rows[plan.text_start :], pair[1], preferred_element_type=F32)
    return by_stream(plan, image_part, text_part, is_text)


def stream_dot_back(plan, grads, pair, is_text):
    image_part = lax.dot_general(grads[: plan.image_end], pair[0], CONTRACT_LAST, preferred_element_type=F32)
    text_part = lax.dot_general(grads[plan.text_start :], pair[1], CONTRACT_LAST, preferred_element_type=F32)
    return by_stream(plan, image_part, text_part, is_text)


def weight_terms(plan, rows, grads, is_text):
    zero = jnp.zeros((), grads.dtype)
    image = jnp.where(is_text[: plan.image_end, None], zero, grads[: plan.image_end])
    text = jnp.where(is_text[plan.text_start :, None], grads[plan.text_start :], zero)
    image_term = lax.dot_general(rows[: plan.image_end], image, CONTRACT_FIRST, preferred_element_type=F32)
    text_term = lax.dot_general(rows[plan.text_start :], text, CONTRACT_FIRST, preferred_element_type=F32)
    return jnp.stack([image_term, text_term])


def pick(table, text_rows):
    return jnp.where(text_rows[:, None], table[1][None, :], table[0][None, :])


def on_device(
    tokens,
    conditioning,
    text_lengths,
    modulation_weight,
    project_weight,
    merge_weight,
    up_weight,
    down_weight,
    cotangent,
):
    rows_dev, width = tokens.shape
    mod_rows = modulation_weight.shape[0]
    plan = Plan(lax.axis_size("dev"), conditioning.shape[0], rows_dev, width)
    device = lax.axis_index("dev")
    seq, rank = plan.place_of(device)
    feature_start = device * mod_rows % width

    ends = jnp.cumsum(IMG + text_lengths)
    starts = jnp.concatenate([jnp.zeros((1,), jnp.int32), ends[:-1]])
    positions = device * rows_dev + jnp.arange(rows_dev, dtype=jnp.int32)
    row_seq = jnp.sum((starts[None, :] <= positions[:, None]).astype(jnp.int32), axis=1) - 1
    offset = plan.span * seq - plan.edge + jnp.arange(plan.rows, dtype=jnp.int32) - starts[seq]
    valid = (offset >= 0) & (offset < IMG + text_lengths[seq])
    is_text = offset >= IMG
    bias = jnp.where(valid, 0.0, MASKED).astype(F32)[None, :]
    own_valid = own_rows(plan, valid[:, None], rank)[:, 0]
    own_text = own_rows(plan, is_text[:, None], rank)[:, 0]

    cond_float = conditioning.astype(F32)
    silu_low = jax.nn.silu(cond_float).astype(BF16)
    silu_part = lax.dynamic_slice_in_dim(silu_low, feature_start, mod_rows, 1)
    mod_part = jnp.dot(silu_part, modulation_weight, preferred_element_type=F32)

    merge_pair = merge_slices(plan, merge_weight, rank)
    project_pieces, up_pieces = swap_in(plan, project_weight, up_weight)
    project_pieces, up_pieces, merge_pair = lax.optimization_barrier((project_pieces, up_pieces, merge_pair))
    project_pair = over_sequences(plan, project_pieces)
    up_pair = over_sequences(plan, up_pieces)
    down_pair = down_slices(plan, down_weight)

    token_window, grad_window, mods = entry(plan, tokens, cotangent, mod_part)
    shift_a, scale_a, gate_a, shift_b, scale_b, gate_b = jnp.split(mods, 6, axis=1)
    grad_window = jnp.where(valid[:, None], grad_window, jnp.zeros((), BF16))

    normed_full, _ = layer_norm(token_window.astype(F32))
    hidden_a = (normed_full * (1.0 + pick(scale_a, is_text)) + pick(shift_a, is_text)).astype(BF16)
    projected = stream_dot(plan, hidden_a, project_pair, is_text).astype(BF16)
    queries, keys, values = jnp.split(projected, 3, axis=1)
    attended = attend(plan, queries, keys, values, bias)

    own_tokens = own_rows(plan, token_window, rank)
    own_grad = own_rows(plan, grad_window, rank)
    text_mask = own_text.astype(F32)[:, None]
    merged, hidden_b = middle_rows(
        plan, stream_dot(plan, attended, merge_pair, is_text), own_tokens, gate_a, scale_b, shift_b, text_mask
    )
    middle = own_tokens.astype(F32) + pick(gate_a, own_text) * merged
    normed_b, inv_b = layer_norm(middle)

    upper = stream_dot(plan, hidden_b, up_pair, is_text)
    activated = jax.nn.gelu(upper, approximate=True).astype(BF16)
    grad_lowered = (pick(gate_b, is_text) * grad_window.astype(F32)).astype(BF16)
    down_term = weight_terms(plan, activated, grad_lowered, is_text).astype(BF16)
    down_term = down_term.reshape(plan.sequences, -1, width)
    down_term, grad_lowered = lax.optimization_barrier((down_term, grad_lowered))
    down_sum = over_sequences_sum(plan, down_term)
    grad_activated = stream_dot_back(plan, grad_lowered, down_pair, is_text)
    gelu_pull = jax.vjp(lambda value_in: jax.nn.gelu(value_in, approximate=True), upper)[1]
    grad_upper = gelu_pull(grad_activated)[0].astype(BF16)
    up_term = terms_to_send(plan, weight_terms(plan, hidden_b, grad_upper, is_text), mod_rows)
    back_part = stream_dot_back(plan, grad_upper, up_pair, is_text)
    back_part, up_term = lax.optimization_barrier((back_part, up_term))
    up_sum = over_sequences_sum(plan, up_term)
    grad_hidden_b, grad_middle, grad_merged = back_rows(
        plan, back_part, own_grad, middle, gate_a, scale_b, text_mask
    )
    foreign = (row_seq != seq)[:, None]
    lowered, out_here, out_there = output_rows(
        plan, stream_dot(plan, activated, down_pair, is_text), middle, gate_b, text_mask
    )
    layer_out = jnp.where(foreign, out_there, out_here)
    grad_attended = stream_dot_back(plan, grad_merged, merge_pair, is_text).astype(BF16)
    merge_grad = merge_grads(plan, weight_terms(plan, attended, grad_merged, is_text), rank)

    grad_projected = jnp.concatenate(attend_back(plan, queries, keys, values, grad_attended, bias), axis=1)
    grad_projected, down_sum = lax.optimization_barrier((grad_projected, down_sum))
    down_grad = down_sum.astype(F32)
    project_term = terms_to_send(plan, weight_terms(plan, hidden_a, grad_projected, is_text), mod_rows)
    last_part = stream_dot_back(plan, grad_projected, project_pair, is_text)
    last_part, project_term = lax.optimization_barrier((last_part, project_term))
    project_sum = over_sequences_sum(plan, project_term)

    masks = jnp.stack([own_valid & ~own_text, own_valid & own_text], axis=1).astype(F32)
    rest = jnp.concatenate(
        [
            jnp.stack([jnp.sum(value * masks[:, j : j + 1], axis=0) for j in range(2)])
            for value in (
                grad_middle * merged,
                grad_hidden_b,
                grad_hidden_b * normed_b,
                own_grad.astype(F32) * lowered,
            )
        ],
        axis=1,
    )
    rest, up_sum = lax.optimization_barrier((rest, up_sum))
    back_here, back_there, grad_table = last_rows(
        plan, last_part, own_tokens, grad_middle, scale_a, text_mask, masks, rest
    )
    tokens_grad = jnp.where(foreign, back_there, back_here)
    own_grads = grad_table.astype(BF16)
    up_grad = swap_out(plan, up_sum, lambda p, r: up_columns(p, r, up_weight.shape[1]), "up_out", 7)
    project_grad = swap_out(plan, project_sum, project_columns, "project_out", 6)
    modulation_grad = lax.dot_general(silu_part, own_grads, CONTRACT_FIRST, preferred_element_type=F32)
    grad_piece = lax.dot_general(own_grads, modulation_weight, CONTRACT_LAST, preferred_element_type=F32)
    everyone = spread(plan, grad_piece.reshape(-1, 128), 13)
    everyone = everyone.reshape(2, plan.devices // 2, plan.sequences, mod_rows)
    grad_silu = (everyone[0] + everyone[1]).transpose(1, 0, 2).reshape(plan.sequences, width)
    conditioning_grad = jax.vjp(jax.nn.silu, cond_float)[1](grad_silu)[0]
    return (
        layer_out,
        tokens_grad,
        conditioning_grad,
        modulation_grad,
        project_grad,
        merge_grad,
        up_grad,
        down_grad,
    )


def solution(mesh):
    shard, whole = P("dev", None), P()
    return jax.shard_map(
        on_device,
        mesh=mesh,
        in_specs=(shard, whole, whole, shard, shard, shard, shard, shard, shard),
        out_specs=(shard, shard, whole, shard, shard, shard, shard, shard),
        check_vma=False,
    )
```

```python
import functools

import jax
import jax.numpy as jnp
import numpy as np
from jax import lax
from jax.experimental import pallas as pl
from jax.experimental.pallas import tpu as pltpu
from jax.sharding import PartitionSpec as P

HEADS = 24
HDIM = 64
IMG = 1024
TXT_MIN = 86
TXT_MAX = 154
EPSILON = 1e-06
F32 = jnp.float32
BF16 = jnp.bfloat16
CONTRACT_LAST = (((1,), (1,)), ((), ()))
PLAIN = (((1,), (0,)), ((), ()))
CONTRACT_FIRST = (((0,), (0,)), ((), ()))
MASKED = -1e30


class Plan:
    def __init__(self, devices, sequences, rows_dev, width):
        self.devices, self.sequences, self.rows_dev, self.width = devices, sequences, rows_dev, width
        self.group = devices // sequences
        self.span = self.group * rows_dev
        mean = self.span - IMG
        up, down = TXT_MAX - mean, mean - TXT_MIN
        drift = 0
        for k in range(sequences + 1):
            drift = max(drift, min(up * k, down * (sequences - k)), min(down * k, up * (sequences - k)))
        self.edge = -(-drift // 64) * 64
        self.rows = self.span + 2 * self.edge
        self.piece = 2 * self.edge // self.group
        self.own = rows_dev + self.piece
        self.image_end = -(-(self.edge + drift + IMG) // 128) * 128
        self.text_start = (self.edge - drift + IMG) // 128 * 128
        self.heads = HEADS // self.group
        self.segments = self.edge_segments()
        self.chip_heads = devices == 4 * self.group

    def device_of(self, seq, rank):
        return seq * self.group + rank

    def place_of(self, device):
        return lax.div(device, self.group), lax.rem(device, self.group)

    def seq_groups(self):
        return [[self.device_of(s, r) for r in range(self.group)] for s in range(self.sequences)]

    def rank_groups(self):
        return [[self.device_of(s, r) for s in range(self.sequences)] for r in range(self.group)]

    def edge_row(self, rank):
        half = self.group // 2
        return jnp.where(rank < half, self.piece * rank, self.edge + self.span + self.piece * (rank - half))

    def main_row(self, rank):
        return self.edge + self.rows_dev * rank

    def edge_segments(self):
        found = []
        for rank in range(self.group):
            half = self.group // 2
            first = self.piece * rank - self.edge if rank < half else self.span + self.piece * (rank - half)
            row = 0
            while row < self.piece:
                owner, owner_row = (first + row) // self.rows_dev, (first + row) % self.rows_dev
                count = min(self.piece - row, self.rows_dev - owner_row)
                found.append((rank, row, count, owner // self.group, owner % self.group, owner_row))
                row += count
        return found


def layer_norm(values):
    mean = jnp.mean(values, axis=-1, keepdims=True)
    centred = values - mean
    variance = jnp.mean(centred * centred, axis=-1, keepdims=True)
    inv_std = lax.rsqrt(variance + EPSILON)
    return (centred * inv_std, inv_std)


def norm_back(grad_normed, normed, inv_std):
    mean_grad = jnp.mean(grad_normed, axis=-1, keepdims=True)
    mean_cross = jnp.mean(grad_normed * normed, axis=-1, keepdims=True)
    return inv_std * (grad_normed - mean_grad - normed * mean_cross)


def softmax_parts(query, key, bias):
    scores = lax.dot_general(query, key, CONTRACT_LAST, preferred_element_type=F32) + bias
    top = jnp.max(scores, axis=1, keepdims=True)
    exponent = jnp.exp(scores - top)
    total = jnp.sum(exponent, axis=1, keepdims=True)
    return exponent * (1.0 / total)


def attend_kernel(heads, q_ref, k_ref, v_ref, bias_ref, out_ref):
    bias = bias_ref[...]
    outs = []
    for head in range(heads):
        cols = slice(head * HDIM, (head + 1) * HDIM)
        query = q_ref[:, cols] * jnp.asarray(HDIM ** (-0.5), BF16)
        probs = softmax_parts(query, k_ref[:, cols], bias).astype(BF16)
        outs.append(jnp.dot(probs, v_ref[:, cols], preferred_element_type=F32))
    out_ref[...] = jnp.concatenate(outs, axis=1).astype(BF16)


def block_rows(rows):
    return 256 if rows % 256 == 0 else 128


def attend(plan, queries, keys, values, bias):
    rows, cols = queries.shape
    block = block_rows(rows)
    whole = pl.BlockSpec((rows, cols), lambda i: (0, 0))
    return pl.pallas_call(
        functools.partial(attend_kernel, plan.heads),
        out_shape=jax.ShapeDtypeStruct((rows, cols), BF16),
        grid=(rows // block,),
        in_specs=[
            pl.BlockSpec((block, cols), lambda i: (i, 0)),
            whole,
            whole,
            pl.BlockSpec((1, rows), lambda i: (0, 0)),
        ],
        out_specs=pl.BlockSpec((block, cols), lambda i: (i, 0)),
        compiler_params=pltpu.CompilerParams(vmem_limit_bytes=48 << 20),
        cost_estimate=pl.CostEstimate(flops=16 * rows * rows * cols, bytes_accessed=8 * rows * cols, transcendentals=0),
        name="attend",
    )(queries, keys, values, bias)


def attend_back_kernel(heads, steps, q_ref, k_ref, v_ref, g_ref, bias_ref, gq_ref, gk_ref, gv_ref, key_sum, value_sum):
    step = pl.program_id(0)
    scale = jnp.asarray(HDIM ** (-0.5), BF16)

    @pl.when(step == 0)
    def _():
        key_sum[...] = jnp.zeros_like(key_sum)
        value_sum[...] = jnp.zeros_like(value_sum)

    bias = bias_ref[...]
    grads = []
    for head in range(heads):
        cols = slice(head * HDIM, (head + 1) * HDIM)
        query = q_ref[:, cols] * scale
        key = k_ref[:, cols]
        grad_out = g_ref[:, cols]
        probs = softmax_parts(query, key, bias)
        grad_probs = lax.dot_general(grad_out, v_ref[:, cols], CONTRACT_LAST, preferred_element_type=F32)
        inner = jnp.sum(probs * grad_probs, axis=1, keepdims=True)
        grad_scores = (probs * (grad_probs - inner)).astype(BF16)
        grads.append(jnp.dot(grad_scores, key, preferred_element_type=F32) * HDIM ** (-0.5))
        key_sum[head] += lax.dot_general(query, grad_scores, CONTRACT_FIRST, preferred_element_type=F32)
        value_sum[head] += lax.dot_general(grad_out, probs.astype(BF16), CONTRACT_FIRST, preferred_element_type=F32)
    gq_ref[...] = jnp.concatenate(grads, axis=1).astype(BF16)

    @pl.when(step == steps - 1)
    def _():
        rows = gk_ref.shape[0]
        gk_ref[...] = key_sum[...].reshape(heads * HDIM, rows).T.astype(BF16)
        gv_ref[...] = value_sum[...].reshape(heads * HDIM, rows).T.astype(BF16)


def attend_back(plan, queries, keys, values, grad_out, bias):
    rows, cols = queries.shape
    block = block_rows(rows)
    whole = pl.BlockSpec((rows, cols), lambda i: (0, 0))
    part = pl.BlockSpec((block, cols), lambda i: (i, 0))
    shape = jax.ShapeDtypeStruct((rows, cols), BF16)
    return pl.pallas_call(
        functools.partial(attend_back_kernel, plan.heads, rows // block),
        out_shape=(shape, shape, shape),
        grid=(rows // block,),
        in_specs=[part, whole, whole, part, pl.BlockSpec((1, rows), lambda i: (0, 0))],
        out_specs=(part, whole, whole),
        scratch_shapes=[pltpu.VMEM((plan.heads, HDIM, rows), F32)] * 2,
        compiler_params=pltpu.CompilerParams(vmem_limit_bytes=56 << 20),
        cost_estimate=pl.CostEstimate(flops=40 * rows * rows * cols, bytes_accessed=14 * rows * cols, transcendentals=0),
        name="attend_back",
    )(queries, keys, values, grad_out, bias)


VMEM = pl.BlockSpec(memory_space=pltpu.VMEM)


def own_rows(plan, window, rank):
    main = lax.dynamic_slice_in_dim(window, plan.main_row(rank), plan.rows_dev, 0)
    edge = lax.dynamic_slice_in_dim(window, plan.edge_row(rank), plan.piece, 0)
    return jnp.concatenate([main, edge], axis=0)


def remote(source, target, send_sem, recv_sem, device):
    return pltpu.make_async_remote_copy(
        src_ref=source,
        dst_ref=target,
        send_sem=send_sem,
        recv_sem=recv_sem,
        device_id=(device,),
        device_id_type=pl.DeviceIdType.MESH,
    )


def here(plan):
    return plan.place_of(lax.axis_index("dev"))


def other(rank, step, size):
    return lax.rem(rank + step, size)


def meet(devices):
    barrier = pltpu.get_barrier_semaphore()
    for device in devices:
        pl.semaphore_signal(barrier, inc=1, device_id=(device,), device_id_type=pl.DeviceIdType.MESH)
    pl.semaphore_wait(barrier, len(devices))


def group_devices(plan, seq, rank):
    return [plan.device_of(seq, other(rank, step, plan.group)) for step in range(1, plan.group)]


def column_devices(plan, seq, rank):
    return [plan.device_of(other(seq, step, plan.sequences), rank) for step in range(1, plan.sequences)]


def every_device(plan, device):
    return [other(device, step, plan.devices) for step in range(1, plan.devices)]


def call(kernel, name, ident, out_shape, scratch, operands, in_specs=None, out_specs=None):
    outs = out_shape if isinstance(out_shape, tuple) else (out_shape,)
    return pl.pallas_call(
        kernel,
        out_shape=out_shape,
        in_specs=in_specs or [VMEM] * len(operands),
        out_specs=out_specs or (tuple([VMEM] * len(outs)) if isinstance(out_shape, tuple) else VMEM),
        scratch_shapes=scratch,
        compiler_params=pltpu.CompilerParams(
            collective_id=ident, has_side_effects=True, vmem_limit_bytes=40 << 20
        ),
        name=name,
    )(*operands)


def aligned(start):
    return pl.multiple_of(start, 16)


def block_parts(plan, ref, rank):
    return (
        ref.at[pl.ds(aligned(plan.main_row(rank)), plan.rows_dev)],
        ref.at[pl.ds(aligned(plan.edge_row(rank)), plan.piece)],
    )


def own_parts(plan, ref):
    return ref.at[pl.ds(0, plan.rows_dev)], ref.at[pl.ds(plan.rows_dev, plan.piece)]


def load_block(plan, ref, rank):
    main, edge = block_parts(plan, ref, rank)
    return jnp.concatenate([main[...], edge[...]], axis=0)


def sum_scratch(plan):
    half, own, width = plan.group // 2, plan.own, plan.width
    return [
        pltpu.VMEM((half, own, width), F32),
        pltpu.VMEM((half, own, width), F32),
        pltpu.VMEM((half, own, width), BF16),
        pltpu.VMEM((half, own, width), BF16),
        pltpu.SemaphoreType.DMA((half,)),
        pltpu.SemaphoreType.DMA((half,)),
        pltpu.SemaphoreType.DMA((half,)),
        pltpu.SemaphoreType.DMA((half,)),
    ]


SUM_SCRATCH = 8


def product(plan, rows, pair, text, dims, rank):
    block = load_block(plan, rows, rank)
    mask = load_block(plan, text, rank)
    parts = [lax.dot_general(block, pair[j], dims, preferred_element_type=F32) for j in range(2)]
    return jnp.where(mask > 0, parts[1], parts[0])


def scatter_sum(plan, seq, rank, rows, pair, text, dims, away, near, going, coming, pair_send, pair_recv, far_send, far_recv):
    half = plan.group // 2
    chip, core = lax.div(rank, 2), lax.rem(rank, 2)
    partner = plan.device_of(seq, 2 * chip + 1 - core)
    order = list(range(1, half)) + [0]

    def for_partner(step):
        away[step] = product(plan, rows, pair, text, dims, 2 * other(chip, step, half) + 1 - core)
        copy = remote(away.at[step], near.at[step], pair_send.at[step], pair_recv.at[step], partner)
        copy.start()
        return copy

    pairs, sends = [for_partner(order[0])], []
    for i, step in enumerate(order):
        chip_to = other(chip, step, half)
        mine = product(plan, rows, pair, text, dims, 2 * chip_to + core)
        if i + 1 < half:
            pairs.append(for_partner(order[i + 1]))
        pairs[i].wait_recv()
        both = mine + near[step]
        if step == 0:
            total = both
        else:
            going[step] = both.astype(BF16)
            copy = remote(
                going.at[step], coming.at[step], far_send.at[step], far_recv.at[step], plan.device_of(seq, 2 * chip_to + core)
            )
            copy.start()
            sends.append(copy)
    for step, copy in zip(order, sends):
        copy.wait_recv()
        total = total + coming[step].astype(F32)
    for copy in pairs + sends:
        copy.wait_send()
    return total


def share_scratch(plan):
    return [pltpu.SemaphoreType.DMA((plan.group, 2))] * 2 + [pltpu.SemaphoreType.DMA((plan.group, 2))]


def share_rows(plan, seq, rank, parts, window, send, recv, pass_send):
    half = plan.group // 2
    chip, core = lax.div(rank, 2), lax.rem(rank, 2)
    partner_rank = 2 * chip + 1 - core
    partner = plan.device_of(seq, partner_rank)

    def send_own(to_device, slot):
        copies = [
            remote(source, target, send.at[slot, i], recv.at[slot, i], to_device)
            for i, (source, target) in enumerate(zip(parts, block_parts(plan, window, rank)))
        ]
        for copy in copies:
            copy.start()
        return copies

    flying = {}
    for step in range(1, half):
        flying[step] = send_own(plan.device_of(seq, 2 * other(chip, step, half) + core), step)
    flying[0] = send_own(partner, 0)
    for source, target in zip(parts, block_parts(plan, window, rank)):
        target[...] = source[...]
    passed = []
    for step in range(1, half):
        for copy in flying[step]:
            copy.wait_recv()
        came = 2 * other(chip, half - step, half) + core
        copies = [
            remote(place, place, pass_send.at[step, i], recv.at[half + step, i], partner)
            for i, place in enumerate(block_parts(plan, window, came))
        ]
        for copy in copies:
            copy.start()
        passed.extend(copies)
    for copy in flying[0]:
        copy.wait_recv()
    for copy in passed:
        copy.wait_recv()
    for copies in flying.values():
        for copy in copies:
            copy.wait_send()
    for copy in passed:
        copy.wait_send()


def entry_kernel(plan, tokens, grads, mod_part, *refs):
    if plan.chip_heads:
        merge, merge_out, *refs = refs[:1] + refs[4:5] + refs[1:4] + refs[5:]
        merge_send, merge_recv, *refs = refs[-2:] + refs[:-2]
    (token_window, grad_window, mods, token_own, grad_own, plane, across, chunk, edge_send, edge_recv,
     t_send, t_recv, t_pass, g_send, g_recv, g_pass, m_send, m_recv) = refs
    device = lax.axis_index("dev")
    seq, rank = plan.place_of(device)
    meet(every_device(plan, device))
    swaps = []
    if plan.chip_heads:
        core = lax.rem(rank, 2)
        partner = plan.device_of(seq, 2 * lax.div(rank, 2) + 1 - core)
        for stream in range(2):
            copy = remote(
                merge.at[2 * stream + 1 - core],
                merge_out.at[stream, core],
                merge_send.at[stream],
                merge_recv.at[stream],
                partner,
            )
            copy.start()
            swaps.append(copy)
            merge_out[stream, core] = merge[2 * stream + core]
    hops = []
    for step in range(1, plan.group):
        to = other(rank, step, plan.group)
        copy = remote(mod_part.at[to], plane.at[step], m_send.at[0, step], m_recv.at[0, step], plan.device_of(seq, to))
        copy.start()
        hops.append(copy)
    arrays = ((tokens, token_own), (grads, grad_own))
    count = len(plan.segments)
    for which, (source, own) in enumerate(arrays):
        for index, (to_rank, row, rows, step, owner, owner_row) in enumerate(plan.segments):
            @pl.when(rank == owner)
            def _():
                remote(
                    source.at[pl.ds(owner_row, rows)],
                    own.at[pl.ds(row, rows)],
                    edge_send.at[which * count + index],
                    edge_recv.at[which * count + index],
                    plan.device_of(lax.rem(seq + plan.sequences - step, plan.sequences), to_rank),
                ).start()
    for copy in hops:
        copy.wait_recv()
    total = mod_part[rank]
    for step in range(1, plan.group):
        total = total + plane[step]
    plane[0] = total
    hops_across = []
    for step in range(1, plan.sequences):
        to = other(seq, step, plan.sequences)
        copy = remote(plane.at[0, to], across.at[seq], m_send.at[1, step], m_recv.at[1, step], plan.device_of(to, rank))
        copy.start()
        hops_across.append(copy)
    across[seq] = plane[0, seq]
    for which, (source, own) in enumerate(arrays):
        for index, (to_rank, row, rows, step, owner, owner_row) in enumerate(plan.segments):
            @pl.when(rank == to_rank)
            def _():
                remote(
                    source.at[pl.ds(owner_row, rows)],
                    own.at[pl.ds(row, rows)],
                    edge_send.at[which * count + index],
                    edge_recv.at[which * count + index],
                    plan.device_of(lax.rem(seq + plan.sequences + step, plan.sequences), owner),
                ).wait_recv()
    share_rows(plan, seq, rank, (tokens, token_own), token_window, t_send, t_recv, t_pass)
    for copy in hops_across:
        copy.wait_recv()
    half = plan.sequences // 2
    for stream in range(2):
        total = across[stream * half]
        for i in range(1, half):
            total = total + across[stream * half + i]
        chunk[stream] = total
    hops_back = []
    for step in range(1, plan.group):
        to = other(rank, step, plan.group)
        copy = remote(chunk, mods.at[rank], m_send.at[2, step], m_recv.at[2, step], plan.device_of(seq, to))
        copy.start()
        hops_back.append(copy)
    mods[rank] = chunk[...]
    share_rows(plan, seq, rank, (grads, grad_own), grad_window, g_send, g_recv, g_pass)
    for copy in hops_back:
        copy.wait_recv()
    for copy in hops + hops_across + hops_back:
        copy.wait_send()
    for copy in swaps:
        copy.wait()
    for which, (source, own) in enumerate(arrays):
        for index, (to_rank, row, rows, step, owner, owner_row) in enumerate(plan.segments):
            @pl.when(rank == owner)
            def _():
                remote(
                    source.at[pl.ds(owner_row, rows)],
                    own.at[pl.ds(row, rows)],
                    edge_send.at[which * count + index],
                    edge_recv.at[which * count + index],
                    plan.device_of(lax.rem(seq + plan.sequences - step, plan.sequences), to_rank),
                ).wait_send()


def entry(plan, tokens, grads, mod_part, merge):
    lanes = mod_part.shape[1] // plan.group // 128
    pieces = mod_part.reshape(plan.sequences, plan.group, lanes, 128).transpose(1, 0, 2, 3)
    window = jax.ShapeDtypeStruct((plan.rows, plan.width), BF16)
    dma = pltpu.SemaphoreType.DMA
    most = max(plan.group, plan.sequences)
    shapes = (window, window, jax.ShapeDtypeStruct((plan.group, 2, lanes, 128), F32))
    operands = (tokens, grads, pieces)
    scratch = (
        [
            pltpu.VMEM((plan.piece, plan.width), BF16),
            pltpu.VMEM((plan.piece, plan.width), BF16),
            pltpu.VMEM((plan.group, plan.sequences, lanes, 128), F32),
            pltpu.VMEM((plan.sequences, lanes, 128), F32),
            pltpu.VMEM((2, lanes, 128), F32),
            dma((2 * len(plan.segments),)),
            dma((2 * len(plan.segments),)),
        ]
        + share_scratch(plan)
        + share_scratch(plan)
        + [dma((3, most)), dma((3, most))]
    )
    if plan.chip_heads:
        shapes += (jax.ShapeDtypeStruct((2, 2) + merge.shape[1:], BF16),)
        operands += (merge,)
        scratch += [dma((2,)), dma((2,))]
    token_window, grad_window, mods, *rest = call(
        functools.partial(entry_kernel, plan), "entry", 1, shapes, scratch, operands
    )
    merge_pair = rest[0].reshape(2, -1, plan.width) if plan.chip_heads else merge
    return token_window, grad_window, mods.transpose(1, 0, 2, 3).reshape(2, -1), merge_pair


def project_columns(plan, rank):
    share = plan.width // plan.group
    first = (rank % 2) * (plan.width // 2) + (rank // 2) * share
    return [part * plan.width + first for part in range(3)], share


def up_columns(plan, rank, cols):
    planes = plan.sequences // 2
    share = cols // planes // plan.group
    return [plane * plan.group * share + rank * share for plane in range(planes)], share


def start_swap(plan, seq, rank, source, target, send, recv):
    copies = []
    for step in range(1, plan.group):
        to = other(rank, step, plan.group)
        copy = remote(source.at[to], target.at[rank], send.at[step], recv.at[step], plan.device_of(seq, to))
        copy.start()
        copies.append(copy)
    target[rank] = source[rank]
    return copies


def swap_in_kernel(plan, project, up, project_out, up_out, project_cut, up_cut, p_send, p_recv, u_send, u_recv):
    seq, rank = here(plan)
    for to in range(plan.group):
        starts, share = project_columns(plan, to)
        project_cut[to] = jnp.concatenate([project[:, c : c + share] for c in starts], axis=1)
    meet(group_devices(plan, seq, rank))
    copies = start_swap(plan, seq, rank, project_cut, project_out, p_send, p_recv)
    for to in range(plan.group):
        starts, share = up_columns(plan, to, up.shape[1])
        up_cut[to] = jnp.concatenate([up[:, c : c + share] for c in starts], axis=1)
    copies += start_swap(plan, seq, rank, up_cut, up_out, u_send, u_recv)
    for copy in copies:
        copy.wait()


def swap_in(plan, project, up):
    rows = project.shape[0]
    dma = pltpu.SemaphoreType.DMA
    shapes = [(plan.group, rows, project.shape[1] // plan.group), (plan.group, rows, up.shape[1] // plan.group)]
    return call(
        functools.partial(swap_in_kernel, plan),
        "swap_in",
        4,
        tuple(jax.ShapeDtypeStruct(shape, BF16) for shape in shapes),
        [pltpu.VMEM(shape, BF16) for shape in shapes] + [dma((plan.group,))] * 4,
        (project, up),
    )


def swap_out_kernel(plan, columns, pieces, out, got, send, recv):
    seq, rank = here(plan)
    meet(group_devices(plan, seq, rank))
    copies = start_swap(plan, seq, rank, pieces, got, send, recv)
    for copy in copies:
        copy.wait()
    for source in range(plan.group):
        starts, share = columns(plan, source)
        piece = got[source].astype(F32)
        for i, c in enumerate(starts):
            out[:, c : c + share] = piece[:, i * share : (i + 1) * share]


def swap_out(plan, pieces, columns, name, ident):
    dma = pltpu.SemaphoreType.DMA
    group, rows, cols = pieces.shape
    return call(
        functools.partial(swap_out_kernel, plan, columns),
        name,
        ident,
        jax.ShapeDtypeStruct((rows, group * cols), F32),
        [pltpu.VMEM(pieces.shape, BF16), dma((plan.group,)), dma((plan.group,))],
        (pieces,),
    )


def pick_rows(table, text):
    return jnp.where(text > 0, table[1:2, :], table[0:1, :])


def norm_rows(values):
    mean = jnp.mean(values, axis=1, keepdims=True)
    centred = values - mean
    inv = lax.rsqrt(jnp.mean(centred * centred, axis=1, keepdims=True) + EPSILON)
    return centred * inv, inv


def middle_kernel(plan, rows, pair, window_text, tokens, gate_a, scale_b, shift_b, text, merged, window, own, *scratch):
    seq, rank = here(plan)
    meet(group_devices(plan, seq, rank))
    total = scatter_sum(plan, seq, rank, rows, pair, window_text, PLAIN, *scratch[:SUM_SCRATCH])
    merged[...] = total
    mask = text[...]
    middle = tokens[...].astype(F32) + pick_rows(gate_a[...], mask) * total
    normed, _ = norm_rows(middle)
    own[...] = (normed * (1.0 + pick_rows(scale_b[...], mask)) + pick_rows(shift_b[...], mask)).astype(BF16)
    share_rows(plan, seq, rank, own_parts(plan, own), window, *scratch[SUM_SCRATCH:])


def own_shape(plan, dtype=F32):
    return jax.ShapeDtypeStruct((plan.own, plan.width), dtype)


def window_shape(plan):
    return jax.ShapeDtypeStruct((plan.rows, plan.width), BF16)


def middle_rows(plan, rows, pair, window_text, tokens, gate_a, scale_b, shift_b, text):
    return call(
        functools.partial(middle_kernel, plan),
        "middle",
        2,
        (own_shape(plan), window_shape(plan)),
        [pltpu.VMEM((plan.own, plan.width), BF16)] + sum_scratch(plan) + share_scratch(plan),
        (rows, pair, window_text, tokens, gate_a, scale_b, shift_b, text),
    )


def back_kernel(plan, rows, pair, window_text, grad, middle, gate_a, scale_b, text, grad_hidden, grad_middle, window, own, *scratch):
    seq, rank = here(plan)
    meet(group_devices(plan, seq, rank))
    total = scatter_sum(plan, seq, rank, rows, pair, window_text, CONTRACT_LAST, *scratch[:SUM_SCRATCH])
    grad_hidden[...] = total
    mask = text[...]
    normed, inv = norm_rows(middle[...])
    inner = total * (1.0 + pick_rows(scale_b[...], mask))
    mean_grad = jnp.mean(inner, axis=1, keepdims=True)
    mean_cross = jnp.mean(inner * normed, axis=1, keepdims=True)
    result = grad[...].astype(F32) + inv * (inner - mean_grad - normed * mean_cross)
    grad_middle[...] = result
    own[...] = (pick_rows(gate_a[...], mask) * result).astype(BF16)
    share_rows(plan, seq, rank, own_parts(plan, own), window, *scratch[SUM_SCRATCH:])


def back_rows(plan, rows, pair, window_text, grad, middle, gate_a, scale_b, text):
    return call(
        functools.partial(back_kernel, plan),
        "back",
        3,
        (own_shape(plan), own_shape(plan), window_shape(plan)),
        [pltpu.VMEM((plan.own, plan.width), BF16)] + sum_scratch(plan) + share_scratch(plan),
        (rows, pair, window_text, grad, middle, gate_a, scale_b, text),
    )


def edge_copy(plan, seq, source, first_row, target, send, recv, index):
    from_rank, row, rows, step, owner, owner_row = plan.segments[index]
    return remote(
        source.at[pl.ds(first_row + row, rows)],
        target.at[pl.ds(owner_row, rows)],
        send.at[index],
        recv.at[index],
        plan.device_of(lax.rem(seq + plan.sequences + step, plan.sequences), owner),
    )


def start_edges(plan, seq, rank, *refs):
    for index, segment in enumerate(plan.segments):
        @pl.when(rank == segment[0])
        def _():
            edge_copy(plan, seq, *refs, index).start()


def finish_edges(plan, seq, rank, *refs):
    for index, segment in enumerate(plan.segments):
        @pl.when(rank == segment[4])
        def _():
            edge_copy(plan, seq, *refs, index).wait_recv()

        @pl.when(rank == segment[0])
        def _():
            edge_copy(plan, seq, *refs, index).wait_send()


def edge_scratch(plan):
    return [pltpu.SemaphoreType.DMA((len(plan.segments),))] * 2


def output_kernel(plan, rows, pair, window_text, middle, gate_b, text, *refs):
    if plan.chip_heads:
        term, lowered, out, extra, term_out, own, term_send, term_recv, *scratch = refs
    else:
        lowered, out, extra, own, *scratch = refs
    device = lax.axis_index("dev")
    seq, rank = plan.place_of(device)
    extra[...] = jnp.zeros_like(extra)
    meet(every_device(plan, device))
    swaps = []
    if plan.chip_heads:
        core = lax.rem(rank, 2)
        partner = plan.device_of(seq, 2 * lax.div(rank, 2) + 1 - core)
        for stream in range(2):
            copy = remote(
                term.at[stream, 1 - core], term_out.at[2 * stream + core], term_send.at[stream], term_recv.at[stream], partner
            )
            copy.start()
            swaps.append(copy)
            term_out[2 * stream + core] = term[stream, core]
    total = scatter_sum(plan, seq, rank, rows, pair, window_text, PLAIN, *scratch[:SUM_SCRATCH])
    lowered[...] = total
    own[...] = (middle[...] + pick_rows(gate_b[...], text[...]) * total).astype(BF16)
    edges = (own, plan.rows_dev, extra) + tuple(scratch[SUM_SCRATCH:])
    start_edges(plan, seq, rank, *edges)
    out[...] = own[pl.ds(0, plan.rows_dev)]
    for copy in swaps:
        copy.wait()
    finish_edges(plan, seq, rank, *edges)


def output_rows(plan, rows, pair, window_text, middle, gate_b, text, term):
    placed = jax.ShapeDtypeStruct((plan.rows_dev, plan.width), BF16)
    shapes = (own_shape(plan), placed, placed)
    operands = (rows, pair, window_text, middle, gate_b, text)
    scratch = [pltpu.VMEM((plan.own, plan.width), BF16)]
    if plan.chip_heads:
        share = plan.width // plan.group // 2
        shapes += (jax.ShapeDtypeStruct((plan.sequences, share, plan.width), BF16),)
        operands += (term.reshape(2, 2, share, plan.width),)
        scratch += [pltpu.SemaphoreType.DMA((2,))] * 2
    scratch += sum_scratch(plan) + edge_scratch(plan)
    outs = call(functools.partial(output_kernel, plan), "output", 8, shapes, scratch, operands)
    return outs if plan.chip_heads else outs + [None] if isinstance(outs, list) else outs + (None,)


def stream_sums(values, masks):
    return jnp.concatenate([jnp.sum(values * mask, axis=0, keepdims=True) for mask in masks], axis=0)


def last_kernel(plan, rows, pair, window_text, tokens, grad_middle, scale_a, text, masks, rest, out, extra, table,
                own, local, first, second, mine, t_send, t_recv, *scratch):
    device = lax.axis_index("dev")
    seq, rank = plan.place_of(device)
    stream = lax.div(2 * seq, plan.sequences)
    extra[...] = jnp.zeros_like(extra)
    meet(every_device(plan, device))
    total = scatter_sum(plan, seq, rank, rows, pair, window_text, CONTRACT_LAST, *scratch[:SUM_SCRATCH])
    normed, inv = norm_rows(tokens[...].astype(F32))
    streams = (masks[:, 0:1], masks[:, 1:2])
    local[:, : plan.width] = stream_sums(total, streams)
    local[:, plan.width : 2 * plan.width] = stream_sums(total * normed, streams)
    local[:, 2 * plan.width :] = rest[...]
    cols = 6 * plan.width // plan.group

    def chunk(index):
        return pl.ds(pl.multiple_of(index * cols, 128), cols)

    hops = []
    for step in range(1, plan.group):
        to = other(rank, step, plan.group)
        copy = remote(local.at[:, chunk(to)], first.at[step], t_send.at[0, step], t_recv.at[0, step], plan.device_of(seq, to))
        copy.start()
        hops.append(copy)
    inner = total * (1.0 + pick_rows(scale_a[...], text[...]))
    mean_grad = jnp.mean(inner, axis=1, keepdims=True)
    mean_cross = jnp.mean(inner * normed, axis=1, keepdims=True)
    own[...] = grad_middle[...] + inv * (inner - mean_grad - normed * mean_cross)
    refs = (own, plan.rows_dev, extra) + scratch[SUM_SCRATCH:]
    start_edges(plan, seq, rank, *refs)
    for copy in hops:
        copy.wait_recv()
    sums = local[:, chunk(rank)]
    for step in range(1, plan.group):
        sums = sums + first[step]
    for i in range(2):
        mine[i] = sums[i : i + 1]
    across = []
    for step in range(1, plan.sequences):
        to = other(seq, step, plan.sequences)
        to_stream = lax.div(2 * to, plan.sequences)
        copy = remote(mine.at[to_stream], second.at[seq], t_send.at[1, step], t_recv.at[1, step], plan.device_of(to, rank))
        copy.start()
        across.append(copy)
    second[seq] = mine[stream]
    out[...] = own[pl.ds(0, plan.rows_dev)]
    for copy in across:
        copy.wait_recv()
    last = []
    for step in range(1, plan.group):
        to = other(rank, step, plan.group)
        copy = remote(second, table.at[rank], t_send.at[2, step], t_recv.at[2, step], plan.device_of(seq, to))
        copy.start()
        last.append(copy)
    table[rank] = second[...]
    for copy in last:
        copy.wait_recv()
    for copy in hops + across + last:
        copy.wait_send()
    finish_edges(plan, seq, rank, *refs)


def last_rows(plan, rows, pair, window_text, tokens, grad_middle, scale_a, text, masks, rest):
    placed = jax.ShapeDtypeStruct((plan.rows_dev, plan.width), F32)
    cols = 6 * plan.width // plan.group
    dma = pltpu.SemaphoreType.DMA
    most = max(plan.group, plan.sequences)
    out, extra, table = call(
        functools.partial(last_kernel, plan),
        "last",
        10,
        (placed, placed, jax.ShapeDtypeStruct((plan.group, plan.sequences, 1, cols), F32)),
        [
            pltpu.VMEM((plan.own, plan.width), F32),
            pltpu.VMEM((2, 6 * plan.width), F32),
            pltpu.VMEM((plan.group, 2, cols), F32),
            pltpu.VMEM((plan.sequences, 1, cols), F32),
            pltpu.VMEM((2, 1, cols), F32),
            dma((3, most)),
            dma((3, most)),
        ]
        + sum_scratch(plan)
        + edge_scratch(plan),
        (rows, pair, window_text, tokens, grad_middle, scale_a, text, masks, rest),
    )
    return out, extra, table[:, :, 0].transpose(1, 0, 2).reshape(plan.sequences, -1)


def spread_kernel(plan, piece, everyone, send, recv):
    device = lax.axis_index("dev")
    seq, rank = plan.place_of(device)
    meet(group_devices(plan, seq, rank) + column_devices(plan, seq, rank))
    copies = []
    everyone[seq, rank] = piece[...]
    for step in range(1, plan.group):
        to = other(rank, step, plan.group)
        copy = remote(piece, everyone.at[seq, rank], send.at[0, step], recv.at[0, step], plan.device_of(seq, to))
        copy.start()
        copies.append(copy)
    for copy in copies:
        copy.wait_recv()
    across = []
    for step in range(1, plan.sequences):
        to = other(seq, step, plan.sequences)
        copy = remote(everyone.at[seq], everyone.at[seq], send.at[1, step], recv.at[1, step], plan.device_of(to, rank))
        copy.start()
        across.append(copy)
    for copy in across:
        copy.wait_recv()
    for copy in copies + across:
        copy.wait_send()


def spread(plan, piece, ident):
    dma = pltpu.SemaphoreType.DMA
    most = max(plan.group, plan.sequences)
    return call(
        functools.partial(spread_kernel, plan),
        "spread",
        ident,
        jax.ShapeDtypeStruct((plan.sequences, plan.group) + piece.shape, piece.dtype),
        [dma((2, most)), dma((2, most))],
        (piece,),
    )


def over_sequences(plan, pieces):
    full = lax.all_gather(pieces, "dev", axis=0, axis_index_groups=plan.rank_groups())
    return full.reshape(2, plan.width, pieces.shape[2])


def terms_to_send(plan, grad, rows):
    return grad.astype(BF16).reshape(plan.sequences, plan.group, rows, grad.shape[2])


def over_sequences_sum(plan, pieces):
    return lax.psum_scatter(pieces, "dev", scatter_dimension=0, axis_index_groups=plan.rank_groups())


def merge_rows(plan, weight, rank):
    if plan.chip_heads:
        return lax.all_gather(weight, "dev", axis=0, axis_index_groups=plan.rank_groups())
    share = plan.width // plan.group
    full = lax.all_gather(weight, "dev", axis=0, tiled=True)
    full = full.reshape(2, 2, plan.group // 2, share, weight.shape[1])
    full = lax.dynamic_index_in_dim(full, lax.rem(rank, 2), 1, keepdims=False)
    return lax.dynamic_index_in_dim(full, lax.div(rank, 2), 1, keepdims=False)


def merge_sum(plan, term, term_out, rank):
    if plan.chip_heads:
        return over_sequences_sum(plan, term_out)
    half = plan.group // 2
    _, share, cols = term.shape
    mine = [jnp.where(lax.rem(rank, 2) == k, term, jnp.zeros((), BF16)) for k in range(2)]
    full = jnp.zeros((2, 2, half, share, cols), BF16)
    full = lax.dynamic_update_slice_in_dim(full, jnp.stack(mine, axis=1)[:, :, None], lax.div(rank, 2), 2)
    return lax.psum_scatter(full.reshape(-1, cols), "dev", scatter_dimension=0, tiled=True)


def down_slices(plan, weight):
    full = lax.all_gather(weight, "dev", axis=0, axis_index_groups=plan.rank_groups())
    return full.reshape(2, -1, weight.shape[1])


def by_stream(plan, image_part, text_part, is_text):
    start, end = plan.text_start, plan.image_end
    mixed = jnp.where(is_text[start:end, None], text_part[: end - start], image_part[start:])
    return jnp.concatenate([image_part[:start], mixed, text_part[end - start :]], axis=0)


def stream_dot(plan, rows, pair, is_text):
    image_part = jnp.dot(rows[: plan.image_end], pair[0], preferred_element_type=F32)
    text_part = jnp.dot(rows[plan.text_start :], pair[1], preferred_element_type=F32)
    return by_stream(plan, image_part, text_part, is_text)


def stream_dot_back(plan, grads, pair, is_text):
    image_part = lax.dot_general(grads[: plan.image_end], pair[0], CONTRACT_LAST, preferred_element_type=F32)
    text_part = lax.dot_general(grads[plan.text_start :], pair[1], CONTRACT_LAST, preferred_element_type=F32)
    return by_stream(plan, image_part, text_part, is_text)


def weight_terms(plan, rows, grads, is_text):
    zero = jnp.zeros((), grads.dtype)
    image = jnp.where(is_text[: plan.image_end, None], zero, grads[: plan.image_end])
    text = jnp.where(is_text[plan.text_start :, None], grads[plan.text_start :], zero)
    image_term = lax.dot_general(rows[: plan.image_end], image, CONTRACT_FIRST, preferred_element_type=F32)
    text_term = lax.dot_general(rows[plan.text_start :], text, CONTRACT_FIRST, preferred_element_type=F32)
    return jnp.stack([image_term, text_term])


def pick(table, text_rows):
    return jnp.where(text_rows[:, None], table[1][None, :], table[0][None, :])


def on_device(
    tokens,
    conditioning,
    text_lengths,
    modulation_weight,
    project_weight,
    merge_weight,
    up_weight,
    down_weight,
    cotangent,
):
    rows_dev, width = tokens.shape
    mod_rows = modulation_weight.shape[0]
    plan = Plan(lax.axis_size("dev"), conditioning.shape[0], rows_dev, width)
    device = lax.axis_index("dev")
    seq, rank = plan.place_of(device)
    feature_start = device * mod_rows % width

    ends = jnp.cumsum(IMG + text_lengths)
    starts = jnp.concatenate([jnp.zeros((1,), jnp.int32), ends[:-1]])
    positions = device * rows_dev + jnp.arange(rows_dev, dtype=jnp.int32)
    row_seq = jnp.sum((starts[None, :] <= positions[:, None]).astype(jnp.int32), axis=1) - 1
    offset = plan.span * seq - plan.edge + jnp.arange(plan.rows, dtype=jnp.int32) - starts[seq]
    valid = (offset >= 0) & (offset < IMG + text_lengths[seq])
    is_text = offset >= IMG
    bias = jnp.where(valid, 0.0, MASKED).astype(F32)[None, :]
    own_valid = own_rows(plan, valid[:, None], rank)[:, 0]
    own_text = own_rows(plan, is_text[:, None], rank)[:, 0]

    cond_float = conditioning.astype(F32)
    silu_low = jax.nn.silu(cond_float).astype(BF16)
    silu_part = lax.dynamic_slice_in_dim(silu_low, feature_start, mod_rows, 1)
    mod_part = jnp.dot(silu_part, modulation_weight, preferred_element_type=F32)

    merge_pair = merge_rows(plan, merge_weight, rank)
    project_pieces, up_pieces = swap_in(plan, project_weight, up_weight)
    project_pieces, up_pieces, merge_pair = lax.optimization_barrier((project_pieces, up_pieces, merge_pair))
    project_pair = over_sequences(plan, project_pieces)
    up_pair = over_sequences(plan, up_pieces)
    down_pair = down_slices(plan, down_weight)

    token_window, grad_window, mods, merge_pair = entry(plan, tokens, cotangent, mod_part, merge_pair)
    shift_a, scale_a, gate_a, shift_b, scale_b, gate_b = jnp.split(mods, 6, axis=1)
    grad_window = jnp.where(valid[:, None], grad_window, jnp.zeros((), BF16))

    normed_full, _ = layer_norm(token_window.astype(F32))
    hidden_a = (normed_full * (1.0 + pick(scale_a, is_text)) + pick(shift_a, is_text)).astype(BF16)
    projected = stream_dot(plan, hidden_a, project_pair, is_text).astype(BF16)
    queries, keys, values = jnp.split(projected, 3, axis=1)
    attended = attend(plan, queries, keys, values, bias)

    own_tokens = own_rows(plan, token_window, rank)
    own_grad = own_rows(plan, grad_window, rank)
    text_mask = own_text.astype(F32)[:, None]
    window_text = is_text.astype(F32)[:, None]
    merged, hidden_b = middle_rows(
        plan, attended, merge_pair, window_text, own_tokens, gate_a, scale_b, shift_b, text_mask
    )
    middle = own_tokens.astype(F32) + pick(gate_a, own_text) * merged
    normed_b, inv_b = layer_norm(middle)

    upper = stream_dot(plan, hidden_b, up_pair, is_text)
    activated = jax.nn.gelu(upper, approximate=True).astype(BF16)
    grad_lowered = (pick(gate_b, is_text) * grad_window.astype(F32)).astype(BF16)
    down_term = weight_terms(plan, activated, grad_lowered, is_text).astype(BF16)
    down_term = down_term.reshape(plan.sequences, -1, width)
    down_term, grad_lowered = lax.optimization_barrier((down_term, grad_lowered))
    down_sum = over_sequences_sum(plan, down_term)
    grad_activated = stream_dot_back(plan, grad_lowered, down_pair, is_text)
    gelu_pull = jax.vjp(lambda value_in: jax.nn.gelu(value_in, approximate=True), upper)[1]
    grad_upper = gelu_pull(grad_activated)[0].astype(BF16)
    up_term = terms_to_send(plan, weight_terms(plan, hidden_b, grad_upper, is_text), mod_rows)
    grad_upper, up_term = lax.optimization_barrier((grad_upper, up_term))
    up_sum = over_sequences_sum(plan, up_term)
    grad_hidden_b, grad_middle, grad_merged = back_rows(
        plan, grad_upper, up_pair, window_text, own_grad, middle, gate_a, scale_b, text_mask
    )
    foreign = (row_seq != seq)[:, None]
    grad_attended = stream_dot_back(plan, grad_merged, merge_pair, is_text).astype(BF16)
    merge_term = weight_terms(plan, attended, grad_merged, is_text).astype(BF16)

    grad_projected = jnp.concatenate(attend_back(plan, queries, keys, values, grad_attended, bias), axis=1)
    grad_projected, down_sum = lax.optimization_barrier((grad_projected, down_sum))
    down_grad = down_sum.astype(F32)
    project_term = terms_to_send(plan, weight_terms(plan, hidden_a, grad_projected, is_text), mod_rows)
    grad_projected, project_term = lax.optimization_barrier((grad_projected, project_term))
    project_sum = over_sequences_sum(plan, project_term)
    activated, project_term = lax.optimization_barrier((activated, project_term))
    lowered, out_here, out_there, merge_out = output_rows(
        plan, activated, down_pair, window_text, middle, gate_b, text_mask, merge_term
    )
    layer_out = jnp.where(foreign, out_there, out_here)

    masks = jnp.stack([own_valid & ~own_text, own_valid & own_text], axis=1).astype(F32)
    rest = jnp.concatenate(
        [
            jnp.stack([jnp.sum(value * masks[:, j : j + 1], axis=0) for j in range(2)])
            for value in (
                grad_middle * merged,
                grad_hidden_b,
                grad_hidden_b * normed_b,
                own_grad.astype(F32) * lowered,
            )
        ],
        axis=1,
    )
    rest, up_sum = lax.optimization_barrier((rest, up_sum))
    back_here, back_there, grad_table = last_rows(
        plan, grad_projected, project_pair, window_text, own_tokens, grad_middle, scale_a, text_mask, masks, rest
    )
    tokens_grad = jnp.where(foreign, back_there, back_here)
    own_grads = grad_table.astype(BF16)
    modulation_grad = lax.dot_general(silu_part, own_grads, CONTRACT_FIRST, preferred_element_type=F32)
    grad_piece = lax.dot_general(own_grads, modulation_weight, CONTRACT_LAST, preferred_element_type=F32)
    merge_out, merge_term, project_sum, own_grads = lax.optimization_barrier(
        (merge_out, merge_term, project_sum, own_grads)
    )
    merge_grad = merge_sum(plan, merge_term, merge_out, rank).reshape(merge_weight.shape).astype(F32)
    up_grad = swap_out(plan, up_sum, lambda p, r: up_columns(p, r, up_weight.shape[1]), "up_out", 7)
    project_grad = swap_out(plan, project_sum, project_columns, "project_out", 6)
    everyone = spread(plan, grad_piece.reshape(-1, 128), 13)
    everyone = everyone.reshape(2, plan.devices // 2, plan.sequences, mod_rows)
    grad_silu = (everyone[0] + everyone[1]).transpose(1, 0, 2).reshape(plan.sequences, width)
    conditioning_grad = jax.vjp(jax.nn.silu, cond_float)[1](grad_silu)[0]
    return (
        layer_out,
        tokens_grad,
        conditioning_grad,
        modulation_grad,
        project_grad,
        merge_grad,
        up_grad,
        down_grad,
    )


def solution(mesh):
    shard, whole = P("dev", None), P()
    return jax.shard_map(
        on_device,
        mesh=mesh,
        in_specs=(shard, whole, whole, shard, shard, shard, shard, shard, shard),
        out_specs=(shard, shard, whole, shard, shard, shard, shard, shard),
        check_vma=False,
    )
```

```python
import functools

import jax
import jax.numpy as jnp
import numpy as np
from jax import lax
from jax.experimental import pallas as pl
from jax.experimental.pallas import tpu as pltpu
from jax.sharding import PartitionSpec as P

HEADS = 24
HDIM = 64
IMG = 1024
TXT_MIN = 86
TXT_MAX = 154
EPSILON = 1e-06
F32 = jnp.float32
BF16 = jnp.bfloat16
CONTRACT_LAST = (((1,), (1,)), ((), ()))
PLAIN = (((1,), (0,)), ((), ()))
CONTRACT_FIRST = (((0,), (0,)), ((), ()))
MASKED = -1e30


class Plan:
    def __init__(self, devices, sequences, rows_dev, width):
        self.devices, self.sequences, self.rows_dev, self.width = devices, sequences, rows_dev, width
        self.group = devices // sequences
        self.span = self.group * rows_dev
        mean = self.span - IMG
        up, down = TXT_MAX - mean, mean - TXT_MIN
        drift = 0
        for k in range(sequences + 1):
            drift = max(drift, min(up * k, down * (sequences - k)), min(down * k, up * (sequences - k)))
        self.edge = -(-drift // 64) * 64
        self.rows = self.span + 2 * self.edge
        self.piece = 2 * self.edge // self.group
        self.own = rows_dev + self.piece
        self.image_end = -(-(self.edge + drift + IMG) // 128) * 128
        self.text_start = (self.edge - drift + IMG) // 128 * 128
        self.heads = HEADS // self.group
        self.segments = self.edge_segments()
        self.chip_heads = devices == 4 * self.group

    def device_of(self, seq, rank):
        return seq * self.group + rank

    def place_of(self, device):
        return lax.div(device, self.group), lax.rem(device, self.group)

    def seq_groups(self):
        return [[self.device_of(s, r) for r in range(self.group)] for s in range(self.sequences)]

    def rank_groups(self):
        return [[self.device_of(s, r) for s in range(self.sequences)] for r in range(self.group)]

    def edge_row(self, rank):
        half = self.group // 2
        return jnp.where(rank < half, self.piece * rank, self.edge + self.span + self.piece * (rank - half))

    def main_row(self, rank):
        return self.edge + self.rows_dev * rank

    def edge_segments(self):
        found = []
        for rank in range(self.group):
            half = self.group // 2
            first = self.piece * rank - self.edge if rank < half else self.span + self.piece * (rank - half)
            row = 0
            while row < self.piece:
                owner, owner_row = (first + row) // self.rows_dev, (first + row) % self.rows_dev
                count = min(self.piece - row, self.rows_dev - owner_row)
                found.append((rank, row, count, owner // self.group, owner % self.group, owner_row))
                row += count
        return found


def layer_norm(values):
    mean = jnp.mean(values, axis=-1, keepdims=True)
    centred = values - mean
    variance = jnp.mean(centred * centred, axis=-1, keepdims=True)
    inv_std = lax.rsqrt(variance + EPSILON)
    return (centred * inv_std, inv_std)


def norm_back(grad_normed, normed, inv_std):
    mean_grad = jnp.mean(grad_normed, axis=-1, keepdims=True)
    mean_cross = jnp.mean(grad_normed * normed, axis=-1, keepdims=True)
    return inv_std * (grad_normed - mean_grad - normed * mean_cross)


def softmax_parts(query, key, bias):
    scores = lax.dot_general(query, key, CONTRACT_LAST, preferred_element_type=F32) + bias
    top = jnp.max(scores, axis=1, keepdims=True)
    exponent = jnp.exp(scores - top)
    total = jnp.sum(exponent, axis=1, keepdims=True)
    return exponent * (1.0 / total)


def head_columns(heads, part, head):
    first = (part * heads + head) * HDIM
    return slice(first, first + HDIM)


def attend_kernel(heads, block, projected, bias_ref, out_ref):
    rows = pl.ds(pl.multiple_of(pl.program_id(0) * block, block), block)
    bias = bias_ref[...]
    outs = []
    for head in range(heads):
        query = projected[rows, head_columns(heads, 0, head)] * jnp.asarray(HDIM ** (-0.5), BF16)
        probs = softmax_parts(query, projected[:, head_columns(heads, 1, head)], bias).astype(BF16)
        outs.append(jnp.dot(probs, projected[:, head_columns(heads, 2, head)], preferred_element_type=F32))
    out_ref[...] = jnp.concatenate(outs, axis=1).astype(BF16)


def block_rows(rows):
    return 256 if rows % 256 == 0 else 128


def constant(shape):
    return pl.BlockSpec(shape, lambda i: (0,) * len(shape))


def attend(plan, projected, bias):
    rows, cols = projected.shape[0], projected.shape[1] // 3
    block = block_rows(rows)
    return pl.pallas_call(
        functools.partial(attend_kernel, plan.heads, block),
        out_shape=jax.ShapeDtypeStruct((rows, cols), BF16),
        grid=(rows // block,),
        in_specs=[constant(projected.shape), constant(bias.shape)],
        out_specs=pl.BlockSpec((block, cols), lambda i: (i, 0)),
        compiler_params=pltpu.CompilerParams(vmem_limit_bytes=48 << 20),
        cost_estimate=pl.CostEstimate(flops=16 * rows * rows * cols, bytes_accessed=8 * rows * cols, transcendentals=0),
        name="attend",
    )(projected, bias)


def attend_back_kernel(
    heads, steps, block, projected, grad_merged, merge_pair, text, bias_ref, out, key_sum, value_sum
):
    step = pl.program_id(0)
    scale = jnp.asarray(HDIM ** (-0.5), BF16)

    @pl.when(step == 0)
    def _():
        key_sum[...] = jnp.zeros_like(key_sum)
        value_sum[...] = jnp.zeros_like(value_sum)

    rows = pl.ds(pl.multiple_of(step * block, block), block)
    bias = bias_ref[...]
    image, other_stream = [
        lax.dot_general(grad_merged[...], merge_pair[j], CONTRACT_LAST, preferred_element_type=F32) for j in range(2)
    ]
    grad_attended = jnp.where(text[...] > 0, other_stream, image).astype(BF16)
    grads = []
    for head in range(heads):
        query = projected[rows, head_columns(heads, 0, head)] * scale
        key = projected[:, head_columns(heads, 1, head)]
        grad_out = grad_attended[:, head * HDIM : (head + 1) * HDIM]
        probs = softmax_parts(query, key, bias)
        grad_probs = lax.dot_general(
            grad_out, projected[:, head_columns(heads, 2, head)], CONTRACT_LAST, preferred_element_type=F32
        )
        inner = jnp.sum(probs * grad_probs, axis=1, keepdims=True)
        grad_scores = (probs * (grad_probs - inner)).astype(BF16)
        grads.append(jnp.dot(grad_scores, key, preferred_element_type=F32) * HDIM ** (-0.5))
        key_sum[head] += lax.dot_general(query, grad_scores, CONTRACT_FIRST, preferred_element_type=F32)
        value_sum[head] += lax.dot_general(grad_out, probs.astype(BF16), CONTRACT_FIRST, preferred_element_type=F32)
    cols = heads * HDIM
    out[rows, :cols] = jnp.concatenate(grads, axis=1).astype(BF16)

    @pl.when(step == steps - 1)
    def _():
        total = out.shape[0]
        out[:, cols : 2 * cols] = key_sum[...].reshape(cols, total).T.astype(BF16)
        out[:, 2 * cols :] = value_sum[...].reshape(cols, total).T.astype(BF16)


def attend_back(plan, projected, grad_merged, merge_pair, text, bias):
    rows, cols = projected.shape[0], projected.shape[1] // 3
    block = block_rows(rows)
    return pl.pallas_call(
        functools.partial(attend_back_kernel, plan.heads, rows // block, block),
        out_shape=jax.ShapeDtypeStruct(projected.shape, BF16),
        grid=(rows // block,),
        in_specs=[
            constant(projected.shape),
            pl.BlockSpec((block, plan.width), lambda i: (i, 0)),
            constant(merge_pair.shape),
            pl.BlockSpec((block, 1), lambda i: (i, 0)),
            constant(bias.shape),
        ],
        out_specs=constant(projected.shape),
        scratch_shapes=[pltpu.VMEM((plan.heads, HDIM, rows), F32)] * 2,
        compiler_params=pltpu.CompilerParams(vmem_limit_bytes=56 << 20),
        cost_estimate=pl.CostEstimate(flops=40 * rows * rows * cols, bytes_accessed=14 * rows * cols, transcendentals=0),
        name="attend_back",
    )(projected, grad_merged, merge_pair, text, bias)


def fold_rows(piece):
    half = piece.shape[0] // 2
    return jnp.concatenate([piece[:half], piece[half:]], axis=1)


def unfold_rows(piece):
    half = piece.shape[1] // 2
    return jnp.concatenate([piece[:, :half], piece[:, half:]], axis=0)


def project_terms_kernel(plan, rows_of, hidden, grads, text, out):
    cols = grads.shape[1]
    spans = ((0, plan.image_end), (plan.text_start, plan.rows))
    chunk = 4 * 96
    for stream, (first, last) in enumerate(spans):
        mask = text[pl.ds(first, last - first)]
        keep = (mask > 0) if stream else (mask <= 0)
        part = jnp.where(keep, grads[pl.ds(first, last - first)], jnp.zeros((), BF16))
        for start in range(0, plan.width, chunk):
            term = lax.dot_general(
                hidden[pl.ds(first, last - first), start : start + chunk], part, CONTRACT_FIRST, preferred_element_type=F32
            ).astype(BF16)
            for i in range(chunk // rows_of):
                owner = (stream * plan.width + start) // rows_of + i
                out[owner] = fold_rows(term[i * rows_of : (i + 1) * rows_of])


def project_terms(plan, hidden, grads, text, rows):
    cols = grads.shape[1]
    shape = (plan.devices, rows // 2, 2 * cols)
    out = pl.pallas_call(
        functools.partial(project_terms_kernel, plan, rows),
        out_shape=jax.ShapeDtypeStruct(shape, BF16),
        in_specs=[pl.BlockSpec(memory_space=pltpu.VMEM)] * 3,
        out_specs=pl.BlockSpec(memory_space=pltpu.VMEM),
        compiler_params=pltpu.CompilerParams(vmem_limit_bytes=40 << 20),
        cost_estimate=pl.CostEstimate(flops=4 * plan.rows * plan.width * cols, bytes_accessed=1 << 23, transcendentals=0),
        name="project_terms",
    )(hidden, grads, text)
    return out.reshape((plan.sequences, plan.group) + shape[1:])


VMEM = pl.BlockSpec(memory_space=pltpu.VMEM)


def own_rows(plan, window, rank):
    main = lax.dynamic_slice_in_dim(window, plan.main_row(rank), plan.rows_dev, 0)
    edge = lax.dynamic_slice_in_dim(window, plan.edge_row(rank), plan.piece, 0)
    return jnp.concatenate([main, edge], axis=0)


def remote(source, target, send_sem, recv_sem, device):
    return pltpu.make_async_remote_copy(
        src_ref=source,
        dst_ref=target,
        send_sem=send_sem,
        recv_sem=recv_sem,
        device_id=(device,),
        device_id_type=pl.DeviceIdType.MESH,
    )


def here(plan):
    return plan.place_of(lax.axis_index("dev"))


def other(rank, step, size):
    return lax.rem(rank + step, size)


def meet(devices):
    barrier = pltpu.get_barrier_semaphore()
    for device in devices:
        pl.semaphore_signal(barrier, inc=1, device_id=(device,), device_id_type=pl.DeviceIdType.MESH)
    pl.semaphore_wait(barrier, len(devices))


def group_devices(plan, seq, rank):
    return [plan.device_of(seq, other(rank, step, plan.group)) for step in range(1, plan.group)]


def column_devices(plan, seq, rank):
    return [plan.device_of(other(seq, step, plan.sequences), rank) for step in range(1, plan.sequences)]


def every_device(plan, device):
    return [other(device, step, plan.devices) for step in range(1, plan.devices)]


def call(kernel, name, ident, out_shape, scratch, operands, in_specs=None, out_specs=None):
    outs = out_shape if isinstance(out_shape, tuple) else (out_shape,)
    return pl.pallas_call(
        kernel,
        out_shape=out_shape,
        in_specs=in_specs or [VMEM] * len(operands),
        out_specs=out_specs or (tuple([VMEM] * len(outs)) if isinstance(out_shape, tuple) else VMEM),
        scratch_shapes=scratch,
        compiler_params=pltpu.CompilerParams(
            collective_id=ident, has_side_effects=True, vmem_limit_bytes=40 << 20
        ),
        name=name,
    )(*operands)


def aligned(start):
    return pl.multiple_of(start, 16)


def block_parts(plan, ref, rank):
    return (
        ref.at[pl.ds(aligned(plan.main_row(rank)), plan.rows_dev)],
        ref.at[pl.ds(aligned(plan.edge_row(rank)), plan.piece)],
    )


def own_parts(plan, ref):
    return ref.at[pl.ds(0, plan.rows_dev)], ref.at[pl.ds(plan.rows_dev, plan.piece)]


def load_block(plan, ref, rank):
    main, edge = block_parts(plan, ref, rank)
    return jnp.concatenate([main[...], edge[...]], axis=0)


def sum_scratch(plan):
    half, own, width = plan.group // 2, plan.own, plan.width
    return [
        pltpu.VMEM((half, own, width), F32),
        pltpu.VMEM((half, own, width), F32),
        pltpu.VMEM((half, own, width), BF16),
        pltpu.VMEM((half, own, width), BF16),
        pltpu.SemaphoreType.DMA((half,)),
        pltpu.SemaphoreType.DMA((half,)),
        pltpu.SemaphoreType.DMA((half,)),
        pltpu.SemaphoreType.DMA((half,)),
    ]


SUM_SCRATCH = 8


def product(plan, rows, pair, text, dims, rank):
    block = load_block(plan, rows, rank)
    mask = load_block(plan, text, rank)
    parts = [lax.dot_general(block, pair[j], dims, preferred_element_type=F32) for j in range(2)]
    return jnp.where(mask > 0, parts[1], parts[0])


def scatter_sum(plan, seq, rank, rows, pair, text, dims, away, near, going, coming, pair_send, pair_recv, far_send, far_recv):
    half = plan.group // 2
    chip, core = lax.div(rank, 2), lax.rem(rank, 2)
    partner = plan.device_of(seq, 2 * chip + 1 - core)
    order = list(range(1, half)) + [0]

    def for_partner(step):
        away[step] = product(plan, rows, pair, text, dims, 2 * other(chip, step, half) + 1 - core)
        copy = remote(away.at[step], near.at[step], pair_send.at[step], pair_recv.at[step], partner)
        copy.start()
        return copy

    pairs, sends = [for_partner(order[0])], []
    for i, step in enumerate(order):
        chip_to = other(chip, step, half)
        mine = product(plan, rows, pair, text, dims, 2 * chip_to + core)
        if i + 1 < half:
            pairs.append(for_partner(order[i + 1]))
        pairs[i].wait_recv()
        both = mine + near[step]
        if step == 0:
            total = both
        else:
            going[step] = both.astype(BF16)
            copy = remote(
                going.at[step], coming.at[step], far_send.at[step], far_recv.at[step], plan.device_of(seq, 2 * chip_to + core)
            )
            copy.start()
            sends.append(copy)
    for step, copy in zip(order, sends):
        copy.wait_recv()
        total = total + coming[step].astype(F32)
    for copy in pairs + sends:
        copy.wait_send()
    return total


def share_scratch(plan):
    return [pltpu.SemaphoreType.DMA((plan.group, 2))] * 2 + [pltpu.SemaphoreType.DMA((plan.group, 2))]


def share_rows(plan, seq, rank, parts, window, send, recv, pass_send):
    half = plan.group // 2
    chip, core = lax.div(rank, 2), lax.rem(rank, 2)
    partner_rank = 2 * chip + 1 - core
    partner = plan.device_of(seq, partner_rank)

    def send_own(to_device, slot):
        copies = [
            remote(source, target, send.at[slot, i], recv.at[slot, i], to_device)
            for i, (source, target) in enumerate(zip(parts, block_parts(plan, window, rank)))
        ]
        for copy in copies:
            copy.start()
        return copies

    flying = {}
    for step in range(1, half):
        flying[step] = send_own(plan.device_of(seq, 2 * other(chip, step, half) + core), step)
    flying[0] = send_own(partner, 0)
    for source, target in zip(parts, block_parts(plan, window, rank)):
        target[...] = source[...]
    passed = []
    for step in range(1, half):
        for copy in flying[step]:
            copy.wait_recv()
        came = 2 * other(chip, half - step, half) + core
        copies = [
            remote(place, place, pass_send.at[step, i], recv.at[half + step, i], partner)
            for i, place in enumerate(block_parts(plan, window, came))
        ]
        for copy in copies:
            copy.start()
        passed.extend(copies)
    for copy in flying[0]:
        copy.wait_recv()
    for copy in passed:
        copy.wait_recv()
    for copies in flying.values():
        for copy in copies:
            copy.wait_send()
    for copy in passed:
        copy.wait_send()


def entry_kernel(plan, tokens, grads, mod_part, *refs):
    if plan.chip_heads:
        merge, merge_out, *refs = refs[:1] + refs[4:5] + refs[1:4] + refs[5:]
        merge_send, merge_recv, *refs = refs[-2:] + refs[:-2]
    (token_window, grad_window, mods, token_own, grad_own, plane, across, chunk, edge_send, edge_recv,
     t_send, t_recv, t_pass, g_send, g_recv, g_pass, m_send, m_recv) = refs
    device = lax.axis_index("dev")
    seq, rank = plan.place_of(device)
    meet(every_device(plan, device))
    swaps = []
    if plan.chip_heads:
        core = lax.rem(rank, 2)
        partner = plan.device_of(seq, 2 * lax.div(rank, 2) + 1 - core)
        for stream in range(2):
            copy = remote(
                merge.at[2 * stream + 1 - core],
                merge_out.at[stream, core],
                merge_send.at[stream],
                merge_recv.at[stream],
                partner,
            )
            copy.start()
            swaps.append(copy)
            merge_out[stream, core] = merge[2 * stream + core]
    hops = []
    for step in range(1, plan.group):
        to = other(rank, step, plan.group)
        copy = remote(mod_part.at[to], plane.at[step], m_send.at[0, step], m_recv.at[0, step], plan.device_of(seq, to))
        copy.start()
        hops.append(copy)
    arrays = ((tokens, token_own), (grads, grad_own))
    count = len(plan.segments)
    for which, (source, own) in enumerate(arrays):
        for index, (to_rank, row, rows, step, owner, owner_row) in enumerate(plan.segments):
            @pl.when(rank == owner)
            def _():
                remote(
                    source.at[pl.ds(owner_row, rows)],
                    own.at[pl.ds(row, rows)],
                    edge_send.at[which * count + index],
                    edge_recv.at[which * count + index],
                    plan.device_of(lax.rem(seq + plan.sequences - step, plan.sequences), to_rank),
                ).start()
    for copy in hops:
        copy.wait_recv()
    total = mod_part[rank]
    for step in range(1, plan.group):
        total = total + plane[step]
    plane[0] = total
    hops_across = []
    for step in range(1, plan.sequences):
        to = other(seq, step, plan.sequences)
        copy = remote(plane.at[0, to], across.at[seq], m_send.at[1, step], m_recv.at[1, step], plan.device_of(to, rank))
        copy.start()
        hops_across.append(copy)
    across[seq] = plane[0, seq]
    for which, (source, own) in enumerate(arrays):
        for index, (to_rank, row, rows, step, owner, owner_row) in enumerate(plan.segments):
            @pl.when(rank == to_rank)
            def _():
                remote(
                    source.at[pl.ds(owner_row, rows)],
                    own.at[pl.ds(row, rows)],
                    edge_send.at[which * count + index],
                    edge_recv.at[which * count + index],
                    plan.device_of(lax.rem(seq + plan.sequences + step, plan.sequences), owner),
                ).wait_recv()
    share_rows(plan, seq, rank, (tokens, token_own), token_window, t_send, t_recv, t_pass)
    for copy in hops_across:
        copy.wait_recv()
    half = plan.sequences // 2
    for stream in range(2):
        total = across[stream * half]
        for i in range(1, half):
            total = total + across[stream * half + i]
        chunk[stream] = total
    hops_back = []
    for step in range(1, plan.group):
        to = other(rank, step, plan.group)
        copy = remote(chunk, mods.at[rank], m_send.at[2, step], m_recv.at[2, step], plan.device_of(seq, to))
        copy.start()
        hops_back.append(copy)
    mods[rank] = chunk[...]
    share_rows(plan, seq, rank, (grads, grad_own), grad_window, g_send, g_recv, g_pass)
    for copy in hops_back:
        copy.wait_recv()
    for copy in hops + hops_across + hops_back:
        copy.wait_send()
    for copy in swaps:
        copy.wait()
    for which, (source, own) in enumerate(arrays):
        for index, (to_rank, row, rows, step, owner, owner_row) in enumerate(plan.segments):
            @pl.when(rank == owner)
            def _():
                remote(
                    source.at[pl.ds(owner_row, rows)],
                    own.at[pl.ds(row, rows)],
                    edge_send.at[which * count + index],
                    edge_recv.at[which * count + index],
                    plan.device_of(lax.rem(seq + plan.sequences - step, plan.sequences), to_rank),
                ).wait_send()


def entry(plan, tokens, grads, mod_part, merge):
    lanes = mod_part.shape[1] // plan.group // 128
    pieces = mod_part.reshape(plan.sequences, plan.group, lanes, 128).transpose(1, 0, 2, 3)
    window = jax.ShapeDtypeStruct((plan.rows, plan.width), BF16)
    dma = pltpu.SemaphoreType.DMA
    most = max(plan.group, plan.sequences)
    shapes = (window, window, jax.ShapeDtypeStruct((plan.group, 2, lanes, 128), F32))
    operands = (tokens, grads, pieces)
    scratch = (
        [
            pltpu.VMEM((plan.piece, plan.width), BF16),
            pltpu.VMEM((plan.piece, plan.width), BF16),
            pltpu.VMEM((plan.group, plan.sequences, lanes, 128), F32),
            pltpu.VMEM((plan.sequences, lanes, 128), F32),
            pltpu.VMEM((2, lanes, 128), F32),
            dma((2 * len(plan.segments),)),
            dma((2 * len(plan.segments),)),
        ]
        + share_scratch(plan)
        + share_scratch(plan)
        + [dma((3, most)), dma((3, most))]
    )
    if plan.chip_heads:
        shapes += (jax.ShapeDtypeStruct((2, 2) + merge.shape[1:], BF16),)
        operands += (merge,)
        scratch += [dma((2,)), dma((2,))]
    token_window, grad_window, mods, *rest = call(
        functools.partial(entry_kernel, plan), "entry", 1, shapes, scratch, operands
    )
    merge_pair = rest[0].reshape(2, -1, plan.width) if plan.chip_heads else merge
    return token_window, grad_window, mods.transpose(1, 0, 2, 3).reshape(2, -1), merge_pair


def project_columns(plan, rank):
    share = plan.width // plan.group
    first = (rank % 2) * (plan.width // 2) + (rank // 2) * share
    return [part * plan.width + first for part in range(3)], share


def up_columns(plan, rank, cols):
    planes = plan.sequences // 2
    share = cols // planes // plan.group
    return [plane * plan.group * share + rank * share for plane in range(planes)], share


def start_swap(plan, seq, rank, source, target, send, recv):
    copies = []
    for step in range(1, plan.group):
        to = other(rank, step, plan.group)
        copy = remote(source.at[to], target.at[rank], send.at[step], recv.at[step], plan.device_of(seq, to))
        copy.start()
        copies.append(copy)
    target[rank] = source[rank]
    return copies


def swap_in_kernel(plan, project, up, project_out, up_out, project_cut, up_cut, p_send, p_recv, u_send, u_recv):
    seq, rank = here(plan)
    for to in range(plan.group):
        starts, share = project_columns(plan, to)
        project_cut[to] = fold_rows(jnp.concatenate([project[:, c : c + share] for c in starts], axis=1))
    meet(group_devices(plan, seq, rank))
    copies = start_swap(plan, seq, rank, project_cut, project_out, p_send, p_recv)
    for to in range(plan.group):
        starts, share = up_columns(plan, to, up.shape[1])
        up_cut[to] = jnp.concatenate([up[:, c : c + share] for c in starts], axis=1)
    copies += start_swap(plan, seq, rank, up_cut, up_out, u_send, u_recv)
    for copy in copies:
        copy.wait()


def swap_in(plan, project, up):
    rows = project.shape[0]
    dma = pltpu.SemaphoreType.DMA
    shapes = [
        (plan.group, rows // 2, 2 * project.shape[1] // plan.group),
        (plan.group, rows, up.shape[1] // plan.group),
    ]
    return call(
        functools.partial(swap_in_kernel, plan),
        "swap_in",
        4,
        tuple(jax.ShapeDtypeStruct(shape, BF16) for shape in shapes),
        [pltpu.VMEM(shape, BF16) for shape in shapes] + [dma((plan.group,))] * 4,
        (project, up),
    )


def place_columns(plan, got, out, columns, unfold):
    for source in range(plan.group):
        starts, share = columns(plan, source)
        piece = got[source]
        piece = (unfold_rows(piece) if unfold else piece).astype(F32)
        for i, c in enumerate(starts):
            out[:, c : c + share] = piece[:, i * share : (i + 1) * share]


def finish_kernel(plan, up, project, piece, up_out, project_out, everyone, up_got, project_got,
                  u_send, u_recv, p_send, p_recv, send, recv):
    seq, rank = here(plan)
    meet(group_devices(plan, seq, rank) + column_devices(plan, seq, rank))
    near = []
    everyone[seq, rank] = piece[...]
    for step in range(1, plan.group):
        to = other(rank, step, plan.group)
        copy = remote(piece, everyone.at[seq, rank], send.at[0, step], recv.at[0, step], plan.device_of(seq, to))
        copy.start()
        near.append(copy)
    ups = start_swap(plan, seq, rank, up, up_got, u_send, u_recv)
    projects = start_swap(plan, seq, rank, project, project_got, p_send, p_recv)
    for copy in near:
        copy.wait_recv()
    far = []
    for step in range(1, plan.sequences):
        to = other(seq, step, plan.sequences)
        copy = remote(everyone.at[seq], everyone.at[seq], send.at[1, step], recv.at[1, step], plan.device_of(to, rank))
        copy.start()
        far.append(copy)
    for copy in ups:
        copy.wait()
    place_columns(plan, up_got, up_out, lambda p, r: up_columns(p, r, up_out.shape[1]), False)
    for copy in projects:
        copy.wait()
    place_columns(plan, project_got, project_out, project_columns, True)
    for copy in far:
        copy.wait_recv()
    for copy in near + far:
        copy.wait_send()


def finish(plan, up, project, piece):
    dma = pltpu.SemaphoreType.DMA
    most = max(plan.group, plan.sequences)
    rows = up.shape[1]
    return call(
        functools.partial(finish_kernel, plan),
        "finish",
        6,
        (
            jax.ShapeDtypeStruct((rows, plan.group * up.shape[2]), F32),
            jax.ShapeDtypeStruct((rows, plan.group * project.shape[2] // 2), F32),
            jax.ShapeDtypeStruct((plan.sequences, plan.group) + piece.shape, F32),
        ),
        [pltpu.VMEM(up.shape, BF16), pltpu.VMEM(project.shape, BF16)]
        + [dma((plan.group,))] * 4
        + [dma((2, most))] * 2,
        (up, project, piece),
    )


def pick_rows(table, text):
    return jnp.where(text > 0, table[1:2, :], table[0:1, :])


def norm_rows(values):
    mean = jnp.mean(values, axis=1, keepdims=True)
    centred = values - mean
    inv = lax.rsqrt(jnp.mean(centred * centred, axis=1, keepdims=True) + EPSILON)
    return centred * inv, inv


def middle_kernel(plan, rows, pair, window_text, tokens, gate_a, scale_b, shift_b, text, merged, window, own, *scratch):
    seq, rank = here(plan)
    meet(group_devices(plan, seq, rank))
    total = scatter_sum(plan, seq, rank, rows, pair, window_text, PLAIN, *scratch[:SUM_SCRATCH])
    merged[...] = total
    mask = text[...]
    middle = tokens[...].astype(F32) + pick_rows(gate_a[...], mask) * total
    normed, _ = norm_rows(middle)
    own[...] = (normed * (1.0 + pick_rows(scale_b[...], mask)) + pick_rows(shift_b[...], mask)).astype(BF16)
    share_rows(plan, seq, rank, own_parts(plan, own), window, *scratch[SUM_SCRATCH:])


def own_shape(plan, dtype=F32):
    return jax.ShapeDtypeStruct((plan.own, plan.width), dtype)


def window_shape(plan):
    return jax.ShapeDtypeStruct((plan.rows, plan.width), BF16)


def middle_rows(plan, rows, pair, window_text, tokens, gate_a, scale_b, shift_b, text):
    return call(
        functools.partial(middle_kernel, plan),
        "middle",
        2,
        (own_shape(plan), window_shape(plan)),
        [pltpu.VMEM((plan.own, plan.width), BF16)] + sum_scratch(plan) + share_scratch(plan),
        (rows, pair, window_text, tokens, gate_a, scale_b, shift_b, text),
    )


def back_kernel(plan, rows, pair, window_text, grad, middle, gate_a, scale_b, text, grad_hidden, grad_middle, window, own, *scratch):
    seq, rank = here(plan)
    meet(group_devices(plan, seq, rank))
    total = scatter_sum(plan, seq, rank, rows, pair, window_text, CONTRACT_LAST, *scratch[:SUM_SCRATCH])
    grad_hidden[...] = total
    mask = text[...]
    normed, inv = norm_rows(middle[...])
    inner = total * (1.0 + pick_rows(scale_b[...], mask))
    mean_grad = jnp.mean(inner, axis=1, keepdims=True)
    mean_cross = jnp.mean(inner * normed, axis=1, keepdims=True)
    result = grad[...].astype(F32) + inv * (inner - mean_grad - normed * mean_cross)
    grad_middle[...] = result
    own[...] = (pick_rows(gate_a[...], mask) * result).astype(BF16)
    share_rows(plan, seq, rank, own_parts(plan, own), window, *scratch[SUM_SCRATCH:])


def back_rows(plan, rows, pair, window_text, grad, middle, gate_a, scale_b, text):
    return call(
        functools.partial(back_kernel, plan),
        "back",
        3,
        (own_shape(plan), own_shape(plan), window_shape(plan)),
        [pltpu.VMEM((plan.own, plan.width), BF16)] + sum_scratch(plan) + share_scratch(plan),
        (rows, pair, window_text, grad, middle, gate_a, scale_b, text),
    )


def edge_copy(plan, seq, source, first_row, target, send, recv, index):
    from_rank, row, rows, step, owner, owner_row = plan.segments[index]
    return remote(
        source.at[pl.ds(first_row + row, rows)],
        target.at[pl.ds(owner_row, rows)],
        send.at[index],
        recv.at[index],
        plan.device_of(lax.rem(seq + plan.sequences + step, plan.sequences), owner),
    )


def start_edges(plan, seq, rank, *refs):
    for index, segment in enumerate(plan.segments):
        @pl.when(rank == segment[0])
        def _():
            edge_copy(plan, seq, *refs, index).start()


def finish_edges(plan, seq, rank, *refs):
    for index, segment in enumerate(plan.segments):
        @pl.when(rank == segment[4])
        def _():
            edge_copy(plan, seq, *refs, index).wait_recv()

        @pl.when(rank == segment[0])
        def _():
            edge_copy(plan, seq, *refs, index).wait_send()


def edge_scratch(plan):
    return [pltpu.SemaphoreType.DMA((len(plan.segments),))] * 2


def output_kernel(plan, rows, pair, window_text, middle, gate_b, text, *refs):
    if plan.chip_heads:
        term, lowered, out, extra, term_out, own, term_send, term_recv, *scratch = refs
    else:
        lowered, out, extra, own, *scratch = refs
    device = lax.axis_index("dev")
    seq, rank = plan.place_of(device)
    extra[...] = jnp.zeros_like(extra)
    meet(every_device(plan, device))
    swaps = []
    if plan.chip_heads:
        core = lax.rem(rank, 2)
        partner = plan.device_of(seq, 2 * lax.div(rank, 2) + 1 - core)
        for stream in range(2):
            copy = remote(
                term.at[stream, 1 - core], term_out.at[2 * stream + core], term_send.at[stream], term_recv.at[stream], partner
            )
            copy.start()
            swaps.append(copy)
            term_out[2 * stream + core] = term[stream, core]
    total = scatter_sum(plan, seq, rank, rows, pair, window_text, PLAIN, *scratch[:SUM_SCRATCH])
    lowered[...] = total
    own[...] = (middle[...] + pick_rows(gate_b[...], text[...]) * total).astype(BF16)
    edges = (own, plan.rows_dev, extra) + tuple(scratch[SUM_SCRATCH:])
    start_edges(plan, seq, rank, *edges)
    out[...] = own[pl.ds(0, plan.rows_dev)]
    for copy in swaps:
        copy.wait()
    finish_edges(plan, seq, rank, *edges)


def output_rows(plan, rows, pair, window_text, middle, gate_b, text, term):
    placed = jax.ShapeDtypeStruct((plan.rows_dev, plan.width), BF16)
    shapes = (own_shape(plan), placed, placed)
    operands = (rows, pair, window_text, middle, gate_b, text)
    scratch = [pltpu.VMEM((plan.own, plan.width), BF16)]
    if plan.chip_heads:
        share = plan.width // plan.group // 2
        shapes += (jax.ShapeDtypeStruct((plan.sequences, share, plan.width), BF16),)
        operands += (term.reshape(2, 2, share, plan.width),)
        scratch += [pltpu.SemaphoreType.DMA((2,))] * 2
    scratch += sum_scratch(plan) + edge_scratch(plan)
    outs = call(functools.partial(output_kernel, plan), "output", 8, shapes, scratch, operands)
    return outs if plan.chip_heads else outs + [None] if isinstance(outs, list) else outs + (None,)


def stream_sums(values, masks):
    return jnp.concatenate([jnp.sum(values * mask, axis=0, keepdims=True) for mask in masks], axis=0)


def last_kernel(plan, rows, pair, window_text, tokens, grad_middle, scale_a, text, masks, rest, out, extra, table,
                own, local, first, second, mine, t_send, t_recv, *scratch):
    device = lax.axis_index("dev")
    seq, rank = plan.place_of(device)
    stream = lax.div(2 * seq, plan.sequences)
    extra[...] = jnp.zeros_like(extra)
    meet(every_device(plan, device))
    total = scatter_sum(plan, seq, rank, rows, pair, window_text, CONTRACT_LAST, *scratch[:SUM_SCRATCH])
    normed, inv = norm_rows(tokens[...].astype(F32))
    streams = (masks[:, 0:1], masks[:, 1:2])
    local[:, : plan.width] = stream_sums(total, streams)
    local[:, plan.width : 2 * plan.width] = stream_sums(total * normed, streams)
    local[:, 2 * plan.width :] = rest[...]
    cols = 6 * plan.width // plan.group

    def chunk(index):
        return pl.ds(pl.multiple_of(index * cols, 128), cols)

    hops = []
    for step in range(1, plan.group):
        to = other(rank, step, plan.group)
        copy = remote(local.at[:, chunk(to)], first.at[step], t_send.at[0, step], t_recv.at[0, step], plan.device_of(seq, to))
        copy.start()
        hops.append(copy)
    inner = total * (1.0 + pick_rows(scale_a[...], text[...]))
    mean_grad = jnp.mean(inner, axis=1, keepdims=True)
    mean_cross = jnp.mean(inner * normed, axis=1, keepdims=True)
    own[...] = grad_middle[...] + inv * (inner - mean_grad - normed * mean_cross)
    refs = (own, plan.rows_dev, extra) + scratch[SUM_SCRATCH:]
    start_edges(plan, seq, rank, *refs)
    for copy in hops:
        copy.wait_recv()
    sums = local[:, chunk(rank)]
    for step in range(1, plan.group):
        sums = sums + first[step]
    for i in range(2):
        mine[i] = sums[i : i + 1]
    across = []
    for step in range(1, plan.sequences):
        to = other(seq, step, plan.sequences)
        to_stream = lax.div(2 * to, plan.sequences)
        copy = remote(mine.at[to_stream], second.at[seq], t_send.at[1, step], t_recv.at[1, step], plan.device_of(to, rank))
        copy.start()
        across.append(copy)
    second[seq] = mine[stream]
    out[...] = own[pl.ds(0, plan.rows_dev)]
    for copy in across:
        copy.wait_recv()
    last = []
    for step in range(1, plan.group):
        to = other(rank, step, plan.group)
        copy = remote(second, table.at[rank], t_send.at[2, step], t_recv.at[2, step], plan.device_of(seq, to))
        copy.start()
        last.append(copy)
    table[rank] = second[...]
    for copy in last:
        copy.wait_recv()
    for copy in hops + across + last:
        copy.wait_send()
    finish_edges(plan, seq, rank, *refs)


def last_rows(plan, rows, pair, window_text, tokens, grad_middle, scale_a, text, masks, rest):
    placed = jax.ShapeDtypeStruct((plan.rows_dev, plan.width), F32)
    cols = 6 * plan.width // plan.group
    dma = pltpu.SemaphoreType.DMA
    most = max(plan.group, plan.sequences)
    out, extra, table = call(
        functools.partial(last_kernel, plan),
        "last",
        10,
        (placed, placed, jax.ShapeDtypeStruct((plan.group, plan.sequences, 1, cols), F32)),
        [
            pltpu.VMEM((plan.own, plan.width), F32),
            pltpu.VMEM((2, 6 * plan.width), F32),
            pltpu.VMEM((plan.group, 2, cols), F32),
            pltpu.VMEM((plan.sequences, 1, cols), F32),
            pltpu.VMEM((2, 1, cols), F32),
            dma((3, most)),
            dma((3, most)),
        ]
        + sum_scratch(plan)
        + edge_scratch(plan),
        (rows, pair, window_text, tokens, grad_middle, scale_a, text, masks, rest),
    )
    return out, extra, table[:, :, 0].transpose(1, 0, 2).reshape(plan.sequences, -1)


def over_sequences(plan, pieces):
    full = lax.all_gather(pieces, "dev", axis=0, axis_index_groups=plan.rank_groups())
    return full.reshape((plan.devices,) + pieces.shape[1:])


def terms_to_send(plan, grad, rows):
    return grad.astype(BF16).reshape(plan.sequences, plan.group, rows, grad.shape[2])


def over_sequences_sum(plan, pieces):
    return lax.psum_scatter(pieces, "dev", scatter_dimension=0, axis_index_groups=plan.rank_groups())


def merge_rows(plan, weight, rank):
    if plan.chip_heads:
        return lax.all_gather(weight, "dev", axis=0, axis_index_groups=plan.rank_groups())
    share = plan.width // plan.group
    full = lax.all_gather(weight, "dev", axis=0, tiled=True)
    full = full.reshape(2, 2, plan.group // 2, share, weight.shape[1])
    full = lax.dynamic_index_in_dim(full, lax.rem(rank, 2), 1, keepdims=False)
    return lax.dynamic_index_in_dim(full, lax.div(rank, 2), 1, keepdims=False)


def merge_sum(plan, term, term_out, rank):
    if plan.chip_heads:
        return over_sequences_sum(plan, term_out)
    half = plan.group // 2
    _, share, cols = term.shape
    mine = [jnp.where(lax.rem(rank, 2) == k, term, jnp.zeros((), BF16)) for k in range(2)]
    full = jnp.zeros((2, 2, half, share, cols), BF16)
    full = lax.dynamic_update_slice_in_dim(full, jnp.stack(mine, axis=1)[:, :, None], lax.div(rank, 2), 2)
    return lax.psum_scatter(full.reshape(-1, cols), "dev", scatter_dimension=0, tiled=True)


def down_slices(plan, weight):
    full = lax.all_gather(weight, "dev", axis=0, axis_index_groups=plan.rank_groups())
    return full.reshape(2, -1, weight.shape[1])


def by_stream(plan, image_part, text_part, is_text):
    start, end = plan.text_start, plan.image_end
    mixed = jnp.where(is_text[start:end, None], text_part[: end - start], image_part[start:])
    return jnp.concatenate([image_part[:start], mixed, text_part[end - start :]], axis=0)


def stream_dot(plan, rows, pair, is_text):
    image_part = jnp.dot(rows[: plan.image_end], pair[0], preferred_element_type=F32)
    text_part = jnp.dot(rows[plan.text_start :], pair[1], preferred_element_type=F32)
    return by_stream(plan, image_part, text_part, is_text)


def stream_dot_back(plan, grads, pair, is_text):
    image_part = lax.dot_general(grads[: plan.image_end], pair[0], CONTRACT_LAST, preferred_element_type=F32)
    text_part = lax.dot_general(grads[plan.text_start :], pair[1], CONTRACT_LAST, preferred_element_type=F32)
    return by_stream(plan, image_part, text_part, is_text)


def weight_terms(plan, rows, grads, is_text):
    zero = jnp.zeros((), grads.dtype)
    image = jnp.where(is_text[: plan.image_end, None], zero, grads[: plan.image_end])
    text = jnp.where(is_text[plan.text_start :, None], grads[plan.text_start :], zero)
    image_term = lax.dot_general(rows[: plan.image_end], image, CONTRACT_FIRST, preferred_element_type=F32)
    text_term = lax.dot_general(rows[plan.text_start :], text, CONTRACT_FIRST, preferred_element_type=F32)
    return jnp.stack([image_term, text_term])


def pick(table, text_rows):
    return jnp.where(text_rows[:, None], table[1][None, :], table[0][None, :])


def on_device(
    tokens,
    conditioning,
    text_lengths,
    modulation_weight,
    project_weight,
    merge_weight,
    up_weight,
    down_weight,
    cotangent,
):
    rows_dev, width = tokens.shape
    mod_rows = modulation_weight.shape[0]
    plan = Plan(lax.axis_size("dev"), conditioning.shape[0], rows_dev, width)
    device = lax.axis_index("dev")
    seq, rank = plan.place_of(device)
    feature_start = device * mod_rows % width

    ends = jnp.cumsum(IMG + text_lengths)
    starts = jnp.concatenate([jnp.zeros((1,), jnp.int32), ends[:-1]])
    positions = device * rows_dev + jnp.arange(rows_dev, dtype=jnp.int32)
    row_seq = jnp.sum((starts[None, :] <= positions[:, None]).astype(jnp.int32), axis=1) - 1
    offset = plan.span * seq - plan.edge + jnp.arange(plan.rows, dtype=jnp.int32) - starts[seq]
    valid = (offset >= 0) & (offset < IMG + text_lengths[seq])
    is_text = offset >= IMG
    bias = jnp.where(valid, 0.0, MASKED).astype(F32)[None, :]
    own_valid = own_rows(plan, valid[:, None], rank)[:, 0]
    own_text = own_rows(plan, is_text[:, None], rank)[:, 0]

    cond_float = conditioning.astype(F32)
    silu_low = jax.nn.silu(cond_float).astype(BF16)
    silu_part = lax.dynamic_slice_in_dim(silu_low, feature_start, mod_rows, 1)
    mod_part = jnp.dot(silu_part, modulation_weight, preferred_element_type=F32)

    merge_pair = merge_rows(plan, merge_weight, rank)
    project_pieces, up_pieces = swap_in(plan, project_weight, up_weight)
    project_pieces, up_pieces, merge_pair = lax.optimization_barrier((project_pieces, up_pieces, merge_pair))
    project_pair = over_sequences(plan, project_pieces)
    share = project_pair.shape[2] // 2
    project_pair = jnp.concatenate([project_pair[:, :, :share], project_pair[:, :, share:]], axis=1)
    project_pair = project_pair.reshape(2, width, share)
    up_pair = over_sequences(plan, up_pieces).reshape(2, width, -1)
    down_pair = down_slices(plan, down_weight)

    token_window, grad_window, mods, merge_pair = entry(plan, tokens, cotangent, mod_part, merge_pair)
    shift_a, scale_a, gate_a, shift_b, scale_b, gate_b = jnp.split(mods, 6, axis=1)
    grad_window = jnp.where(valid[:, None], grad_window, jnp.zeros((), BF16))

    normed_full, _ = layer_norm(token_window.astype(F32))
    hidden_a = (normed_full * (1.0 + pick(scale_a, is_text)) + pick(shift_a, is_text)).astype(BF16)
    projected = stream_dot(plan, hidden_a, project_pair, is_text).astype(BF16)
    attended = attend(plan, projected, bias)

    own_tokens = own_rows(plan, token_window, rank)
    own_grad = own_rows(plan, grad_window, rank)
    text_mask = own_text.astype(F32)[:, None]
    window_text = is_text.astype(F32)[:, None]
    merged, hidden_b = middle_rows(
        plan, attended, merge_pair, window_text, own_tokens, gate_a, scale_b, shift_b, text_mask
    )
    middle = own_tokens.astype(F32) + pick(gate_a, own_text) * merged
    normed_b, inv_b = layer_norm(middle)

    upper = stream_dot(plan, hidden_b, up_pair, is_text)
    activated = jax.nn.gelu(upper, approximate=True).astype(BF16)
    grad_lowered = (pick(gate_b, is_text) * grad_window.astype(F32)).astype(BF16)
    down_term = weight_terms(plan, activated, grad_lowered, is_text).astype(BF16)
    down_term = down_term.reshape(plan.sequences, -1, width)
    down_term, grad_lowered = lax.optimization_barrier((down_term, grad_lowered))
    down_sum = over_sequences_sum(plan, down_term)
    grad_activated = stream_dot_back(plan, grad_lowered, down_pair, is_text)
    gelu_pull = jax.vjp(lambda value_in: jax.nn.gelu(value_in, approximate=True), upper)[1]
    grad_upper = gelu_pull(grad_activated)[0].astype(BF16)
    up_term = terms_to_send(plan, weight_terms(plan, hidden_b, grad_upper, is_text), mod_rows)
    grad_upper, up_term = lax.optimization_barrier((grad_upper, up_term))
    up_sum = over_sequences_sum(plan, up_term)
    grad_hidden_b, grad_middle, grad_merged = back_rows(
        plan, grad_upper, up_pair, window_text, own_grad, middle, gate_a, scale_b, text_mask
    )
    foreign = (row_seq != seq)[:, None]
    merge_term = weight_terms(plan, attended, grad_merged, is_text).astype(BF16)

    grad_projected = attend_back(plan, projected, grad_merged, merge_pair, window_text, bias)
    grad_projected, down_sum = lax.optimization_barrier((grad_projected, down_sum))
    down_grad = down_sum.astype(F32)
    project_term = project_terms(plan, hidden_a, grad_projected, window_text, mod_rows)
    grad_projected, project_term = lax.optimization_barrier((grad_projected, project_term))
    project_sum = over_sequences_sum(plan, project_term)
    activated, project_term = lax.optimization_barrier((activated, project_term))
    lowered, out_here, out_there, merge_out = output_rows(
        plan, activated, down_pair, window_text, middle, gate_b, text_mask, merge_term
    )
    layer_out = jnp.where(foreign, out_there, out_here)

    masks = jnp.stack([own_valid & ~own_text, own_valid & own_text], axis=1).astype(F32)
    rest = jnp.concatenate(
        [
            jnp.stack([jnp.sum(value * masks[:, j : j + 1], axis=0) for j in range(2)])
            for value in (
                grad_middle * merged,
                grad_hidden_b,
                grad_hidden_b * normed_b,
                own_grad.astype(F32) * lowered,
            )
        ],
        axis=1,
    )
    rest, up_sum = lax.optimization_barrier((rest, up_sum))
    back_here, back_there, grad_table = last_rows(
        plan, grad_projected, project_pair, window_text, own_tokens, grad_middle, scale_a, text_mask, masks, rest
    )
    tokens_grad = jnp.where(foreign, back_there, back_here)
    own_grads = grad_table.astype(BF16)
    modulation_grad = lax.dot_general(silu_part, own_grads, CONTRACT_FIRST, preferred_element_type=F32)
    grad_piece = lax.dot_general(own_grads, modulation_weight, CONTRACT_LAST, preferred_element_type=F32)
    merge_out, merge_term, project_sum, modulation_grad, down_grad, layer_out, tokens_grad = lax.optimization_barrier(
        (merge_out, merge_term, project_sum, modulation_grad, down_grad, layer_out, tokens_grad)
    )
    merge_grad = merge_sum(plan, merge_term, merge_out, rank).reshape(merge_weight.shape).astype(F32)
    up_grad, project_grad, everyone = finish(plan, up_sum, project_sum, grad_piece.reshape(-1, 128))
    everyone = everyone.reshape(2, plan.devices // 2, plan.sequences, mod_rows)
    grad_silu = (everyone[0] + everyone[1]).transpose(1, 0, 2).reshape(plan.sequences, width)
    conditioning_grad = jax.vjp(jax.nn.silu, cond_float)[1](grad_silu)[0]
    return (
        layer_out,
        tokens_grad,
        conditioning_grad,
        modulation_grad,
        project_grad,
        merge_grad,
        up_grad,
        down_grad,
    )


def solution(mesh):
    shard, whole = P("dev", None), P()
    return jax.shard_map(
        on_device,
        mesh=mesh,
        in_specs=(shard, whole, whole, shard, shard, shard, shard, shard, shard),
        out_specs=(shard, shard, whole, shard, shard, shard, shard, shard),
        check_vma=False,
    )
```

```python
import functools
import types

import jax
import jax.numpy as jnp
import numpy as np
from jax import lax
from jax.experimental import pallas as pl
from jax.experimental.pallas import tpu as pltpu
from jax.sharding import PartitionSpec as P

HEADS = 24
HDIM = 64
IMG = 1024
TXT_MIN = 86
TXT_MAX = 154
EPSILON = 1e-06
F32 = jnp.float32
BF16 = jnp.bfloat16
CONTRACT_LAST = (((1,), (1,)), ((), ()))
PLAIN = (((1,), (0,)), ((), ()))
CONTRACT_FIRST = (((0,), (0,)), ((), ()))
MASKED = -1e30


class Plan:
    def __init__(self, devices, sequences, rows_dev, width):
        self.devices, self.sequences, self.rows_dev, self.width = devices, sequences, rows_dev, width
        self.group = devices // sequences
        self.span = self.group * rows_dev
        mean = self.span - IMG
        up, down = TXT_MAX - mean, mean - TXT_MIN
        drift = 0
        for k in range(sequences + 1):
            drift = max(drift, min(up * k, down * (sequences - k)), min(down * k, up * (sequences - k)))
        self.edge = -(-drift // 64) * 64
        self.rows = self.span + 2 * self.edge
        self.piece = 2 * self.edge // self.group
        self.own = rows_dev + self.piece
        self.image_end = -(-(self.edge + drift + IMG) // 128) * 128
        self.text_start = (self.edge - drift + IMG) // 128 * 128
        self.heads = HEADS // self.group
        self.segments = self.edge_segments()
        self.chip_heads = devices == 4 * self.group

    def device_of(self, seq, rank):
        return seq * self.group + rank

    def place_of(self, device):
        return lax.div(device, self.group), lax.rem(device, self.group)

    def seq_groups(self):
        return [[self.device_of(s, r) for r in range(self.group)] for s in range(self.sequences)]

    def rank_groups(self):
        return [[self.device_of(s, r) for s in range(self.sequences)] for r in range(self.group)]

    def edge_row(self, rank):
        half = self.group // 2
        return jnp.where(rank < half, self.piece * rank, self.edge + self.span + self.piece * (rank - half))

    def main_row(self, rank):
        return self.edge + self.rows_dev * rank

    def edge_segments(self):
        found = []
        for rank in range(self.group):
            half = self.group // 2
            first = self.piece * rank - self.edge if rank < half else self.span + self.piece * (rank - half)
            row = 0
            while row < self.piece:
                owner, owner_row = (first + row) // self.rows_dev, (first + row) % self.rows_dev
                count = min(self.piece - row, self.rows_dev - owner_row)
                found.append((rank, row, count, owner // self.group, owner % self.group, owner_row))
                row += count
        return found


def layer_norm(values):
    mean = jnp.mean(values, axis=-1, keepdims=True)
    centred = values - mean
    variance = jnp.mean(centred * centred, axis=-1, keepdims=True)
    inv_std = lax.rsqrt(variance + EPSILON)
    return (centred * inv_std, inv_std)


def norm_back(grad_normed, normed, inv_std):
    mean_grad = jnp.mean(grad_normed, axis=-1, keepdims=True)
    mean_cross = jnp.mean(grad_normed * normed, axis=-1, keepdims=True)
    return inv_std * (grad_normed - mean_grad - normed * mean_cross)


def softmax_parts(query, key, bias):
    scores = lax.dot_general(query, key, CONTRACT_LAST, preferred_element_type=F32) + bias
    top = jnp.max(scores, axis=1, keepdims=True)
    exponent = jnp.exp(scores - top)
    total = jnp.sum(exponent, axis=1, keepdims=True)
    return exponent * (1.0 / total)


def head_columns(heads, part, head):
    first = (part * heads + head) * HDIM
    return slice(first, first + HDIM)


def attend_kernel(heads, block, projected, bias_ref, out_ref):
    rows = pl.ds(pl.multiple_of(pl.program_id(0) * block, block), block)
    bias = bias_ref[...]
    outs = []
    for head in range(heads):
        query = projected[rows, head_columns(heads, 0, head)] * jnp.asarray(HDIM ** (-0.5), BF16)
        probs = softmax_parts(query, projected[:, head_columns(heads, 1, head)], bias).astype(BF16)
        outs.append(jnp.dot(probs, projected[:, head_columns(heads, 2, head)], preferred_element_type=F32))
    out_ref[...] = jnp.concatenate(outs, axis=1).astype(BF16)


def block_rows(rows):
    return 256 if rows % 256 == 0 else 128


def constant(shape):
    return pl.BlockSpec(shape, lambda i: (0,) * len(shape))


def attend(plan, projected, bias):
    rows, cols = projected.shape[0], projected.shape[1] // 3
    block = block_rows(rows)
    return pl.pallas_call(
        functools.partial(attend_kernel, plan.heads, block),
        out_shape=jax.ShapeDtypeStruct((rows, cols), BF16),
        grid=(rows // block,),
        in_specs=[constant(projected.shape), constant(bias.shape)],
        out_specs=pl.BlockSpec((block, cols), lambda i: (i, 0)),
        compiler_params=pltpu.CompilerParams(vmem_limit_bytes=48 << 20),
        cost_estimate=pl.CostEstimate(flops=16 * rows * rows * cols, bytes_accessed=8 * rows * cols, transcendentals=0),
        name="attend",
    )(projected, bias)


def attend_back_kernel(
    heads, steps, block, projected, grad_merged, merge_pair, text, bias_ref, out, key_sum, value_sum
):
    step = pl.program_id(0)
    scale = jnp.asarray(HDIM ** (-0.5), BF16)

    @pl.when(step == 0)
    def _():
        key_sum[...] = jnp.zeros_like(key_sum)
        value_sum[...] = jnp.zeros_like(value_sum)

    rows = pl.ds(pl.multiple_of(step * block, block), block)
    bias = bias_ref[...]
    image, other_stream = [
        lax.dot_general(grad_merged[...], merge_pair[j], CONTRACT_LAST, preferred_element_type=F32) for j in range(2)
    ]
    grad_attended = jnp.where(text[...] > 0, other_stream, image).astype(BF16)
    grads = []
    for head in range(heads):
        query = projected[rows, head_columns(heads, 0, head)] * scale
        key = projected[:, head_columns(heads, 1, head)]
        grad_out = grad_attended[:, head * HDIM : (head + 1) * HDIM]
        probs = softmax_parts(query, key, bias)
        grad_probs = lax.dot_general(
            grad_out, projected[:, head_columns(heads, 2, head)], CONTRACT_LAST, preferred_element_type=F32
        )
        inner = jnp.sum(probs * grad_probs, axis=1, keepdims=True)
        grad_scores = (probs * (grad_probs - inner)).astype(BF16)
        grads.append(jnp.dot(grad_scores, key, preferred_element_type=F32) * HDIM ** (-0.5))
        key_sum[head] += lax.dot_general(query, grad_scores, CONTRACT_FIRST, preferred_element_type=F32)
        value_sum[head] += lax.dot_general(grad_out, probs.astype(BF16), CONTRACT_FIRST, preferred_element_type=F32)
    cols = heads * HDIM
    out[rows, :cols] = jnp.concatenate(grads, axis=1).astype(BF16)

    @pl.when(step == steps - 1)
    def _():
        total = out.shape[0]
        out[:, cols : 2 * cols] = key_sum[...].reshape(cols, total).T.astype(BF16)
        out[:, 2 * cols :] = value_sum[...].reshape(cols, total).T.astype(BF16)


def attend_back(plan, projected, grad_merged, merge_pair, text, bias):
    rows, cols = projected.shape[0], projected.shape[1] // 3
    block = block_rows(rows)
    return pl.pallas_call(
        functools.partial(attend_back_kernel, plan.heads, rows // block, block),
        out_shape=jax.ShapeDtypeStruct(projected.shape, BF16),
        grid=(rows // block,),
        in_specs=[
            constant(projected.shape),
            pl.BlockSpec((block, plan.width), lambda i: (i, 0)),
            constant(merge_pair.shape),
            pl.BlockSpec((block, 1), lambda i: (i, 0)),
            constant(bias.shape),
        ],
        out_specs=constant(projected.shape),
        scratch_shapes=[pltpu.VMEM((plan.heads, HDIM, rows), F32)] * 2,
        compiler_params=pltpu.CompilerParams(vmem_limit_bytes=56 << 20),
        cost_estimate=pl.CostEstimate(flops=40 * rows * rows * cols, bytes_accessed=14 * rows * cols, transcendentals=0),
        name="attend_back",
    )(projected, grad_merged, merge_pair, text, bias)


def fold_rows(piece):
    half = piece.shape[0] // 2
    return jnp.concatenate([piece[:half], piece[half:]], axis=1)


def unfold_rows(piece):
    half = piece.shape[1] // 2
    return jnp.concatenate([piece[:, :half], piece[:, half:]], axis=0)


def terms_kernel(plan, fold, chunk, rows, grads, text, out, kept):
    width = rows.shape[1]
    for stream, (first, last) in enumerate(((0, plan.image_end), (plan.text_start, plan.rows))):
        count = last - first
        mask = text[pl.ds(first, count)]
        keep = (mask > 0) if stream else (mask <= 0)
        kept[pl.ds(0, count)] = jnp.where(keep, grads[pl.ds(first, count)], jnp.zeros((), BF16))

        def step(i, carry):
            start = pl.multiple_of(i * chunk, chunk)
            term = lax.dot_general(
                rows[pl.ds(first, count), pl.ds(start, chunk)],
                kept[pl.ds(0, count)],
                CONTRACT_FIRST,
                preferred_element_type=F32,
            ).astype(BF16)
            if fold:
                for j in range(chunk // fold):
                    out[(stream * width) // fold + i * (chunk // fold) + j] = fold_rows(term[j * fold : (j + 1) * fold])
            else:
                out[stream, pl.ds(start, chunk)] = term
            return carry

        if width == chunk:
            step(0, 0)
        else:
            lax.fori_loop(0, width // chunk, step, 0)


def weight_terms(plan, rows, grads, text, name, fold=0):
    width, cols = rows.shape[1], grads.shape[1]
    chunk = 384 if width % 384 == 0 else width
    shape = (2 * width // fold, fold // 2, 2 * cols) if fold else (2, width, cols)
    return pl.pallas_call(
        functools.partial(terms_kernel, plan, fold, chunk),
        out_shape=jax.ShapeDtypeStruct(shape, BF16),
        in_specs=[pl.BlockSpec(memory_space=pltpu.VMEM)] * 3,
        out_specs=pl.BlockSpec(memory_space=pltpu.VMEM),
        scratch_shapes=[pltpu.VMEM((plan.image_end, cols), BF16)],
        compiler_params=pltpu.CompilerParams(vmem_limit_bytes=40 << 20),
        cost_estimate=pl.CostEstimate(flops=3 * plan.rows * width * cols, bytes_accessed=1 << 23, transcendentals=0),
        name=name,
    )(rows, grads, text)


VMEM = pl.BlockSpec(memory_space=pltpu.VMEM)


def own_rows(plan, window, rank):
    main = lax.dynamic_slice_in_dim(window, plan.main_row(rank), plan.rows_dev, 0)
    edge = lax.dynamic_slice_in_dim(window, plan.edge_row(rank), plan.piece, 0)
    return jnp.concatenate([main, edge], axis=0)


def remote(source, target, send_sem, recv_sem, device):
    return pltpu.make_async_remote_copy(
        src_ref=source,
        dst_ref=target,
        send_sem=send_sem,
        recv_sem=recv_sem,
        device_id=(device,),
        device_id_type=pl.DeviceIdType.MESH,
    )


def here(plan):
    return plan.place_of(lax.axis_index("dev"))


def other(rank, step, size):
    return lax.rem(rank + step, size)


def meet(devices):
    barrier = pltpu.get_barrier_semaphore()
    for device in devices:
        pl.semaphore_signal(barrier, inc=1, device_id=(device,), device_id_type=pl.DeviceIdType.MESH)
    pl.semaphore_wait(barrier, len(devices))


def group_devices(plan, seq, rank):
    return [plan.device_of(seq, other(rank, step, plan.group)) for step in range(1, plan.group)]


def column_devices(plan, seq, rank):
    return [plan.device_of(other(seq, step, plan.sequences), rank) for step in range(1, plan.sequences)]


def every_device(plan, device):
    return [other(device, step, plan.devices) for step in range(1, plan.devices)]


def call(kernel, name, ident, out_shape, scratch, operands, in_specs=None, out_specs=None, vmem=40 << 20):
    outs = out_shape if isinstance(out_shape, tuple) else (out_shape,)
    return pl.pallas_call(
        kernel,
        out_shape=out_shape,
        in_specs=in_specs or [VMEM] * len(operands),
        out_specs=out_specs or (tuple([VMEM] * len(outs)) if isinstance(out_shape, tuple) else VMEM),
        scratch_shapes=scratch,
        compiler_params=pltpu.CompilerParams(
            collective_id=ident, has_side_effects=True, vmem_limit_bytes=vmem
        ),
        name=name,
    )(*operands)


def aligned(start):
    return pl.multiple_of(start, 16)


def block_parts(plan, ref, rank):
    return (
        ref.at[pl.ds(aligned(plan.main_row(rank)), plan.rows_dev)],
        ref.at[pl.ds(aligned(plan.edge_row(rank)), plan.piece)],
    )


def own_parts(plan, ref):
    return ref.at[pl.ds(0, plan.rows_dev)], ref.at[pl.ds(plan.rows_dev, plan.piece)]


def load_block(plan, ref, rank):
    main, edge = block_parts(plan, ref, rank)
    return jnp.concatenate([main[...], edge[...]], axis=0)


def sum_scratch(plan):
    half, own, width = plan.group // 2, plan.own, plan.width
    return [
        pltpu.VMEM((half, own, width), F32),
        pltpu.VMEM((half, own, width), F32),
        pltpu.VMEM((own, width), F32),
        pltpu.VMEM((half - 1, own, width), BF16),
        pltpu.VMEM((half - 1, own, width), BF16),
        pltpu.SemaphoreType.DMA((half,)),
        pltpu.SemaphoreType.DMA((half,)),
        pltpu.SemaphoreType.DMA((half,)),
        pltpu.SemaphoreType.DMA((half,)),
    ]


SUM_SCRATCH = 9


def product(plan, rows, pair, text, dims, rank, out):
    block = load_block(plan, rows, rank)
    text_row = load_block(plan, text, rank) > 0
    chunk = plan.width // 4

    def step(i, carry):
        cols = pl.ds(pl.multiple_of(i * chunk, chunk), chunk)
        parts = []
        for stream in range(2):
            weight = pair[stream, cols, :] if dims is CONTRACT_LAST else pair[stream, :, cols]
            parts.append(lax.dot_general(block, weight, dims, preferred_element_type=F32))
        out[:, cols] = jnp.where(text_row, parts[1], parts[0])
        return carry

    lax.fori_loop(0, 4, step, 0)


def scatter_sum(*args):
    return scatter_start(*args)()


def scatter_start(plan, seq, rank, rows, pair, text, dims, away, near, mine, going, coming,
                  pair_send, pair_recv, far_send, far_recv):
    half = plan.group // 2
    chip, core = lax.div(rank, 2), lax.rem(rank, 2)
    partner = plan.device_of(seq, 2 * chip + 1 - core)
    order = list(range(1, half)) + [0]

    def pair_copy(step):
        return remote(away.at[step], near.at[step], pair_send.at[step], pair_recv.at[step], partner)

    def far_copy(step):
        to = plan.device_of(seq, 2 * other(chip, step, half) + core)
        return remote(going.at[step - 1], coming.at[step - 1], far_send.at[step], far_recv.at[step], to)

    def for_owner(step):
        product(plan, rows, pair, text, dims, 2 * other(chip, step, half) + core, mine)
        pair_copy(step).wait_recv()
        mine[...] += near[step]

    def turn(i, carry):
        step = other(i, 1, half)
        product(plan, rows, pair, text, dims, 2 * other(chip, step, half) + 1 - core, away.at[step])
        pair_copy(step).start()

        @pl.when(i > 0)
        def _():
            for_owner(i)
            going[i - 1] = mine[...].astype(BF16)
            far_copy(i).start()

        return carry

    lax.fori_loop(0, half, turn, 0)

    def result():
        for_owner(0)
        total = mine[...]
        for step in range(1, half):
            far_copy(step).wait_recv()
            total = total + coming[step - 1].astype(F32)
        for step in range(half):
            pair_copy(step).wait_send()
        for step in range(1, half):
            far_copy(step).wait_send()
        return total

    return result


def share_scratch(plan):
    return [pltpu.SemaphoreType.DMA((plan.group, 2))] * 2 + [pltpu.SemaphoreType.DMA((plan.group, 2))]


def share_rows(plan, seq, rank, parts, window, send, recv, pass_send):
    half = plan.group // 2
    chip, core = lax.div(rank, 2), lax.rem(rank, 2)
    partner_rank = 2 * chip + 1 - core
    partner = plan.device_of(seq, partner_rank)

    def send_own(to_device, slot):
        copies = [
            remote(source, target, send.at[slot, i], recv.at[slot, i], to_device)
            for i, (source, target) in enumerate(zip(parts, block_parts(plan, window, rank)))
        ]
        for copy in copies:
            copy.start()
        return copies

    flying = {}
    for step in range(1, half):
        flying[step] = send_own(plan.device_of(seq, 2 * other(chip, step, half) + core), step)
    flying[0] = send_own(partner, 0)
    for source, target in zip(parts, block_parts(plan, window, rank)):
        target[...] = source[...]
    passed = []
    for step in range(1, half):
        for copy in flying[step]:
            copy.wait_recv()
        came = 2 * other(chip, half - step, half) + core
        copies = [
            remote(place, place, pass_send.at[step, i], recv.at[half + step, i], partner)
            for i, place in enumerate(block_parts(plan, window, came))
        ]
        for copy in copies:
            copy.start()
        passed.extend(copies)
    for copy in flying[0]:
        copy.wait_recv()
    for copy in passed:
        copy.wait_recv()
    for copies in flying.values():
        for copy in copies:
            copy.wait_send()
    for copy in passed:
        copy.wait_send()


def entry_kernel(plan, tokens, grads, mod_part, *refs):
    if plan.chip_heads:
        merge, merge_out, *refs = refs[:1] + refs[4:5] + refs[1:4] + refs[5:]
        merge_send, merge_recv, *refs = refs[-2:] + refs[:-2]
    (token_window, grad_window, mods, token_own, grad_own, plane, across, chunk, edge_send, edge_recv,
     t_send, t_recv, t_pass, g_send, g_recv, g_pass, m_send, m_recv) = refs
    device = lax.axis_index("dev")
    seq, rank = plan.place_of(device)
    meet(every_device(plan, device))
    swaps = []
    if plan.chip_heads:
        core = lax.rem(rank, 2)
        partner = plan.device_of(seq, 2 * lax.div(rank, 2) + 1 - core)
        for stream in range(2):
            copy = remote(
                merge.at[2 * stream + 1 - core],
                merge_out.at[stream, core],
                merge_send.at[stream],
                merge_recv.at[stream],
                partner,
            )
            copy.start()
            swaps.append(copy)
            merge_out[stream, core] = merge[2 * stream + core]
    hops = []
    for step in range(1, plan.group):
        to = other(rank, step, plan.group)
        copy = remote(mod_part.at[to], plane.at[step], m_send.at[0, step], m_recv.at[0, step], plan.device_of(seq, to))
        copy.start()
        hops.append(copy)
    arrays = ((tokens, token_own), (grads, grad_own))
    count = len(plan.segments)
    for which, (source, own) in enumerate(arrays):
        for index, (to_rank, row, rows, step, owner, owner_row) in enumerate(plan.segments):
            @pl.when(rank == owner)
            def _():
                remote(
                    source.at[pl.ds(owner_row, rows)],
                    own.at[pl.ds(row, rows)],
                    edge_send.at[which * count + index],
                    edge_recv.at[which * count + index],
                    plan.device_of(lax.rem(seq + plan.sequences - step, plan.sequences), to_rank),
                ).start()
    for copy in hops:
        copy.wait_recv()
    total = mod_part[rank]
    for step in range(1, plan.group):
        total = total + plane[step]
    plane[0] = total
    hops_across = []
    for step in range(1, plan.sequences):
        to = other(seq, step, plan.sequences)
        copy = remote(plane.at[0, to], across.at[seq], m_send.at[1, step], m_recv.at[1, step], plan.device_of(to, rank))
        copy.start()
        hops_across.append(copy)
    across[seq] = plane[0, seq]
    for which, (source, own) in enumerate(arrays):
        for index, (to_rank, row, rows, step, owner, owner_row) in enumerate(plan.segments):
            @pl.when(rank == to_rank)
            def _():
                remote(
                    source.at[pl.ds(owner_row, rows)],
                    own.at[pl.ds(row, rows)],
                    edge_send.at[which * count + index],
                    edge_recv.at[which * count + index],
                    plan.device_of(lax.rem(seq + plan.sequences + step, plan.sequences), owner),
                ).wait_recv()
    share_rows(plan, seq, rank, (tokens, token_own), token_window, t_send, t_recv, t_pass)
    for copy in hops_across:
        copy.wait_recv()
    half = plan.sequences // 2
    for stream in range(2):
        total = across[stream * half]
        for i in range(1, half):
            total = total + across[stream * half + i]
        chunk[stream] = total
    hops_back = []
    for step in range(1, plan.group):
        to = other(rank, step, plan.group)
        copy = remote(chunk, mods.at[rank], m_send.at[2, step], m_recv.at[2, step], plan.device_of(seq, to))
        copy.start()
        hops_back.append(copy)
    mods[rank] = chunk[...]
    share_rows(plan, seq, rank, (grads, grad_own), grad_window, g_send, g_recv, g_pass)
    for copy in hops_back:
        copy.wait_recv()
    for copy in hops + hops_across + hops_back:
        copy.wait_send()
    for copy in swaps:
        copy.wait()
    for which, (source, own) in enumerate(arrays):
        for index, (to_rank, row, rows, step, owner, owner_row) in enumerate(plan.segments):
            @pl.when(rank == owner)
            def _():
                remote(
                    source.at[pl.ds(owner_row, rows)],
                    own.at[pl.ds(row, rows)],
                    edge_send.at[which * count + index],
                    edge_recv.at[which * count + index],
                    plan.device_of(lax.rem(seq + plan.sequences - step, plan.sequences), to_rank),
                ).wait_send()


def entry(plan, tokens, grads, mod_part, merge):
    lanes = mod_part.shape[1] // plan.group // 128
    pieces = mod_part.reshape(plan.sequences, plan.group, lanes, 128).transpose(1, 0, 2, 3)
    window = jax.ShapeDtypeStruct((plan.rows, plan.width), BF16)
    dma = pltpu.SemaphoreType.DMA
    most = max(plan.group, plan.sequences)
    shapes = (window, window, jax.ShapeDtypeStruct((plan.group, 2, lanes, 128), F32))
    operands = (tokens, grads, pieces)
    scratch = (
        [
            pltpu.VMEM((plan.piece, plan.width), BF16),
            pltpu.VMEM((plan.piece, plan.width), BF16),
            pltpu.VMEM((plan.group, plan.sequences, lanes, 128), F32),
            pltpu.VMEM((plan.sequences, lanes, 128), F32),
            pltpu.VMEM((2, lanes, 128), F32),
            dma((2 * len(plan.segments),)),
            dma((2 * len(plan.segments),)),
        ]
        + share_scratch(plan)
        + share_scratch(plan)
        + [dma((3, most)), dma((3, most))]
    )
    if plan.chip_heads:
        shapes += (jax.ShapeDtypeStruct((2, 2) + merge.shape[1:], BF16),)
        operands += (merge,)
        scratch += [dma((2,)), dma((2,))]
    token_window, grad_window, mods, *rest = call(
        functools.partial(entry_kernel, plan), "entry", 1, shapes, scratch, operands
    )
    merge_pair = rest[0].reshape(2, -1, plan.width) if plan.chip_heads else merge
    return token_window, grad_window, mods.transpose(1, 0, 2, 3).reshape(2, -1), merge_pair


def project_columns(plan, rank):
    share = plan.width // plan.group
    first = (rank % 2) * (plan.width // 2) + (rank // 2) * share
    return [part * plan.width + first for part in range(3)], share


def up_columns(plan, rank, cols):
    planes = plan.sequences // 2
    share = cols // planes // plan.group
    return [plane * plan.group * share + rank * share for plane in range(planes)], share


def start_swap(plan, seq, rank, source, target, send, recv):
    copies = []
    for step in range(1, plan.group):
        to = other(rank, step, plan.group)
        copy = remote(source.at[to], target.at[rank], send.at[step], recv.at[step], plan.device_of(seq, to))
        copy.start()
        copies.append(copy)
    target[rank] = source[rank]
    return copies


def swap_in_kernel(plan, project, up, project_out, up_out, project_cut, up_cut, p_send, p_recv, u_send, u_recv):
    seq, rank = here(plan)
    for to in range(plan.group):
        starts, share = project_columns(plan, to)
        project_cut[to] = fold_rows(jnp.concatenate([project[:, c : c + share] for c in starts], axis=1))
    meet(group_devices(plan, seq, rank))
    copies = start_swap(plan, seq, rank, project_cut, project_out, p_send, p_recv)
    for to in range(plan.group):
        starts, share = up_columns(plan, to, up.shape[1])
        up_cut[to] = jnp.concatenate([up[:, c : c + share] for c in starts], axis=1)
    copies += start_swap(plan, seq, rank, up_cut, up_out, u_send, u_recv)
    for copy in copies:
        copy.wait()


def swap_in(plan, project, up):
    rows = project.shape[0]
    dma = pltpu.SemaphoreType.DMA
    shapes = [
        (plan.group, rows // 2, 2 * project.shape[1] // plan.group),
        (plan.group, rows, up.shape[1] // plan.group),
    ]
    return call(
        functools.partial(swap_in_kernel, plan),
        "swap_in",
        4,
        tuple(jax.ShapeDtypeStruct(shape, BF16) for shape in shapes),
        [pltpu.VMEM(shape, BF16) for shape in shapes] + [dma((plan.group,))] * 4,
        (project, up),
    )


def place_columns(plan, got, out, columns, unfold):
    for source in range(plan.group):
        starts, share = columns(plan, source)
        piece = unfold_rows(got[source]) if unfold else got[source]
        for i, c in enumerate(starts):
            out[:, c : c + share] = piece[:, i * share : (i + 1) * share]


def finish_kernel(plan, up, project, up_out, project_out, up_got, project_got, u_send, u_recv, p_send, p_recv):
    seq, rank = here(plan)
    meet(group_devices(plan, seq, rank))
    ups = start_swap(plan, seq, rank, up, up_got, u_send, u_recv)
    projects = start_swap(plan, seq, rank, project, project_got, p_send, p_recv)
    for copy in ups:
        copy.wait()
    place_columns(plan, up_got, up_out, lambda p, r: up_columns(p, r, up_out.shape[1]), False)
    for copy in projects:
        copy.wait()
    place_columns(plan, project_got, project_out, project_columns, True)


def finish(plan, up, project):
    dma = pltpu.SemaphoreType.DMA
    rows = up.shape[1]
    up_grad, project_grad = call(
        functools.partial(finish_kernel, plan),
        "finish",
        6,
        (
            jax.ShapeDtypeStruct((rows, plan.group * up.shape[2]), BF16),
            jax.ShapeDtypeStruct((rows, plan.group * project.shape[2] // 2), BF16),
        ),
        [pltpu.VMEM(up.shape, BF16), pltpu.VMEM(project.shape, BF16)] + [dma((plan.group,))] * 4,
        (up, project),
    )
    return up_grad.astype(F32), project_grad.astype(F32)


def pick_rows(table, text):
    return jnp.where(text > 0, table[1:2, :], table[0:1, :])


def norm_rows(values):
    mean = jnp.mean(values, axis=1, keepdims=True)
    centred = values - mean
    inv = lax.rsqrt(jnp.mean(centred * centred, axis=1, keepdims=True) + EPSILON)
    return centred * inv, inv


def middle_kernel(plan, rows, pair, window_text, tokens, gate_a, scale_b, shift_b, text, merged, window, own, *scratch):
    seq, rank = here(plan)
    meet(group_devices(plan, seq, rank))
    total = scatter_sum(plan, seq, rank, rows, pair, window_text, PLAIN, *scratch[:SUM_SCRATCH])
    merged[...] = total
    mask = text[...]
    middle = tokens[...].astype(F32) + pick_rows(gate_a[...], mask) * total
    normed, _ = norm_rows(middle)
    own[...] = (normed * (1.0 + pick_rows(scale_b[...], mask)) + pick_rows(shift_b[...], mask)).astype(BF16)
    share_rows(plan, seq, rank, own_parts(plan, own), window, *scratch[SUM_SCRATCH:])


def own_shape(plan, dtype=F32):
    return jax.ShapeDtypeStruct((plan.own, plan.width), dtype)


def window_shape(plan):
    return jax.ShapeDtypeStruct((plan.rows, plan.width), BF16)


def middle_rows(plan, rows, pair, window_text, tokens, gate_a, scale_b, shift_b, text):
    return call(
        functools.partial(middle_kernel, plan),
        "middle",
        2,
        (own_shape(plan), window_shape(plan)),
        [pltpu.VMEM((plan.own, plan.width), BF16)] + sum_scratch(plan) + share_scratch(plan),
        (rows, pair, window_text, tokens, gate_a, scale_b, shift_b, text),
    )


def back_kernel(plan, rows, pair, window_text, grad, middle, gate_a, scale_b, text, grad_hidden, grad_middle, window, own, *scratch):
    seq, rank = here(plan)
    meet(group_devices(plan, seq, rank))
    total = scatter_sum(plan, seq, rank, rows, pair, window_text, CONTRACT_LAST, *scratch[:SUM_SCRATCH])
    grad_hidden[...] = total
    mask = text[...]
    normed, inv = norm_rows(middle[...])
    inner = total * (1.0 + pick_rows(scale_b[...], mask))
    mean_grad = jnp.mean(inner, axis=1, keepdims=True)
    mean_cross = jnp.mean(inner * normed, axis=1, keepdims=True)
    result = grad[...].astype(F32) + inv * (inner - mean_grad - normed * mean_cross)
    grad_middle[...] = result
    own[...] = (pick_rows(gate_a[...], mask) * result).astype(BF16)
    share_rows(plan, seq, rank, own_parts(plan, own), window, *scratch[SUM_SCRATCH:])


def back_rows(plan, rows, pair, window_text, grad, middle, gate_a, scale_b, text):
    return call(
        functools.partial(back_kernel, plan),
        "back",
        3,
        (own_shape(plan), own_shape(plan), window_shape(plan)),
        [pltpu.VMEM((plan.own, plan.width), BF16)] + sum_scratch(plan) + share_scratch(plan),
        (rows, pair, window_text, grad, middle, gate_a, scale_b, text),
    )


def edge_copy(plan, seq, source, first_row, target, send, recv, index):
    from_rank, row, rows, step, owner, owner_row = plan.segments[index]
    return remote(
        source.at[pl.ds(first_row + row, rows)],
        target.at[pl.ds(owner_row, rows)],
        send.at[index],
        recv.at[index],
        plan.device_of(lax.rem(seq + plan.sequences + step, plan.sequences), owner),
    )


def start_edges(plan, seq, rank, *refs):
    for index, segment in enumerate(plan.segments):
        @pl.when(rank == segment[0])
        def _():
            edge_copy(plan, seq, *refs, index).start()


def finish_edges(plan, seq, rank, *refs):
    for index, segment in enumerate(plan.segments):
        @pl.when(rank == segment[4])
        def _():
            edge_copy(plan, seq, *refs, index).wait_recv()

        @pl.when(rank == segment[0])
        def _():
            edge_copy(plan, seq, *refs, index).wait_send()


def edge_scratch(plan):
    return [pltpu.SemaphoreType.DMA((len(plan.segments),))] * 2


def stream_sums(values, masks):
    return jnp.concatenate([jnp.sum(values * mask, axis=0, keepdims=True) for mask in masks], axis=0)


def last_kernel(plan, names, *refs):
    at = types.SimpleNamespace(**dict(zip(names, refs)))
    low_scratch = refs[len(names) : len(names) + SUM_SCRATCH]
    back_scratch = refs[len(names) + SUM_SCRATCH : len(names) + 2 * SUM_SCRATCH]
    device = lax.axis_index("dev")
    seq, rank = plan.place_of(device)
    stream = lax.div(2 * seq, plan.sequences)
    at.layer_extra[...] = jnp.zeros_like(at.layer_extra)
    at.token_extra[...] = jnp.zeros_like(at.token_extra)
    meet(every_device(plan, device))
    low_sum = scatter_start(plan, seq, rank, at.activated, at.down_pair, at.window_text, PLAIN, *low_scratch)
    back_sum = scatter_start(plan, seq, rank, at.grads, at.project_pair, at.window_text, CONTRACT_LAST, *back_scratch)
    swaps = []
    if plan.chip_heads:
        core = lax.rem(rank, 2)
        partner = plan.device_of(seq, 2 * lax.div(rank, 2) + 1 - core)
        for j in range(2):
            copy = remote(
                at.term.at[j, 1 - core], at.term_out.at[2 * j + core], at.term_send.at[j], at.term_recv.at[j], partner
            )
            copy.start()
            swaps.append(copy)
            at.term_out[2 * j + core] = at.term[j, core]
    text = at.text[...]
    streams = (at.masks[:, 0:1], at.masks[:, 1:2])
    width = plan.width

    lowered = low_sum()
    at.layer_own[...] = (at.middle[...] + pick_rows(at.gate_b[...], text) * lowered).astype(BF16)
    layer_edges = (at.layer_own, plan.rows_dev, at.layer_extra, at.l_send, at.l_recv)
    start_edges(plan, seq, rank, *layer_edges)
    at.local[:, 5 * width :] = stream_sums(at.grad[...].astype(F32) * lowered, streams)
    at.local[:, 2 * width : 5 * width] = at.rest[...]
    at.layer[...] = at.layer_own[pl.ds(0, plan.rows_dev)]

    total = back_sum()
    normed, inv = norm_rows(at.tokens[...].astype(F32))
    at.local[:, :width] = stream_sums(total, streams)
    at.local[:, width : 2 * width] = stream_sums(total * normed, streams)
    cols = 6 * width // plan.group

    def chunk(index):
        return pl.ds(pl.multiple_of(index * cols, 128), cols)

    hops = []
    for step in range(1, plan.group):
        to = other(rank, step, plan.group)
        copy = remote(
            at.local.at[:, chunk(to)], at.first.at[step], at.t_send.at[0, step], at.t_recv.at[0, step], plan.device_of(seq, to)
        )
        copy.start()
        hops.append(copy)
    inner = total * (1.0 + pick_rows(at.scale_a[...], text))
    mean_grad = jnp.mean(inner, axis=1, keepdims=True)
    mean_cross = jnp.mean(inner * normed, axis=1, keepdims=True)
    at.token_own[...] = at.grad_middle[...] + inv * (inner - mean_grad - normed * mean_cross)
    token_edges = (at.token_own, plan.rows_dev, at.token_extra, at.e_send, at.e_recv)
    start_edges(plan, seq, rank, *token_edges)
    for copy in hops:
        copy.wait_recv()
    sums = at.local[:, chunk(rank)]
    for step in range(1, plan.group):
        sums = sums + at.first[step]
    for i in range(2):
        at.mine[i] = sums[i : i + 1]
    across = []
    for step in range(1, plan.sequences):
        to = other(seq, step, plan.sequences)
        to_stream = lax.div(2 * to, plan.sequences)
        copy = remote(
            at.mine.at[to_stream], at.second.at[seq], at.t_send.at[1, step], at.t_recv.at[1, step], plan.device_of(to, rank)
        )
        copy.start()
        across.append(copy)
    at.second[seq] = at.mine[stream]
    at.token[...] = at.token_own[pl.ds(0, plan.rows_dev)]
    for copy in across:
        copy.wait_recv()
    last = []
    for step in range(1, plan.group):
        to = other(rank, step, plan.group)
        copy = remote(at.second, at.table.at[rank], at.t_send.at[2, step], at.t_recv.at[2, step], plan.device_of(seq, to))
        copy.start()
        last.append(copy)
    at.table[rank] = at.second[...]
    for copy in last:
        copy.wait_recv()

    piece = None
    for index in range(plan.group):
        grads = jnp.concatenate([at.table[index, s] for s in range(plan.sequences)], axis=0).astype(BF16)
        part = lax.dot_general(
            grads, at.weight[:, index * cols : (index + 1) * cols], CONTRACT_LAST, preferred_element_type=F32
        )
        piece = part if piece is None else piece + part
    at.piece[...] = piece
    at.everyone[seq, rank] = piece
    spread = []
    for step in range(1, plan.group):
        to = other(rank, step, plan.group)
        copy = remote(
            at.piece, at.everyone.at[seq, rank], at.c_send.at[0, step], at.c_recv.at[0, step], plan.device_of(seq, to)
        )
        copy.start()
        spread.append(copy)
    for copy in spread:
        copy.wait_recv()
    for step in range(1, plan.sequences):
        to = other(seq, step, plan.sequences)
        copy = remote(
            at.everyone.at[seq], at.everyone.at[seq], at.c_send.at[1, step], at.c_recv.at[1, step], plan.device_of(to, rank)
        )
        copy.start()
        spread.append(copy)
    for copy in spread[plan.group - 1 :]:
        copy.wait_recv()
    for copy in hops + across + last + spread:
        copy.wait_send()
    for copy in swaps:
        copy.wait()
    finish_edges(plan, seq, rank, *layer_edges)
    finish_edges(plan, seq, rank, *token_edges)


def last_rows(plan, term, weight, **operands):
    rows, share = weight.shape[0], plan.width // plan.group // 2
    cols = 6 * plan.width // plan.group
    most = max(plan.group, plan.sequences)
    dma = pltpu.SemaphoreType.DMA

    def placed(dtype):
        return jax.ShapeDtypeStruct((plan.rows_dev, plan.width), dtype)

    operands = dict(operands, weight=weight)
    outs = dict(
        layer=placed(BF16),
        layer_extra=placed(BF16),
        token=placed(F32),
        token_extra=placed(F32),
        table=jax.ShapeDtypeStruct((plan.group, plan.sequences, 1, cols), F32),
        everyone=jax.ShapeDtypeStruct((plan.sequences, plan.group, plan.sequences, rows), F32),
    )
    edges = len(plan.segments)
    scratch = dict(
        layer_own=pltpu.VMEM((plan.own, plan.width), BF16),
        token_own=pltpu.VMEM((plan.own, plan.width), F32),
        local=pltpu.VMEM((2, 6 * plan.width), F32),
        first=pltpu.VMEM((plan.group, 2, cols), F32),
        second=pltpu.VMEM((plan.sequences, 1, cols), F32),
        mine=pltpu.VMEM((2, 1, cols), F32),
        piece=pltpu.VMEM((plan.sequences, rows), F32),
        t_send=dma((3, most)),
        t_recv=dma((3, most)),
        c_send=dma((2, most)),
        c_recv=dma((2, most)),
        l_send=dma((edges,)),
        l_recv=dma((edges,)),
        e_send=dma((edges,)),
        e_recv=dma((edges,)),
    )
    if plan.chip_heads:
        operands["term"] = term.reshape(2, 2, share, plan.width)
        outs["term_out"] = jax.ShapeDtypeStruct((plan.sequences, share, plan.width), BF16)
        scratch.update(term_send=dma((2,)), term_recv=dma((2,)))
    names = tuple(operands) + tuple(outs) + tuple(scratch)
    got = call(
        functools.partial(last_kernel, plan, names),
        "last",
        10,
        tuple(outs.values()),
        list(scratch.values()) + sum_scratch(plan) + sum_scratch(plan),
        tuple(operands.values()),
        vmem=58 << 20,
    )
    got = types.SimpleNamespace(**dict(zip(outs, got)))
    got.table = got.table[:, :, 0].transpose(1, 0, 2).reshape(plan.sequences, -1)
    got.term = got.term_out if plan.chip_heads else term
    return got


def over_sequences(plan, pieces):
    full = lax.all_gather(pieces, "dev", axis=0, axis_index_groups=plan.rank_groups())
    return full.reshape((plan.devices,) + pieces.shape[1:])


def over_sequences_sum(plan, pieces):
    return lax.psum_scatter(pieces, "dev", scatter_dimension=0, axis_index_groups=plan.rank_groups())


def merge_rows(plan, weight, rank):
    if plan.chip_heads:
        return lax.all_gather(weight, "dev", axis=0, axis_index_groups=plan.rank_groups())
    share = plan.width // plan.group
    full = lax.all_gather(weight, "dev", axis=0, tiled=True)
    full = full.reshape(2, 2, plan.group // 2, share, weight.shape[1])
    full = lax.dynamic_index_in_dim(full, lax.rem(rank, 2), 1, keepdims=False)
    return lax.dynamic_index_in_dim(full, lax.div(rank, 2), 1, keepdims=False)


def merge_sum(plan, term, rank):
    if plan.chip_heads:
        return over_sequences_sum(plan, term)
    half = plan.group // 2
    _, share, cols = term.shape
    mine = [jnp.where(lax.rem(rank, 2) == k, term, jnp.zeros((), BF16)) for k in range(2)]
    full = jnp.zeros((2, 2, half, share, cols), BF16)
    full = lax.dynamic_update_slice_in_dim(full, jnp.stack(mine, axis=1)[:, :, None], lax.div(rank, 2), 2)
    return lax.psum_scatter(full.reshape(-1, cols), "dev", scatter_dimension=0, tiled=True)


def down_slices(plan, weight):
    full = lax.all_gather(weight, "dev", axis=0, axis_index_groups=plan.rank_groups())
    return full.reshape(2, -1, weight.shape[1])


def by_stream(plan, image_part, text_part, is_text):
    start, end = plan.text_start, plan.image_end
    mixed = jnp.where(is_text[start:end, None], text_part[: end - start], image_part[start:])
    return jnp.concatenate([image_part[:start], mixed, text_part[end - start :]], axis=0)


def stream_dot(plan, rows, pair, is_text):
    image_part = jnp.dot(rows[: plan.image_end], pair[0], preferred_element_type=F32)
    text_part = jnp.dot(rows[plan.text_start :], pair[1], preferred_element_type=F32)
    return by_stream(plan, image_part, text_part, is_text)


def stream_dot_back(plan, grads, pair, is_text):
    image_part = lax.dot_general(grads[: plan.image_end], pair[0], CONTRACT_LAST, preferred_element_type=F32)
    text_part = lax.dot_general(grads[plan.text_start :], pair[1], CONTRACT_LAST, preferred_element_type=F32)
    return by_stream(plan, image_part, text_part, is_text)


def pick(table, text_rows):
    return jnp.where(text_rows[:, None], table[1][None, :], table[0][None, :])


def on_device(
    tokens,
    conditioning,
    text_lengths,
    modulation_weight,
    project_weight,
    merge_weight,
    up_weight,
    down_weight,
    cotangent,
):
    rows_dev, width = tokens.shape
    mod_rows = modulation_weight.shape[0]
    plan = Plan(lax.axis_size("dev"), conditioning.shape[0], rows_dev, width)
    device = lax.axis_index("dev")
    seq, rank = plan.place_of(device)
    feature_start = device * mod_rows % width

    ends = jnp.cumsum(IMG + text_lengths)
    starts = jnp.concatenate([jnp.zeros((1,), jnp.int32), ends[:-1]])
    positions = device * rows_dev + jnp.arange(rows_dev, dtype=jnp.int32)
    row_seq = jnp.sum((starts[None, :] <= positions[:, None]).astype(jnp.int32), axis=1) - 1
    offset = plan.span * seq - plan.edge + jnp.arange(plan.rows, dtype=jnp.int32) - starts[seq]
    valid = (offset >= 0) & (offset < IMG + text_lengths[seq])
    is_text = offset >= IMG
    bias = jnp.where(valid, 0.0, MASKED).astype(F32)[None, :]
    window_text = is_text.astype(F32)[:, None]
    own_valid = own_rows(plan, valid[:, None], rank)[:, 0]
    own_text = own_rows(plan, is_text[:, None], rank)[:, 0]

    cond_float = conditioning.astype(F32)
    silu_low = jax.nn.silu(cond_float).astype(BF16)
    silu_part = lax.dynamic_slice_in_dim(silu_low, feature_start, mod_rows, 1)
    mod_part = jnp.dot(silu_part, modulation_weight, preferred_element_type=F32)

    merge_pair = merge_rows(plan, merge_weight, rank)
    project_pieces, up_pieces = swap_in(plan, project_weight, up_weight)
    project_pieces, up_pieces, merge_pair = lax.optimization_barrier((project_pieces, up_pieces, merge_pair))
    project_pair = over_sequences(plan, project_pieces)
    share = project_pair.shape[2] // 2
    project_pair = jnp.concatenate([project_pair[:, :, :share], project_pair[:, :, share:]], axis=1)
    project_pair = lax.optimization_barrier(project_pair.reshape(2, width, share))
    up_pair = over_sequences(plan, up_pieces).reshape(2, width, -1)
    down_pair = down_slices(plan, down_weight)

    token_window, grad_window, mods, merge_pair = entry(plan, tokens, cotangent, mod_part, merge_pair)
    shift_a, scale_a, gate_a, shift_b, scale_b, gate_b = jnp.split(mods, 6, axis=1)
    grad_window = jnp.where(valid[:, None], grad_window, jnp.zeros((), BF16))

    normed_full, _ = layer_norm(token_window.astype(F32))
    hidden_a = (normed_full * (1.0 + pick(scale_a, is_text)) + pick(shift_a, is_text)).astype(BF16)
    projected = stream_dot(plan, hidden_a, project_pair, is_text).astype(BF16)
    attended = attend(plan, projected, bias)

    own_tokens = own_rows(plan, token_window, rank)
    own_grad = own_rows(plan, grad_window, rank)
    text_mask = own_text.astype(F32)[:, None]
    merged, hidden_b = middle_rows(
        plan, attended, merge_pair, window_text, own_tokens, gate_a, scale_b, shift_b, text_mask
    )
    middle = own_tokens.astype(F32) + pick(gate_a, own_text) * merged
    normed_b, inv_b = layer_norm(middle)

    upper = stream_dot(plan, hidden_b, up_pair, is_text)
    activated = jax.nn.gelu(upper, approximate=True).astype(BF16)
    grad_lowered = (pick(gate_b, is_text) * grad_window.astype(F32)).astype(BF16)
    down_term = weight_terms(plan, activated, grad_lowered, window_text, "down_terms")
    down_term = down_term.reshape(plan.sequences, -1, width)
    down_term, grad_lowered = lax.optimization_barrier((down_term, grad_lowered))
    down_sum = over_sequences_sum(plan, down_term)
    grad_activated = stream_dot_back(plan, grad_lowered, down_pair, is_text)
    gelu_pull = jax.vjp(lambda value_in: jax.nn.gelu(value_in, approximate=True), upper)[1]
    grad_upper = gelu_pull(grad_activated)[0].astype(BF16)
    up_term = weight_terms(plan, hidden_b, grad_upper, window_text, "up_terms")
    up_term = up_term.reshape(plan.sequences, plan.group, mod_rows, -1)
    grad_upper, up_term = lax.optimization_barrier((grad_upper, up_term))
    up_sum = over_sequences_sum(plan, up_term)
    grad_hidden_b, grad_middle, grad_merged = back_rows(
        plan, grad_upper, up_pair, window_text, own_grad, middle, gate_a, scale_b, text_mask
    )
    merge_term = weight_terms(plan, attended, grad_merged, window_text, "merge_terms")

    grad_projected = attend_back(plan, projected, grad_merged, merge_pair, window_text, bias)
    grad_projected, down_sum = lax.optimization_barrier((grad_projected, down_sum))
    down_grad = down_sum.astype(F32)
    project_term = weight_terms(plan, hidden_a, grad_projected, window_text, "project_terms", mod_rows)
    project_term = project_term.reshape((plan.sequences, plan.group) + project_term.shape[1:])
    grad_projected, project_term = lax.optimization_barrier((grad_projected, project_term))
    project_sum = over_sequences_sum(plan, project_term)

    masks = jnp.stack([own_valid & ~own_text, own_valid & own_text], axis=1).astype(F32)
    rest = jnp.concatenate(
        [
            jnp.stack([jnp.sum(value * masks[:, j : j + 1], axis=0) for j in range(2)])
            for value in (grad_middle * merged, grad_hidden_b, grad_hidden_b * normed_b)
        ],
        axis=1,
    )
    got = last_rows(
        plan,
        merge_term,
        modulation_weight,
        activated=activated,
        down_pair=down_pair,
        grads=grad_projected,
        project_pair=project_pair,
        window_text=window_text,
        tokens=own_tokens,
        middle=middle,
        grad=own_grad,
        grad_middle=grad_middle,
        gate_b=gate_b,
        scale_a=scale_a,
        text=text_mask,
        masks=masks,
        rest=rest,
    )
    foreign = (row_seq != seq)[:, None]
    layer_out = jnp.where(foreign, got.layer_extra, got.layer)
    tokens_grad = jnp.where(foreign, got.token_extra, got.token)
    own_grads = got.table.astype(BF16)
    modulation_grad = lax.dot_general(silu_part, own_grads, CONTRACT_FIRST, preferred_element_type=F32)
    everyone = got.everyone.reshape(2, plan.devices // 2, plan.sequences, mod_rows)
    grad_silu = (everyone[0] + everyone[1]).transpose(1, 0, 2).reshape(plan.sequences, width)
    conditioning_grad = jax.vjp(jax.nn.silu, cond_float)[1](grad_silu)[0]
    modulation_grad, up_sum = lax.optimization_barrier((modulation_grad, up_sum))
    merge_out, project_sum, *done = lax.optimization_barrier(
        (got.term, project_sum, modulation_grad, down_grad, layer_out, tokens_grad, conditioning_grad)
    )
    modulation_grad, down_grad, layer_out, tokens_grad, conditioning_grad = done
    merge_grad = merge_sum(plan, merge_out, rank).reshape(merge_weight.shape).astype(F32)
    up_grad, project_grad = finish(plan, up_sum, project_sum)
    return (
        layer_out,
        tokens_grad,
        conditioning_grad,
        modulation_grad,
        project_grad,
        merge_grad,
        up_grad,
        down_grad,
    )


def solution(mesh):
    shard, whole = P("dev", None), P()
    return jax.shard_map(
        on_device,
        mesh=mesh,
        in_specs=(shard, whole, whole, shard, shard, shard, shard, shard, shard),
        out_specs=(shard, shard, whole, shard, shard, shard, shard, shard),
        check_vma=False,
    )
```

```python
import functools
import types

import jax
import jax.numpy as jnp
import numpy as np
from jax import lax
from jax.experimental import pallas as pl
from jax.experimental.pallas import tpu as pltpu
from jax.sharding import PartitionSpec as P

HEADS = 24
HDIM = 64
IMG = 1024
TXT_MIN = 86
TXT_MAX = 154
EPSILON = 1e-06
F32 = jnp.float32
BF16 = jnp.bfloat16
CONTRACT_LAST = (((1,), (1,)), ((), ()))
PLAIN = (((1,), (0,)), ((), ()))
CONTRACT_FIRST = (((0,), (0,)), ((), ()))
MASKED = -1e30


class Plan:
    def __init__(self, devices, sequences, rows_dev, width):
        self.devices, self.sequences, self.rows_dev, self.width = devices, sequences, rows_dev, width
        self.group = devices // sequences
        self.span = self.group * rows_dev
        mean = self.span - IMG
        up, down = TXT_MAX - mean, mean - TXT_MIN
        drift = 0
        for k in range(sequences + 1):
            drift = max(drift, min(up * k, down * (sequences - k)), min(down * k, up * (sequences - k)))
        self.edge = -(-drift // 64) * 64
        self.rows = self.span + 2 * self.edge
        self.piece = 2 * self.edge // self.group
        self.own = rows_dev + self.piece
        self.image_end = -(-(self.edge + drift + IMG) // 128) * 128
        self.text_start = (self.edge - drift + IMG) // 128 * 128
        self.heads = HEADS // self.group
        self.segments = self.edge_segments()
        self.chip_heads = devices == 4 * self.group

    def device_of(self, seq, rank):
        return seq * self.group + rank

    def place_of(self, device):
        return lax.div(device, self.group), lax.rem(device, self.group)

    def seq_groups(self):
        return [[self.device_of(s, r) for r in range(self.group)] for s in range(self.sequences)]

    def rank_groups(self):
        return [[self.device_of(s, r) for s in range(self.sequences)] for r in range(self.group)]

    def edge_row(self, rank):
        half = self.group // 2
        return jnp.where(rank < half, self.piece * rank, self.edge + self.span + self.piece * (rank - half))

    def main_row(self, rank):
        return self.edge + self.rows_dev * rank

    def edge_segments(self):
        found = []
        for rank in range(self.group):
            half = self.group // 2
            first = self.piece * rank - self.edge if rank < half else self.span + self.piece * (rank - half)
            row = 0
            while row < self.piece:
                owner, owner_row = (first + row) // self.rows_dev, (first + row) % self.rows_dev
                count = min(self.piece - row, self.rows_dev - owner_row)
                found.append((rank, row, count, owner // self.group, owner % self.group, owner_row))
                row += count
        return found


def layer_norm(values):
    mean = jnp.mean(values, axis=-1, keepdims=True)
    centred = values - mean
    variance = jnp.mean(centred * centred, axis=-1, keepdims=True)
    inv_std = lax.rsqrt(variance + EPSILON)
    return (centred * inv_std, inv_std)


def norm_back(grad_normed, normed, inv_std):
    mean_grad = jnp.mean(grad_normed, axis=-1, keepdims=True)
    mean_cross = jnp.mean(grad_normed * normed, axis=-1, keepdims=True)
    return inv_std * (grad_normed - mean_grad - normed * mean_cross)


def softmax_parts(query, key, bias):
    scores = lax.dot_general(query, key, CONTRACT_LAST, preferred_element_type=F32) + bias
    top = jnp.max(scores, axis=1, keepdims=True)
    exponent = jnp.exp(scores - top)
    total = jnp.sum(exponent, axis=1, keepdims=True)
    return exponent * (1.0 / total)


def head_columns(heads, part, head):
    first = (part * heads + head) * HDIM
    return slice(first, first + HDIM)


def attend_kernel(heads, block, projected, bias_ref, out_ref):
    rows = pl.ds(pl.multiple_of(pl.program_id(0) * block, block), block)
    bias = bias_ref[...]
    outs = []
    for head in range(heads):
        query = projected[rows, head_columns(heads, 0, head)] * jnp.asarray(HDIM ** (-0.5), BF16)
        probs = softmax_parts(query, projected[:, head_columns(heads, 1, head)], bias).astype(BF16)
        outs.append(jnp.dot(probs, projected[:, head_columns(heads, 2, head)], preferred_element_type=F32))
    out_ref[...] = jnp.concatenate(outs, axis=1).astype(BF16)


def block_rows(rows):
    return 256 if rows % 256 == 0 else 128


def constant(shape):
    return pl.BlockSpec(shape, lambda i: (0,) * len(shape))


def attend(plan, projected, bias):
    rows, cols = projected.shape[0], projected.shape[1] // 3
    block = block_rows(rows)
    return pl.pallas_call(
        functools.partial(attend_kernel, plan.heads, block),
        out_shape=jax.ShapeDtypeStruct((rows, cols), BF16),
        grid=(rows // block,),
        in_specs=[constant(projected.shape), constant(bias.shape)],
        out_specs=pl.BlockSpec((block, cols), lambda i: (i, 0)),
        compiler_params=pltpu.CompilerParams(vmem_limit_bytes=48 << 20),
        cost_estimate=pl.CostEstimate(flops=16 * rows * rows * cols, bytes_accessed=8 * rows * cols, transcendentals=0),
        name="attend",
    )(projected, bias)


def attend_back_kernel(
    heads, steps, block, projected, grad_merged, merge_pair, text, bias_ref, out, key_sum, value_sum
):
    step = pl.program_id(0)
    scale = jnp.asarray(HDIM ** (-0.5), BF16)

    @pl.when(step == 0)
    def _():
        key_sum[...] = jnp.zeros_like(key_sum)
        value_sum[...] = jnp.zeros_like(value_sum)

    rows = pl.ds(pl.multiple_of(step * block, block), block)
    bias = bias_ref[...]
    image, other_stream = [
        lax.dot_general(grad_merged[...], merge_pair[j], CONTRACT_LAST, preferred_element_type=F32) for j in range(2)
    ]
    grad_attended = jnp.where(text[...] > 0, other_stream, image).astype(BF16)
    grads = []
    for head in range(heads):
        query = projected[rows, head_columns(heads, 0, head)] * scale
        key = projected[:, head_columns(heads, 1, head)]
        grad_out = grad_attended[:, head * HDIM : (head + 1) * HDIM]
        probs = softmax_parts(query, key, bias)
        grad_probs = lax.dot_general(
            grad_out, projected[:, head_columns(heads, 2, head)], CONTRACT_LAST, preferred_element_type=F32
        )
        inner = jnp.sum(probs * grad_probs, axis=1, keepdims=True)
        grad_scores = (probs * (grad_probs - inner)).astype(BF16)
        grads.append(jnp.dot(grad_scores, key, preferred_element_type=F32) * HDIM ** (-0.5))
        key_sum[head] += lax.dot_general(query, grad_scores, CONTRACT_FIRST, preferred_element_type=F32)
        value_sum[head] += lax.dot_general(grad_out, probs.astype(BF16), CONTRACT_FIRST, preferred_element_type=F32)
    cols = heads * HDIM
    out[rows, :cols] = jnp.concatenate(grads, axis=1).astype(BF16)

    @pl.when(step == steps - 1)
    def _():
        total = out.shape[0]
        out[:, cols : 2 * cols] = key_sum[...].reshape(cols, total).T.astype(BF16)
        out[:, 2 * cols :] = value_sum[...].reshape(cols, total).T.astype(BF16)


def attend_back(plan, projected, grad_merged, merge_pair, text, bias):
    rows, cols = projected.shape[0], projected.shape[1] // 3
    block = block_rows(rows)
    return pl.pallas_call(
        functools.partial(attend_back_kernel, plan.heads, rows // block, block),
        out_shape=jax.ShapeDtypeStruct(projected.shape, BF16),
        grid=(rows // block,),
        in_specs=[
            constant(projected.shape),
            pl.BlockSpec((block, plan.width), lambda i: (i, 0)),
            constant(merge_pair.shape),
            pl.BlockSpec((block, 1), lambda i: (i, 0)),
            constant(bias.shape),
        ],
        out_specs=constant(projected.shape),
        scratch_shapes=[pltpu.VMEM((plan.heads, HDIM, rows), F32)] * 2,
        compiler_params=pltpu.CompilerParams(vmem_limit_bytes=56 << 20),
        cost_estimate=pl.CostEstimate(flops=40 * rows * rows * cols, bytes_accessed=14 * rows * cols, transcendentals=0),
        name="attend_back",
    )(projected, grad_merged, merge_pair, text, bias)


def fold_rows(piece):
    half = piece.shape[0] // 2
    return jnp.concatenate([piece[:half], piece[half:]], axis=1)


def unfold_rows(piece):
    half = piece.shape[1] // 2
    return jnp.concatenate([piece[:, :half], piece[:, half:]], axis=0)


def terms_kernel(plan, fold, chunk, rows, grads, text, out, kept):
    width = rows.shape[1]
    for stream, (first, last) in enumerate(((0, plan.image_end), (plan.text_start, plan.rows))):
        count = last - first
        mask = text[pl.ds(first, count)]
        keep = (mask > 0) if stream else (mask <= 0)
        kept[pl.ds(0, count)] = jnp.where(keep, grads[pl.ds(first, count)], jnp.zeros((), BF16))

        def step(i, carry):
            start = pl.multiple_of(i * chunk, chunk)
            term = lax.dot_general(
                rows[pl.ds(first, count), pl.ds(start, chunk)],
                kept[pl.ds(0, count)],
                CONTRACT_FIRST,
                preferred_element_type=F32,
            ).astype(BF16)
            if fold:
                for j in range(chunk // fold):
                    out[(stream * width) // fold + i * (chunk // fold) + j] = fold_rows(term[j * fold : (j + 1) * fold])
            else:
                out[stream, pl.ds(start, chunk)] = term
            return carry

        if width == chunk:
            step(0, 0)
        else:
            lax.fori_loop(0, width // chunk, step, 0)


def weight_terms(plan, rows, grads, text, name, fold=0):
    width, cols = rows.shape[1], grads.shape[1]
    chunk = 384 if width % 384 == 0 else width
    shape = (2 * width // fold, fold // 2, 2 * cols) if fold else (2, width, cols)
    return pl.pallas_call(
        functools.partial(terms_kernel, plan, fold, chunk),
        out_shape=jax.ShapeDtypeStruct(shape, BF16),
        in_specs=[pl.BlockSpec(memory_space=pltpu.VMEM)] * 3,
        out_specs=pl.BlockSpec(memory_space=pltpu.VMEM),
        scratch_shapes=[pltpu.VMEM((plan.image_end, cols), BF16)],
        compiler_params=pltpu.CompilerParams(vmem_limit_bytes=40 << 20),
        cost_estimate=pl.CostEstimate(flops=3 * plan.rows * width * cols, bytes_accessed=1 << 23, transcendentals=0),
        name=name,
    )(rows, grads, text)


VMEM = pl.BlockSpec(memory_space=pltpu.VMEM)


def own_rows(plan, window, rank):
    main = lax.dynamic_slice_in_dim(window, plan.main_row(rank), plan.rows_dev, 0)
    edge = lax.dynamic_slice_in_dim(window, plan.edge_row(rank), plan.piece, 0)
    return jnp.concatenate([main, edge], axis=0)


def remote(source, target, send_sem, recv_sem, device):
    return pltpu.make_async_remote_copy(
        src_ref=source,
        dst_ref=target,
        send_sem=send_sem,
        recv_sem=recv_sem,
        device_id=(device,),
        device_id_type=pl.DeviceIdType.MESH,
    )


def here(plan):
    return plan.place_of(lax.axis_index("dev"))


def other(rank, step, size):
    return lax.rem(rank + step, size)


def meet(devices):
    barrier = pltpu.get_barrier_semaphore()
    for device in devices:
        pl.semaphore_signal(barrier, inc=1, device_id=(device,), device_id_type=pl.DeviceIdType.MESH)
    pl.semaphore_wait(barrier, len(devices))


def group_devices(plan, seq, rank):
    return [plan.device_of(seq, other(rank, step, plan.group)) for step in range(1, plan.group)]


def column_devices(plan, seq, rank):
    return [plan.device_of(other(seq, step, plan.sequences), rank) for step in range(1, plan.sequences)]


def every_device(plan, device):
    return [other(device, step, plan.devices) for step in range(1, plan.devices)]


def call(kernel, name, ident, out_shape, scratch, operands, in_specs=None, out_specs=None, vmem=40 << 20):
    outs = out_shape if isinstance(out_shape, tuple) else (out_shape,)
    return pl.pallas_call(
        kernel,
        out_shape=out_shape,
        in_specs=in_specs or [VMEM] * len(operands),
        out_specs=out_specs or (tuple([VMEM] * len(outs)) if isinstance(out_shape, tuple) else VMEM),
        scratch_shapes=scratch,
        compiler_params=pltpu.CompilerParams(
            collective_id=ident, has_side_effects=True, vmem_limit_bytes=vmem
        ),
        name=name,
    )(*operands)


def aligned(start):
    return pl.multiple_of(start, 16)


def block_parts(plan, ref, rank):
    return (
        ref.at[pl.ds(aligned(plan.main_row(rank)), plan.rows_dev)],
        ref.at[pl.ds(aligned(plan.edge_row(rank)), plan.piece)],
    )


def own_parts(plan, ref):
    return ref.at[pl.ds(0, plan.rows_dev)], ref.at[pl.ds(plan.rows_dev, plan.piece)]


def load_block(plan, ref, rank):
    main, edge = block_parts(plan, ref, rank)
    return jnp.concatenate([main[...], edge[...]], axis=0)


def sum_scratch(plan, wire=BF16):
    half, own, width = plan.group // 2, plan.own, plan.width
    return [
        pltpu.VMEM((half, own, width), F32),
        pltpu.VMEM((half, own, width), F32),
        pltpu.VMEM((own, width), F32),
        pltpu.VMEM((half - 1, own, width), wire),
        pltpu.VMEM((half - 1, own, width), wire),
        pltpu.SemaphoreType.DMA((half,)),
        pltpu.SemaphoreType.DMA((half,)),
        pltpu.SemaphoreType.DMA((half,)),
        pltpu.SemaphoreType.DMA((half,)),
    ]


SUM_SCRATCH = 9


def product(plan, rows, pair, text, dims, rank, out):
    block = load_block(plan, rows, rank)
    text_row = load_block(plan, text, rank) > 0
    chunk = plan.width // 4

    def step(i, carry):
        cols = pl.ds(pl.multiple_of(i * chunk, chunk), chunk)
        parts = []
        for stream in range(2):
            weight = pair[stream, cols, :] if dims is CONTRACT_LAST else pair[stream, :, cols]
            parts.append(lax.dot_general(block, weight, dims, preferred_element_type=F32))
        out[:, cols] = jnp.where(text_row, parts[1], parts[0])
        return carry

    lax.fori_loop(0, 4, step, 0)


def scatter_sum(*args):
    return scatter_start(*args)()


def scatter_start(plan, seq, rank, rows, pair, text, dims, away, near, mine, going, coming,
                  pair_send, pair_recv, far_send, far_recv):
    half = plan.group // 2
    chip, core = lax.div(rank, 2), lax.rem(rank, 2)
    partner = plan.device_of(seq, 2 * chip + 1 - core)
    order = list(range(1, half)) + [0]

    def pair_copy(step):
        return remote(away.at[step], near.at[step], pair_send.at[step], pair_recv.at[step], partner)

    def far_copy(step):
        to = plan.device_of(seq, 2 * other(chip, step, half) + core)
        return remote(going.at[step - 1], coming.at[step - 1], far_send.at[step], far_recv.at[step], to)

    def for_owner(step):
        product(plan, rows, pair, text, dims, 2 * other(chip, step, half) + core, mine)
        pair_copy(step).wait_recv()
        mine[...] += near[step]

    def turn(i, carry):
        step = other(i, 1, half)
        product(plan, rows, pair, text, dims, 2 * other(chip, step, half) + 1 - core, away.at[step])
        pair_copy(step).start()

        @pl.when(i > 0)
        def _():
            for_owner(i)
            going[i - 1] = mine[...].astype(going.dtype)
            far_copy(i).start()

        return carry

    lax.fori_loop(0, half, turn, 0)

    def result():
        for_owner(0)
        total = mine[...]
        for step in range(1, half):
            far_copy(step).wait_recv()
            total = total + coming[step - 1].astype(F32)
        for step in range(half):
            pair_copy(step).wait_send()
        for step in range(1, half):
            far_copy(step).wait_send()
        return total

    return result


def share_scratch(plan):
    return [pltpu.SemaphoreType.DMA((plan.group, 2))] * 2 + [pltpu.SemaphoreType.DMA((plan.group, 2))]


def share_rows(plan, seq, rank, parts, window, send, recv, pass_send):
    half = plan.group // 2
    chip, core = lax.div(rank, 2), lax.rem(rank, 2)
    partner_rank = 2 * chip + 1 - core
    partner = plan.device_of(seq, partner_rank)

    def send_own(to_device, slot):
        copies = [
            remote(source, target, send.at[slot, i], recv.at[slot, i], to_device)
            for i, (source, target) in enumerate(zip(parts, block_parts(plan, window, rank)))
        ]
        for copy in copies:
            copy.start()
        return copies

    flying = {}
    for step in range(1, half):
        flying[step] = send_own(plan.device_of(seq, 2 * other(chip, step, half) + core), step)
    flying[0] = send_own(partner, 0)
    for source, target in zip(parts, block_parts(plan, window, rank)):
        target[...] = source[...]
    passed = []
    for step in range(1, half):
        for copy in flying[step]:
            copy.wait_recv()
        came = 2 * other(chip, half - step, half) + core
        copies = [
            remote(place, place, pass_send.at[step, i], recv.at[half + step, i], partner)
            for i, place in enumerate(block_parts(plan, window, came))
        ]
        for copy in copies:
            copy.start()
        passed.extend(copies)
    for copy in flying[0]:
        copy.wait_recv()
    for copy in passed:
        copy.wait_recv()
    for copies in flying.values():
        for copy in copies:
            copy.wait_send()
    for copy in passed:
        copy.wait_send()


def entry_kernel(plan, tokens, grads, mod_part, *refs):
    if plan.chip_heads:
        merge, merge_out, *refs = refs[:1] + refs[4:5] + refs[1:4] + refs[5:]
        merge_send, merge_recv, *refs = refs[-2:] + refs[:-2]
    (token_window, grad_window, mods, token_own, grad_own, plane, across, chunk, edge_send, edge_recv,
     t_send, t_recv, t_pass, g_send, g_recv, g_pass, m_send, m_recv) = refs
    device = lax.axis_index("dev")
    seq, rank = plan.place_of(device)
    meet(every_device(plan, device))
    swaps = []
    if plan.chip_heads:
        core = lax.rem(rank, 2)
        partner = plan.device_of(seq, 2 * lax.div(rank, 2) + 1 - core)
        for stream in range(2):
            copy = remote(
                merge.at[2 * stream + 1 - core],
                merge_out.at[stream, core],
                merge_send.at[stream],
                merge_recv.at[stream],
                partner,
            )
            copy.start()
            swaps.append(copy)
            merge_out[stream, core] = merge[2 * stream + core]
    hops = []
    for step in range(1, plan.group):
        to = other(rank, step, plan.group)
        copy = remote(mod_part.at[to], plane.at[step], m_send.at[0, step], m_recv.at[0, step], plan.device_of(seq, to))
        copy.start()
        hops.append(copy)
    arrays = ((tokens, token_own), (grads, grad_own))
    count = len(plan.segments)
    for which, (source, own) in enumerate(arrays):
        for index, (to_rank, row, rows, step, owner, owner_row) in enumerate(plan.segments):
            @pl.when(rank == owner)
            def _():
                remote(
                    source.at[pl.ds(owner_row, rows)],
                    own.at[pl.ds(row, rows)],
                    edge_send.at[which * count + index],
                    edge_recv.at[which * count + index],
                    plan.device_of(lax.rem(seq + plan.sequences - step, plan.sequences), to_rank),
                ).start()
    for copy in hops:
        copy.wait_recv()
    total = mod_part[rank]
    for step in range(1, plan.group):
        total = total + plane[step]
    plane[0] = total
    hops_across = []
    for step in range(1, plan.sequences):
        to = other(seq, step, plan.sequences)
        copy = remote(plane.at[0, to], across.at[seq], m_send.at[1, step], m_recv.at[1, step], plan.device_of(to, rank))
        copy.start()
        hops_across.append(copy)
    across[seq] = plane[0, seq]
    for which, (source, own) in enumerate(arrays):
        for index, (to_rank, row, rows, step, owner, owner_row) in enumerate(plan.segments):
            @pl.when(rank == to_rank)
            def _():
                remote(
                    source.at[pl.ds(owner_row, rows)],
                    own.at[pl.ds(row, rows)],
                    edge_send.at[which * count + index],
                    edge_recv.at[which * count + index],
                    plan.device_of(lax.rem(seq + plan.sequences + step, plan.sequences), owner),
                ).wait_recv()
    share_rows(plan, seq, rank, (tokens, token_own), token_window, t_send, t_recv, t_pass)
    for copy in hops_across:
        copy.wait_recv()
    half = plan.sequences // 2
    for stream in range(2):
        total = across[stream * half]
        for i in range(1, half):
            total = total + across[stream * half + i]
        chunk[stream] = total
    hops_back = []
    for step in range(1, plan.group):
        to = other(rank, step, plan.group)
        copy = remote(chunk, mods.at[rank], m_send.at[2, step], m_recv.at[2, step], plan.device_of(seq, to))
        copy.start()
        hops_back.append(copy)
    mods[rank] = chunk[...]
    share_rows(plan, seq, rank, (grads, grad_own), grad_window, g_send, g_recv, g_pass)
    for copy in hops_back:
        copy.wait_recv()
    for copy in hops + hops_across + hops_back:
        copy.wait_send()
    for copy in swaps:
        copy.wait()
    for which, (source, own) in enumerate(arrays):
        for index, (to_rank, row, rows, step, owner, owner_row) in enumerate(plan.segments):
            @pl.when(rank == owner)
            def _():
                remote(
                    source.at[pl.ds(owner_row, rows)],
                    own.at[pl.ds(row, rows)],
                    edge_send.at[which * count + index],
                    edge_recv.at[which * count + index],
                    plan.device_of(lax.rem(seq + plan.sequences - step, plan.sequences), to_rank),
                ).wait_send()


def entry(plan, tokens, grads, mod_part, merge):
    lanes = mod_part.shape[1] // plan.group // 128
    pieces = mod_part.reshape(plan.sequences, plan.group, lanes, 128).transpose(1, 0, 2, 3)
    window = jax.ShapeDtypeStruct((plan.rows, plan.width), BF16)
    dma = pltpu.SemaphoreType.DMA
    most = max(plan.group, plan.sequences)
    shapes = (window, window, jax.ShapeDtypeStruct((plan.group, 2, lanes, 128), F32))
    operands = (tokens, grads, pieces)
    scratch = (
        [
            pltpu.VMEM((plan.piece, plan.width), BF16),
            pltpu.VMEM((plan.piece, plan.width), BF16),
            pltpu.VMEM((plan.group, plan.sequences, lanes, 128), F32),
            pltpu.VMEM((plan.sequences, lanes, 128), F32),
            pltpu.VMEM((2, lanes, 128), F32),
            dma((2 * len(plan.segments),)),
            dma((2 * len(plan.segments),)),
        ]
        + share_scratch(plan)
        + share_scratch(plan)
        + [dma((3, most)), dma((3, most))]
    )
    if plan.chip_heads:
        shapes += (jax.ShapeDtypeStruct((2, 2) + merge.shape[1:], BF16),)
        operands += (merge,)
        scratch += [dma((2,)), dma((2,))]
    token_window, grad_window, mods, *rest = call(
        functools.partial(entry_kernel, plan), "entry", 1, shapes, scratch, operands
    )
    merge_pair = rest[0].reshape(2, -1, plan.width) if plan.chip_heads else merge
    return token_window, grad_window, mods.transpose(1, 0, 2, 3).reshape(2, -1), merge_pair


def project_columns(plan, rank):
    share = plan.width // plan.group
    first = (rank % 2) * (plan.width // 2) + (rank // 2) * share
    return [part * plan.width + first for part in range(3)], share


def up_columns(plan, rank, cols):
    planes = plan.sequences // 2
    share = cols // planes // plan.group
    return [plane * plan.group * share + rank * share for plane in range(planes)], share


def start_swap(plan, seq, rank, source, target, send, recv):
    copies = []
    for step in range(1, plan.group):
        to = other(rank, step, plan.group)
        copy = remote(source.at[to], target.at[rank], send.at[step], recv.at[step], plan.device_of(seq, to))
        copy.start()
        copies.append(copy)
    target[rank] = source[rank]
    return copies


def swap_in_kernel(plan, project, up, project_out, up_out, project_cut, up_cut, p_send, p_recv, u_send, u_recv):
    seq, rank = here(plan)
    for to in range(plan.group):
        starts, share = project_columns(plan, to)
        project_cut[to] = fold_rows(jnp.concatenate([project[:, c : c + share] for c in starts], axis=1))
    meet(group_devices(plan, seq, rank))
    copies = start_swap(plan, seq, rank, project_cut, project_out, p_send, p_recv)
    for to in range(plan.group):
        starts, share = up_columns(plan, to, up.shape[1])
        up_cut[to] = jnp.concatenate([up[:, c : c + share] for c in starts], axis=1)
    copies += start_swap(plan, seq, rank, up_cut, up_out, u_send, u_recv)
    for copy in copies:
        copy.wait()


def swap_in(plan, project, up):
    rows = project.shape[0]
    dma = pltpu.SemaphoreType.DMA
    shapes = [
        (plan.group, rows // 2, 2 * project.shape[1] // plan.group),
        (plan.group, rows, up.shape[1] // plan.group),
    ]
    return call(
        functools.partial(swap_in_kernel, plan),
        "swap_in",
        4,
        tuple(jax.ShapeDtypeStruct(shape, BF16) for shape in shapes),
        [pltpu.VMEM(shape, BF16) for shape in shapes] + [dma((plan.group,))] * 4,
        (project, up),
    )


def place_columns(plan, got, out, columns, unfold):
    for source in range(plan.group):
        starts, share = columns(plan, source)
        piece = unfold_rows(got[source]) if unfold else got[source]
        for i, c in enumerate(starts):
            out[:, c : c + share] = piece[:, i * share : (i + 1) * share]


def finish_kernel(plan, up, project, up_out, project_out, up_got, project_got, u_send, u_recv, p_send, p_recv):
    seq, rank = here(plan)
    meet(group_devices(plan, seq, rank))
    ups = start_swap(plan, seq, rank, up, up_got, u_send, u_recv)
    projects = start_swap(plan, seq, rank, project, project_got, p_send, p_recv)
    for copy in ups:
        copy.wait()
    place_columns(plan, up_got, up_out, lambda p, r: up_columns(p, r, up_out.shape[1]), False)
    for copy in projects:
        copy.wait()
    place_columns(plan, project_got, project_out, project_columns, True)


def finish(plan, up, project):
    dma = pltpu.SemaphoreType.DMA
    rows = up.shape[1]
    up_grad, project_grad = call(
        functools.partial(finish_kernel, plan),
        "finish",
        6,
        (
            jax.ShapeDtypeStruct((rows, plan.group * up.shape[2]), BF16),
            jax.ShapeDtypeStruct((rows, plan.group * project.shape[2] // 2), BF16),
        ),
        [pltpu.VMEM(up.shape, BF16), pltpu.VMEM(project.shape, BF16)] + [dma((plan.group,))] * 4,
        (up, project),
    )
    return up_grad.astype(F32), project_grad.astype(F32)


def pick_rows(table, text):
    return jnp.where(text > 0, table[1:2, :], table[0:1, :])


def norm_rows(values):
    mean = jnp.mean(values, axis=1, keepdims=True)
    centred = values - mean
    inv = lax.rsqrt(jnp.mean(centred * centred, axis=1, keepdims=True) + EPSILON)
    return centred * inv, inv


def middle_kernel(plan, rows, pair, window_text, tokens, gate_a, scale_b, shift_b, text, merged, window, own, *scratch):
    seq, rank = here(plan)
    meet(group_devices(plan, seq, rank))
    total = scatter_sum(plan, seq, rank, rows, pair, window_text, PLAIN, *scratch[:SUM_SCRATCH])
    merged[...] = total
    mask = text[...]
    middle = tokens[...].astype(F32) + pick_rows(gate_a[...], mask) * total
    normed, _ = norm_rows(middle)
    own[...] = (normed * (1.0 + pick_rows(scale_b[...], mask)) + pick_rows(shift_b[...], mask)).astype(BF16)
    share_rows(plan, seq, rank, own_parts(plan, own), window, *scratch[SUM_SCRATCH:])


def own_shape(plan, dtype=F32):
    return jax.ShapeDtypeStruct((plan.own, plan.width), dtype)


def window_shape(plan):
    return jax.ShapeDtypeStruct((plan.rows, plan.width), BF16)


def middle_rows(plan, rows, pair, window_text, tokens, gate_a, scale_b, shift_b, text):
    return call(
        functools.partial(middle_kernel, plan),
        "middle",
        2,
        (own_shape(plan), window_shape(plan)),
        [pltpu.VMEM((plan.own, plan.width), BF16)] + sum_scratch(plan, F32) + share_scratch(plan),
        (rows, pair, window_text, tokens, gate_a, scale_b, shift_b, text),
    )


def back_kernel(plan, rows, pair, window_text, grad, middle, gate_a, scale_b, text, grad_hidden, grad_middle, window, own, *scratch):
    seq, rank = here(plan)
    meet(group_devices(plan, seq, rank))
    total = scatter_sum(plan, seq, rank, rows, pair, window_text, CONTRACT_LAST, *scratch[:SUM_SCRATCH])
    grad_hidden[...] = total
    mask = text[...]
    normed, inv = norm_rows(middle[...])
    inner = total * (1.0 + pick_rows(scale_b[...], mask))
    mean_grad = jnp.mean(inner, axis=1, keepdims=True)
    mean_cross = jnp.mean(inner * normed, axis=1, keepdims=True)
    result = grad[...].astype(F32) + inv * (inner - mean_grad - normed * mean_cross)
    grad_middle[...] = result
    own[...] = (pick_rows(gate_a[...], mask) * result).astype(BF16)
    share_rows(plan, seq, rank, own_parts(plan, own), window, *scratch[SUM_SCRATCH:])


def back_rows(plan, rows, pair, window_text, grad, middle, gate_a, scale_b, text):
    return call(
        functools.partial(back_kernel, plan),
        "back",
        3,
        (own_shape(plan), own_shape(plan), window_shape(plan)),
        [pltpu.VMEM((plan.own, plan.width), BF16)] + sum_scratch(plan) + share_scratch(plan),
        (rows, pair, window_text, grad, middle, gate_a, scale_b, text),
    )


def edge_copy(plan, seq, source, first_row, target, send, recv, index):
    from_rank, row, rows, step, owner, owner_row = plan.segments[index]
    return remote(
        source.at[pl.ds(first_row + row, rows)],
        target.at[pl.ds(owner_row, rows)],
        send.at[index],
        recv.at[index],
        plan.device_of(lax.rem(seq + plan.sequences + step, plan.sequences), owner),
    )


def start_edges(plan, seq, rank, *refs):
    for index, segment in enumerate(plan.segments):
        @pl.when(rank == segment[0])
        def _():
            edge_copy(plan, seq, *refs, index).start()


def finish_edges(plan, seq, rank, *refs):
    for index, segment in enumerate(plan.segments):
        @pl.when(rank == segment[4])
        def _():
            edge_copy(plan, seq, *refs, index).wait_recv()

        @pl.when(rank == segment[0])
        def _():
            edge_copy(plan, seq, *refs, index).wait_send()


def edge_scratch(plan):
    return [pltpu.SemaphoreType.DMA((len(plan.segments),))] * 2


def stream_sums(values, masks):
    return jnp.concatenate([jnp.sum(values * mask, axis=0, keepdims=True) for mask in masks], axis=0)


def last_kernel(plan, names, *refs):
    at = types.SimpleNamespace(**dict(zip(names, refs)))
    low_scratch = refs[len(names) : len(names) + SUM_SCRATCH]
    back_scratch = refs[len(names) + SUM_SCRATCH : len(names) + 2 * SUM_SCRATCH]
    device = lax.axis_index("dev")
    seq, rank = plan.place_of(device)
    stream = lax.div(2 * seq, plan.sequences)
    at.layer_extra[...] = jnp.zeros_like(at.layer_extra)
    at.token_extra[...] = jnp.zeros_like(at.token_extra)
    meet(every_device(plan, device))
    low_sum = scatter_start(plan, seq, rank, at.activated, at.down_pair, at.window_text, PLAIN, *low_scratch)
    back_sum = scatter_start(plan, seq, rank, at.grads, at.project_pair, at.window_text, CONTRACT_LAST, *back_scratch)
    swaps = []
    if plan.chip_heads:
        core = lax.rem(rank, 2)
        partner = plan.device_of(seq, 2 * lax.div(rank, 2) + 1 - core)
        for j in range(2):
            copy = remote(
                at.term.at[j, 1 - core], at.term_out.at[2 * j + core], at.term_send.at[j], at.term_recv.at[j], partner
            )
            copy.start()
            swaps.append(copy)
            at.term_out[2 * j + core] = at.term[j, core]
    text = at.text[...]
    streams = (at.masks[:, 0:1], at.masks[:, 1:2])
    width = plan.width

    lowered = low_sum()
    at.layer_own[...] = (at.middle[...] + pick_rows(at.gate_b[...], text) * lowered).astype(BF16)
    layer_edges = (at.layer_own, plan.rows_dev, at.layer_extra, at.l_send, at.l_recv)
    start_edges(plan, seq, rank, *layer_edges)
    at.local[:, 5 * width :] = stream_sums(at.grad[...].astype(F32) * lowered, streams)
    at.local[:, 2 * width : 5 * width] = at.rest[...]
    at.layer[...] = at.layer_own[pl.ds(0, plan.rows_dev)]

    total = back_sum()
    normed, inv = norm_rows(at.tokens[...].astype(F32))
    at.local[:, :width] = stream_sums(total, streams)
    at.local[:, width : 2 * width] = stream_sums(total * normed, streams)
    cols = 6 * width // plan.group

    def chunk(index):
        return pl.ds(pl.multiple_of(index * cols, 128), cols)

    hops = []
    for step in range(1, plan.group):
        to = other(rank, step, plan.group)
        copy = remote(
            at.local.at[:, chunk(to)], at.first.at[step], at.t_send.at[0, step], at.t_recv.at[0, step], plan.device_of(seq, to)
        )
        copy.start()
        hops.append(copy)
    inner = total * (1.0 + pick_rows(at.scale_a[...], text))
    mean_grad = jnp.mean(inner, axis=1, keepdims=True)
    mean_cross = jnp.mean(inner * normed, axis=1, keepdims=True)
    at.token_own[...] = at.grad_middle[...] + inv * (inner - mean_grad - normed * mean_cross)
    token_edges = (at.token_own, plan.rows_dev, at.token_extra, at.e_send, at.e_recv)
    start_edges(plan, seq, rank, *token_edges)
    for copy in hops:
        copy.wait_recv()
    sums = at.local[:, chunk(rank)]
    for step in range(1, plan.group):
        sums = sums + at.first[step]
    for i in range(2):
        at.mine[i] = sums[i : i + 1]
    across = []
    for step in range(1, plan.sequences):
        to = other(seq, step, plan.sequences)
        to_stream = lax.div(2 * to, plan.sequences)
        copy = remote(
            at.mine.at[to_stream], at.second.at[seq], at.t_send.at[1, step], at.t_recv.at[1, step], plan.device_of(to, rank)
        )
        copy.start()
        across.append(copy)
    at.second[seq] = at.mine[stream]
    at.token[...] = at.token_own[pl.ds(0, plan.rows_dev)]
    for copy in across:
        copy.wait_recv()
    last = []
    for step in range(1, plan.group):
        to = other(rank, step, plan.group)
        copy = remote(at.second, at.table.at[rank], at.t_send.at[2, step], at.t_recv.at[2, step], plan.device_of(seq, to))
        copy.start()
        last.append(copy)
    at.table[rank] = at.second[...]
    for copy in last:
        copy.wait_recv()

    piece = None
    for index in range(plan.group):
        grads = jnp.concatenate([at.table[index, s] for s in range(plan.sequences)], axis=0).astype(BF16)
        part = lax.dot_general(
            grads, at.weight[:, index * cols : (index + 1) * cols], CONTRACT_LAST, preferred_element_type=F32
        )
        piece = part if piece is None else piece + part
    at.piece[...] = piece
    at.everyone[seq, rank] = piece
    spread = []
    for step in range(1, plan.group):
        to = other(rank, step, plan.group)
        copy = remote(
            at.piece, at.everyone.at[seq, rank], at.c_send.at[0, step], at.c_recv.at[0, step], plan.device_of(seq, to)
        )
        copy.start()
        spread.append(copy)
    for copy in spread:
        copy.wait_recv()
    for step in range(1, plan.sequences):
        to = other(seq, step, plan.sequences)
        copy = remote(
            at.everyone.at[seq], at.everyone.at[seq], at.c_send.at[1, step], at.c_recv.at[1, step], plan.device_of(to, rank)
        )
        copy.start()
        spread.append(copy)
    for copy in spread[plan.group - 1 :]:
        copy.wait_recv()
    for copy in hops + across + last + spread:
        copy.wait_send()
    for copy in swaps:
        copy.wait()
    finish_edges(plan, seq, rank, *layer_edges)
    finish_edges(plan, seq, rank, *token_edges)


def last_rows(plan, term, weight, **operands):
    rows, share = weight.shape[0], plan.width // plan.group // 2
    cols = 6 * plan.width // plan.group
    most = max(plan.group, plan.sequences)
    dma = pltpu.SemaphoreType.DMA

    def placed(dtype):
        return jax.ShapeDtypeStruct((plan.rows_dev, plan.width), dtype)

    operands = dict(operands, weight=weight)
    outs = dict(
        layer=placed(BF16),
        layer_extra=placed(BF16),
        token=placed(F32),
        token_extra=placed(F32),
        table=jax.ShapeDtypeStruct((plan.group, plan.sequences, 1, cols), F32),
        everyone=jax.ShapeDtypeStruct((plan.sequences, plan.group, plan.sequences, rows), F32),
    )
    edges = len(plan.segments)
    scratch = dict(
        layer_own=pltpu.VMEM((plan.own, plan.width), BF16),
        token_own=pltpu.VMEM((plan.own, plan.width), F32),
        local=pltpu.VMEM((2, 6 * plan.width), F32),
        first=pltpu.VMEM((plan.group, 2, cols), F32),
        second=pltpu.VMEM((plan.sequences, 1, cols), F32),
        mine=pltpu.VMEM((2, 1, cols), F32),
        piece=pltpu.VMEM((plan.sequences, rows), F32),
        t_send=dma((3, most)),
        t_recv=dma((3, most)),
        c_send=dma((2, most)),
        c_recv=dma((2, most)),
        l_send=dma((edges,)),
        l_recv=dma((edges,)),
        e_send=dma((edges,)),
        e_recv=dma((edges,)),
    )
    if plan.chip_heads:
        operands["term"] = term.reshape(2, 2, share, plan.width)
        outs["term_out"] = jax.ShapeDtypeStruct((plan.sequences, share, plan.width), BF16)
        scratch.update(term_send=dma((2,)), term_recv=dma((2,)))
    names = tuple(operands) + tuple(outs) + tuple(scratch)
    got = call(
        functools.partial(last_kernel, plan, names),
        "last",
        10,
        tuple(outs.values()),
        list(scratch.values()) + sum_scratch(plan) + sum_scratch(plan),
        tuple(operands.values()),
        vmem=58 << 20,
    )
    got = types.SimpleNamespace(**dict(zip(outs, got)))
    got.table = got.table[:, :, 0].transpose(1, 0, 2).reshape(plan.sequences, -1)
    got.term = got.term_out if plan.chip_heads else term
    return got


def over_sequences(plan, pieces):
    full = lax.all_gather(pieces, "dev", axis=0, axis_index_groups=plan.rank_groups())
    return full.reshape((plan.devices,) + pieces.shape[1:])


def over_sequences_sum(plan, pieces):
    return lax.psum_scatter(pieces, "dev", scatter_dimension=0, axis_index_groups=plan.rank_groups())


def merge_rows(plan, weight, rank):
    if plan.chip_heads:
        return lax.all_gather(weight, "dev", axis=0, axis_index_groups=plan.rank_groups())
    share = plan.width // plan.group
    full = lax.all_gather(weight, "dev", axis=0, tiled=True)
    full = full.reshape(2, 2, plan.group // 2, share, weight.shape[1])
    full = lax.dynamic_index_in_dim(full, lax.rem(rank, 2), 1, keepdims=False)
    return lax.dynamic_index_in_dim(full, lax.div(rank, 2), 1, keepdims=False)


def merge_sum(plan, term, rank):
    if plan.chip_heads:
        return over_sequences_sum(plan, term)
    half = plan.group // 2
    _, share, cols = term.shape
    mine = [jnp.where(lax.rem(rank, 2) == k, term, jnp.zeros((), BF16)) for k in range(2)]
    full = jnp.zeros((2, 2, half, share, cols), BF16)
    full = lax.dynamic_update_slice_in_dim(full, jnp.stack(mine, axis=1)[:, :, None], lax.div(rank, 2), 2)
    return lax.psum_scatter(full.reshape(-1, cols), "dev", scatter_dimension=0, tiled=True)


def down_slices(plan, weight):
    full = lax.all_gather(weight, "dev", axis=0, axis_index_groups=plan.rank_groups())
    return full.reshape(2, -1, weight.shape[1])


def by_stream(plan, image_part, text_part, is_text):
    start, end = plan.text_start, plan.image_end
    mixed = jnp.where(is_text[start:end, None], text_part[: end - start], image_part[start:])
    return jnp.concatenate([image_part[:start], mixed, text_part[end - start :]], axis=0)


def stream_dot(plan, rows, pair, is_text):
    image_part = jnp.dot(rows[: plan.image_end], pair[0], preferred_element_type=F32)
    text_part = jnp.dot(rows[plan.text_start :], pair[1], preferred_element_type=F32)
    return by_stream(plan, image_part, text_part, is_text)


def stream_dot_back(plan, grads, pair, is_text):
    image_part = lax.dot_general(grads[: plan.image_end], pair[0], CONTRACT_LAST, preferred_element_type=F32)
    text_part = lax.dot_general(grads[plan.text_start :], pair[1], CONTRACT_LAST, preferred_element_type=F32)
    return by_stream(plan, image_part, text_part, is_text)


def pick(table, text_rows):
    return jnp.where(text_rows[:, None], table[1][None, :], table[0][None, :])


def on_device(
    tokens,
    conditioning,
    text_lengths,
    modulation_weight,
    project_weight,
    merge_weight,
    up_weight,
    down_weight,
    cotangent,
):
    rows_dev, width = tokens.shape
    mod_rows = modulation_weight.shape[0]
    plan = Plan(lax.axis_size("dev"), conditioning.shape[0], rows_dev, width)
    device = lax.axis_index("dev")
    seq, rank = plan.place_of(device)
    feature_start = device * mod_rows % width

    ends = jnp.cumsum(IMG + text_lengths)
    starts = jnp.concatenate([jnp.zeros((1,), jnp.int32), ends[:-1]])
    positions = device * rows_dev + jnp.arange(rows_dev, dtype=jnp.int32)
    row_seq = jnp.sum((starts[None, :] <= positions[:, None]).astype(jnp.int32), axis=1) - 1
    offset = plan.span * seq - plan.edge + jnp.arange(plan.rows, dtype=jnp.int32) - starts[seq]
    valid = (offset >= 0) & (offset < IMG + text_lengths[seq])
    is_text = offset >= IMG
    bias = jnp.where(valid, 0.0, MASKED).astype(F32)[None, :]
    window_text = is_text.astype(F32)[:, None]
    own_valid = own_rows(plan, valid[:, None], rank)[:, 0]
    own_text = own_rows(plan, is_text[:, None], rank)[:, 0]

    cond_float = conditioning.astype(F32)
    silu_low = jax.nn.silu(cond_float).astype(BF16)
    silu_part = lax.dynamic_slice_in_dim(silu_low, feature_start, mod_rows, 1)
    mod_part = jnp.dot(silu_part, modulation_weight, preferred_element_type=F32)

    merge_pair = merge_rows(plan, merge_weight, rank)
    project_pieces, up_pieces = swap_in(plan, project_weight, up_weight)
    project_pieces, up_pieces, merge_pair = lax.optimization_barrier((project_pieces, up_pieces, merge_pair))
    project_pair = over_sequences(plan, project_pieces)
    share = project_pair.shape[2] // 2
    project_pair = jnp.concatenate([project_pair[:, :, :share], project_pair[:, :, share:]], axis=1)
    project_pair = lax.optimization_barrier(project_pair.reshape(2, width, share))
    up_pair = over_sequences(plan, up_pieces).reshape(2, width, -1)
    down_pair = down_slices(plan, down_weight)

    token_window, grad_window, mods, merge_pair = entry(plan, tokens, cotangent, mod_part, merge_pair)
    shift_a, scale_a, gate_a, shift_b, scale_b, gate_b = jnp.split(mods, 6, axis=1)
    grad_window = jnp.where(valid[:, None], grad_window, jnp.zeros((), BF16))

    normed_full, _ = layer_norm(token_window.astype(F32))
    hidden_a = (normed_full * (1.0 + pick(scale_a, is_text)) + pick(shift_a, is_text)).astype(BF16)
    projected = stream_dot(plan, hidden_a, project_pair, is_text).astype(BF16)
    attended = attend(plan, projected, bias)

    own_tokens = own_rows(plan, token_window, rank)
    own_grad = own_rows(plan, grad_window, rank)
    text_mask = own_text.astype(F32)[:, None]
    merged, hidden_b = middle_rows(
        plan, attended, merge_pair, window_text, own_tokens, gate_a, scale_b, shift_b, text_mask
    )
    middle = own_tokens.astype(F32) + pick(gate_a, own_text) * merged
    normed_b, inv_b = layer_norm(middle)

    upper = stream_dot(plan, hidden_b, up_pair, is_text)
    activated = jax.nn.gelu(upper, approximate=True).astype(BF16)
    grad_lowered = (pick(gate_b, is_text) * grad_window.astype(F32)).astype(BF16)
    down_term = weight_terms(plan, activated, grad_lowered, window_text, "down_terms")
    down_term = down_term.reshape(plan.sequences, -1, width)
    down_term, grad_lowered = lax.optimization_barrier((down_term, grad_lowered))
    down_sum = over_sequences_sum(plan, down_term)
    grad_activated = stream_dot_back(plan, grad_lowered, down_pair, is_text)
    gelu_pull = jax.vjp(lambda value_in: jax.nn.gelu(value_in, approximate=True), upper)[1]
    grad_upper = gelu_pull(grad_activated)[0].astype(BF16)
    up_term = weight_terms(plan, hidden_b, grad_upper, window_text, "up_terms")
    up_term = up_term.reshape(plan.sequences, plan.group, mod_rows, -1)
    grad_upper, up_term = lax.optimization_barrier((grad_upper, up_term))
    up_sum = over_sequences_sum(plan, up_term)
    grad_hidden_b, grad_middle, grad_merged = back_rows(
        plan, grad_upper, up_pair, window_text, own_grad, middle, gate_a, scale_b, text_mask
    )
    merge_term = weight_terms(plan, attended, grad_merged, window_text, "merge_terms")

    grad_projected = attend_back(plan, projected, grad_merged, merge_pair, window_text, bias)
    grad_projected, down_sum = lax.optimization_barrier((grad_projected, down_sum))
    down_grad = down_sum.astype(F32)
    project_term = weight_terms(plan, hidden_a, grad_projected, window_text, "project_terms", mod_rows)
    project_term = project_term.reshape((plan.sequences, plan.group) + project_term.shape[1:])
    grad_projected, project_term = lax.optimization_barrier((grad_projected, project_term))
    project_sum = over_sequences_sum(plan, project_term)

    masks = jnp.stack([own_valid & ~own_text, own_valid & own_text], axis=1).astype(F32)
    rest = jnp.concatenate(
        [
            jnp.stack([jnp.sum(value * masks[:, j : j + 1], axis=0) for j in range(2)])
            for value in (grad_middle * merged, grad_hidden_b, grad_hidden_b * normed_b)
        ],
        axis=1,
    )
    got = last_rows(
        plan,
        merge_term,
        modulation_weight,
        activated=activated,
        down_pair=down_pair,
        grads=grad_projected,
        project_pair=project_pair,
        window_text=window_text,
        tokens=own_tokens,
        middle=middle,
        grad=own_grad,
        grad_middle=grad_middle,
        gate_b=gate_b,
        scale_a=scale_a,
        text=text_mask,
        masks=masks,
        rest=rest,
    )
    foreign = (row_seq != seq)[:, None]
    layer_out = jnp.where(foreign, got.layer_extra, got.layer)
    tokens_grad = jnp.where(foreign, got.token_extra, got.token)
    own_grads = got.table.astype(BF16)
    modulation_grad = lax.dot_general(silu_part, own_grads, CONTRACT_FIRST, preferred_element_type=F32)
    everyone = got.everyone.reshape(2, plan.devices // 2, plan.sequences, mod_rows)
    grad_silu = (everyone[0] + everyone[1]).transpose(1, 0, 2).reshape(plan.sequences, width)
    conditioning_grad = jax.vjp(jax.nn.silu, cond_float)[1](grad_silu)[0]
    modulation_grad, up_sum = lax.optimization_barrier((modulation_grad, up_sum))
    merge_out, project_sum, *done = lax.optimization_barrier(
        (got.term, project_sum, modulation_grad, down_grad, layer_out, tokens_grad, conditioning_grad)
    )
    modulation_grad, down_grad, layer_out, tokens_grad, conditioning_grad = done
    merge_grad = merge_sum(plan, merge_out, rank).reshape(merge_weight.shape).astype(F32)
    up_grad, project_grad = finish(plan, up_sum, project_sum)
    return (
        layer_out,
        tokens_grad,
        conditioning_grad,
        modulation_grad,
        project_grad,
        merge_grad,
        up_grad,
        down_grad,
    )


def solution(mesh):
    shard, whole = P("dev", None), P()
    return jax.shard_map(
        on_device,
        mesh=mesh,
        in_specs=(shard, whole, whole, shard, shard, shard, shard, shard, shard),
        out_specs=(shard, shard, whole, shard, shard, shard, shard, shard),
        check_vma=False,
    )
```

```python
import functools
import types

import jax
import jax.numpy as jnp
import numpy as np
from jax import lax
from jax.experimental import pallas as pl
from jax.experimental.pallas import tpu as pltpu
from jax.sharding import PartitionSpec as P

HEADS = 24
HDIM = 64
IMG = 1024
TXT_MIN = 86
TXT_MAX = 154
EPSILON = 1e-06
F32 = jnp.float32
BF16 = jnp.bfloat16
CONTRACT_LAST = (((1,), (1,)), ((), ()))
PLAIN = (((1,), (0,)), ((), ()))
CONTRACT_FIRST = (((0,), (0,)), ((), ()))
MASKED = -1e30


class Plan:
    def __init__(self, devices, sequences, rows_dev, width):
        self.devices, self.sequences, self.rows_dev, self.width = devices, sequences, rows_dev, width
        self.group = devices // sequences
        self.span = self.group * rows_dev
        mean = self.span - IMG
        up, down = TXT_MAX - mean, mean - TXT_MIN
        drift = 0
        for k in range(sequences + 1):
            drift = max(drift, min(up * k, down * (sequences - k)), min(down * k, up * (sequences - k)))
        self.edge = -(-drift // 64) * 64
        self.rows = self.span + 2 * self.edge
        self.piece = 2 * self.edge // self.group
        self.own = rows_dev + self.piece
        self.image_end = -(-(self.edge + drift + IMG) // 128) * 128
        self.text_start = (self.edge - drift + IMG) // 128 * 128
        self.heads = HEADS // self.group
        self.segments = self.edge_segments()
        self.chip_heads = devices == 4 * self.group

    def device_of(self, seq, rank):
        return seq * self.group + rank

    def place_of(self, device):
        return lax.div(device, self.group), lax.rem(device, self.group)

    def seq_groups(self):
        return [[self.device_of(s, r) for r in range(self.group)] for s in range(self.sequences)]

    def rank_groups(self):
        return [[self.device_of(s, r) for s in range(self.sequences)] for r in range(self.group)]

    def edge_row(self, rank):
        half = self.group // 2
        return jnp.where(rank < half, self.piece * rank, self.edge + self.span + self.piece * (rank - half))

    def main_row(self, rank):
        return self.edge + self.rows_dev * rank

    def edge_segments(self):
        found = []
        for rank in range(self.group):
            half = self.group // 2
            first = self.piece * rank - self.edge if rank < half else self.span + self.piece * (rank - half)
            row = 0
            while row < self.piece:
                owner, owner_row = (first + row) // self.rows_dev, (first + row) % self.rows_dev
                count = min(self.piece - row, self.rows_dev - owner_row)
                found.append((rank, row, count, owner // self.group, owner % self.group, owner_row))
                row += count
        return found


def layer_norm(values):
    mean = jnp.mean(values, axis=-1, keepdims=True)
    centred = values - mean
    variance = jnp.mean(centred * centred, axis=-1, keepdims=True)
    inv_std = lax.rsqrt(variance + EPSILON)
    return (centred * inv_std, inv_std)


def norm_back(grad_normed, normed, inv_std):
    mean_grad = jnp.mean(grad_normed, axis=-1, keepdims=True)
    mean_cross = jnp.mean(grad_normed * normed, axis=-1, keepdims=True)
    return inv_std * (grad_normed - mean_grad - normed * mean_cross)


def softmax_parts(query, key, bias):
    scores = lax.dot_general(query, key, CONTRACT_LAST, preferred_element_type=F32) + bias
    top = jnp.max(scores, axis=1, keepdims=True)
    exponent = jnp.exp(scores - top)
    total = jnp.sum(exponent, axis=1, keepdims=True)
    return exponent * (1.0 / total)


def head_columns(heads, part, head):
    first = (part * heads + head) * HDIM
    return slice(first, first + HDIM)


def attend_kernel(heads, block, projected, bias_ref, out_ref):
    rows = pl.ds(pl.multiple_of(pl.program_id(0) * block, block), block)
    bias = bias_ref[...]
    outs = []
    for head in range(heads):
        query = projected[rows, head_columns(heads, 0, head)] * jnp.asarray(HDIM ** (-0.5), BF16)
        probs = softmax_parts(query, projected[:, head_columns(heads, 1, head)], bias).astype(BF16)
        outs.append(jnp.dot(probs, projected[:, head_columns(heads, 2, head)], preferred_element_type=F32))
    out_ref[...] = jnp.concatenate(outs, axis=1).astype(BF16)


def block_rows(rows):
    return 256 if rows % 256 == 0 else 128


def constant(shape):
    return pl.BlockSpec(shape, lambda i: (0,) * len(shape))


def attend(plan, projected, bias):
    rows, cols = projected.shape[0], projected.shape[1] // 3
    block = block_rows(rows)
    return pl.pallas_call(
        functools.partial(attend_kernel, plan.heads, block),
        out_shape=jax.ShapeDtypeStruct((rows, cols), BF16),
        grid=(rows // block,),
        in_specs=[constant(projected.shape), constant(bias.shape)],
        out_specs=pl.BlockSpec((block, cols), lambda i: (i, 0)),
        compiler_params=pltpu.CompilerParams(vmem_limit_bytes=48 << 20),
        cost_estimate=pl.CostEstimate(flops=16 * rows * rows * cols, bytes_accessed=8 * rows * cols, transcendentals=0),
        name="attend",
    )(projected, bias)


def attend_back_kernel(
    heads, steps, block, projected, grad_merged, merge_pair, text, bias_ref, out, key_sum, value_sum
):
    step = pl.program_id(0)
    scale = jnp.asarray(HDIM ** (-0.5), BF16)

    @pl.when(step == 0)
    def _():
        key_sum[...] = jnp.zeros_like(key_sum)
        value_sum[...] = jnp.zeros_like(value_sum)

    rows = pl.ds(pl.multiple_of(step * block, block), block)
    bias = bias_ref[...]
    image, other_stream = [
        lax.dot_general(grad_merged[...], merge_pair[j], CONTRACT_LAST, preferred_element_type=F32) for j in range(2)
    ]
    grad_attended = jnp.where(text[...] > 0, other_stream, image).astype(BF16)
    grads = []
    for head in range(heads):
        query = projected[rows, head_columns(heads, 0, head)] * scale
        key = projected[:, head_columns(heads, 1, head)]
        grad_out = grad_attended[:, head * HDIM : (head + 1) * HDIM]
        probs = softmax_parts(query, key, bias)
        grad_probs = lax.dot_general(
            grad_out, projected[:, head_columns(heads, 2, head)], CONTRACT_LAST, preferred_element_type=F32
        )
        inner = jnp.sum(probs * grad_probs, axis=1, keepdims=True)
        grad_scores = (probs * (grad_probs - inner)).astype(BF16)
        grads.append(jnp.dot(grad_scores, key, preferred_element_type=F32) * HDIM ** (-0.5))
        key_sum[head] += lax.dot_general(query, grad_scores, CONTRACT_FIRST, preferred_element_type=F32)
        value_sum[head] += lax.dot_general(grad_out, probs.astype(BF16), CONTRACT_FIRST, preferred_element_type=F32)
    cols = heads * HDIM
    out[rows, :cols] = jnp.concatenate(grads, axis=1).astype(BF16)

    @pl.when(step == steps - 1)
    def _():
        total = out.shape[0]
        out[:, cols : 2 * cols] = key_sum[...].reshape(cols, total).T.astype(BF16)
        out[:, 2 * cols :] = value_sum[...].reshape(cols, total).T.astype(BF16)


def attend_back(plan, projected, grad_merged, merge_pair, text, bias):
    rows, cols = projected.shape[0], projected.shape[1] // 3
    block = block_rows(rows)
    return pl.pallas_call(
        functools.partial(attend_back_kernel, plan.heads, rows // block, block),
        out_shape=jax.ShapeDtypeStruct(projected.shape, BF16),
        grid=(rows // block,),
        in_specs=[
            constant(projected.shape),
            pl.BlockSpec((block, plan.width), lambda i: (i, 0)),
            constant(merge_pair.shape),
            pl.BlockSpec((block, 1), lambda i: (i, 0)),
            constant(bias.shape),
        ],
        out_specs=constant(projected.shape),
        scratch_shapes=[pltpu.VMEM((plan.heads, HDIM, rows), F32)] * 2,
        compiler_params=pltpu.CompilerParams(vmem_limit_bytes=56 << 20),
        cost_estimate=pl.CostEstimate(flops=40 * rows * rows * cols, bytes_accessed=14 * rows * cols, transcendentals=0),
        name="attend_back",
    )(projected, grad_merged, merge_pair, text, bias)


def fold_rows(piece):
    half = piece.shape[0] // 2
    return jnp.concatenate([piece[:half], piece[half:]], axis=1)


def unfold_rows(piece):
    half = piece.shape[1] // 2
    return jnp.concatenate([piece[:, :half], piece[:, half:]], axis=0)


def terms_kernel(plan, fold, chunk, rows, grads, text, out, kept):
    width = rows.shape[1]
    for stream, (first, last) in enumerate(((0, plan.image_end), (plan.text_start, plan.rows))):
        count = last - first
        mask = text[pl.ds(first, count)]
        keep = (mask > 0) if stream else (mask <= 0)
        kept[pl.ds(0, count)] = jnp.where(keep, grads[pl.ds(first, count)], jnp.zeros((), BF16))

        def step(i, carry):
            start = pl.multiple_of(i * chunk, chunk)
            term = lax.dot_general(
                rows[pl.ds(first, count), pl.ds(start, chunk)],
                kept[pl.ds(0, count)],
                CONTRACT_FIRST,
                preferred_element_type=F32,
            ).astype(BF16)
            if fold:
                for j in range(chunk // fold):
                    out[(stream * width) // fold + i * (chunk // fold) + j] = fold_rows(term[j * fold : (j + 1) * fold])
            else:
                out[stream, pl.ds(start, chunk)] = term
            return carry

        if width == chunk:
            step(0, 0)
        else:
            lax.fori_loop(0, width // chunk, step, 0)


def weight_terms(plan, rows, grads, text, name, fold=0):
    width, cols = rows.shape[1], grads.shape[1]
    chunk = 384 if width % 384 == 0 else width
    shape = (2 * width // fold, fold // 2, 2 * cols) if fold else (2, width, cols)
    return pl.pallas_call(
        functools.partial(terms_kernel, plan, fold, chunk),
        out_shape=jax.ShapeDtypeStruct(shape, BF16),
        in_specs=[pl.BlockSpec(memory_space=pltpu.VMEM)] * 3,
        out_specs=pl.BlockSpec(memory_space=pltpu.VMEM),
        scratch_shapes=[pltpu.VMEM((plan.image_end, cols), BF16)],
        compiler_params=pltpu.CompilerParams(vmem_limit_bytes=40 << 20),
        cost_estimate=pl.CostEstimate(flops=3 * plan.rows * width * cols, bytes_accessed=1 << 23, transcendentals=0),
        name=name,
    )(rows, grads, text)


VMEM = pl.BlockSpec(memory_space=pltpu.VMEM)


def own_rows(plan, window, rank):
    main = lax.dynamic_slice_in_dim(window, plan.main_row(rank), plan.rows_dev, 0)
    edge = lax.dynamic_slice_in_dim(window, plan.edge_row(rank), plan.piece, 0)
    return jnp.concatenate([main, edge], axis=0)


def remote(source, target, send_sem, recv_sem, device):
    return pltpu.make_async_remote_copy(
        src_ref=source,
        dst_ref=target,
        send_sem=send_sem,
        recv_sem=recv_sem,
        device_id=(device,),
        device_id_type=pl.DeviceIdType.MESH,
    )


def here(plan):
    return plan.place_of(lax.axis_index("dev"))


def other(rank, step, size):
    return lax.rem(rank + step, size)


def meet(devices):
    barrier = pltpu.get_barrier_semaphore()
    for device in devices:
        pl.semaphore_signal(barrier, inc=1, device_id=(device,), device_id_type=pl.DeviceIdType.MESH)
    pl.semaphore_wait(barrier, len(devices))


def group_devices(plan, seq, rank):
    return [plan.device_of(seq, other(rank, step, plan.group)) for step in range(1, plan.group)]


def column_devices(plan, seq, rank):
    return [plan.device_of(other(seq, step, plan.sequences), rank) for step in range(1, plan.sequences)]


def every_device(plan, device):
    return [other(device, step, plan.devices) for step in range(1, plan.devices)]


def call(kernel, name, ident, out_shape, scratch, operands, in_specs=None, out_specs=None, vmem=40 << 20):
    outs = out_shape if isinstance(out_shape, tuple) else (out_shape,)
    return pl.pallas_call(
        kernel,
        out_shape=out_shape,
        in_specs=in_specs or [VMEM] * len(operands),
        out_specs=out_specs or (tuple([VMEM] * len(outs)) if isinstance(out_shape, tuple) else VMEM),
        scratch_shapes=scratch,
        compiler_params=pltpu.CompilerParams(
            collective_id=ident, has_side_effects=True, vmem_limit_bytes=vmem
        ),
        name=name,
    )(*operands)


def aligned(start):
    return pl.multiple_of(start, 16)


def block_parts(plan, ref, rank):
    return (
        ref.at[pl.ds(aligned(plan.main_row(rank)), plan.rows_dev)],
        ref.at[pl.ds(aligned(plan.edge_row(rank)), plan.piece)],
    )


def own_parts(plan, ref):
    return ref.at[pl.ds(0, plan.rows_dev)], ref.at[pl.ds(plan.rows_dev, plan.piece)]


def load_block(plan, ref, rank):
    main, edge = block_parts(plan, ref, rank)
    return jnp.concatenate([main[...], edge[...]], axis=0)


def sum_scratch(plan, wire=BF16):
    half, own, width = plan.group // 2, plan.own, plan.width
    return [
        pltpu.VMEM((half, own, width), F32),
        pltpu.VMEM((half, own, width), F32),
        pltpu.VMEM((own, width), F32),
        pltpu.VMEM((half - 1, own, width), wire),
        pltpu.VMEM((half - 1, own, width), wire),
        pltpu.SemaphoreType.DMA((half,)),
        pltpu.SemaphoreType.DMA((half,)),
        pltpu.SemaphoreType.DMA((half,)),
        pltpu.SemaphoreType.DMA((half,)),
    ]


SUM_SCRATCH = 9


def product(plan, rows, pair, text, dims, rank, out):
    block = load_block(plan, rows, rank)
    text_row = load_block(plan, text, rank) > 0
    chunk = plan.width // 4

    def step(i, carry):
        cols = pl.ds(pl.multiple_of(i * chunk, chunk), chunk)
        parts = []
        for stream in range(2):
            weight = pair[stream, cols, :] if dims is CONTRACT_LAST else pair[stream, :, cols]
            parts.append(lax.dot_general(block, weight, dims, preferred_element_type=F32))
        out[:, cols] = jnp.where(text_row, parts[1], parts[0])
        return carry

    lax.fori_loop(0, 4, step, 0)


def scatter_sum(*args):
    return scatter_start(*args)()


def scatter_start(plan, seq, rank, rows, pair, text, dims, away, near, mine, going, coming,
                  pair_send, pair_recv, far_send, far_recv):
    half = plan.group // 2
    chip, core = lax.div(rank, 2), lax.rem(rank, 2)
    partner = plan.device_of(seq, 2 * chip + 1 - core)
    order = list(range(1, half)) + [0]

    def pair_copy(step):
        return remote(away.at[step], near.at[step], pair_send.at[step], pair_recv.at[step], partner)

    def far_copy(step):
        to = plan.device_of(seq, 2 * other(chip, step, half) + core)
        return remote(going.at[step - 1], coming.at[step - 1], far_send.at[step], far_recv.at[step], to)

    def for_owner(step):
        product(plan, rows, pair, text, dims, 2 * other(chip, step, half) + core, mine)
        pair_copy(step).wait_recv()
        mine[...] += near[step]

    def turn(i, carry):
        step = other(i, 1, half)
        product(plan, rows, pair, text, dims, 2 * other(chip, step, half) + 1 - core, away.at[step])
        pair_copy(step).start()

        @pl.when(i > 0)
        def _():
            for_owner(i)
            going[i - 1] = mine[...].astype(going.dtype)
            far_copy(i).start()

        return carry

    lax.fori_loop(0, half, turn, 0)

    def result():
        for_owner(0)
        total = mine[...]
        for step in range(1, half):
            far_copy(step).wait_recv()
            total = total + coming[step - 1].astype(F32)
        for step in range(half):
            pair_copy(step).wait_send()
        for step in range(1, half):
            far_copy(step).wait_send()
        return total

    return result


def share_scratch(plan):
    return [pltpu.SemaphoreType.DMA((plan.group, 2))] * 2 + [pltpu.SemaphoreType.DMA((plan.group, 2))]


def share_rows(plan, seq, rank, parts, window, send, recv, pass_send):
    half = plan.group // 2
    chip, core = lax.div(rank, 2), lax.rem(rank, 2)
    partner_rank = 2 * chip + 1 - core
    partner = plan.device_of(seq, partner_rank)

    def send_own(to_device, slot):
        copies = [
            remote(source, target, send.at[slot, i], recv.at[slot, i], to_device)
            for i, (source, target) in enumerate(zip(parts, block_parts(plan, window, rank)))
        ]
        for copy in copies:
            copy.start()
        return copies

    flying = {}
    for step in range(1, half):
        flying[step] = send_own(plan.device_of(seq, 2 * other(chip, step, half) + core), step)
    flying[0] = send_own(partner, 0)
    for source, target in zip(parts, block_parts(plan, window, rank)):
        target[...] = source[...]
    passed = []
    for step in range(1, half):
        for copy in flying[step]:
            copy.wait_recv()
        came = 2 * other(chip, half - step, half) + core
        copies = [
            remote(place, place, pass_send.at[step, i], recv.at[half + step, i], partner)
            for i, place in enumerate(block_parts(plan, window, came))
        ]
        for copy in copies:
            copy.start()
        passed.extend(copies)
    for copy in flying[0]:
        copy.wait_recv()
    for copy in passed:
        copy.wait_recv()
    for copies in flying.values():
        for copy in copies:
            copy.wait_send()
    for copy in passed:
        copy.wait_send()


def entry_kernel(plan, tokens, grads, mod_part, *refs):
    if plan.chip_heads:
        merge, merge_out, *refs = refs[:1] + refs[4:5] + refs[1:4] + refs[5:]
        merge_send, merge_recv, *refs = refs[-2:] + refs[:-2]
    (token_window, grad_window, mods, token_own, grad_own, plane, across, chunk, edge_send, edge_recv,
     t_send, t_recv, t_pass, g_send, g_recv, g_pass, m_send, m_recv) = refs
    device = lax.axis_index("dev")
    seq, rank = plan.place_of(device)
    meet(every_device(plan, device))
    swaps = []
    if plan.chip_heads:
        core = lax.rem(rank, 2)
        partner = plan.device_of(seq, 2 * lax.div(rank, 2) + 1 - core)
        for stream in range(2):
            copy = remote(
                merge.at[2 * stream + 1 - core],
                merge_out.at[stream, core],
                merge_send.at[stream],
                merge_recv.at[stream],
                partner,
            )
            copy.start()
            swaps.append(copy)
            merge_out[stream, core] = merge[2 * stream + core]
    hops = []
    for step in range(1, plan.group):
        to = other(rank, step, plan.group)
        copy = remote(mod_part.at[to], plane.at[step], m_send.at[0, step], m_recv.at[0, step], plan.device_of(seq, to))
        copy.start()
        hops.append(copy)
    arrays = ((tokens, token_own), (grads, grad_own))
    count = len(plan.segments)
    for which, (source, own) in enumerate(arrays):
        for index, (to_rank, row, rows, step, owner, owner_row) in enumerate(plan.segments):
            @pl.when(rank == owner)
            def _():
                remote(
                    source.at[pl.ds(owner_row, rows)],
                    own.at[pl.ds(row, rows)],
                    edge_send.at[which * count + index],
                    edge_recv.at[which * count + index],
                    plan.device_of(lax.rem(seq + plan.sequences - step, plan.sequences), to_rank),
                ).start()
    for copy in hops:
        copy.wait_recv()
    total = mod_part[rank]
    for step in range(1, plan.group):
        total = total + plane[step]
    plane[0] = total
    hops_across = []
    for step in range(1, plan.sequences):
        to = other(seq, step, plan.sequences)
        copy = remote(plane.at[0, to], across.at[seq], m_send.at[1, step], m_recv.at[1, step], plan.device_of(to, rank))
        copy.start()
        hops_across.append(copy)
    across[seq] = plane[0, seq]
    for which, (source, own) in enumerate(arrays):
        for index, (to_rank, row, rows, step, owner, owner_row) in enumerate(plan.segments):
            @pl.when(rank == to_rank)
            def _():
                remote(
                    source.at[pl.ds(owner_row, rows)],
                    own.at[pl.ds(row, rows)],
                    edge_send.at[which * count + index],
                    edge_recv.at[which * count + index],
                    plan.device_of(lax.rem(seq + plan.sequences + step, plan.sequences), owner),
                ).wait_recv()
    share_rows(plan, seq, rank, (tokens, token_own), token_window, t_send, t_recv, t_pass)
    for copy in hops_across:
        copy.wait_recv()
    half = plan.sequences // 2
    for stream in range(2):
        total = across[stream * half]
        for i in range(1, half):
            total = total + across[stream * half + i]
        chunk[stream] = total
    hops_back = []
    for step in range(1, plan.group):
        to = other(rank, step, plan.group)
        copy = remote(chunk, mods.at[rank], m_send.at[2, step], m_recv.at[2, step], plan.device_of(seq, to))
        copy.start()
        hops_back.append(copy)
    mods[rank] = chunk[...]
    share_rows(plan, seq, rank, (grads, grad_own), grad_window, g_send, g_recv, g_pass)
    for copy in hops_back:
        copy.wait_recv()
    for copy in hops + hops_across + hops_back:
        copy.wait_send()
    for copy in swaps:
        copy.wait()
    for which, (source, own) in enumerate(arrays):
        for index, (to_rank, row, rows, step, owner, owner_row) in enumerate(plan.segments):
            @pl.when(rank == owner)
            def _():
                remote(
                    source.at[pl.ds(owner_row, rows)],
                    own.at[pl.ds(row, rows)],
                    edge_send.at[which * count + index],
                    edge_recv.at[which * count + index],
                    plan.device_of(lax.rem(seq + plan.sequences - step, plan.sequences), to_rank),
                ).wait_send()


def entry(plan, tokens, grads, mod_part, merge):
    lanes = mod_part.shape[1] // plan.group // 128
    pieces = mod_part.reshape(plan.sequences, plan.group, lanes, 128).transpose(1, 0, 2, 3)
    window = jax.ShapeDtypeStruct((plan.rows, plan.width), BF16)
    dma = pltpu.SemaphoreType.DMA
    most = max(plan.group, plan.sequences)
    shapes = (window, window, jax.ShapeDtypeStruct((plan.group, 2, lanes, 128), F32))
    operands = (tokens, grads, pieces)
    scratch = (
        [
            pltpu.VMEM((plan.piece, plan.width), BF16),
            pltpu.VMEM((plan.piece, plan.width), BF16),
            pltpu.VMEM((plan.group, plan.sequences, lanes, 128), F32),
            pltpu.VMEM((plan.sequences, lanes, 128), F32),
            pltpu.VMEM((2, lanes, 128), F32),
            dma((2 * len(plan.segments),)),
            dma((2 * len(plan.segments),)),
        ]
        + share_scratch(plan)
        + share_scratch(plan)
        + [dma((3, most)), dma((3, most))]
    )
    if plan.chip_heads:
        shapes += (jax.ShapeDtypeStruct((2, 2) + merge.shape[1:], BF16),)
        operands += (merge,)
        scratch += [dma((2,)), dma((2,))]
    token_window, grad_window, mods, *rest = call(
        functools.partial(entry_kernel, plan), "entry", 1, shapes, scratch, operands
    )
    merge_pair = rest[0].reshape(2, -1, plan.width) if plan.chip_heads else merge
    return token_window, grad_window, mods.transpose(1, 0, 2, 3).reshape(2, -1), merge_pair


def project_columns(plan, rank):
    share = plan.width // plan.group
    first = (rank % 2) * (plan.width // 2) + (rank // 2) * share
    return [part * plan.width + first for part in range(3)], share


def up_columns(plan, rank, cols):
    planes = plan.sequences // 2
    share = cols // planes // plan.group
    return [plane * plan.group * share + rank * share for plane in range(planes)], share


def start_swap(plan, seq, rank, source, target, send, recv):
    copies = []
    for step in range(1, plan.group):
        to = other(rank, step, plan.group)
        copy = remote(source.at[to], target.at[rank], send.at[step], recv.at[step], plan.device_of(seq, to))
        copy.start()
        copies.append(copy)
    target[rank] = source[rank]
    return copies


def swap_in_kernel(plan, project, up, down, project_out, up_out, down_out, project_cut, up_cut,
                   p_send, p_recv, u_send, u_recv, d_send, d_recv):
    seq, rank = here(plan)
    for to in range(plan.group):
        starts, share = project_columns(plan, to)
        project_cut[to] = fold_rows(jnp.concatenate([project[:, c : c + share] for c in starts], axis=1))
    meet(group_devices(plan, seq, rank) + column_devices(plan, seq, rank))
    copies = start_swap(plan, seq, rank, project_cut, project_out, p_send, p_recv)
    for step in range(1, plan.sequences):
        to = other(seq, step, plan.sequences)
        copy = remote(down, down_out.at[seq], d_send.at[step], d_recv.at[step], plan.device_of(to, rank))
        copy.start()
        copies.append(copy)
    for to in range(plan.group):
        starts, share = up_columns(plan, to, up.shape[1])
        up_cut[to] = jnp.concatenate([up[:, c : c + share] for c in starts], axis=1)
    copies += start_swap(plan, seq, rank, up_cut, up_out, u_send, u_recv)
    down_out[seq] = down[...]
    for copy in copies:
        copy.wait()


def swap_in(plan, project, up, down):
    rows = project.shape[0]
    dma = pltpu.SemaphoreType.DMA
    shapes = [
        (plan.group, rows // 2, 2 * project.shape[1] // plan.group),
        (plan.group, rows, up.shape[1] // plan.group),
    ]
    whole = (plan.sequences,) + down.shape
    return call(
        functools.partial(swap_in_kernel, plan),
        "swap_in",
        4,
        tuple(jax.ShapeDtypeStruct(shape, BF16) for shape in shapes + [whole]),
        [pltpu.VMEM(shape, BF16) for shape in shapes] + [dma((plan.group,))] * 4 + [dma((plan.sequences,))] * 2,
        (project, up, down),
    )


def place_columns(plan, got, out, columns, unfold):
    for source in range(plan.group):
        starts, share = columns(plan, source)
        piece = unfold_rows(got[source]) if unfold else got[source]
        for i, c in enumerate(starts):
            out[:, c : c + share] = piece[:, i * share : (i + 1) * share]


def finish_kernel(plan, up, project, up_out, project_out, up_got, project_got, u_send, u_recv, p_send, p_recv):
    seq, rank = here(plan)
    meet(group_devices(plan, seq, rank))
    ups = start_swap(plan, seq, rank, up, up_got, u_send, u_recv)
    projects = start_swap(plan, seq, rank, project, project_got, p_send, p_recv)
    for copy in ups:
        copy.wait()
    place_columns(plan, up_got, up_out, lambda p, r: up_columns(p, r, up_out.shape[1]), False)
    for copy in projects:
        copy.wait()
    place_columns(plan, project_got, project_out, project_columns, True)


def finish(plan, up, project):
    dma = pltpu.SemaphoreType.DMA
    rows = up.shape[1]
    up_grad, project_grad = call(
        functools.partial(finish_kernel, plan),
        "finish",
        6,
        (
            jax.ShapeDtypeStruct((rows, plan.group * up.shape[2]), BF16),
            jax.ShapeDtypeStruct((rows, plan.group * project.shape[2] // 2), BF16),
        ),
        [pltpu.VMEM(up.shape, BF16), pltpu.VMEM(project.shape, BF16)] + [dma((plan.group,))] * 4,
        (up, project),
    )
    return up_grad.astype(F32), project_grad.astype(F32)


def pick_rows(table, text):
    return jnp.where(text > 0, table[1:2, :], table[0:1, :])


def norm_rows(values):
    mean = jnp.mean(values, axis=1, keepdims=True)
    centred = values - mean
    inv = lax.rsqrt(jnp.mean(centred * centred, axis=1, keepdims=True) + EPSILON)
    return centred * inv, inv


def middle_kernel(plan, rows, pair, window_text, tokens, gate_a, scale_b, shift_b, text, merged, window, own, *scratch):
    seq, rank = here(plan)
    meet(group_devices(plan, seq, rank))
    total = scatter_sum(plan, seq, rank, rows, pair, window_text, PLAIN, *scratch[:SUM_SCRATCH])
    merged[...] = total
    mask = text[...]
    middle = tokens[...].astype(F32) + pick_rows(gate_a[...], mask) * total
    normed, _ = norm_rows(middle)
    own[...] = (normed * (1.0 + pick_rows(scale_b[...], mask)) + pick_rows(shift_b[...], mask)).astype(BF16)
    share_rows(plan, seq, rank, own_parts(plan, own), window, *scratch[SUM_SCRATCH:])


def own_shape(plan, dtype=F32):
    return jax.ShapeDtypeStruct((plan.own, plan.width), dtype)


def window_shape(plan):
    return jax.ShapeDtypeStruct((plan.rows, plan.width), BF16)


def middle_rows(plan, rows, pair, window_text, tokens, gate_a, scale_b, shift_b, text):
    return call(
        functools.partial(middle_kernel, plan),
        "middle",
        2,
        (own_shape(plan), window_shape(plan)),
        [pltpu.VMEM((plan.own, plan.width), BF16)] + sum_scratch(plan, F32) + share_scratch(plan),
        (rows, pair, window_text, tokens, gate_a, scale_b, shift_b, text),
    )


def back_kernel(plan, rows, pair, window_text, grad, middle, gate_a, scale_b, text, grad_hidden, grad_middle, window, own, *scratch):
    seq, rank = here(plan)
    meet(group_devices(plan, seq, rank))
    total = scatter_sum(plan, seq, rank, rows, pair, window_text, CONTRACT_LAST, *scratch[:SUM_SCRATCH])
    grad_hidden[...] = total
    mask = text[...]
    normed, inv = norm_rows(middle[...])
    inner = total * (1.0 + pick_rows(scale_b[...], mask))
    mean_grad = jnp.mean(inner, axis=1, keepdims=True)
    mean_cross = jnp.mean(inner * normed, axis=1, keepdims=True)
    result = grad[...].astype(F32) + inv * (inner - mean_grad - normed * mean_cross)
    grad_middle[...] = result
    own[...] = (pick_rows(gate_a[...], mask) * result).astype(BF16)
    share_rows(plan, seq, rank, own_parts(plan, own), window, *scratch[SUM_SCRATCH:])


def back_rows(plan, rows, pair, window_text, grad, middle, gate_a, scale_b, text):
    return call(
        functools.partial(back_kernel, plan),
        "back",
        3,
        (own_shape(plan), own_shape(plan), window_shape(plan)),
        [pltpu.VMEM((plan.own, plan.width), BF16)] + sum_scratch(plan) + share_scratch(plan),
        (rows, pair, window_text, grad, middle, gate_a, scale_b, text),
    )


def edge_copy(plan, seq, source, first_row, target, send, recv, index):
    from_rank, row, rows, step, owner, owner_row = plan.segments[index]
    return remote(
        source.at[pl.ds(first_row + row, rows)],
        target.at[pl.ds(owner_row, rows)],
        send.at[index],
        recv.at[index],
        plan.device_of(lax.rem(seq + plan.sequences + step, plan.sequences), owner),
    )


def start_edges(plan, seq, rank, *refs):
    for index, segment in enumerate(plan.segments):
        @pl.when(rank == segment[0])
        def _():
            edge_copy(plan, seq, *refs, index).start()


def finish_edges(plan, seq, rank, *refs):
    for index, segment in enumerate(plan.segments):
        @pl.when(rank == segment[4])
        def _():
            edge_copy(plan, seq, *refs, index).wait_recv()

        @pl.when(rank == segment[0])
        def _():
            edge_copy(plan, seq, *refs, index).wait_send()


def edge_scratch(plan):
    return [pltpu.SemaphoreType.DMA((len(plan.segments),))] * 2


def stream_sums(values, masks):
    return jnp.concatenate([jnp.sum(values * mask, axis=0, keepdims=True) for mask in masks], axis=0)


def last_kernel(plan, names, *refs):
    at = types.SimpleNamespace(**dict(zip(names, refs)))
    low_scratch = refs[len(names) : len(names) + SUM_SCRATCH]
    back_scratch = refs[len(names) + SUM_SCRATCH : len(names) + 2 * SUM_SCRATCH]
    device = lax.axis_index("dev")
    seq, rank = plan.place_of(device)
    stream = lax.div(2 * seq, plan.sequences)
    at.layer_extra[...] = jnp.zeros_like(at.layer_extra)
    at.token_extra[...] = jnp.zeros_like(at.token_extra)
    meet(every_device(plan, device))
    low_sum = scatter_start(plan, seq, rank, at.activated, at.down_pair, at.window_text, PLAIN, *low_scratch)
    back_sum = scatter_start(plan, seq, rank, at.grads, at.project_pair, at.window_text, CONTRACT_LAST, *back_scratch)
    swaps = []
    if plan.chip_heads:
        core = lax.rem(rank, 2)
        partner = plan.device_of(seq, 2 * lax.div(rank, 2) + 1 - core)
        for j in range(2):
            copy = remote(
                at.term.at[j, 1 - core], at.term_out.at[2 * j + core], at.term_send.at[j], at.term_recv.at[j], partner
            )
            copy.start()
            swaps.append(copy)
            at.term_out[2 * j + core] = at.term[j, core]
    text = at.text[...]
    streams = (at.masks[:, 0:1], at.masks[:, 1:2])
    width = plan.width

    lowered = low_sum()
    at.layer_own[...] = (at.middle[...] + pick_rows(at.gate_b[...], text) * lowered).astype(BF16)
    layer_edges = (at.layer_own, plan.rows_dev, at.layer_extra, at.l_send, at.l_recv)
    start_edges(plan, seq, rank, *layer_edges)
    at.local[:, 5 * width :] = stream_sums(at.grad[...].astype(F32) * lowered, streams)
    at.local[:, 2 * width : 5 * width] = at.rest[...]
    at.layer[...] = at.layer_own[pl.ds(0, plan.rows_dev)]

    total = back_sum()
    normed, inv = norm_rows(at.tokens[...].astype(F32))
    at.local[:, :width] = stream_sums(total, streams)
    at.local[:, width : 2 * width] = stream_sums(total * normed, streams)
    cols = 6 * width // plan.group

    def chunk(index):
        return pl.ds(pl.multiple_of(index * cols, 128), cols)

    hops = []
    for step in range(1, plan.group):
        to = other(rank, step, plan.group)
        copy = remote(
            at.local.at[:, chunk(to)], at.first.at[step], at.t_send.at[0, step], at.t_recv.at[0, step], plan.device_of(seq, to)
        )
        copy.start()
        hops.append(copy)
    inner = total * (1.0 + pick_rows(at.scale_a[...], text))
    mean_grad = jnp.mean(inner, axis=1, keepdims=True)
    mean_cross = jnp.mean(inner * normed, axis=1, keepdims=True)
    at.token_own[...] = at.grad_middle[...] + inv * (inner - mean_grad - normed * mean_cross)
    token_edges = (at.token_own, plan.rows_dev, at.token_extra, at.e_send, at.e_recv)
    start_edges(plan, seq, rank, *token_edges)
    for copy in hops:
        copy.wait_recv()
    sums = at.local[:, chunk(rank)]
    for step in range(1, plan.group):
        sums = sums + at.first[step]
    for i in range(2):
        at.mine[i] = sums[i : i + 1]
    across = []
    for step in range(1, plan.sequences):
        to = other(seq, step, plan.sequences)
        to_stream = lax.div(2 * to, plan.sequences)
        copy = remote(
            at.mine.at[to_stream], at.second.at[seq], at.t_send.at[1, step], at.t_recv.at[1, step], plan.device_of(to, rank)
        )
        copy.start()
        across.append(copy)
    at.second[seq] = at.mine[stream]
    at.token[...] = at.token_own[pl.ds(0, plan.rows_dev)]
    for copy in across:
        copy.wait_recv()
    last = []
    for step in range(1, plan.group):
        to = other(rank, step, plan.group)
        copy = remote(at.second, at.table.at[rank], at.t_send.at[2, step], at.t_recv.at[2, step], plan.device_of(seq, to))
        copy.start()
        last.append(copy)
    at.table[rank] = at.second[...]
    for copy in last:
        copy.wait_recv()

    piece = None
    for index in range(plan.group):
        grads = jnp.concatenate([at.table[index, s] for s in range(plan.sequences)], axis=0).astype(BF16)
        part = lax.dot_general(
            grads, at.weight[:, index * cols : (index + 1) * cols], CONTRACT_LAST, preferred_element_type=F32
        )
        piece = part if piece is None else piece + part
    at.piece[...] = piece
    at.everyone[seq, rank] = piece
    spread = []
    for step in range(1, plan.group):
        to = other(rank, step, plan.group)
        copy = remote(
            at.piece, at.everyone.at[seq, rank], at.c_send.at[0, step], at.c_recv.at[0, step], plan.device_of(seq, to)
        )
        copy.start()
        spread.append(copy)
    for copy in spread:
        copy.wait_recv()
    for step in range(1, plan.sequences):
        to = other(seq, step, plan.sequences)
        copy = remote(
            at.everyone.at[seq], at.everyone.at[seq], at.c_send.at[1, step], at.c_recv.at[1, step], plan.device_of(to, rank)
        )
        copy.start()
        spread.append(copy)
    for copy in spread[plan.group - 1 :]:
        copy.wait_recv()
    for copy in hops + across + last + spread:
        copy.wait_send()
    for copy in swaps:
        copy.wait()
    finish_edges(plan, seq, rank, *layer_edges)
    finish_edges(plan, seq, rank, *token_edges)


def last_rows(plan, term, weight, **operands):
    rows, share = weight.shape[0], plan.width // plan.group // 2
    cols = 6 * plan.width // plan.group
    most = max(plan.group, plan.sequences)
    dma = pltpu.SemaphoreType.DMA

    def placed(dtype):
        return jax.ShapeDtypeStruct((plan.rows_dev, plan.width), dtype)

    operands = dict(operands, weight=weight)
    outs = dict(
        layer=placed(BF16),
        layer_extra=placed(BF16),
        token=placed(F32),
        token_extra=placed(F32),
        table=jax.ShapeDtypeStruct((plan.group, plan.sequences, 1, cols), F32),
        everyone=jax.ShapeDtypeStruct((plan.sequences, plan.group, plan.sequences, rows), F32),
    )
    edges = len(plan.segments)
    scratch = dict(
        layer_own=pltpu.VMEM((plan.own, plan.width), BF16),
        token_own=pltpu.VMEM((plan.own, plan.width), F32),
        local=pltpu.VMEM((2, 6 * plan.width), F32),
        first=pltpu.VMEM((plan.group, 2, cols), F32),
        second=pltpu.VMEM((plan.sequences, 1, cols), F32),
        mine=pltpu.VMEM((2, 1, cols), F32),
        piece=pltpu.VMEM((plan.sequences, rows), F32),
        t_send=dma((3, most)),
        t_recv=dma((3, most)),
        c_send=dma((2, most)),
        c_recv=dma((2, most)),
        l_send=dma((edges,)),
        l_recv=dma((edges,)),
        e_send=dma((edges,)),
        e_recv=dma((edges,)),
    )
    if plan.chip_heads:
        operands["term"] = term.reshape(2, 2, share, plan.width)
        outs["term_out"] = jax.ShapeDtypeStruct((plan.sequences, share, plan.width), BF16)
        scratch.update(term_send=dma((2,)), term_recv=dma((2,)))
    names = tuple(operands) + tuple(outs) + tuple(scratch)
    got = call(
        functools.partial(last_kernel, plan, names),
        "last",
        10,
        tuple(outs.values()),
        list(scratch.values()) + sum_scratch(plan) + sum_scratch(plan),
        tuple(operands.values()),
        vmem=58 << 20,
    )
    got = types.SimpleNamespace(**dict(zip(outs, got)))
    got.table = got.table[:, :, 0].transpose(1, 0, 2).reshape(plan.sequences, -1)
    got.term = got.term_out if plan.chip_heads else term
    return got


def over_sequences(plan, pieces):
    full = lax.all_gather(pieces, "dev", axis=0, axis_index_groups=plan.rank_groups())
    return full.reshape((plan.devices,) + pieces.shape[1:])


def over_sequences_sum(plan, pieces):
    return lax.psum_scatter(pieces, "dev", scatter_dimension=0, axis_index_groups=plan.rank_groups())


def merge_rows(plan, weight, rank):
    if plan.chip_heads:
        return lax.all_gather(weight, "dev", axis=0, axis_index_groups=plan.rank_groups())
    share = plan.width // plan.group
    full = lax.all_gather(weight, "dev", axis=0, tiled=True)
    full = full.reshape(2, 2, plan.group // 2, share, weight.shape[1])
    full = lax.dynamic_index_in_dim(full, lax.rem(rank, 2), 1, keepdims=False)
    return lax.dynamic_index_in_dim(full, lax.div(rank, 2), 1, keepdims=False)


def merge_sum(plan, term, rank):
    if plan.chip_heads:
        return over_sequences_sum(plan, term)
    half = plan.group // 2
    _, share, cols = term.shape
    mine = [jnp.where(lax.rem(rank, 2) == k, term, jnp.zeros((), BF16)) for k in range(2)]
    full = jnp.zeros((2, 2, half, share, cols), BF16)
    full = lax.dynamic_update_slice_in_dim(full, jnp.stack(mine, axis=1)[:, :, None], lax.div(rank, 2), 2)
    return lax.psum_scatter(full.reshape(-1, cols), "dev", scatter_dimension=0, tiled=True)


def by_stream(plan, image_part, text_part, is_text):
    start, end = plan.text_start, plan.image_end
    mixed = jnp.where(is_text[start:end, None], text_part[: end - start], image_part[start:])
    return jnp.concatenate([image_part[:start], mixed, text_part[end - start :]], axis=0)


def stream_dot(plan, rows, pair, is_text):
    image_part = jnp.dot(rows[: plan.image_end], pair[0], preferred_element_type=F32)
    text_part = jnp.dot(rows[plan.text_start :], pair[1], preferred_element_type=F32)
    return by_stream(plan, image_part, text_part, is_text)


def stream_dot_back(plan, grads, pair, is_text):
    image_part = lax.dot_general(grads[: plan.image_end], pair[0], CONTRACT_LAST, preferred_element_type=F32)
    text_part = lax.dot_general(grads[plan.text_start :], pair[1], CONTRACT_LAST, preferred_element_type=F32)
    return by_stream(plan, image_part, text_part, is_text)


def pick(table, text_rows):
    return jnp.where(text_rows[:, None], table[1][None, :], table[0][None, :])


def on_device(
    tokens,
    conditioning,
    text_lengths,
    modulation_weight,
    project_weight,
    merge_weight,
    up_weight,
    down_weight,
    cotangent,
):
    rows_dev, width = tokens.shape
    mod_rows = modulation_weight.shape[0]
    plan = Plan(lax.axis_size("dev"), conditioning.shape[0], rows_dev, width)
    device = lax.axis_index("dev")
    seq, rank = plan.place_of(device)
    feature_start = device * mod_rows % width

    ends = jnp.cumsum(IMG + text_lengths)
    starts = jnp.concatenate([jnp.zeros((1,), jnp.int32), ends[:-1]])
    positions = device * rows_dev + jnp.arange(rows_dev, dtype=jnp.int32)
    row_seq = jnp.sum((starts[None, :] <= positions[:, None]).astype(jnp.int32), axis=1) - 1
    offset = plan.span * seq - plan.edge + jnp.arange(plan.rows, dtype=jnp.int32) - starts[seq]
    valid = (offset >= 0) & (offset < IMG + text_lengths[seq])
    is_text = offset >= IMG
    bias = jnp.where(valid, 0.0, MASKED).astype(F32)[None, :]
    window_text = is_text.astype(F32)[:, None]
    own_valid = own_rows(plan, valid[:, None], rank)[:, 0]
    own_text = own_rows(plan, is_text[:, None], rank)[:, 0]

    cond_float = conditioning.astype(F32)
    silu_low = jax.nn.silu(cond_float).astype(BF16)
    silu_part = lax.dynamic_slice_in_dim(silu_low, feature_start, mod_rows, 1)
    mod_part = jnp.dot(silu_part, modulation_weight, preferred_element_type=F32)

    merge_pair = merge_rows(plan, merge_weight, rank)
    early = down_weight.shape[0] // 6
    project_pieces, up_pieces, down_early = swap_in(plan, project_weight, up_weight, down_weight[:early])
    project_pieces, up_pieces, merge_pair = lax.optimization_barrier((project_pieces, up_pieces, merge_pair))
    project_pair = over_sequences(plan, project_pieces)
    share = project_pair.shape[2] // 2
    project_pair = jnp.concatenate([project_pair[:, :, :share], project_pair[:, :, share:]], axis=1)
    project_pair = lax.optimization_barrier(project_pair.reshape(2, width, share))
    up_pair = over_sequences(plan, up_pieces).reshape(2, width, -1)
    down_late = lax.all_gather(down_weight[early:], "dev", axis=0, axis_index_groups=plan.rank_groups())
    down_pair = jnp.concatenate([down_early, down_late], axis=1).reshape(2, -1, width)
    down_pair = lax.optimization_barrier(down_pair)

    token_window, grad_window, mods, merge_pair = entry(plan, tokens, cotangent, mod_part, merge_pair)
    shift_a, scale_a, gate_a, shift_b, scale_b, gate_b = jnp.split(mods, 6, axis=1)
    grad_window = jnp.where(valid[:, None], grad_window, jnp.zeros((), BF16))

    normed_full, _ = layer_norm(token_window.astype(F32))
    hidden_a = (normed_full * (1.0 + pick(scale_a, is_text)) + pick(shift_a, is_text)).astype(BF16)
    projected = stream_dot(plan, hidden_a, project_pair, is_text).astype(BF16)
    attended = attend(plan, projected, bias)

    own_tokens = own_rows(plan, token_window, rank)
    own_grad = own_rows(plan, grad_window, rank)
    text_mask = own_text.astype(F32)[:, None]
    merged, hidden_b = middle_rows(
        plan, attended, merge_pair, window_text, own_tokens, gate_a, scale_b, shift_b, text_mask
    )
    middle = own_tokens.astype(F32) + pick(gate_a, own_text) * merged
    normed_b, inv_b = layer_norm(middle)

    upper = stream_dot(plan, hidden_b, up_pair, is_text)
    activated = jax.nn.gelu(upper, approximate=True).astype(BF16)
    grad_lowered = (pick(gate_b, is_text) * grad_window.astype(F32)).astype(BF16)
    down_term = weight_terms(plan, activated, grad_lowered, window_text, "down_terms")
    down_term = down_term.reshape(plan.sequences, -1, width)
    down_term, grad_lowered = lax.optimization_barrier((down_term, grad_lowered))
    down_sum = over_sequences_sum(plan, down_term)
    grad_activated = stream_dot_back(plan, grad_lowered, down_pair, is_text)
    gelu_pull = jax.vjp(lambda value_in: jax.nn.gelu(value_in, approximate=True), upper)[1]
    grad_upper = gelu_pull(grad_activated)[0].astype(BF16)
    up_term = weight_terms(plan, hidden_b, grad_upper, window_text, "up_terms")
    up_term = up_term.reshape(plan.sequences, plan.group, mod_rows, -1)
    grad_upper, up_term = lax.optimization_barrier((grad_upper, up_term))
    up_sum = over_sequences_sum(plan, up_term)
    grad_hidden_b, grad_middle, grad_merged = back_rows(
        plan, grad_upper, up_pair, window_text, own_grad, middle, gate_a, scale_b, text_mask
    )
    merge_term = weight_terms(plan, attended, grad_merged, window_text, "merge_terms")

    grad_projected = attend_back(plan, projected, grad_merged, merge_pair, window_text, bias)
    grad_projected, down_sum = lax.optimization_barrier((grad_projected, down_sum))
    down_grad = down_sum.astype(F32)
    project_term = weight_terms(plan, hidden_a, grad_projected, window_text, "project_terms", mod_rows)
    project_term = project_term.reshape((plan.sequences, plan.group) + project_term.shape[1:])
    grad_projected, project_term = lax.optimization_barrier((grad_projected, project_term))
    project_sum = over_sequences_sum(plan, project_term)

    masks = jnp.stack([own_valid & ~own_text, own_valid & own_text], axis=1).astype(F32)
    rest = jnp.concatenate(
        [
            jnp.stack([jnp.sum(value * masks[:, j : j + 1], axis=0) for j in range(2)])
            for value in (grad_middle * merged, grad_hidden_b, grad_hidden_b * normed_b)
        ],
        axis=1,
    )
    got = last_rows(
        plan,
        merge_term,
        modulation_weight,
        activated=activated,
        down_pair=down_pair,
        grads=grad_projected,
        project_pair=project_pair,
        window_text=window_text,
        tokens=own_tokens,
        middle=middle,
        grad=own_grad,
        grad_middle=grad_middle,
        gate_b=gate_b,
        scale_a=scale_a,
        text=text_mask,
        masks=masks,
        rest=rest,
    )
    foreign = (row_seq != seq)[:, None]
    layer_out = jnp.where(foreign, got.layer_extra, got.layer)
    tokens_grad = jnp.where(foreign, got.token_extra, got.token)
    own_grads = got.table.astype(BF16)
    modulation_grad = lax.dot_general(silu_part, own_grads, CONTRACT_FIRST, preferred_element_type=F32)
    everyone = got.everyone.reshape(2, plan.devices // 2, plan.sequences, mod_rows)
    grad_silu = (everyone[0] + everyone[1]).transpose(1, 0, 2).reshape(plan.sequences, width)
    conditioning_grad = jax.vjp(jax.nn.silu, cond_float)[1](grad_silu)[0]
    modulation_grad, up_sum = lax.optimization_barrier((modulation_grad, up_sum))
    merge_out, project_sum, *done = lax.optimization_barrier(
        (got.term, project_sum, modulation_grad, down_grad, layer_out, tokens_grad, conditioning_grad)
    )
    modulation_grad, down_grad, layer_out, tokens_grad, conditioning_grad = done
    merge_grad = merge_sum(plan, merge_out, rank).reshape(merge_weight.shape).astype(F32)
    up_grad, project_grad = finish(plan, up_sum, project_sum)
    return (
        layer_out,
        tokens_grad,
        conditioning_grad,
        modulation_grad,
        project_grad,
        merge_grad,
        up_grad,
        down_grad,
    )


def solution(mesh):
    shard, whole = P("dev", None), P()
    return jax.shard_map(
        on_device,
        mesh=mesh,
        in_specs=(shard, whole, whole, shard, shard, shard, shard, shard, shard),
        out_specs=(shard, shard, whole, shard, shard, shard, shard, shard),
        check_vma=False,
    )
```

```python
import functools
import types

import jax
import jax.numpy as jnp
import numpy as np
from jax import lax
from jax.experimental import pallas as pl
from jax.experimental.pallas import tpu as pltpu
from jax.sharding import PartitionSpec as P

HEADS = 24
HDIM = 64
IMG = 1024
TXT_MIN = 86
TXT_MAX = 154
EPSILON = 1e-06
F32 = jnp.float32
BF16 = jnp.bfloat16
CONTRACT_LAST = (((1,), (1,)), ((), ()))
PLAIN = (((1,), (0,)), ((), ()))
CONTRACT_FIRST = (((0,), (0,)), ((), ()))
MASKED = -1e30


class Plan:
    def __init__(self, devices, sequences, rows_dev, width):
        self.devices, self.sequences, self.rows_dev, self.width = devices, sequences, rows_dev, width
        self.group = devices // sequences
        self.span = self.group * rows_dev
        mean = self.span - IMG
        up, down = TXT_MAX - mean, mean - TXT_MIN
        drift = 0
        for k in range(sequences + 1):
            drift = max(drift, min(up * k, down * (sequences - k)), min(down * k, up * (sequences - k)))
        self.edge = -(-drift // 64) * 64
        self.rows = self.span + 2 * self.edge
        self.piece = 2 * self.edge // self.group
        self.own = rows_dev + self.piece
        self.image_end = -(-(self.edge + drift + IMG) // 128) * 128
        self.text_start = (self.edge - drift + IMG) // 128 * 128
        self.heads = HEADS // self.group
        self.segments = self.edge_segments()
        self.chip_heads = devices == 4 * self.group

    def device_of(self, seq, rank):
        return seq * self.group + rank

    def place_of(self, device):
        return lax.div(device, self.group), lax.rem(device, self.group)

    def seq_groups(self):
        return [[self.device_of(s, r) for r in range(self.group)] for s in range(self.sequences)]

    def rank_groups(self):
        return [[self.device_of(s, r) for s in range(self.sequences)] for r in range(self.group)]

    def edge_row(self, rank):
        half = self.group // 2
        return jnp.where(rank < half, self.piece * rank, self.edge + self.span + self.piece * (rank - half))

    def main_row(self, rank):
        return self.edge + self.rows_dev * rank

    def edge_segments(self):
        found = []
        for rank in range(self.group):
            half = self.group // 2
            first = self.piece * rank - self.edge if rank < half else self.span + self.piece * (rank - half)
            row = 0
            while row < self.piece:
                owner, owner_row = (first + row) // self.rows_dev, (first + row) % self.rows_dev
                count = min(self.piece - row, self.rows_dev - owner_row)
                found.append((rank, row, count, owner // self.group, owner % self.group, owner_row))
                row += count
        return found


def layer_norm(values):
    mean = jnp.mean(values, axis=-1, keepdims=True)
    centred = values - mean
    variance = jnp.mean(centred * centred, axis=-1, keepdims=True)
    inv_std = lax.rsqrt(variance + EPSILON)
    return (centred * inv_std, inv_std)


def norm_back(grad_normed, normed, inv_std):
    mean_grad = jnp.mean(grad_normed, axis=-1, keepdims=True)
    mean_cross = jnp.mean(grad_normed * normed, axis=-1, keepdims=True)
    return inv_std * (grad_normed - mean_grad - normed * mean_cross)


def softmax_parts(query, key, bias):
    scores = lax.dot_general(query, key, CONTRACT_LAST, preferred_element_type=F32) + bias
    top = jnp.max(scores, axis=1, keepdims=True)
    exponent = jnp.exp(scores - top)
    total = jnp.sum(exponent, axis=1, keepdims=True)
    return exponent * (1.0 / total)


def head_columns(heads, part, head):
    first = (part * heads + head) * HDIM
    return slice(first, first + HDIM)


def attend_kernel(heads, block, projected, bias_ref, out_ref):
    rows = pl.ds(pl.multiple_of(pl.program_id(0) * block, block), block)
    bias = bias_ref[...]
    outs = []
    for head in range(heads):
        query = projected[rows, head_columns(heads, 0, head)] * jnp.asarray(HDIM ** (-0.5), BF16)
        probs = softmax_parts(query, projected[:, head_columns(heads, 1, head)], bias).astype(BF16)
        outs.append(jnp.dot(probs, projected[:, head_columns(heads, 2, head)], preferred_element_type=F32))
    out_ref[...] = jnp.concatenate(outs, axis=1).astype(BF16)


def block_rows(rows):
    return 128


def constant(shape):
    return pl.BlockSpec(shape, lambda i: (0,) * len(shape))


def attend(plan, projected, bias):
    rows, cols = projected.shape[0], projected.shape[1] // 3
    block = block_rows(rows)
    return pl.pallas_call(
        functools.partial(attend_kernel, plan.heads, block),
        out_shape=jax.ShapeDtypeStruct((rows, cols), BF16),
        grid=(rows // block,),
        in_specs=[constant(projected.shape), constant(bias.shape)],
        out_specs=pl.BlockSpec((block, cols), lambda i: (i, 0)),
        compiler_params=pltpu.CompilerParams(vmem_limit_bytes=48 << 20),
        cost_estimate=pl.CostEstimate(flops=16 * rows * rows * cols, bytes_accessed=8 * rows * cols, transcendentals=0),
        name="attend",
    )(projected, bias)


def attend_back_kernel(
    heads, steps, block, projected, grad_merged, merge_pair, text, bias_ref, out, key_sum, value_sum
):
    step = pl.program_id(0)
    scale = jnp.asarray(HDIM ** (-0.5), BF16)

    @pl.when(step == 0)
    def _():
        key_sum[...] = jnp.zeros_like(key_sum)
        value_sum[...] = jnp.zeros_like(value_sum)

    rows = pl.ds(pl.multiple_of(step * block, block), block)
    bias = bias_ref[...]
    image, other_stream = [
        lax.dot_general(grad_merged[...], merge_pair[j], CONTRACT_LAST, preferred_element_type=F32) for j in range(2)
    ]
    grad_attended = jnp.where(text[...] > 0, other_stream, image).astype(BF16)
    grads = []
    for head in range(heads):
        query = projected[rows, head_columns(heads, 0, head)] * scale
        key = projected[:, head_columns(heads, 1, head)]
        grad_out = grad_attended[:, head * HDIM : (head + 1) * HDIM]
        probs = softmax_parts(query, key, bias)
        grad_probs = lax.dot_general(
            grad_out, projected[:, head_columns(heads, 2, head)], CONTRACT_LAST, preferred_element_type=F32
        )
        inner = jnp.sum(probs * grad_probs, axis=1, keepdims=True)
        grad_scores = (probs * (grad_probs - inner)).astype(BF16)
        grads.append(jnp.dot(grad_scores, key, preferred_element_type=F32) * HDIM ** (-0.5))
        key_sum[head] += lax.dot_general(query, grad_scores, CONTRACT_FIRST, preferred_element_type=F32)
        value_sum[head] += lax.dot_general(grad_out, probs.astype(BF16), CONTRACT_FIRST, preferred_element_type=F32)
    cols = heads * HDIM
    out[rows, :cols] = jnp.concatenate(grads, axis=1).astype(BF16)

    @pl.when(step == steps - 1)
    def _():
        total = out.shape[0]
        out[:, cols : 2 * cols] = key_sum[...].reshape(cols, total).T.astype(BF16)
        out[:, 2 * cols :] = value_sum[...].reshape(cols, total).T.astype(BF16)


def attend_back(plan, projected, grad_merged, merge_pair, text, bias):
    rows, cols = projected.shape[0], projected.shape[1] // 3
    block = block_rows(rows)
    return pl.pallas_call(
        functools.partial(attend_back_kernel, plan.heads, rows // block, block),
        out_shape=jax.ShapeDtypeStruct(projected.shape, BF16),
        grid=(rows // block,),
        in_specs=[
            constant(projected.shape),
            pl.BlockSpec((block, plan.width), lambda i: (i, 0)),
            constant(merge_pair.shape),
            pl.BlockSpec((block, 1), lambda i: (i, 0)),
            constant(bias.shape),
        ],
        out_specs=constant(projected.shape),
        scratch_shapes=[pltpu.VMEM((plan.heads, HDIM, rows), F32)] * 2,
        compiler_params=pltpu.CompilerParams(vmem_limit_bytes=56 << 20),
        cost_estimate=pl.CostEstimate(flops=40 * rows * rows * cols, bytes_accessed=14 * rows * cols, transcendentals=0),
        name="attend_back",
    )(projected, grad_merged, merge_pair, text, bias)


def fold_rows(piece):
    half = piece.shape[0] // 2
    return jnp.concatenate([piece[:half], piece[half:]], axis=1)


def unfold_rows(piece):
    half = piece.shape[1] // 2
    return jnp.concatenate([piece[:, :half], piece[:, half:]], axis=0)


def terms_kernel(plan, fold, chunk, rows, grads, text, out, kept):
    width = rows.shape[1]
    for stream, (first, last) in enumerate(((0, plan.image_end), (plan.text_start, plan.rows))):
        count = last - first
        mask = text[pl.ds(first, count)]
        keep = (mask > 0) if stream else (mask <= 0)
        kept[pl.ds(0, count)] = jnp.where(keep, grads[pl.ds(first, count)], jnp.zeros((), BF16))

        def step(i, carry):
            start = pl.multiple_of(i * chunk, chunk)
            term = lax.dot_general(
                rows[pl.ds(first, count), pl.ds(start, chunk)],
                kept[pl.ds(0, count)],
                CONTRACT_FIRST,
                preferred_element_type=F32,
            ).astype(BF16)
            if fold:
                for j in range(chunk // fold):
                    out[(stream * width) // fold + i * (chunk // fold) + j] = fold_rows(term[j * fold : (j + 1) * fold])
            else:
                out[stream, pl.ds(start, chunk)] = term
            return carry

        if width == chunk:
            step(0, 0)
        else:
            lax.fori_loop(0, width // chunk, step, 0)


def weight_terms(plan, rows, grads, text, name, fold=0):
    width, cols = rows.shape[1], grads.shape[1]
    chunk = 384 if fold else 256 if width % 256 == 0 else width
    shape = (2 * width // fold, fold // 2, 2 * cols) if fold else (2, width, cols)
    return pl.pallas_call(
        functools.partial(terms_kernel, plan, fold, chunk),
        out_shape=jax.ShapeDtypeStruct(shape, BF16),
        in_specs=[pl.BlockSpec(memory_space=pltpu.VMEM)] * 3,
        out_specs=pl.BlockSpec(memory_space=pltpu.VMEM),
        scratch_shapes=[pltpu.VMEM((plan.image_end, cols), BF16)],
        compiler_params=pltpu.CompilerParams(vmem_limit_bytes=40 << 20),
        cost_estimate=pl.CostEstimate(flops=3 * plan.rows * width * cols, bytes_accessed=1 << 23, transcendentals=0),
        name=name,
    )(rows, grads, text)


def gelu(values):
    return jax.nn.gelu(values, approximate=True)


def in_blocks(plan, size, body):
    def step(i, carry):
        body(i, pl.ds(pl.multiple_of(i * size, size), size))
        return carry

    lax.fori_loop(0, plan.rows // size, step, 0)


def blockwise(plan, i, size, block, pair, dims, mask, out):
    @pl.when(i * size < plan.image_end)
    def _():
        out[...] = lax.dot_general(block, pair[0], dims, preferred_element_type=F32)

    @pl.when(i * size + size > plan.text_start)
    def _():
        out[...] = jnp.where(mask > 0, lax.dot_general(block, pair[1], dims, preferred_element_type=F32), out[...])


def project_kernel(plan, size, rows, pair, text, shift, scale, hidden, out, held):
    def body(i, place):
        mask = text[place]
        normed, _ = norm_rows(rows[place].astype(F32))
        block = (normed * (1.0 + pick_rows(scale[...], mask)) + pick_rows(shift[...], mask)).astype(BF16)
        hidden[place] = block
        blockwise(plan, i, size, block, pair, PLAIN, mask, held)
        out[place] = held[...].astype(BF16)

    in_blocks(plan, size, body)


def up_kernel(plan, size, rows, pair, text, upper, activated):
    def body(i, place):
        blockwise(plan, i, size, rows[place], pair, PLAIN, text[place], upper.at[place])
        activated[place] = gelu(upper[place]).astype(BF16)

    in_blocks(plan, size, body)


def down_back_kernel(plan, size, rows, pair, text, upper, out, held):
    def body(i, place):
        blockwise(plan, i, size, rows[place], pair, CONTRACT_LAST, text[place], held)
        out[place] = jax.vjp(gelu, upper[place])[1](held[...])[0].astype(BF16)

    in_blocks(plan, size, body)


def stream_rows(plan, kernel, size, cols, held, name, outs, *operands):
    spec = pl.BlockSpec(memory_space=pltpu.VMEM)
    shapes = tuple(jax.ShapeDtypeStruct((plan.rows, width), dtype) for width, dtype in outs)
    return pl.pallas_call(
        functools.partial(kernel, plan, size),
        out_shape=shapes,
        in_specs=[spec] * len(operands),
        out_specs=(spec,) * len(shapes),
        scratch_shapes=[pltpu.VMEM((size, cols), F32)] if held else [],
        compiler_params=pltpu.CompilerParams(vmem_limit_bytes=40 << 20),
        cost_estimate=pl.CostEstimate(
            flops=2 * plan.rows * plan.width * cols, bytes_accessed=1 << 24, transcendentals=0
        ),
        name=name,
    )(*operands)


VMEM = pl.BlockSpec(memory_space=pltpu.VMEM)


def own_rows(plan, window, rank):
    main = lax.dynamic_slice_in_dim(window, plan.main_row(rank), plan.rows_dev, 0)
    edge = lax.dynamic_slice_in_dim(window, plan.edge_row(rank), plan.piece, 0)
    return jnp.concatenate([main, edge], axis=0)


def remote(source, target, send_sem, recv_sem, device):
    return pltpu.make_async_remote_copy(
        src_ref=source,
        dst_ref=target,
        send_sem=send_sem,
        recv_sem=recv_sem,
        device_id=(device,),
        device_id_type=pl.DeviceIdType.MESH,
    )


def here(plan):
    return plan.place_of(lax.axis_index("dev"))


def other(rank, step, size):
    return lax.rem(rank + step, size)


def meet(devices):
    barrier = pltpu.get_barrier_semaphore()
    for device in devices:
        pl.semaphore_signal(barrier, inc=1, device_id=(device,), device_id_type=pl.DeviceIdType.MESH)
    pl.semaphore_wait(barrier, len(devices))


def group_devices(plan, seq, rank):
    return [plan.device_of(seq, other(rank, step, plan.group)) for step in range(1, plan.group)]


def column_devices(plan, seq, rank):
    return [plan.device_of(other(seq, step, plan.sequences), rank) for step in range(1, plan.sequences)]


def every_device(plan, device):
    return [other(device, step, plan.devices) for step in range(1, plan.devices)]


def call(kernel, name, ident, out_shape, scratch, operands, in_specs=None, out_specs=None, vmem=40 << 20):
    outs = out_shape if isinstance(out_shape, tuple) else (out_shape,)
    return pl.pallas_call(
        kernel,
        out_shape=out_shape,
        in_specs=in_specs or [VMEM] * len(operands),
        out_specs=out_specs or (tuple([VMEM] * len(outs)) if isinstance(out_shape, tuple) else VMEM),
        scratch_shapes=scratch,
        compiler_params=pltpu.CompilerParams(
            collective_id=ident, has_side_effects=True, vmem_limit_bytes=vmem
        ),
        name=name,
    )(*operands)


def aligned(start):
    return pl.multiple_of(start, 16)


def block_parts(plan, ref, rank):
    return (
        ref.at[pl.ds(aligned(plan.main_row(rank)), plan.rows_dev)],
        ref.at[pl.ds(aligned(plan.edge_row(rank)), plan.piece)],
    )


def own_parts(plan, ref):
    return ref.at[pl.ds(0, plan.rows_dev)], ref.at[pl.ds(plan.rows_dev, plan.piece)]


def load_block(plan, ref, rank):
    main, edge = block_parts(plan, ref, rank)
    return jnp.concatenate([main[...], edge[...]], axis=0)


def sum_scratch(plan, wire=BF16):
    half, own, width = plan.group // 2, plan.own, plan.width
    return [
        pltpu.VMEM((half + 1, own, width), F32),
        pltpu.VMEM((half, own, width), F32),
        pltpu.VMEM((half - 1, own, width), wire),
        pltpu.VMEM((half - 1, own, width), wire),
        pltpu.SemaphoreType.DMA((half,)),
        pltpu.SemaphoreType.DMA((half,)),
        pltpu.SemaphoreType.DMA((half,)),
        pltpu.SemaphoreType.DMA((half,)),
    ]


SUM_SCRATCH = 8


def product(plan, rows, pair, text, dims, rank, out):
    block = load_block(plan, rows, rank)
    text_row = load_block(plan, text, rank) > 0
    chunk = 256

    def step(i, carry):
        cols = pl.ds(pl.multiple_of(i * chunk, chunk), chunk)
        parts = []
        for stream in range(2):
            weight = pair[stream, cols, :] if dims is CONTRACT_LAST else pair[stream, :, cols]
            parts.append(lax.dot_general(block, weight, dims, preferred_element_type=F32))
        out[:, cols] = jnp.where(text_row, parts[1], parts[0])
        return carry

    lax.fori_loop(0, plan.width // chunk, step, 0)


def scatter_sum(*args):
    return scatter_start(*args)()


def scatter_start(plan, seq, rank, rows, pair, text, dims, away, near, going, coming,
                  pair_send, pair_recv, far_send, far_recv):
    half = plan.group // 2
    chip, core = lax.div(rank, 2), lax.rem(rank, 2)
    partner = plan.device_of(seq, 2 * chip + 1 - core)
    order = list(range(1, half)) + [0]

    def pair_copy(step):
        return remote(away.at[step], near.at[step], pair_send.at[step], pair_recv.at[step], partner)

    def far_copy(step):
        to = plan.device_of(seq, 2 * other(chip, step, half) + core)
        return remote(going.at[step - 1], coming.at[step - 1], far_send.at[step], far_recv.at[step], to)

    def turn(i, carry):
        for_partner = (i < 2) | (lax.rem(i, 2) == 1) & (i < 2 * half - 1)
        place = jnp.where(i < 2, i, jnp.where(for_partner, lax.div(i + 1, 2), lax.div(i, 2) - 1))
        place = jnp.where(i == 2 * half - 1, half - 1, place)
        step = other(place, 1, half)
        block = 2 * other(chip, step, half) + jnp.where(for_partner, 1 - core, core)
        product(plan, rows, pair, text, dims, block, away.at[jnp.where(for_partner, step, half)])

        @pl.when(for_partner)
        def _():
            pair_copy(step).start()

        @pl.when(jnp.logical_not(for_partner))
        def _():
            pair_copy(step).wait_recv()
            away[half] = away[half] + near[step]

        @pl.when(jnp.logical_not(for_partner) & (place < half - 1))
        def _():
            going[step - 1] = away[half].astype(going.dtype)
            far_copy(step).start()

        return carry

    lax.fori_loop(0, 2 * half, turn, 0)

    def result():
        total = away[half]
        for step in range(1, half):
            far_copy(step).wait_recv()
            total = total + coming[step - 1].astype(F32)
        for step in range(half):
            pair_copy(step).wait_send()
        for step in range(1, half):
            far_copy(step).wait_send()
        return total

    return result


def share_scratch(plan):
    return [pltpu.SemaphoreType.DMA((plan.group, 2))] * 2 + [pltpu.SemaphoreType.DMA((plan.group, 2))]


def share_rows(plan, seq, rank, parts, window, send, recv, pass_send):
    half = plan.group // 2
    chip, core = lax.div(rank, 2), lax.rem(rank, 2)
    partner_rank = 2 * chip + 1 - core
    partner = plan.device_of(seq, partner_rank)

    def send_own(to_device, slot):
        copies = [
            remote(source, target, send.at[slot, i], recv.at[slot, i], to_device)
            for i, (source, target) in enumerate(zip(parts, block_parts(plan, window, rank)))
        ]
        for copy in copies:
            copy.start()
        return copies

    flying = {}
    for step in range(1, half):
        flying[step] = send_own(plan.device_of(seq, 2 * other(chip, step, half) + core), step)
    flying[0] = send_own(partner, 0)
    for source, target in zip(parts, block_parts(plan, window, rank)):
        target[...] = source[...]
    passed = []
    for step in range(1, half):
        for copy in flying[step]:
            copy.wait_recv()
        came = 2 * other(chip, half - step, half) + core
        copies = [
            remote(place, place, pass_send.at[step, i], recv.at[half + step, i], partner)
            for i, place in enumerate(block_parts(plan, window, came))
        ]
        for copy in copies:
            copy.start()
        passed.extend(copies)
    for copy in flying[0]:
        copy.wait_recv()
    for copy in passed:
        copy.wait_recv()
    for copies in flying.values():
        for copy in copies:
            copy.wait_send()
    for copy in passed:
        copy.wait_send()


def entry_kernel(plan, tokens, grads, mod_part, *refs):
    if plan.chip_heads:
        merge, merge_out, *refs = refs[:1] + refs[4:5] + refs[1:4] + refs[5:]
        merge_send, merge_recv, *refs = refs[-2:] + refs[:-2]
    (token_window, grad_window, mods, token_own, grad_own, plane, across, chunk, edge_send, edge_recv,
     t_send, t_recv, t_pass, g_send, g_recv, g_pass, m_send, m_recv) = refs
    device = lax.axis_index("dev")
    seq, rank = plan.place_of(device)
    meet(every_device(plan, device))
    swaps = []
    if plan.chip_heads:
        core = lax.rem(rank, 2)
        partner = plan.device_of(seq, 2 * lax.div(rank, 2) + 1 - core)
        for stream in range(2):
            copy = remote(
                merge.at[2 * stream + 1 - core],
                merge_out.at[stream, core],
                merge_send.at[stream],
                merge_recv.at[stream],
                partner,
            )
            copy.start()
            swaps.append(copy)
            merge_out[stream, core] = merge[2 * stream + core]
    hops = []
    for step in range(1, plan.group):
        to = other(rank, step, plan.group)
        copy = remote(mod_part.at[to], plane.at[step], m_send.at[0, step], m_recv.at[0, step], plan.device_of(seq, to))
        copy.start()
        hops.append(copy)
    arrays = ((tokens, token_own), (grads, grad_own))
    count = len(plan.segments)
    for which, (source, own) in enumerate(arrays):
        for index, (to_rank, row, rows, step, owner, owner_row) in enumerate(plan.segments):
            @pl.when(rank == owner)
            def _():
                remote(
                    source.at[pl.ds(owner_row, rows)],
                    own.at[pl.ds(row, rows)],
                    edge_send.at[which * count + index],
                    edge_recv.at[which * count + index],
                    plan.device_of(lax.rem(seq + plan.sequences - step, plan.sequences), to_rank),
                ).start()
    for copy in hops:
        copy.wait_recv()
    total = mod_part[rank]
    for step in range(1, plan.group):
        total = total + plane[step]
    plane[0] = total
    hops_across = []
    for step in range(1, plan.sequences):
        to = other(seq, step, plan.sequences)
        copy = remote(plane.at[0, to], across.at[seq], m_send.at[1, step], m_recv.at[1, step], plan.device_of(to, rank))
        copy.start()
        hops_across.append(copy)
    across[seq] = plane[0, seq]
    for which, (source, own) in enumerate(arrays):
        for index, (to_rank, row, rows, step, owner, owner_row) in enumerate(plan.segments):
            @pl.when(rank == to_rank)
            def _():
                remote(
                    source.at[pl.ds(owner_row, rows)],
                    own.at[pl.ds(row, rows)],
                    edge_send.at[which * count + index],
                    edge_recv.at[which * count + index],
                    plan.device_of(lax.rem(seq + plan.sequences + step, plan.sequences), owner),
                ).wait_recv()
    share_rows(plan, seq, rank, (tokens, token_own), token_window, t_send, t_recv, t_pass)
    for copy in hops_across:
        copy.wait_recv()
    half = plan.sequences // 2
    for stream in range(2):
        total = across[stream * half]
        for i in range(1, half):
            total = total + across[stream * half + i]
        chunk[stream] = total
    hops_back = []
    for step in range(1, plan.group):
        to = other(rank, step, plan.group)
        copy = remote(chunk, mods.at[rank], m_send.at[2, step], m_recv.at[2, step], plan.device_of(seq, to))
        copy.start()
        hops_back.append(copy)
    mods[rank] = chunk[...]
    share_rows(plan, seq, rank, (grads, grad_own), grad_window, g_send, g_recv, g_pass)
    for copy in hops_back:
        copy.wait_recv()
    for copy in hops + hops_across + hops_back:
        copy.wait_send()
    for copy in swaps:
        copy.wait()
    for which, (source, own) in enumerate(arrays):
        for index, (to_rank, row, rows, step, owner, owner_row) in enumerate(plan.segments):
            @pl.when(rank == owner)
            def _():
                remote(
                    source.at[pl.ds(owner_row, rows)],
                    own.at[pl.ds(row, rows)],
                    edge_send.at[which * count + index],
                    edge_recv.at[which * count + index],
                    plan.device_of(lax.rem(seq + plan.sequences - step, plan.sequences), to_rank),
                ).wait_send()


def entry(plan, tokens, grads, mod_part, merge):
    lanes = mod_part.shape[1] // plan.group // 128
    pieces = mod_part.reshape(plan.sequences, plan.group, lanes, 128).transpose(1, 0, 2, 3)
    window = jax.ShapeDtypeStruct((plan.rows, plan.width), BF16)
    dma = pltpu.SemaphoreType.DMA
    most = max(plan.group, plan.sequences)
    shapes = (window, window, jax.ShapeDtypeStruct((plan.group, 2, lanes, 128), F32))
    operands = (tokens, grads, pieces)
    scratch = (
        [
            pltpu.VMEM((plan.piece, plan.width), BF16),
            pltpu.VMEM((plan.piece, plan.width), BF16),
            pltpu.VMEM((plan.group, plan.sequences, lanes, 128), F32),
            pltpu.VMEM((plan.sequences, lanes, 128), F32),
            pltpu.VMEM((2, lanes, 128), F32),
            dma((2 * len(plan.segments),)),
            dma((2 * len(plan.segments),)),
        ]
        + share_scratch(plan)
        + share_scratch(plan)
        + [dma((3, most)), dma((3, most))]
    )
    if plan.chip_heads:
        shapes += (jax.ShapeDtypeStruct((2, 2) + merge.shape[1:], BF16),)
        operands += (merge,)
        scratch += [dma((2,)), dma((2,))]
    token_window, grad_window, mods, *rest = call(
        functools.partial(entry_kernel, plan), "entry", 1, shapes, scratch, operands
    )
    merge_pair = rest[0].reshape(2, -1, plan.width) if plan.chip_heads else merge
    return token_window, grad_window, mods.transpose(1, 0, 2, 3).reshape(2, -1), merge_pair


def project_columns(plan, rank):
    share = plan.width // plan.group
    first = (rank % 2) * (plan.width // 2) + (rank // 2) * share
    return [part * plan.width + first for part in range(3)], share


def up_columns(plan, rank, cols):
    planes = plan.sequences // 2
    share = cols // planes // plan.group
    return [plane * plan.group * share + rank * share for plane in range(planes)], share


def start_swap(plan, seq, rank, source, target, send, recv):
    copies = []
    for step in range(1, plan.group):
        to = other(rank, step, plan.group)
        copy = remote(source.at[to], target.at[rank], send.at[step], recv.at[step], plan.device_of(seq, to))
        copy.start()
        copies.append(copy)
    target[rank] = source[rank]
    return copies


def swap_in_kernel(plan, project, up, project_out, up_out, project_cut, up_cut, p_send, p_recv, u_send, u_recv):
    seq, rank = here(plan)
    for to in range(plan.group):
        starts, share = project_columns(plan, to)
        project_cut[to] = fold_rows(jnp.concatenate([project[:, c : c + share] for c in starts], axis=1))
    meet(group_devices(plan, seq, rank))
    copies = start_swap(plan, seq, rank, project_cut, project_out, p_send, p_recv)
    for to in range(plan.group):
        starts, share = up_columns(plan, to, up.shape[1])
        up_cut[to] = jnp.concatenate([up[:, c : c + share] for c in starts], axis=1)
    copies += start_swap(plan, seq, rank, up_cut, up_out, u_send, u_recv)
    for copy in copies:
        copy.wait()


def swap_in(plan, project, up):
    rows = project.shape[0]
    dma = pltpu.SemaphoreType.DMA
    shapes = [
        (plan.group, rows // 2, 2 * project.shape[1] // plan.group),
        (plan.group, rows, up.shape[1] // plan.group),
    ]
    return call(
        functools.partial(swap_in_kernel, plan),
        "swap_in",
        4,
        tuple(jax.ShapeDtypeStruct(shape, BF16) for shape in shapes),
        [pltpu.VMEM(shape, BF16) for shape in shapes] + [dma((plan.group,))] * 4,
        (project, up),
    )


def place_columns(plan, got, out, columns, unfold):
    for source in range(plan.group):
        starts, share = columns(plan, source)
        piece = unfold_rows(got[source]) if unfold else got[source]
        for i, c in enumerate(starts):
            out[:, c : c + share] = piece[:, i * share : (i + 1) * share]


def finish_kernel(plan, up, project, up_out, project_out, up_got, project_got, u_send, u_recv, p_send, p_recv):
    seq, rank = here(plan)
    meet(group_devices(plan, seq, rank))
    ups = start_swap(plan, seq, rank, up, up_got, u_send, u_recv)
    projects = start_swap(plan, seq, rank, project, project_got, p_send, p_recv)
    for copy in ups:
        copy.wait()
    place_columns(plan, up_got, up_out, lambda p, r: up_columns(p, r, up_out.shape[1]), False)
    for copy in projects:
        copy.wait()
    place_columns(plan, project_got, project_out, project_columns, True)


def finish(plan, up, project):
    dma = pltpu.SemaphoreType.DMA
    rows = up.shape[1]
    up_grad, project_grad = call(
        functools.partial(finish_kernel, plan),
        "finish",
        6,
        (
            jax.ShapeDtypeStruct((rows, plan.group * up.shape[2]), BF16),
            jax.ShapeDtypeStruct((rows, plan.group * project.shape[2] // 2), BF16),
        ),
        [pltpu.VMEM(up.shape, BF16), pltpu.VMEM(project.shape, BF16)] + [dma((plan.group,))] * 4,
        (up, project),
    )
    return up_grad.astype(F32), project_grad.astype(F32)


def pick_rows(table, text):
    return jnp.where(text > 0, table[1:2, :], table[0:1, :])


def norm_rows(values):
    mean = jnp.mean(values, axis=1, keepdims=True)
    centred = values - mean
    inv = lax.rsqrt(jnp.mean(centred * centred, axis=1, keepdims=True) + EPSILON)
    return centred * inv, inv


def middle_kernel(plan, rows, pair, window_text, tokens, gate_a, scale_b, shift_b, text, merged, window, own, *scratch):
    seq, rank = here(plan)
    meet(group_devices(plan, seq, rank))
    total = scatter_sum(plan, seq, rank, rows, pair, window_text, PLAIN, *scratch[:SUM_SCRATCH])
    merged[...] = total
    mask = text[...]
    middle = tokens[...].astype(F32) + pick_rows(gate_a[...], mask) * total
    normed, _ = norm_rows(middle)
    own[...] = (normed * (1.0 + pick_rows(scale_b[...], mask)) + pick_rows(shift_b[...], mask)).astype(BF16)
    share_rows(plan, seq, rank, own_parts(plan, own), window, *scratch[SUM_SCRATCH:])


def own_shape(plan, dtype=F32):
    return jax.ShapeDtypeStruct((plan.own, plan.width), dtype)


def window_shape(plan):
    return jax.ShapeDtypeStruct((plan.rows, plan.width), BF16)


def middle_rows(plan, rows, pair, window_text, tokens, gate_a, scale_b, shift_b, text):
    return call(
        functools.partial(middle_kernel, plan),
        "middle",
        2,
        (own_shape(plan), window_shape(plan)),
        [pltpu.VMEM((plan.own, plan.width), BF16)] + sum_scratch(plan, F32) + share_scratch(plan),
        (rows, pair, window_text, tokens, gate_a, scale_b, shift_b, text),
    )


def back_kernel(plan, rows, pair, window_text, grad, middle, gate_a, scale_b, text, grad_hidden, grad_middle, window, own, *scratch):
    seq, rank = here(plan)
    meet(group_devices(plan, seq, rank))
    total = scatter_sum(plan, seq, rank, rows, pair, window_text, CONTRACT_LAST, *scratch[:SUM_SCRATCH])
    grad_hidden[...] = total
    mask = text[...]
    normed, inv = norm_rows(middle[...])
    inner = total * (1.0 + pick_rows(scale_b[...], mask))
    mean_grad = jnp.mean(inner, axis=1, keepdims=True)
    mean_cross = jnp.mean(inner * normed, axis=1, keepdims=True)
    result = grad[...].astype(F32) + inv * (inner - mean_grad - normed * mean_cross)
    grad_middle[...] = result
    own[...] = (pick_rows(gate_a[...], mask) * result).astype(BF16)
    share_rows(plan, seq, rank, own_parts(plan, own), window, *scratch[SUM_SCRATCH:])


def back_rows(plan, rows, pair, window_text, grad, middle, gate_a, scale_b, text):
    return call(
        functools.partial(back_kernel, plan),
        "back",
        3,
        (own_shape(plan), own_shape(plan), window_shape(plan)),
        [pltpu.VMEM((plan.own, plan.width), BF16)] + sum_scratch(plan) + share_scratch(plan),
        (rows, pair, window_text, grad, middle, gate_a, scale_b, text),
    )


def edge_copy(plan, seq, source, first_row, target, send, recv, index):
    from_rank, row, rows, step, owner, owner_row = plan.segments[index]
    return remote(
        source.at[pl.ds(first_row + row, rows)],
        target.at[pl.ds(owner_row, rows)],
        send.at[index],
        recv.at[index],
        plan.device_of(lax.rem(seq + plan.sequences + step, plan.sequences), owner),
    )


def start_edges(plan, seq, rank, *refs):
    for index, segment in enumerate(plan.segments):
        @pl.when(rank == segment[0])
        def _():
            edge_copy(plan, seq, *refs, index).start()


def finish_edges(plan, seq, rank, *refs):
    for index, segment in enumerate(plan.segments):
        @pl.when(rank == segment[4])
        def _():
            edge_copy(plan, seq, *refs, index).wait_recv()

        @pl.when(rank == segment[0])
        def _():
            edge_copy(plan, seq, *refs, index).wait_send()


def edge_scratch(plan):
    return [pltpu.SemaphoreType.DMA((len(plan.segments),))] * 2


def stream_sums(values, masks):
    return jnp.concatenate([jnp.sum(values * mask, axis=0, keepdims=True) for mask in masks], axis=0)


def last_kernel(plan, names, *refs):
    at = types.SimpleNamespace(**dict(zip(names, refs)))
    low_scratch = refs[len(names) : len(names) + SUM_SCRATCH]
    back_scratch = refs[len(names) + SUM_SCRATCH : len(names) + 2 * SUM_SCRATCH]
    device = lax.axis_index("dev")
    seq, rank = plan.place_of(device)
    stream = lax.div(2 * seq, plan.sequences)
    at.layer_extra[...] = jnp.zeros_like(at.layer_extra)
    at.token_extra[...] = jnp.zeros_like(at.token_extra)
    meet(every_device(plan, device))
    low_sum = scatter_start(plan, seq, rank, at.activated, at.down_pair, at.window_text, PLAIN, *low_scratch)
    back_sum = scatter_start(plan, seq, rank, at.grads, at.project_pair, at.window_text, CONTRACT_LAST, *back_scratch)
    swaps = []
    if plan.chip_heads:
        core = lax.rem(rank, 2)
        partner = plan.device_of(seq, 2 * lax.div(rank, 2) + 1 - core)
        for j in range(2):
            copy = remote(
                at.term.at[j, 1 - core], at.term_out.at[2 * j + core], at.term_send.at[j], at.term_recv.at[j], partner
            )
            copy.start()
            swaps.append(copy)
            at.term_out[2 * j + core] = at.term[j, core]
    text = at.text[...]
    streams = (at.masks[:, 0:1], at.masks[:, 1:2])
    width = plan.width

    lowered = low_sum()
    at.layer_own[...] = (at.middle[...] + pick_rows(at.gate_b[...], text) * lowered).astype(BF16)
    layer_edges = (at.layer_own, plan.rows_dev, at.layer_extra, at.l_send, at.l_recv)
    start_edges(plan, seq, rank, *layer_edges)
    at.local[:, 5 * width :] = stream_sums(at.grad[...].astype(F32) * lowered, streams)
    at.local[:, 2 * width : 5 * width] = at.rest[...]
    at.layer[...] = at.layer_own[pl.ds(0, plan.rows_dev)]

    total = back_sum()
    normed, inv = norm_rows(at.tokens[...].astype(F32))
    at.local[:, :width] = stream_sums(total, streams)
    at.local[:, width : 2 * width] = stream_sums(total * normed, streams)
    cols = 6 * width // plan.group

    def chunk(index):
        return pl.ds(pl.multiple_of(index * cols, 128), cols)

    hops = []
    for step in range(1, plan.group):
        to = other(rank, step, plan.group)
        copy = remote(
            at.local.at[:, chunk(to)], at.first.at[step], at.t_send.at[0, step], at.t_recv.at[0, step], plan.device_of(seq, to)
        )
        copy.start()
        hops.append(copy)
    inner = total * (1.0 + pick_rows(at.scale_a[...], text))
    mean_grad = jnp.mean(inner, axis=1, keepdims=True)
    mean_cross = jnp.mean(inner * normed, axis=1, keepdims=True)
    at.token_own[...] = at.grad_middle[...] + inv * (inner - mean_grad - normed * mean_cross)
    token_edges = (at.token_own, plan.rows_dev, at.token_extra, at.e_send, at.e_recv)
    start_edges(plan, seq, rank, *token_edges)
    for copy in hops:
        copy.wait_recv()
    sums = at.local[:, chunk(rank)]
    for step in range(1, plan.group):
        sums = sums + at.first[step]
    for i in range(2):
        at.mine[i] = sums[i : i + 1]
    across = []
    for step in range(1, plan.sequences):
        to = other(seq, step, plan.sequences)
        to_stream = lax.div(2 * to, plan.sequences)
        copy = remote(
            at.mine.at[to_stream], at.second.at[seq], at.t_send.at[1, step], at.t_recv.at[1, step], plan.device_of(to, rank)
        )
        copy.start()
        across.append(copy)
    at.second[seq] = at.mine[stream]
    at.token[...] = at.token_own[pl.ds(0, plan.rows_dev)]
    for copy in across:
        copy.wait_recv()
    last = []
    for step in range(1, plan.group):
        to = other(rank, step, plan.group)
        copy = remote(at.second, at.table.at[rank], at.t_send.at[2, step], at.t_recv.at[2, step], plan.device_of(seq, to))
        copy.start()
        last.append(copy)
    at.table[rank] = at.second[...]
    for copy in last:
        copy.wait_recv()

    piece = None
    for index in range(plan.group):
        grads = jnp.concatenate([at.table[index, s] for s in range(plan.sequences)], axis=0).astype(BF16)
        part = lax.dot_general(
            grads, at.weight[:, index * cols : (index + 1) * cols], CONTRACT_LAST, preferred_element_type=F32
        )
        piece = part if piece is None else piece + part
    at.piece[...] = piece
    at.everyone[seq, rank] = piece
    spread = []
    for step in range(1, plan.group):
        to = other(rank, step, plan.group)
        copy = remote(
            at.piece, at.everyone.at[seq, rank], at.c_send.at[0, step], at.c_recv.at[0, step], plan.device_of(seq, to)
        )
        copy.start()
        spread.append(copy)
    for copy in spread:
        copy.wait_recv()
    for step in range(1, plan.sequences):
        to = other(seq, step, plan.sequences)
        copy = remote(
            at.everyone.at[seq], at.everyone.at[seq], at.c_send.at[1, step], at.c_recv.at[1, step], plan.device_of(to, rank)
        )
        copy.start()
        spread.append(copy)
    for copy in spread[plan.group - 1 :]:
        copy.wait_recv()
    for copy in hops + across + last + spread:
        copy.wait_send()
    for copy in swaps:
        copy.wait()
    finish_edges(plan, seq, rank, *layer_edges)
    finish_edges(plan, seq, rank, *token_edges)


def last_rows(plan, term, weight, **operands):
    rows, share = weight.shape[0], plan.width // plan.group // 2
    cols = 6 * plan.width // plan.group
    most = max(plan.group, plan.sequences)
    dma = pltpu.SemaphoreType.DMA

    def placed(dtype):
        return jax.ShapeDtypeStruct((plan.rows_dev, plan.width), dtype)

    operands = dict(operands, weight=weight)
    outs = dict(
        layer=placed(BF16),
        layer_extra=placed(BF16),
        token=placed(F32),
        token_extra=placed(F32),
        table=jax.ShapeDtypeStruct((plan.group, plan.sequences, 1, cols), F32),
        everyone=jax.ShapeDtypeStruct((plan.sequences, plan.group, plan.sequences, rows), F32),
    )
    edges = len(plan.segments)
    scratch = dict(
        layer_own=pltpu.VMEM((plan.own, plan.width), BF16),
        token_own=pltpu.VMEM((plan.own, plan.width), F32),
        local=pltpu.VMEM((2, 6 * plan.width), F32),
        first=pltpu.VMEM((plan.group, 2, cols), F32),
        second=pltpu.VMEM((plan.sequences, 1, cols), F32),
        mine=pltpu.VMEM((2, 1, cols), F32),
        piece=pltpu.VMEM((plan.sequences, rows), F32),
        t_send=dma((3, most)),
        t_recv=dma((3, most)),
        c_send=dma((2, most)),
        c_recv=dma((2, most)),
        l_send=dma((edges,)),
        l_recv=dma((edges,)),
        e_send=dma((edges,)),
        e_recv=dma((edges,)),
    )
    if plan.chip_heads:
        operands["term"] = term.reshape(2, 2, share, plan.width)
        outs["term_out"] = jax.ShapeDtypeStruct((plan.sequences, share, plan.width), BF16)
        scratch.update(term_send=dma((2,)), term_recv=dma((2,)))
    names = tuple(operands) + tuple(outs) + tuple(scratch)
    got = call(
        functools.partial(last_kernel, plan, names),
        "last",
        10,
        tuple(outs.values()),
        list(scratch.values()) + sum_scratch(plan) + sum_scratch(plan),
        tuple(operands.values()),
        vmem=58 << 20,
    )
    got = types.SimpleNamespace(**dict(zip(outs, got)))
    got.table = got.table[:, :, 0].transpose(1, 0, 2).reshape(plan.sequences, -1)
    got.term = got.term_out if plan.chip_heads else term
    return got


def over_sequences(plan, pieces):
    full = lax.all_gather(pieces, "dev", axis=0, axis_index_groups=plan.rank_groups())
    return full.reshape((plan.devices,) + pieces.shape[1:])


def over_sequences_sum(plan, pieces):
    return lax.psum_scatter(pieces, "dev", scatter_dimension=0, axis_index_groups=plan.rank_groups())


def merge_rows(plan, weight, rank):
    if plan.chip_heads:
        return lax.all_gather(weight, "dev", axis=0, axis_index_groups=plan.rank_groups())
    share = plan.width // plan.group
    full = lax.all_gather(weight, "dev", axis=0, tiled=True)
    full = full.reshape(2, 2, plan.group // 2, share, weight.shape[1])
    full = lax.dynamic_index_in_dim(full, lax.rem(rank, 2), 1, keepdims=False)
    return lax.dynamic_index_in_dim(full, lax.div(rank, 2), 1, keepdims=False)


def merge_sum(plan, term, rank):
    if plan.chip_heads:
        return over_sequences_sum(plan, term)
    half = plan.group // 2
    _, share, cols = term.shape
    mine = [jnp.where(lax.rem(rank, 2) == k, term, jnp.zeros((), BF16)) for k in range(2)]
    full = jnp.zeros((2, 2, half, share, cols), BF16)
    full = lax.dynamic_update_slice_in_dim(full, jnp.stack(mine, axis=1)[:, :, None], lax.div(rank, 2), 2)
    return lax.psum_scatter(full.reshape(-1, cols), "dev", scatter_dimension=0, tiled=True)


def down_slices(plan, weight):
    full = lax.all_gather(weight, "dev", axis=0, axis_index_groups=plan.rank_groups())
    return full.reshape(2, -1, weight.shape[1])


def pick(table, text_rows):
    return jnp.where(text_rows[:, None], table[1][None, :], table[0][None, :])


def on_device(
    tokens,
    conditioning,
    text_lengths,
    modulation_weight,
    project_weight,
    merge_weight,
    up_weight,
    down_weight,
    cotangent,
):
    rows_dev, width = tokens.shape
    mod_rows = modulation_weight.shape[0]
    plan = Plan(lax.axis_size("dev"), conditioning.shape[0], rows_dev, width)
    device = lax.axis_index("dev")
    seq, rank = plan.place_of(device)
    feature_start = device * mod_rows % width

    ends = jnp.cumsum(IMG + text_lengths)
    starts = jnp.concatenate([jnp.zeros((1,), jnp.int32), ends[:-1]])
    positions = device * rows_dev + jnp.arange(rows_dev, dtype=jnp.int32)
    row_seq = jnp.sum((starts[None, :] <= positions[:, None]).astype(jnp.int32), axis=1) - 1
    offset = plan.span * seq - plan.edge + jnp.arange(plan.rows, dtype=jnp.int32) - starts[seq]
    valid = (offset >= 0) & (offset < IMG + text_lengths[seq])
    is_text = offset >= IMG
    bias = jnp.where(valid, 0.0, MASKED).astype(F32)[None, :]
    window_text = is_text.astype(F32)[:, None]
    own_valid = own_rows(plan, valid[:, None], rank)[:, 0]
    own_text = own_rows(plan, is_text[:, None], rank)[:, 0]

    cond_float = conditioning.astype(F32)
    silu_low = jax.nn.silu(cond_float).astype(BF16)
    silu_part = lax.dynamic_slice_in_dim(silu_low, feature_start, mod_rows, 1)
    mod_part = jnp.dot(silu_part, modulation_weight, preferred_element_type=F32)

    merge_pair = merge_rows(plan, merge_weight, rank)
    project_pieces, up_pieces = swap_in(plan, project_weight, up_weight)
    project_pieces, up_pieces, merge_pair = lax.optimization_barrier((project_pieces, up_pieces, merge_pair))
    project_pair = over_sequences(plan, project_pieces)
    share = project_pair.shape[2] // 2
    project_pair = jnp.concatenate([project_pair[:, :, :share], project_pair[:, :, share:]], axis=1)
    project_pair = lax.optimization_barrier(project_pair.reshape(2, width, share))
    up_pair = over_sequences(plan, up_pieces).reshape(2, width, -1)
    down_pair = down_slices(plan, down_weight)

    token_window, grad_window, mods, merge_pair = entry(plan, tokens, cotangent, mod_part, merge_pair)
    shift_a, scale_a, gate_a, shift_b, scale_b, gate_b = jnp.split(mods, 6, axis=1)
    grad_window = jnp.where(valid[:, None], grad_window, jnp.zeros((), BF16))

    cols = project_pair.shape[2]
    hidden_a, projected = stream_rows(
        plan, project_kernel, 128, cols, True, "project", ((width, BF16), (cols, BF16)),
        token_window, project_pair, window_text, shift_a, scale_a,
    )
    attended = attend(plan, projected, bias)

    own_tokens = own_rows(plan, token_window, rank)
    own_grad = own_rows(plan, grad_window, rank)
    text_mask = own_text.astype(F32)[:, None]
    merged, hidden_b = middle_rows(
        plan, attended, merge_pair, window_text, own_tokens, gate_a, scale_b, shift_b, text_mask
    )
    middle = own_tokens.astype(F32) + pick(gate_a, own_text) * merged
    normed_b, inv_b = layer_norm(middle)

    units = up_pair.shape[2]
    upper, activated = stream_rows(
        plan, up_kernel, 128, units, False, "up", ((units, F32), (units, BF16)), hidden_b, up_pair, window_text
    )
    grad_lowered = (pick(gate_b, is_text) * grad_window.astype(F32)).astype(BF16)
    down_term = weight_terms(plan, activated, grad_lowered, window_text, "down_terms")
    down_term = down_term.reshape(plan.sequences, -1, width)
    down_term, grad_lowered = lax.optimization_barrier((down_term, grad_lowered))
    down_sum = over_sequences_sum(plan, down_term)
    (grad_upper,) = stream_rows(
        plan, down_back_kernel, 128, units, True, "down_back", ((units, BF16),),
        grad_lowered, down_pair, window_text, upper,
    )
    up_term = weight_terms(plan, hidden_b, grad_upper, window_text, "up_terms")
    up_term = up_term.reshape(plan.sequences, plan.group, mod_rows, -1)
    grad_upper, up_term = lax.optimization_barrier((grad_upper, up_term))
    up_sum = over_sequences_sum(plan, up_term)
    grad_hidden_b, grad_middle, grad_merged = back_rows(
        plan, grad_upper, up_pair, window_text, own_grad, middle, gate_a, scale_b, text_mask
    )
    merge_term = weight_terms(plan, attended, grad_merged, window_text, "merge_terms")

    grad_projected = attend_back(plan, projected, grad_merged, merge_pair, window_text, bias)
    grad_projected, down_sum = lax.optimization_barrier((grad_projected, down_sum))
    down_grad = down_sum.astype(F32)
    project_term = weight_terms(plan, hidden_a, grad_projected, window_text, "project_terms", mod_rows)
    project_term = project_term.reshape((plan.sequences, plan.group) + project_term.shape[1:])
    grad_projected, project_term = lax.optimization_barrier((grad_projected, project_term))
    project_sum = over_sequences_sum(plan, project_term)

    masks = jnp.stack([own_valid & ~own_text, own_valid & own_text], axis=1).astype(F32)
    rest = jnp.concatenate(
        [
            jnp.stack([jnp.sum(value * masks[:, j : j + 1], axis=0) for j in range(2)])
            for value in (grad_middle * merged, grad_hidden_b, grad_hidden_b * normed_b)
        ],
        axis=1,
    )
    got = last_rows(
        plan,
        merge_term,
        modulation_weight,
        activated=activated,
        down_pair=down_pair,
        grads=grad_projected,
        project_pair=project_pair,
        window_text=window_text,
        tokens=own_tokens,
        middle=middle,
        grad=own_grad,
        grad_middle=grad_middle,
        gate_b=gate_b,
        scale_a=scale_a,
        text=text_mask,
        masks=masks,
        rest=rest,
    )
    foreign = (row_seq != seq)[:, None]
    layer_out = jnp.where(foreign, got.layer_extra, got.layer)
    tokens_grad = jnp.where(foreign, got.token_extra, got.token)
    own_grads = got.table.astype(BF16)
    modulation_grad = lax.dot_general(silu_part, own_grads, CONTRACT_FIRST, preferred_element_type=F32)
    everyone = got.everyone.reshape(2, plan.devices // 2, plan.sequences, mod_rows)
    grad_silu = (everyone[0] + everyone[1]).transpose(1, 0, 2).reshape(plan.sequences, width)
    conditioning_grad = jax.vjp(jax.nn.silu, cond_float)[1](grad_silu)[0]
    modulation_grad, up_sum = lax.optimization_barrier((modulation_grad, up_sum))
    merge_out, project_sum, *done = lax.optimization_barrier(
        (got.term, project_sum, modulation_grad, down_grad, layer_out, tokens_grad, conditioning_grad)
    )
    modulation_grad, down_grad, layer_out, tokens_grad, conditioning_grad = done
    merge_grad = merge_sum(plan, merge_out, rank).reshape(merge_weight.shape).astype(F32)
    up_grad, project_grad = finish(plan, up_sum, project_sum)
    return (
        layer_out,
        tokens_grad,
        conditioning_grad,
        modulation_grad,
        project_grad,
        merge_grad,
        up_grad,
        down_grad,
    )


def solution(mesh):
    shard, whole = P("dev", None), P()
    return jax.shard_map(
        on_device,
        mesh=mesh,
        in_specs=(shard, whole, whole, shard, shard, shard, shard, shard, shard),
        out_specs=(shard, shard, whole, shard, shard, shard, shard, shard),
        check_vma=False,
    )
```

```python
import functools
import types

import jax
import jax.numpy as jnp
import numpy as np
from jax import lax
from jax.experimental import pallas as pl
from jax.experimental.pallas import tpu as pltpu
from jax.sharding import PartitionSpec as P

HEADS = 24
HDIM = 64
IMG = 1024
TXT_MIN = 86
TXT_MAX = 154
EPSILON = 1e-06
F32 = jnp.float32
BF16 = jnp.bfloat16
CONTRACT_LAST = (((1,), (1,)), ((), ()))
PLAIN = (((1,), (0,)), ((), ()))
CONTRACT_FIRST = (((0,), (0,)), ((), ()))
MASKED = -1e30


class Plan:
    def __init__(self, devices, sequences, rows_dev, width):
        self.devices, self.sequences, self.rows_dev, self.width = devices, sequences, rows_dev, width
        self.group = devices // sequences
        self.span = self.group * rows_dev
        mean = self.span - IMG
        up, down = TXT_MAX - mean, mean - TXT_MIN
        drift = 0
        for k in range(sequences + 1):
            drift = max(drift, min(up * k, down * (sequences - k)), min(down * k, up * (sequences - k)))
        self.edge = -(-drift // 64) * 64
        self.rows = self.span + 2 * self.edge
        self.piece = 2 * self.edge // self.group
        self.own = rows_dev + self.piece
        self.image_end = -(-(self.edge + drift + IMG) // 128) * 128
        self.text_start = (self.edge - drift + IMG) // 128 * 128
        self.heads = HEADS // self.group
        self.segments = self.edge_segments()
        self.chip_heads = devices == 4 * self.group

    def device_of(self, seq, rank):
        return seq * self.group + rank

    def place_of(self, device):
        return lax.div(device, self.group), lax.rem(device, self.group)

    def seq_groups(self):
        return [[self.device_of(s, r) for r in range(self.group)] for s in range(self.sequences)]

    def rank_groups(self):
        return [[self.device_of(s, r) for s in range(self.sequences)] for r in range(self.group)]

    def edge_row(self, rank):
        half = self.group // 2
        return jnp.where(rank < half, self.piece * rank, self.edge + self.span + self.piece * (rank - half))

    def main_row(self, rank):
        return self.edge + self.rows_dev * rank

    def edge_segments(self):
        found = []
        for rank in range(self.group):
            half = self.group // 2
            first = self.piece * rank - self.edge if rank < half else self.span + self.piece * (rank - half)
            row = 0
            while row < self.piece:
                owner, owner_row = (first + row) // self.rows_dev, (first + row) % self.rows_dev
                count = min(self.piece - row, self.rows_dev - owner_row)
                found.append((rank, row, count, owner // self.group, owner % self.group, owner_row))
                row += count
        return found


def layer_norm(values):
    mean = jnp.mean(values, axis=-1, keepdims=True)
    centred = values - mean
    variance = jnp.mean(centred * centred, axis=-1, keepdims=True)
    inv_std = lax.rsqrt(variance + EPSILON)
    return (centred * inv_std, inv_std)


def norm_back(grad_normed, normed, inv_std):
    mean_grad = jnp.mean(grad_normed, axis=-1, keepdims=True)
    mean_cross = jnp.mean(grad_normed * normed, axis=-1, keepdims=True)
    return inv_std * (grad_normed - mean_grad - normed * mean_cross)


def softmax_parts(query, key, bias):
    scores = lax.dot_general(query, key, CONTRACT_LAST, preferred_element_type=F32) + bias
    top = jnp.max(scores, axis=1, keepdims=True)
    exponent = jnp.exp(scores - top)
    total = jnp.sum(exponent, axis=1, keepdims=True)
    return exponent * (1.0 / total)


def head_columns(heads, part, head):
    first = (part * heads + head) * HDIM
    return slice(first, first + HDIM)


def attend_kernel(heads, block, projected, bias_ref, out_ref):
    rows = pl.ds(pl.multiple_of(pl.program_id(0) * block, block), block)
    bias = bias_ref[...]
    outs = []
    for head in range(heads):
        query = projected[rows, head_columns(heads, 0, head)] * jnp.asarray(HDIM ** (-0.5), BF16)
        probs = softmax_parts(query, projected[:, head_columns(heads, 1, head)], bias).astype(BF16)
        outs.append(jnp.dot(probs, projected[:, head_columns(heads, 2, head)], preferred_element_type=F32))
    out_ref[...] = jnp.concatenate(outs, axis=1).astype(BF16)


def block_rows(rows, most):
    return most if rows % most == 0 else 128


def constant(shape):
    return pl.BlockSpec(shape, lambda i: (0,) * len(shape))


def attend(plan, projected, bias):
    rows, cols = projected.shape[0], projected.shape[1] // 3
    block = block_rows(rows, 128)
    return pl.pallas_call(
        functools.partial(attend_kernel, plan.heads, block),
        out_shape=jax.ShapeDtypeStruct((rows, cols), BF16),
        grid=(rows // block,),
        in_specs=[constant(projected.shape), constant(bias.shape)],
        out_specs=pl.BlockSpec((block, cols), lambda i: (i, 0)),
        compiler_params=pltpu.CompilerParams(vmem_limit_bytes=48 << 20),
        cost_estimate=pl.CostEstimate(flops=16 * rows * rows * cols, bytes_accessed=8 * rows * cols, transcendentals=0),
        name="attend",
    )(projected, bias)


def attend_back_kernel(
    heads, steps, block, projected, grad_merged, merge_pair, text, bias_ref, out, key_sum, value_sum
):
    step = pl.program_id(0)
    scale = jnp.asarray(HDIM ** (-0.5), BF16)

    @pl.when(step == 0)
    def _():
        key_sum[...] = jnp.zeros_like(key_sum)
        value_sum[...] = jnp.zeros_like(value_sum)

    rows = pl.ds(pl.multiple_of(step * block, block), block)
    bias = bias_ref[...]
    image, other_stream = [
        lax.dot_general(grad_merged[...], merge_pair[j], CONTRACT_LAST, preferred_element_type=F32) for j in range(2)
    ]
    grad_attended = jnp.where(text[...] > 0, other_stream, image).astype(BF16)
    grads = []
    for head in range(heads):
        query = projected[rows, head_columns(heads, 0, head)] * scale
        key = projected[:, head_columns(heads, 1, head)]
        grad_out = grad_attended[:, head * HDIM : (head + 1) * HDIM]
        probs = softmax_parts(query, key, bias)
        grad_probs = lax.dot_general(
            grad_out, projected[:, head_columns(heads, 2, head)], CONTRACT_LAST, preferred_element_type=F32
        )
        inner = jnp.sum(probs * grad_probs, axis=1, keepdims=True)
        grad_scores = (probs * (grad_probs - inner)).astype(BF16)
        grads.append(jnp.dot(grad_scores, key, preferred_element_type=F32) * HDIM ** (-0.5))
        key_sum[head] += lax.dot_general(query, grad_scores, CONTRACT_FIRST, preferred_element_type=F32)
        value_sum[head] += lax.dot_general(grad_out, probs.astype(BF16), CONTRACT_FIRST, preferred_element_type=F32)
    cols = heads * HDIM
    out[rows, :cols] = jnp.concatenate(grads, axis=1).astype(BF16)

    @pl.when(step == steps - 1)
    def _():
        total = out.shape[0]
        out[:, cols : 2 * cols] = key_sum[...].reshape(cols, total).T.astype(BF16)
        out[:, 2 * cols :] = value_sum[...].reshape(cols, total).T.astype(BF16)


def attend_back(plan, projected, grad_merged, merge_pair, text, bias):
    rows, cols = projected.shape[0], projected.shape[1] // 3
    block = block_rows(rows, 256)
    return pl.pallas_call(
        functools.partial(attend_back_kernel, plan.heads, rows // block, block),
        out_shape=jax.ShapeDtypeStruct(projected.shape, BF16),
        grid=(rows // block,),
        in_specs=[
            constant(projected.shape),
            pl.BlockSpec((block, plan.width), lambda i: (i, 0)),
            constant(merge_pair.shape),
            pl.BlockSpec((block, 1), lambda i: (i, 0)),
            constant(bias.shape),
        ],
        out_specs=constant(projected.shape),
        scratch_shapes=[pltpu.VMEM((plan.heads, HDIM, rows), F32)] * 2,
        compiler_params=pltpu.CompilerParams(vmem_limit_bytes=56 << 20),
        cost_estimate=pl.CostEstimate(flops=40 * rows * rows * cols, bytes_accessed=14 * rows * cols, transcendentals=0),
        name="attend_back",
    )(projected, grad_merged, merge_pair, text, bias)


def fold_rows(piece):
    half = piece.shape[0] // 2
    return jnp.concatenate([piece[:half], piece[half:]], axis=1)


def unfold_rows(piece):
    half = piece.shape[1] // 2
    return jnp.concatenate([piece[:, :half], piece[:, half:]], axis=0)


def terms_kernel(plan, fold, chunk, rows, grads, text, out, kept):
    width = rows.shape[1]
    for stream, (first, last) in enumerate(((0, plan.image_end), (plan.text_start, plan.rows))):
        count = last - first
        mask = text[pl.ds(first, count)]
        keep = (mask > 0) if stream else (mask <= 0)
        kept[pl.ds(0, count)] = jnp.where(keep, grads[pl.ds(first, count)], jnp.zeros((), BF16))

        def step(i, carry):
            start = pl.multiple_of(i * chunk, chunk)
            term = lax.dot_general(
                rows[pl.ds(first, count), pl.ds(start, chunk)],
                kept[pl.ds(0, count)],
                CONTRACT_FIRST,
                preferred_element_type=F32,
            ).astype(BF16)
            if fold:
                for j in range(chunk // fold):
                    out[(stream * width) // fold + i * (chunk // fold) + j] = fold_rows(term[j * fold : (j + 1) * fold])
            else:
                out[stream, pl.ds(start, chunk)] = term
            return carry

        if width == chunk:
            step(0, 0)
        else:
            lax.fori_loop(0, width // chunk, step, 0)


def weight_terms(plan, rows, grads, text, name, fold=0):
    width, cols = rows.shape[1], grads.shape[1]
    chunk = 384 if fold else 256 if width % 256 == 0 else width
    shape = (2 * width // fold, fold // 2, 2 * cols) if fold else (2, width, cols)
    return pl.pallas_call(
        functools.partial(terms_kernel, plan, fold, chunk),
        out_shape=jax.ShapeDtypeStruct(shape, BF16),
        in_specs=[pl.BlockSpec(memory_space=pltpu.VMEM)] * 3,
        out_specs=pl.BlockSpec(memory_space=pltpu.VMEM),
        scratch_shapes=[pltpu.VMEM((plan.image_end, cols), BF16)],
        compiler_params=pltpu.CompilerParams(vmem_limit_bytes=40 << 20),
        cost_estimate=pl.CostEstimate(flops=3 * plan.rows * width * cols, bytes_accessed=1 << 23, transcendentals=0),
        name=name,
    )(rows, grads, text)


def gelu(values):
    return jax.nn.gelu(values, approximate=True)


def in_blocks(plan, size, body):
    def step(i, carry):
        body(i, pl.ds(pl.multiple_of(i * size, size), size))
        return carry

    lax.fori_loop(0, plan.rows // size, step, 0)


def blockwise(plan, i, size, block, pair, dims, mask, out):
    @pl.when(i * size < plan.image_end)
    def _():
        out[...] = lax.dot_general(block, pair[0], dims, preferred_element_type=F32)

    @pl.when(i * size + size > plan.text_start)
    def _():
        out[...] = jnp.where(mask > 0, lax.dot_general(block, pair[1], dims, preferred_element_type=F32), out[...])


def project_kernel(plan, size, rows, pair, text, shift, scale, hidden, out, held):
    def body(i, place):
        mask = text[place]
        normed, _ = norm_rows(rows[place].astype(F32))
        block = (normed * (1.0 + pick_rows(scale[...], mask)) + pick_rows(shift[...], mask)).astype(BF16)
        hidden[place] = block
        blockwise(plan, i, size, block, pair, PLAIN, mask, held)
        out[place] = held[...].astype(BF16)

    in_blocks(plan, size, body)


def up_kernel(plan, size, rows, pair, text, upper, activated):
    def body(i, place):
        blockwise(plan, i, size, rows[place], pair, PLAIN, text[place], upper.at[place])
        activated[place] = gelu(upper[place]).astype(BF16)

    in_blocks(plan, size, body)


def down_back_kernel(plan, size, rows, pair, text, upper, out, held):
    def body(i, place):
        blockwise(plan, i, size, rows[place], pair, CONTRACT_LAST, text[place], held)
        out[place] = jax.vjp(gelu, upper[place])[1](held[...])[0].astype(BF16)

    in_blocks(plan, size, body)


def stream_rows(plan, kernel, size, cols, held, name, outs, *operands):
    spec = pl.BlockSpec(memory_space=pltpu.VMEM)
    shapes = tuple(jax.ShapeDtypeStruct((plan.rows, width), dtype) for width, dtype in outs)
    return pl.pallas_call(
        functools.partial(kernel, plan, size),
        out_shape=shapes,
        in_specs=[spec] * len(operands),
        out_specs=(spec,) * len(shapes),
        scratch_shapes=[pltpu.VMEM((size, cols), F32)] if held else [],
        compiler_params=pltpu.CompilerParams(vmem_limit_bytes=40 << 20),
        cost_estimate=pl.CostEstimate(
            flops=2 * plan.rows * plan.width * cols, bytes_accessed=1 << 24, transcendentals=0
        ),
        name=name,
    )(*operands)


VMEM = pl.BlockSpec(memory_space=pltpu.VMEM)


def own_rows(plan, window, rank):
    main = lax.dynamic_slice_in_dim(window, plan.main_row(rank), plan.rows_dev, 0)
    edge = lax.dynamic_slice_in_dim(window, plan.edge_row(rank), plan.piece, 0)
    return jnp.concatenate([main, edge], axis=0)


def remote(source, target, send_sem, recv_sem, device):
    return pltpu.make_async_remote_copy(
        src_ref=source,
        dst_ref=target,
        send_sem=send_sem,
        recv_sem=recv_sem,
        device_id=(device,),
        device_id_type=pl.DeviceIdType.MESH,
    )


def here(plan):
    return plan.place_of(lax.axis_index("dev"))


def other(rank, step, size):
    return lax.rem(rank + step, size)


def meet(devices):
    barrier = pltpu.get_barrier_semaphore()
    for device in devices:
        pl.semaphore_signal(barrier, inc=1, device_id=(device,), device_id_type=pl.DeviceIdType.MESH)
    pl.semaphore_wait(barrier, len(devices))


def group_devices(plan, seq, rank):
    return [plan.device_of(seq, other(rank, step, plan.group)) for step in range(1, plan.group)]


def column_devices(plan, seq, rank):
    return [plan.device_of(other(seq, step, plan.sequences), rank) for step in range(1, plan.sequences)]


def every_device(plan, device):
    return [other(device, step, plan.devices) for step in range(1, plan.devices)]


def call(kernel, name, ident, out_shape, scratch, operands, in_specs=None, out_specs=None, vmem=40 << 20):
    outs = out_shape if isinstance(out_shape, tuple) else (out_shape,)
    return pl.pallas_call(
        kernel,
        out_shape=out_shape,
        in_specs=in_specs or [VMEM] * len(operands),
        out_specs=out_specs or (tuple([VMEM] * len(outs)) if isinstance(out_shape, tuple) else VMEM),
        scratch_shapes=scratch,
        compiler_params=pltpu.CompilerParams(
            collective_id=ident, has_side_effects=True, vmem_limit_bytes=vmem
        ),
        name=name,
    )(*operands)


def aligned(start):
    return pl.multiple_of(start, 16)


def block_parts(plan, ref, rank):
    return (
        ref.at[pl.ds(aligned(plan.main_row(rank)), plan.rows_dev)],
        ref.at[pl.ds(aligned(plan.edge_row(rank)), plan.piece)],
    )


def own_parts(plan, ref):
    return ref.at[pl.ds(0, plan.rows_dev)], ref.at[pl.ds(plan.rows_dev, plan.piece)]


def load_block(plan, ref, rank):
    main, edge = block_parts(plan, ref, rank)
    return jnp.concatenate([main[...], edge[...]], axis=0)


def sum_scratch(plan, wire=BF16):
    half, own, width = plan.group // 2, plan.own, plan.width
    return [
        pltpu.VMEM((half + 1, own, width), F32),
        pltpu.VMEM((half, own, width), F32),
        pltpu.VMEM((half - 1, own, width), wire),
        pltpu.VMEM((half - 1, own, width), wire),
        pltpu.SemaphoreType.DMA((half,)),
        pltpu.SemaphoreType.DMA((half,)),
        pltpu.SemaphoreType.DMA((half,)),
        pltpu.SemaphoreType.DMA((half,)),
    ]


SUM_SCRATCH = 8


def product(plan, rows, pair, text, dims, rank, out):
    block = load_block(plan, rows, rank)
    text_row = load_block(plan, text, rank) > 0
    chunk = 256

    def step(i, carry):
        cols = pl.ds(pl.multiple_of(i * chunk, chunk), chunk)
        parts = []
        for stream in range(2):
            weight = pair[stream, cols, :] if dims is CONTRACT_LAST else pair[stream, :, cols]
            parts.append(lax.dot_general(block, weight, dims, preferred_element_type=F32))
        out[:, cols] = jnp.where(text_row, parts[1], parts[0])
        return carry

    lax.fori_loop(0, plan.width // chunk, step, 0)


def scatter_start(plan, seq, rank, rows, pair, text, dims, away, near, going, coming,
                  pair_send, pair_recv, far_send, far_recv):
    half = plan.group // 2
    chip, core = lax.div(rank, 2), lax.rem(rank, 2)
    partner = plan.device_of(seq, 2 * chip + 1 - core)
    order = list(range(1, half)) + [0]

    def pair_copy(step):
        return remote(away.at[step], near.at[step], pair_send.at[step], pair_recv.at[step], partner)

    def far_copy(step):
        to = plan.device_of(seq, 2 * other(chip, step, half) + core)
        return remote(going.at[step - 1], coming.at[step - 1], far_send.at[step], far_recv.at[step], to)

    def turn(i, carry):
        for_partner = (i < 2) | (lax.rem(i, 2) == 1) & (i < 2 * half - 1)
        place = jnp.where(i < 2, i, jnp.where(for_partner, lax.div(i + 1, 2), lax.div(i, 2) - 1))
        place = jnp.where(i == 2 * half - 1, half - 1, place)
        step = other(place, 1, half)
        block = 2 * other(chip, step, half) + jnp.where(for_partner, 1 - core, core)
        product(plan, rows, pair, text, dims, block, away.at[jnp.where(for_partner, step, half)])

        @pl.when(for_partner)
        def _():
            pair_copy(step).start()

        @pl.when(jnp.logical_not(for_partner))
        def _():
            pair_copy(step).wait_recv()
            away[half] = away[half] + near[step]

        @pl.when(jnp.logical_not(for_partner) & (place < half - 1))
        def _():
            going[step - 1] = away[half].astype(going.dtype)
            far_copy(step).start()

        return carry

    lax.fori_loop(0, 2 * half, turn, 0)

    def result(use):
        for step in range(1, half):
            far_copy(step).wait_recv()
        size = 32 if plan.own % 32 == 0 else 16

        def some(i, carry):
            place = pl.ds(pl.multiple_of(i * size, size), size)
            total = away[half, place]
            for step in range(1, half):
                total = total + coming[step - 1, place].astype(F32)
            use(place, total)
            return carry

        lax.fori_loop(0, plan.own // size, some, 0)
        for step in range(half):
            pair_copy(step).wait_send()
        for step in range(1, half):
            far_copy(step).wait_send()

    return result


def share_scratch(plan):
    return [pltpu.SemaphoreType.DMA((plan.group, 2))] * 2 + [pltpu.SemaphoreType.DMA((plan.group, 2))]


def share_rows(plan, seq, rank, parts, window, send, recv, pass_send):
    half = plan.group // 2
    chip, core = lax.div(rank, 2), lax.rem(rank, 2)
    partner_rank = 2 * chip + 1 - core
    partner = plan.device_of(seq, partner_rank)

    def send_own(to_device, slot):
        copies = [
            remote(source, target, send.at[slot, i], recv.at[slot, i], to_device)
            for i, (source, target) in enumerate(zip(parts, block_parts(plan, window, rank)))
        ]
        for copy in copies:
            copy.start()
        return copies

    flying = {}
    for step in range(1, half):
        flying[step] = send_own(plan.device_of(seq, 2 * other(chip, step, half) + core), step)
    flying[0] = send_own(partner, 0)
    for source, target in zip(parts, block_parts(plan, window, rank)):
        target[...] = source[...]
    passed = []
    for step in range(1, half):
        for copy in flying[step]:
            copy.wait_recv()
        came = 2 * other(chip, half - step, half) + core
        copies = [
            remote(place, place, pass_send.at[step, i], recv.at[half + step, i], partner)
            for i, place in enumerate(block_parts(plan, window, came))
        ]
        for copy in copies:
            copy.start()
        passed.extend(copies)
    for copy in flying[0]:
        copy.wait_recv()
    for copy in passed:
        copy.wait_recv()
    for copies in flying.values():
        for copy in copies:
            copy.wait_send()
    for copy in passed:
        copy.wait_send()


def entry_kernel(plan, tokens, grads, mod_part, *refs):
    if plan.chip_heads:
        merge, merge_out, *refs = refs[:1] + refs[4:5] + refs[1:4] + refs[5:]
        merge_send, merge_recv, *refs = refs[-2:] + refs[:-2]
    (token_window, grad_window, mods, token_own, grad_own, plane, across, chunk, edge_send, edge_recv,
     t_send, t_recv, t_pass, g_send, g_recv, g_pass, m_send, m_recv) = refs
    device = lax.axis_index("dev")
    seq, rank = plan.place_of(device)
    meet(every_device(plan, device))
    swaps = []
    if plan.chip_heads:
        core = lax.rem(rank, 2)
        partner = plan.device_of(seq, 2 * lax.div(rank, 2) + 1 - core)
        for stream in range(2):
            copy = remote(
                merge.at[2 * stream + 1 - core],
                merge_out.at[stream, core],
                merge_send.at[stream],
                merge_recv.at[stream],
                partner,
            )
            copy.start()
            swaps.append(copy)
            merge_out[stream, core] = merge[2 * stream + core]
    hops = []
    for step in range(1, plan.group):
        to = other(rank, step, plan.group)
        copy = remote(mod_part.at[to], plane.at[step], m_send.at[0, step], m_recv.at[0, step], plan.device_of(seq, to))
        copy.start()
        hops.append(copy)
    arrays = ((tokens, token_own), (grads, grad_own))
    count = len(plan.segments)
    for which, (source, own) in enumerate(arrays):
        for index, (to_rank, row, rows, step, owner, owner_row) in enumerate(plan.segments):
            @pl.when(rank == owner)
            def _():
                remote(
                    source.at[pl.ds(owner_row, rows)],
                    own.at[pl.ds(row, rows)],
                    edge_send.at[which * count + index],
                    edge_recv.at[which * count + index],
                    plan.device_of(lax.rem(seq + plan.sequences - step, plan.sequences), to_rank),
                ).start()
    for copy in hops:
        copy.wait_recv()
    total = mod_part[rank]
    for step in range(1, plan.group):
        total = total + plane[step]
    plane[0] = total
    hops_across = []
    for step in range(1, plan.sequences):
        to = other(seq, step, plan.sequences)
        copy = remote(plane.at[0, to], across.at[seq], m_send.at[1, step], m_recv.at[1, step], plan.device_of(to, rank))
        copy.start()
        hops_across.append(copy)
    across[seq] = plane[0, seq]
    for which, (source, own) in enumerate(arrays):
        for index, (to_rank, row, rows, step, owner, owner_row) in enumerate(plan.segments):
            @pl.when(rank == to_rank)
            def _():
                remote(
                    source.at[pl.ds(owner_row, rows)],
                    own.at[pl.ds(row, rows)],
                    edge_send.at[which * count + index],
                    edge_recv.at[which * count + index],
                    plan.device_of(lax.rem(seq + plan.sequences + step, plan.sequences), owner),
                ).wait_recv()
    share_rows(plan, seq, rank, (tokens, token_own), token_window, t_send, t_recv, t_pass)
    for copy in hops_across:
        copy.wait_recv()
    half = plan.sequences // 2
    for stream in range(2):
        total = across[stream * half]
        for i in range(1, half):
            total = total + across[stream * half + i]
        chunk[stream] = total
    hops_back = []
    for step in range(1, plan.group):
        to = other(rank, step, plan.group)
        copy = remote(chunk, mods.at[rank], m_send.at[2, step], m_recv.at[2, step], plan.device_of(seq, to))
        copy.start()
        hops_back.append(copy)
    mods[rank] = chunk[...]
    share_rows(plan, seq, rank, (grads, grad_own), grad_window, g_send, g_recv, g_pass)
    for copy in hops_back:
        copy.wait_recv()
    for copy in hops + hops_across + hops_back:
        copy.wait_send()
    for copy in swaps:
        copy.wait()
    for which, (source, own) in enumerate(arrays):
        for index, (to_rank, row, rows, step, owner, owner_row) in enumerate(plan.segments):
            @pl.when(rank == owner)
            def _():
                remote(
                    source.at[pl.ds(owner_row, rows)],
                    own.at[pl.ds(row, rows)],
                    edge_send.at[which * count + index],
                    edge_recv.at[which * count + index],
                    plan.device_of(lax.rem(seq + plan.sequences - step, plan.sequences), to_rank),
                ).wait_send()


def entry(plan, tokens, grads, mod_part, merge):
    lanes = mod_part.shape[1] // plan.group // 128
    pieces = mod_part.reshape(plan.sequences, plan.group, lanes, 128).transpose(1, 0, 2, 3)
    window = jax.ShapeDtypeStruct((plan.rows, plan.width), BF16)
    dma = pltpu.SemaphoreType.DMA
    most = max(plan.group, plan.sequences)
    shapes = (window, window, jax.ShapeDtypeStruct((plan.group, 2, lanes, 128), F32))
    operands = (tokens, grads, pieces)
    scratch = (
        [
            pltpu.VMEM((plan.piece, plan.width), BF16),
            pltpu.VMEM((plan.piece, plan.width), BF16),
            pltpu.VMEM((plan.group, plan.sequences, lanes, 128), F32),
            pltpu.VMEM((plan.sequences, lanes, 128), F32),
            pltpu.VMEM((2, lanes, 128), F32),
            dma((2 * len(plan.segments),)),
            dma((2 * len(plan.segments),)),
        ]
        + share_scratch(plan)
        + share_scratch(plan)
        + [dma((3, most)), dma((3, most))]
    )
    if plan.chip_heads:
        shapes += (jax.ShapeDtypeStruct((2, 2) + merge.shape[1:], BF16),)
        operands += (merge,)
        scratch += [dma((2,)), dma((2,))]
    token_window, grad_window, mods, *rest = call(
        functools.partial(entry_kernel, plan), "entry", 1, shapes, scratch, operands
    )
    merge_pair = rest[0].reshape(2, -1, plan.width) if plan.chip_heads else merge
    return token_window, grad_window, mods.transpose(1, 0, 2, 3).reshape(2, -1), merge_pair


def project_columns(plan, rank):
    share = plan.width // plan.group
    first = (rank % 2) * (plan.width // 2) + (rank // 2) * share
    return [part * plan.width + first for part in range(3)], share


def up_columns(plan, rank, cols):
    planes = plan.sequences // 2
    share = cols // planes // plan.group
    return [plane * plan.group * share + rank * share for plane in range(planes)], share


def start_swap(plan, seq, rank, source, target, send, recv):
    copies = []
    for step in range(1, plan.group):
        to = other(rank, step, plan.group)
        copy = remote(source.at[to], target.at[rank], send.at[step], recv.at[step], plan.device_of(seq, to))
        copy.start()
        copies.append(copy)
    target[rank] = source[rank]
    return copies


def swap_in_kernel(plan, project, up, project_out, up_out, project_cut, up_cut, p_send, p_recv, u_send, u_recv):
    seq, rank = here(plan)
    for to in range(plan.group):
        starts, share = project_columns(plan, to)
        project_cut[to] = fold_rows(jnp.concatenate([project[:, c : c + share] for c in starts], axis=1))
    meet(group_devices(plan, seq, rank))
    copies = start_swap(plan, seq, rank, project_cut, project_out, p_send, p_recv)
    for to in range(plan.group):
        starts, share = up_columns(plan, to, up.shape[1])
        up_cut[to] = jnp.concatenate([up[:, c : c + share] for c in starts], axis=1)
    copies += start_swap(plan, seq, rank, up_cut, up_out, u_send, u_recv)
    for copy in copies:
        copy.wait()


def swap_in(plan, project, up):
    rows = project.shape[0]
    dma = pltpu.SemaphoreType.DMA
    shapes = [
        (plan.group, rows // 2, 2 * project.shape[1] // plan.group),
        (plan.group, rows, up.shape[1] // plan.group),
    ]
    return call(
        functools.partial(swap_in_kernel, plan),
        "swap_in",
        4,
        tuple(jax.ShapeDtypeStruct(shape, BF16) for shape in shapes),
        [pltpu.VMEM(shape, BF16) for shape in shapes] + [dma((plan.group,))] * 4,
        (project, up),
    )


def place_columns(plan, got, out, columns, unfold):
    for source in range(plan.group):
        starts, share = columns(plan, source)
        piece = unfold_rows(got[source]) if unfold else got[source]
        for i, c in enumerate(starts):
            out[:, c : c + share] = piece[:, i * share : (i + 1) * share]


def finish_kernel(plan, up, project, up_out, project_out, up_got, project_got, u_send, u_recv, p_send, p_recv):
    seq, rank = here(plan)
    meet(group_devices(plan, seq, rank))
    ups = start_swap(plan, seq, rank, up, up_got, u_send, u_recv)
    projects = start_swap(plan, seq, rank, project, project_got, p_send, p_recv)
    for copy in ups:
        copy.wait()
    place_columns(plan, up_got, up_out, lambda p, r: up_columns(p, r, up_out.shape[1]), False)
    for copy in projects:
        copy.wait()
    place_columns(plan, project_got, project_out, project_columns, True)


def finish(plan, up, project):
    dma = pltpu.SemaphoreType.DMA
    rows = up.shape[1]
    up_grad, project_grad = call(
        functools.partial(finish_kernel, plan),
        "finish",
        6,
        (
            jax.ShapeDtypeStruct((rows, plan.group * up.shape[2]), BF16),
            jax.ShapeDtypeStruct((rows, plan.group * project.shape[2] // 2), BF16),
        ),
        [pltpu.VMEM(up.shape, BF16), pltpu.VMEM(project.shape, BF16)] + [dma((plan.group,))] * 4,
        (up, project),
    )
    return up_grad.astype(F32), project_grad.astype(F32)


def pick_rows(table, text):
    return jnp.where(text > 0, table[1:2, :], table[0:1, :])


def norm_rows(values):
    mean = jnp.mean(values, axis=1, keepdims=True)
    centred = values - mean
    inv = lax.rsqrt(jnp.mean(centred * centred, axis=1, keepdims=True) + EPSILON)
    return centred * inv, inv


def middle_kernel(plan, rows, pair, window_text, tokens, gate_a, scale_b, shift_b, text, merged, window, own, *scratch):
    seq, rank = here(plan)
    meet(group_devices(plan, seq, rank))
    result = scatter_start(plan, seq, rank, rows, pair, window_text, PLAIN, *scratch[:SUM_SCRATCH])

    def use(place, total):
        merged[place] = total
        mask = text[place]
        middle = tokens[place].astype(F32) + pick_rows(gate_a[...], mask) * total
        normed, _ = norm_rows(middle)
        own[place] = (normed * (1.0 + pick_rows(scale_b[...], mask)) + pick_rows(shift_b[...], mask)).astype(BF16)

    result(use)
    share_rows(plan, seq, rank, own_parts(plan, own), window, *scratch[SUM_SCRATCH:])


def own_shape(plan, dtype=F32):
    return jax.ShapeDtypeStruct((plan.own, plan.width), dtype)


def window_shape(plan):
    return jax.ShapeDtypeStruct((plan.rows, plan.width), BF16)


def middle_rows(plan, rows, pair, window_text, tokens, gate_a, scale_b, shift_b, text):
    return call(
        functools.partial(middle_kernel, plan),
        "middle",
        2,
        (own_shape(plan), window_shape(plan)),
        [pltpu.VMEM((plan.own, plan.width), BF16)] + sum_scratch(plan, F32) + share_scratch(plan),
        (rows, pair, window_text, tokens, gate_a, scale_b, shift_b, text),
    )


def back_kernel(plan, rows, pair, window_text, grad, middle, gate_a, scale_b, text, grad_hidden, grad_middle, window, own, *scratch):
    seq, rank = here(plan)
    meet(group_devices(plan, seq, rank))
    result = scatter_start(plan, seq, rank, rows, pair, window_text, CONTRACT_LAST, *scratch[:SUM_SCRATCH])

    def use(place, total):
        grad_hidden[place] = total
        mask = text[place]
        normed, inv = norm_rows(middle[place])
        inner = total * (1.0 + pick_rows(scale_b[...], mask))
        mean_grad = jnp.mean(inner, axis=1, keepdims=True)
        mean_cross = jnp.mean(inner * normed, axis=1, keepdims=True)
        back = grad[place].astype(F32) + inv * (inner - mean_grad - normed * mean_cross)
        grad_middle[place] = back
        own[place] = (pick_rows(gate_a[...], mask) * back).astype(BF16)

    result(use)
    share_rows(plan, seq, rank, own_parts(plan, own), window, *scratch[SUM_SCRATCH:])


def back_rows(plan, rows, pair, window_text, grad, middle, gate_a, scale_b, text):
    return call(
        functools.partial(back_kernel, plan),
        "back",
        3,
        (own_shape(plan), own_shape(plan), window_shape(plan)),
        [pltpu.VMEM((plan.own, plan.width), BF16)] + sum_scratch(plan) + share_scratch(plan),
        (rows, pair, window_text, grad, middle, gate_a, scale_b, text),
    )


def edge_copy(plan, seq, source, first_row, target, send, recv, index):
    from_rank, row, rows, step, owner, owner_row = plan.segments[index]
    return remote(
        source.at[pl.ds(first_row + row, rows)],
        target.at[pl.ds(owner_row, rows)],
        send.at[index],
        recv.at[index],
        plan.device_of(lax.rem(seq + plan.sequences + step, plan.sequences), owner),
    )


def start_edges(plan, seq, rank, *refs):
    for index, segment in enumerate(plan.segments):
        @pl.when(rank == segment[0])
        def _():
            edge_copy(plan, seq, *refs, index).start()


def finish_edges(plan, seq, rank, *refs):
    for index, segment in enumerate(plan.segments):
        @pl.when(rank == segment[4])
        def _():
            edge_copy(plan, seq, *refs, index).wait_recv()

        @pl.when(rank == segment[0])
        def _():
            edge_copy(plan, seq, *refs, index).wait_send()


def edge_scratch(plan):
    return [pltpu.SemaphoreType.DMA((len(plan.segments),))] * 2


def stream_sums(values, masks):
    return jnp.concatenate([jnp.sum(values * mask, axis=0, keepdims=True) for mask in masks], axis=0)


def last_kernel(plan, names, *refs):
    at = types.SimpleNamespace(**dict(zip(names, refs)))
    low_scratch = refs[len(names) : len(names) + SUM_SCRATCH]
    back_scratch = refs[len(names) + SUM_SCRATCH : len(names) + 2 * SUM_SCRATCH]
    device = lax.axis_index("dev")
    seq, rank = plan.place_of(device)
    stream = lax.div(2 * seq, plan.sequences)
    at.layer_extra[...] = jnp.zeros_like(at.layer_extra)
    at.token_extra[...] = jnp.zeros_like(at.token_extra)
    meet(every_device(plan, device))
    low_sum = scatter_start(plan, seq, rank, at.activated, at.down_pair, at.window_text, PLAIN, *low_scratch)
    back_sum = scatter_start(plan, seq, rank, at.grads, at.project_pair, at.window_text, CONTRACT_LAST, *back_scratch)
    swaps = []
    if plan.chip_heads:
        core = lax.rem(rank, 2)
        partner = plan.device_of(seq, 2 * lax.div(rank, 2) + 1 - core)
        for j in range(2):
            copy = remote(
                at.term.at[j, 1 - core], at.term_out.at[2 * j + core], at.term_send.at[j], at.term_recv.at[j], partner
            )
            copy.start()
            swaps.append(copy)
            at.term_out[2 * j + core] = at.term[j, core]
    width = plan.width
    at.local[...] = jnp.zeros_like(at.local)
    at.local[:, 2 * width : 5 * width] = at.rest[...]

    def add(first, place, values):
        masks = (at.masks[place, 0:1], at.masks[place, 1:2])
        at.local[:, first * width : (first + 1) * width] += stream_sums(values, masks)

    def use_low(place, lowered):
        at.layer_own[place] = (at.middle[place] + pick_rows(at.gate_b[...], at.text[place]) * lowered).astype(BF16)
        add(5, place, at.grad[place].astype(F32) * lowered)

    low_sum(use_low)
    layer_edges = (at.layer_own, plan.rows_dev, at.layer_extra, at.l_send, at.l_recv)
    start_edges(plan, seq, rank, *layer_edges)
    at.layer[...] = at.layer_own[pl.ds(0, plan.rows_dev)]

    def use_back(place, total):
        normed, inv = norm_rows(at.tokens[place].astype(F32))
        add(0, place, total)
        add(1, place, total * normed)
        inner = total * (1.0 + pick_rows(at.scale_a[...], at.text[place]))
        mean_grad = jnp.mean(inner, axis=1, keepdims=True)
        mean_cross = jnp.mean(inner * normed, axis=1, keepdims=True)
        at.token_own[place] = at.grad_middle[place] + inv * (inner - mean_grad - normed * mean_cross)

    back_sum(use_back)
    cols = 6 * width // plan.group

    def chunk(index):
        return pl.ds(pl.multiple_of(index * cols, 128), cols)

    hops = []
    for step in range(1, plan.group):
        to = other(rank, step, plan.group)
        copy = remote(
            at.local.at[:, chunk(to)], at.first.at[step], at.t_send.at[0, step], at.t_recv.at[0, step], plan.device_of(seq, to)
        )
        copy.start()
        hops.append(copy)
    token_edges = (at.token_own, plan.rows_dev, at.token_extra, at.e_send, at.e_recv)
    start_edges(plan, seq, rank, *token_edges)
    for copy in hops:
        copy.wait_recv()
    sums = at.local[:, chunk(rank)]
    for step in range(1, plan.group):
        sums = sums + at.first[step]
    for i in range(2):
        at.mine[i] = sums[i : i + 1]
    across = []
    for step in range(1, plan.sequences):
        to = other(seq, step, plan.sequences)
        to_stream = lax.div(2 * to, plan.sequences)
        copy = remote(
            at.mine.at[to_stream], at.second.at[seq], at.t_send.at[1, step], at.t_recv.at[1, step], plan.device_of(to, rank)
        )
        copy.start()
        across.append(copy)
    at.second[seq] = at.mine[stream]
    at.token[...] = at.token_own[pl.ds(0, plan.rows_dev)]
    for copy in across:
        copy.wait_recv()
    last = []
    for step in range(1, plan.group):
        to = other(rank, step, plan.group)
        copy = remote(at.second, at.table.at[rank], at.t_send.at[2, step], at.t_recv.at[2, step], plan.device_of(seq, to))
        copy.start()
        last.append(copy)
    at.table[rank] = at.second[...]
    for copy in last:
        copy.wait_recv()

    piece = None
    for index in range(plan.group):
        grads = jnp.concatenate([at.table[index, s] for s in range(plan.sequences)], axis=0).astype(BF16)
        part = lax.dot_general(
            grads, at.weight[:, index * cols : (index + 1) * cols], CONTRACT_LAST, preferred_element_type=F32
        )
        piece = part if piece is None else piece + part
    at.piece[...] = piece
    at.everyone[seq, rank] = piece
    spread = []
    for step in range(1, plan.group):
        to = other(rank, step, plan.group)
        copy = remote(
            at.piece, at.everyone.at[seq, rank], at.c_send.at[0, step], at.c_recv.at[0, step], plan.device_of(seq, to)
        )
        copy.start()
        spread.append(copy)
    for copy in spread:
        copy.wait_recv()
    for step in range(1, plan.sequences):
        to = other(seq, step, plan.sequences)
        copy = remote(
            at.everyone.at[seq], at.everyone.at[seq], at.c_send.at[1, step], at.c_recv.at[1, step], plan.device_of(to, rank)
        )
        copy.start()
        spread.append(copy)
    for copy in spread[plan.group - 1 :]:
        copy.wait_recv()
    for copy in hops + across + last + spread:
        copy.wait_send()
    for copy in swaps:
        copy.wait()
    finish_edges(plan, seq, rank, *layer_edges)
    finish_edges(plan, seq, rank, *token_edges)


def last_rows(plan, term, weight, **operands):
    rows, share = weight.shape[0], plan.width // plan.group // 2
    cols = 6 * plan.width // plan.group
    most = max(plan.group, plan.sequences)
    dma = pltpu.SemaphoreType.DMA

    def placed(dtype):
        return jax.ShapeDtypeStruct((plan.rows_dev, plan.width), dtype)

    operands = dict(operands, weight=weight)
    outs = dict(
        layer=placed(BF16),
        layer_extra=placed(BF16),
        token=placed(F32),
        token_extra=placed(F32),
        table=jax.ShapeDtypeStruct((plan.group, plan.sequences, 1, cols), F32),
        everyone=jax.ShapeDtypeStruct((plan.sequences, plan.group, plan.sequences, rows), F32),
    )
    edges = len(plan.segments)
    scratch = dict(
        layer_own=pltpu.VMEM((plan.own, plan.width), BF16),
        token_own=pltpu.VMEM((plan.own, plan.width), F32),
        local=pltpu.VMEM((2, 6 * plan.width), F32),
        first=pltpu.VMEM((plan.group, 2, cols), F32),
        second=pltpu.VMEM((plan.sequences, 1, cols), F32),
        mine=pltpu.VMEM((2, 1, cols), F32),
        piece=pltpu.VMEM((plan.sequences, rows), F32),
        t_send=dma((3, most)),
        t_recv=dma((3, most)),
        c_send=dma((2, most)),
        c_recv=dma((2, most)),
        l_send=dma((edges,)),
        l_recv=dma((edges,)),
        e_send=dma((edges,)),
        e_recv=dma((edges,)),
    )
    if plan.chip_heads:
        operands["term"] = term.reshape(2, 2, share, plan.width)
        outs["term_out"] = jax.ShapeDtypeStruct((plan.sequences, share, plan.width), BF16)
        scratch.update(term_send=dma((2,)), term_recv=dma((2,)))
    names = tuple(operands) + tuple(outs) + tuple(scratch)
    got = call(
        functools.partial(last_kernel, plan, names),
        "last",
        10,
        tuple(outs.values()),
        list(scratch.values()) + sum_scratch(plan) + sum_scratch(plan),
        tuple(operands.values()),
        vmem=58 << 20,
    )
    got = types.SimpleNamespace(**dict(zip(outs, got)))
    got.table = got.table[:, :, 0].transpose(1, 0, 2).reshape(plan.sequences, -1)
    got.term = got.term_out if plan.chip_heads else term
    return got


def over_sequences(plan, pieces):
    full = lax.all_gather(pieces, "dev", axis=0, axis_index_groups=plan.rank_groups())
    return full.reshape((plan.devices,) + pieces.shape[1:])


def over_sequences_sum(plan, pieces):
    return lax.psum_scatter(pieces, "dev", scatter_dimension=0, axis_index_groups=plan.rank_groups())


def merge_rows(plan, weight, rank):
    if plan.chip_heads:
        return lax.all_gather(weight, "dev", axis=0, axis_index_groups=plan.rank_groups())
    share = plan.width // plan.group
    full = lax.all_gather(weight, "dev", axis=0, tiled=True)
    full = full.reshape(2, 2, plan.group // 2, share, weight.shape[1])
    full = lax.dynamic_index_in_dim(full, lax.rem(rank, 2), 1, keepdims=False)
    return lax.dynamic_index_in_dim(full, lax.div(rank, 2), 1, keepdims=False)


def merge_sum(plan, term, rank):
    if plan.chip_heads:
        return over_sequences_sum(plan, term)
    half = plan.group // 2
    _, share, cols = term.shape
    mine = [jnp.where(lax.rem(rank, 2) == k, term, jnp.zeros((), BF16)) for k in range(2)]
    full = jnp.zeros((2, 2, half, share, cols), BF16)
    full = lax.dynamic_update_slice_in_dim(full, jnp.stack(mine, axis=1)[:, :, None], lax.div(rank, 2), 2)
    return lax.psum_scatter(full.reshape(-1, cols), "dev", scatter_dimension=0, tiled=True)


def down_slices(plan, weight):
    full = lax.all_gather(weight, "dev", axis=0, axis_index_groups=plan.rank_groups())
    return full.reshape(2, -1, weight.shape[1])


def pick(table, text_rows):
    return jnp.where(text_rows[:, None], table[1][None, :], table[0][None, :])


def on_device(
    tokens,
    conditioning,
    text_lengths,
    modulation_weight,
    project_weight,
    merge_weight,
    up_weight,
    down_weight,
    cotangent,
):
    rows_dev, width = tokens.shape
    mod_rows = modulation_weight.shape[0]
    plan = Plan(lax.axis_size("dev"), conditioning.shape[0], rows_dev, width)
    device = lax.axis_index("dev")
    seq, rank = plan.place_of(device)
    feature_start = device * mod_rows % width

    ends = jnp.cumsum(IMG + text_lengths)
    starts = jnp.concatenate([jnp.zeros((1,), jnp.int32), ends[:-1]])
    positions = device * rows_dev + jnp.arange(rows_dev, dtype=jnp.int32)
    row_seq = jnp.sum((starts[None, :] <= positions[:, None]).astype(jnp.int32), axis=1) - 1
    offset = plan.span * seq - plan.edge + jnp.arange(plan.rows, dtype=jnp.int32) - starts[seq]
    valid = (offset >= 0) & (offset < IMG + text_lengths[seq])
    is_text = offset >= IMG
    bias = jnp.where(valid, 0.0, MASKED).astype(F32)[None, :]
    window_text = is_text.astype(F32)[:, None]
    own_valid = own_rows(plan, valid[:, None], rank)[:, 0]
    own_text = own_rows(plan, is_text[:, None], rank)[:, 0]

    cond_float = conditioning.astype(F32)
    silu_low = jax.nn.silu(cond_float).astype(BF16)
    silu_part = lax.dynamic_slice_in_dim(silu_low, feature_start, mod_rows, 1)
    mod_part = jnp.dot(silu_part, modulation_weight, preferred_element_type=F32)

    merge_pair = merge_rows(plan, merge_weight, rank)
    project_pieces, up_pieces = swap_in(plan, project_weight, up_weight)
    project_pieces, up_pieces, merge_pair = lax.optimization_barrier((project_pieces, up_pieces, merge_pair))
    project_pair = over_sequences(plan, project_pieces)
    share = project_pair.shape[2] // 2
    project_pair = jnp.concatenate([project_pair[:, :, :share], project_pair[:, :, share:]], axis=1)
    project_pair = lax.optimization_barrier(project_pair.reshape(2, width, share))
    up_pair = over_sequences(plan, up_pieces).reshape(2, width, -1)
    down_pair = down_slices(plan, down_weight)

    token_window, grad_window, mods, merge_pair = entry(plan, tokens, cotangent, mod_part, merge_pair)
    shift_a, scale_a, gate_a, shift_b, scale_b, gate_b = jnp.split(mods, 6, axis=1)
    grad_window = jnp.where(valid[:, None], grad_window, jnp.zeros((), BF16))

    cols = project_pair.shape[2]
    hidden_a, projected = stream_rows(
        plan, project_kernel, 128, cols, True, "project", ((width, BF16), (cols, BF16)),
        token_window, project_pair, window_text, shift_a, scale_a,
    )
    attended = attend(plan, projected, bias)

    own_tokens = own_rows(plan, token_window, rank)
    own_grad = own_rows(plan, grad_window, rank)
    text_mask = own_text.astype(F32)[:, None]
    merged, hidden_b = middle_rows(
        plan, attended, merge_pair, window_text, own_tokens, gate_a, scale_b, shift_b, text_mask
    )
    middle = own_tokens.astype(F32) + pick(gate_a, own_text) * merged
    normed_b, inv_b = layer_norm(middle)

    units = up_pair.shape[2]
    upper, activated = stream_rows(
        plan, up_kernel, 128, units, False, "up", ((units, F32), (units, BF16)), hidden_b, up_pair, window_text
    )
    grad_lowered = (pick(gate_b, is_text) * grad_window.astype(F32)).astype(BF16)
    down_term = weight_terms(plan, activated, grad_lowered, window_text, "down_terms")
    down_term = down_term.reshape(plan.sequences, -1, width)
    down_term, grad_lowered = lax.optimization_barrier((down_term, grad_lowered))
    down_sum = over_sequences_sum(plan, down_term)
    (grad_upper,) = stream_rows(
        plan, down_back_kernel, block_rows(plan.rows, 256), units, True, "down_back", ((units, BF16),),
        grad_lowered, down_pair, window_text, upper,
    )
    up_term = weight_terms(plan, hidden_b, grad_upper, window_text, "up_terms")
    up_term = up_term.reshape(plan.sequences, plan.group, mod_rows, -1)
    grad_upper, up_term = lax.optimization_barrier((grad_upper, up_term))
    up_sum = over_sequences_sum(plan, up_term)
    grad_hidden_b, grad_middle, grad_merged = back_rows(
        plan, grad_upper, up_pair, window_text, own_grad, middle, gate_a, scale_b, text_mask
    )
    merge_term = weight_terms(plan, attended, grad_merged, window_text, "merge_terms")

    grad_projected = attend_back(plan, projected, grad_merged, merge_pair, window_text, bias)
    grad_projected, down_sum = lax.optimization_barrier((grad_projected, down_sum))
    down_grad = down_sum.astype(F32)
    project_term = weight_terms(plan, hidden_a, grad_projected, window_text, "project_terms", mod_rows)
    project_term = project_term.reshape((plan.sequences, plan.group) + project_term.shape[1:])
    grad_projected, project_term = lax.optimization_barrier((grad_projected, project_term))
    project_sum = over_sequences_sum(plan, project_term)

    masks = jnp.stack([own_valid & ~own_text, own_valid & own_text], axis=1).astype(F32)
    rest = jnp.concatenate(
        [
            jnp.stack([jnp.sum(value * masks[:, j : j + 1], axis=0) for j in range(2)])
            for value in (grad_middle * merged, grad_hidden_b, grad_hidden_b * normed_b)
        ],
        axis=1,
    )
    got = last_rows(
        plan,
        merge_term,
        modulation_weight,
        activated=activated,
        down_pair=down_pair,
        grads=grad_projected,
        project_pair=project_pair,
        window_text=window_text,
        tokens=own_tokens,
        middle=middle,
        grad=own_grad,
        grad_middle=grad_middle,
        gate_b=gate_b,
        scale_a=scale_a,
        text=text_mask,
        masks=masks,
        rest=rest,
    )
    foreign = (row_seq != seq)[:, None]
    layer_out = jnp.where(foreign, got.layer_extra, got.layer)
    tokens_grad = jnp.where(foreign, got.token_extra, got.token)
    own_grads = got.table.astype(BF16)
    modulation_grad = lax.dot_general(silu_part, own_grads, CONTRACT_FIRST, preferred_element_type=F32)
    everyone = got.everyone.reshape(2, plan.devices // 2, plan.sequences, mod_rows)
    grad_silu = (everyone[0] + everyone[1]).transpose(1, 0, 2).reshape(plan.sequences, width)
    conditioning_grad = jax.vjp(jax.nn.silu, cond_float)[1](grad_silu)[0]
    modulation_grad, up_sum = lax.optimization_barrier((modulation_grad, up_sum))
    merge_out, project_sum, *done = lax.optimization_barrier(
        (got.term, project_sum, modulation_grad, down_grad, layer_out, tokens_grad, conditioning_grad)
    )
    modulation_grad, down_grad, layer_out, tokens_grad, conditioning_grad = done
    merge_grad = merge_sum(plan, merge_out, rank).reshape(merge_weight.shape).astype(F32)
    up_grad, project_grad = finish(plan, up_sum, project_sum)
    return (
        layer_out,
        tokens_grad,
        conditioning_grad,
        modulation_grad,
        project_grad,
        merge_grad,
        up_grad,
        down_grad,
    )


def solution(mesh):
    shard, whole = P("dev", None), P()
    return jax.shard_map(
        on_device,
        mesh=mesh,
        in_specs=(shard, whole, whole, shard, shard, shard, shard, shard, shard),
        out_specs=(shard, shard, whole, shard, shard, shard, shard, shard),
        check_vma=False,
    )
```

```python
import functools
import types

import jax
import jax.numpy as jnp
import numpy as np
from jax import lax
from jax.experimental import pallas as pl
from jax.experimental.pallas import tpu as pltpu
from jax.sharding import PartitionSpec as P

HEADS = 24
HDIM = 64
IMG = 1024
TXT_MIN = 86
TXT_MAX = 154
EPSILON = 1e-06
F32 = jnp.float32
BF16 = jnp.bfloat16
CONTRACT_LAST = (((1,), (1,)), ((), ()))
PLAIN = (((1,), (0,)), ((), ()))
CONTRACT_FIRST = (((0,), (0,)), ((), ()))
MASKED = -1e30


class Plan:
    def __init__(self, devices, sequences, rows_dev, width):
        self.devices, self.sequences, self.rows_dev, self.width = devices, sequences, rows_dev, width
        self.group = devices // sequences
        self.span = self.group * rows_dev
        mean = self.span - IMG
        up, down = TXT_MAX - mean, mean - TXT_MIN
        drift = 0
        for k in range(sequences + 1):
            drift = max(drift, min(up * k, down * (sequences - k)), min(down * k, up * (sequences - k)))
        self.edge = -(-drift // 64) * 64
        self.rows = self.span + 2 * self.edge
        self.piece = 2 * self.edge // self.group
        self.own = rows_dev + self.piece
        self.image_end = -(-(self.edge + drift + IMG) // 128) * 128
        self.text_start = (self.edge - drift + IMG) // 128 * 128
        self.heads = HEADS // self.group
        self.segments = self.edge_segments()
        self.chip_heads = devices == 4 * self.group

    def device_of(self, seq, rank):
        return seq * self.group + rank

    def place_of(self, device):
        return lax.div(device, self.group), lax.rem(device, self.group)

    def seq_groups(self):
        return [[self.device_of(s, r) for r in range(self.group)] for s in range(self.sequences)]

    def rank_groups(self):
        return [[self.device_of(s, r) for s in range(self.sequences)] for r in range(self.group)]

    def edge_row(self, rank):
        half = self.group // 2
        return jnp.where(rank < half, self.piece * rank, self.edge + self.span + self.piece * (rank - half))

    def main_row(self, rank):
        return self.edge + self.rows_dev * rank

    def edge_segments(self):
        found = []
        for rank in range(self.group):
            half = self.group // 2
            first = self.piece * rank - self.edge if rank < half else self.span + self.piece * (rank - half)
            row = 0
            while row < self.piece:
                owner, owner_row = (first + row) // self.rows_dev, (first + row) % self.rows_dev
                count = min(self.piece - row, self.rows_dev - owner_row)
                found.append((rank, row, count, owner // self.group, owner % self.group, owner_row))
                row += count
        return found


def layer_norm(values):
    mean = jnp.mean(values, axis=-1, keepdims=True)
    centred = values - mean
    variance = jnp.mean(centred * centred, axis=-1, keepdims=True)
    inv_std = lax.rsqrt(variance + EPSILON)
    return (centred * inv_std, inv_std)


def norm_back(grad_normed, normed, inv_std):
    mean_grad = jnp.mean(grad_normed, axis=-1, keepdims=True)
    mean_cross = jnp.mean(grad_normed * normed, axis=-1, keepdims=True)
    return inv_std * (grad_normed - mean_grad - normed * mean_cross)


def softmax_parts(query, key, bias):
    scores = lax.dot_general(query, key, CONTRACT_LAST, preferred_element_type=F32) + bias
    top = jnp.max(scores, axis=1, keepdims=True)
    exponent = jnp.exp(scores - top)
    total = jnp.sum(exponent, axis=1, keepdims=True)
    return exponent * (1.0 / total)


def head_columns(heads, part, head):
    first = (part * heads + head) * HDIM
    return slice(first, first + HDIM)


def attend_kernel(heads, block, projected, bias_ref, out_ref):
    rows = pl.ds(pl.multiple_of(pl.program_id(0) * block, block), block)
    bias = bias_ref[...]
    outs = []
    for head in range(heads):
        query = projected[rows, head_columns(heads, 0, head)] * jnp.asarray(HDIM ** (-0.5), BF16)
        probs = softmax_parts(query, projected[:, head_columns(heads, 1, head)], bias).astype(BF16)
        outs.append(jnp.dot(probs, projected[:, head_columns(heads, 2, head)], preferred_element_type=F32))
    out_ref[...] = jnp.concatenate(outs, axis=1).astype(BF16)


def block_rows(rows, most):
    return most if rows % most == 0 else 128


def constant(shape):
    return pl.BlockSpec(shape, lambda i: (0,) * len(shape))


def attend(plan, projected, bias):
    rows, cols = projected.shape[0], projected.shape[1] // 3
    block = block_rows(rows, 128)
    return pl.pallas_call(
        functools.partial(attend_kernel, plan.heads, block),
        out_shape=jax.ShapeDtypeStruct((rows, cols), BF16),
        grid=(rows // block,),
        in_specs=[constant(projected.shape), constant(bias.shape)],
        out_specs=pl.BlockSpec((block, cols), lambda i: (i, 0)),
        compiler_params=pltpu.CompilerParams(vmem_limit_bytes=48 << 20),
        cost_estimate=pl.CostEstimate(flops=16 * rows * rows * cols, bytes_accessed=8 * rows * cols, transcendentals=0),
        name="attend",
    )(projected, bias)


def attend_back_kernel(
    heads, steps, block, projected, grad_merged, merge_pair, text, bias_ref, out, key_sum, value_sum
):
    step = pl.program_id(0)
    scale = jnp.asarray(HDIM ** (-0.5), BF16)

    @pl.when(step == 0)
    def _():
        key_sum[...] = jnp.zeros_like(key_sum)
        value_sum[...] = jnp.zeros_like(value_sum)

    rows = pl.ds(pl.multiple_of(step * block, block), block)
    bias = bias_ref[...]
    image, other_stream = [
        lax.dot_general(grad_merged[...], merge_pair[j], CONTRACT_LAST, preferred_element_type=F32) for j in range(2)
    ]
    grad_attended = jnp.where(text[...] > 0, other_stream, image).astype(BF16)
    grads = []
    for head in range(heads):
        query = projected[rows, head_columns(heads, 0, head)] * scale
        key = projected[:, head_columns(heads, 1, head)]
        grad_out = grad_attended[:, head * HDIM : (head + 1) * HDIM]
        probs = softmax_parts(query, key, bias)
        grad_probs = lax.dot_general(
            grad_out, projected[:, head_columns(heads, 2, head)], CONTRACT_LAST, preferred_element_type=F32
        )
        inner = jnp.sum(probs * grad_probs, axis=1, keepdims=True)
        grad_scores = (probs * (grad_probs - inner)).astype(BF16)
        grads.append(jnp.dot(grad_scores, key, preferred_element_type=F32) * HDIM ** (-0.5))
        key_sum[head] += lax.dot_general(query, grad_scores, CONTRACT_FIRST, preferred_element_type=F32)
        value_sum[head] += lax.dot_general(grad_out, probs.astype(BF16), CONTRACT_FIRST, preferred_element_type=F32)
    cols = heads * HDIM
    out[rows, :cols] = jnp.concatenate(grads, axis=1).astype(BF16)

    @pl.when(step == steps - 1)
    def _():
        total = out.shape[0]
        out[:, cols : 2 * cols] = key_sum[...].reshape(cols, total).T.astype(BF16)
        out[:, 2 * cols :] = value_sum[...].reshape(cols, total).T.astype(BF16)


def attend_back(plan, projected, grad_merged, merge_pair, text, bias):
    rows, cols = projected.shape[0], projected.shape[1] // 3
    block = block_rows(rows, 256)
    return pl.pallas_call(
        functools.partial(attend_back_kernel, plan.heads, rows // block, block),
        out_shape=jax.ShapeDtypeStruct(projected.shape, BF16),
        grid=(rows // block,),
        in_specs=[
            constant(projected.shape),
            pl.BlockSpec((block, plan.width), lambda i: (i, 0)),
            constant(merge_pair.shape),
            pl.BlockSpec((block, 1), lambda i: (i, 0)),
            constant(bias.shape),
        ],
        out_specs=constant(projected.shape),
        scratch_shapes=[pltpu.VMEM((plan.heads, HDIM, rows), F32)] * 2,
        compiler_params=pltpu.CompilerParams(vmem_limit_bytes=56 << 20),
        cost_estimate=pl.CostEstimate(flops=40 * rows * rows * cols, bytes_accessed=14 * rows * cols, transcendentals=0),
        name="attend_back",
    )(projected, grad_merged, merge_pair, text, bias)


def fold_rows(piece):
    half = piece.shape[0] // 2
    return jnp.concatenate([piece[:half], piece[half:]], axis=1)


def unfold_rows(piece):
    half = piece.shape[1] // 2
    return jnp.concatenate([piece[:, :half], piece[:, half:]], axis=0)


def terms_kernel(plan, fold, chunk, rows, grads, text, out, kept):
    width = rows.shape[1]
    for stream, (first, last) in enumerate(((0, plan.image_end), (plan.text_start, plan.rows))):
        count = last - first
        mask = text[pl.ds(first, count)]
        keep = (mask > 0) if stream else (mask <= 0)
        kept[pl.ds(0, count)] = jnp.where(keep, grads[pl.ds(first, count)], jnp.zeros((), BF16))

        def step(i, carry):
            start = pl.multiple_of(i * chunk, chunk)
            term = lax.dot_general(
                rows[pl.ds(first, count), pl.ds(start, chunk)],
                kept[pl.ds(0, count)],
                CONTRACT_FIRST,
                preferred_element_type=F32,
            ).astype(BF16)
            if fold:
                for j in range(chunk // fold):
                    out[(stream * width) // fold + i * (chunk // fold) + j] = fold_rows(term[j * fold : (j + 1) * fold])
            else:
                out[stream, pl.ds(start, chunk)] = term
            return carry

        if width == chunk:
            step(0, 0)
        else:
            lax.fori_loop(0, width // chunk, step, 0)


def weight_terms(plan, rows, grads, text, name, fold=0):
    width, cols = rows.shape[1], grads.shape[1]
    chunk = 384 if fold else 256 if width % 256 == 0 else width
    shape = (2 * width // fold, fold // 2, 2 * cols) if fold else (2, width, cols)
    return pl.pallas_call(
        functools.partial(terms_kernel, plan, fold, chunk),
        out_shape=jax.ShapeDtypeStruct(shape, BF16),
        in_specs=[pl.BlockSpec(memory_space=pltpu.VMEM)] * 3,
        out_specs=pl.BlockSpec(memory_space=pltpu.VMEM),
        scratch_shapes=[pltpu.VMEM((plan.image_end, cols), BF16)],
        compiler_params=pltpu.CompilerParams(vmem_limit_bytes=40 << 20),
        cost_estimate=pl.CostEstimate(flops=3 * plan.rows * width * cols, bytes_accessed=1 << 23, transcendentals=0),
        name=name,
    )(rows, grads, text)


def gelu(values):
    return jax.nn.gelu(values, approximate=True)


def in_blocks(plan, size, body):
    def step(i, carry):
        body(i, pl.ds(pl.multiple_of(i * size, size), size))
        return carry

    lax.fori_loop(0, plan.rows // size, step, 0)


def blockwise(plan, i, size, block, pair, dims, mask, out):
    @pl.when(i * size < plan.image_end)
    def _():
        out[...] = lax.dot_general(block, pair[0], dims, preferred_element_type=F32)

    @pl.when(i * size + size > plan.text_start)
    def _():
        out[...] = jnp.where(mask > 0, lax.dot_general(block, pair[1], dims, preferred_element_type=F32), out[...])


def project_kernel(plan, size, rows, pair, text, shift, scale, hidden, out, held):
    def body(i, place):
        mask = text[place]
        normed, _ = norm_rows(rows[place].astype(F32))
        block = (normed * (1.0 + pick_rows(scale[...], mask)) + pick_rows(shift[...], mask)).astype(BF16)
        hidden[place] = block
        blockwise(plan, i, size, block, pair, PLAIN, mask, held)
        out[place] = held[...].astype(BF16)

    in_blocks(plan, size, body)


def up_kernel(plan, size, rows, pair, text, upper, activated):
    def body(i, place):
        blockwise(plan, i, size, rows[place], pair, PLAIN, text[place], upper.at[place])
        activated[place] = gelu(upper[place]).astype(BF16)

    in_blocks(plan, size, body)


def down_back_kernel(plan, size, rows, pair, text, upper, out, held):
    def body(i, place):
        blockwise(plan, i, size, rows[place], pair, CONTRACT_LAST, text[place], held)
        out[place] = jax.vjp(gelu, upper[place])[1](held[...])[0].astype(BF16)

    in_blocks(plan, size, body)


def stream_rows(plan, kernel, size, cols, held, name, outs, *operands):
    spec = pl.BlockSpec(memory_space=pltpu.VMEM)
    shapes = tuple(jax.ShapeDtypeStruct((plan.rows, width), dtype) for width, dtype in outs)
    return pl.pallas_call(
        functools.partial(kernel, plan, size),
        out_shape=shapes,
        in_specs=[spec] * len(operands),
        out_specs=(spec,) * len(shapes),
        scratch_shapes=[pltpu.VMEM((size, cols), F32)] if held else [],
        compiler_params=pltpu.CompilerParams(vmem_limit_bytes=40 << 20),
        cost_estimate=pl.CostEstimate(
            flops=2 * plan.rows * plan.width * cols, bytes_accessed=1 << 24, transcendentals=0
        ),
        name=name,
    )(*operands)


VMEM = pl.BlockSpec(memory_space=pltpu.VMEM)


def own_rows(plan, window, rank):
    main = lax.dynamic_slice_in_dim(window, plan.main_row(rank), plan.rows_dev, 0)
    edge = lax.dynamic_slice_in_dim(window, plan.edge_row(rank), plan.piece, 0)
    return jnp.concatenate([main, edge], axis=0)


def remote(source, target, send_sem, recv_sem, device):
    return pltpu.make_async_remote_copy(
        src_ref=source,
        dst_ref=target,
        send_sem=send_sem,
        recv_sem=recv_sem,
        device_id=(device,),
        device_id_type=pl.DeviceIdType.MESH,
    )


def here(plan):
    return plan.place_of(lax.axis_index("dev"))


def other(rank, step, size):
    return lax.rem(rank + step, size)


def meet(devices):
    barrier = pltpu.get_barrier_semaphore()
    for device in devices:
        pl.semaphore_signal(barrier, inc=1, device_id=(device,), device_id_type=pl.DeviceIdType.MESH)
    pl.semaphore_wait(barrier, len(devices))


def group_devices(plan, seq, rank):
    return [plan.device_of(seq, other(rank, step, plan.group)) for step in range(1, plan.group)]


def column_devices(plan, seq, rank):
    return [plan.device_of(other(seq, step, plan.sequences), rank) for step in range(1, plan.sequences)]


def every_device(plan, device):
    return [other(device, step, plan.devices) for step in range(1, plan.devices)]


def call(kernel, name, ident, out_shape, scratch, operands, in_specs=None, out_specs=None, vmem=40 << 20):
    outs = out_shape if isinstance(out_shape, tuple) else (out_shape,)
    return pl.pallas_call(
        kernel,
        out_shape=out_shape,
        in_specs=in_specs or [VMEM] * len(operands),
        out_specs=out_specs or (tuple([VMEM] * len(outs)) if isinstance(out_shape, tuple) else VMEM),
        scratch_shapes=scratch,
        compiler_params=pltpu.CompilerParams(
            collective_id=ident, has_side_effects=True, vmem_limit_bytes=vmem
        ),
        name=name,
    )(*operands)


def aligned(start):
    return pl.multiple_of(start, 16)


def block_parts(plan, ref, rank):
    return (
        ref.at[pl.ds(aligned(plan.main_row(rank)), plan.rows_dev)],
        ref.at[pl.ds(aligned(plan.edge_row(rank)), plan.piece)],
    )


def own_parts(plan, ref):
    return ref.at[pl.ds(0, plan.rows_dev)], ref.at[pl.ds(plan.rows_dev, plan.piece)]


def load_block(plan, ref, rank):
    main, edge = block_parts(plan, ref, rank)
    return jnp.concatenate([main[...], edge[...]], axis=0)


def sum_scratch(plan, wire=BF16):
    half, own, width = plan.group // 2, plan.own, plan.width
    return [
        pltpu.VMEM((half + 1, own, width), F32),
        pltpu.VMEM((half, own, width), F32),
        pltpu.VMEM((half - 1, own, width), wire),
        pltpu.VMEM((half - 1, own, width), wire),
        pltpu.SemaphoreType.DMA((half,)),
        pltpu.SemaphoreType.DMA((half,)),
        pltpu.SemaphoreType.DMA((half,)),
        pltpu.SemaphoreType.DMA((half,)),
    ]


SUM_SCRATCH = 8


def product(plan, rows, pair, text, dims, rank, out):
    block = load_block(plan, rows, rank)
    text_row = load_block(plan, text, rank) > 0
    chunk = 256

    def step(i, carry):
        cols = pl.ds(pl.multiple_of(i * chunk, chunk), chunk)
        parts = []
        for stream in range(2):
            weight = pair[stream, cols, :] if dims is CONTRACT_LAST else pair[stream, :, cols]
            parts.append(lax.dot_general(block, weight, dims, preferred_element_type=F32))
        out[:, cols] = jnp.where(text_row, parts[1], parts[0])
        return carry

    lax.fori_loop(0, plan.width // chunk, step, 0)


def scatter_start(plan, seq, rank, rows, pair, text, dims, away, near, going, coming,
                  pair_send, pair_recv, far_send, far_recv):
    half = plan.group // 2
    chip, core = lax.div(rank, 2), lax.rem(rank, 2)
    partner = plan.device_of(seq, 2 * chip + 1 - core)
    order = list(range(1, half)) + [0]

    def pair_copy(step):
        return remote(away.at[step], near.at[step], pair_send.at[step], pair_recv.at[step], partner)

    def far_copy(step):
        to = plan.device_of(seq, 2 * other(chip, step, half) + core)
        return remote(going.at[step - 1], coming.at[step - 1], far_send.at[step], far_recv.at[step], to)

    def turn(i, carry):
        for_partner = (i < 2) | (lax.rem(i, 2) == 1) & (i < 2 * half - 1)
        place = jnp.where(i < 2, i, jnp.where(for_partner, lax.div(i + 1, 2), lax.div(i, 2) - 1))
        place = jnp.where(i == 2 * half - 1, half - 1, place)
        step = other(place, 1, half)
        block = 2 * other(chip, step, half) + jnp.where(for_partner, 1 - core, core)
        product(plan, rows, pair, text, dims, block, away.at[jnp.where(for_partner, step, half)])

        @pl.when(for_partner)
        def _():
            pair_copy(step).start()

        @pl.when(jnp.logical_not(for_partner))
        def _():
            pair_copy(step).wait_recv()
            away[half] = away[half] + near[step]

        @pl.when(jnp.logical_not(for_partner) & (place < half - 1))
        def _():
            going[step - 1] = away[half].astype(going.dtype)
            far_copy(step).start()

        return carry

    lax.fori_loop(0, 2 * half, turn, 0)

    def result(use):
        for step in range(1, half):
            far_copy(step).wait_recv()
        size = 32 if plan.own % 32 == 0 else 16

        def some(i, carry):
            place = pl.ds(pl.multiple_of(i * size, size), size)
            total = away[half, place]
            for step in range(1, half):
                total = total + coming[step - 1, place].astype(F32)
            use(place, total)
            return carry

        lax.fori_loop(0, plan.own // size, some, 0)
        for step in range(half):
            pair_copy(step).wait_send()
        for step in range(1, half):
            far_copy(step).wait_send()

    return result


def share_scratch(plan):
    return [pltpu.SemaphoreType.DMA((plan.group, 2))] * 2 + [pltpu.SemaphoreType.DMA((plan.group, 2))]


def share_rows(plan, seq, rank, parts, window, send, recv, pass_send):
    half = plan.group // 2
    chip, core = lax.div(rank, 2), lax.rem(rank, 2)
    partner_rank = 2 * chip + 1 - core
    partner = plan.device_of(seq, partner_rank)

    def send_own(to_device, slot):
        copies = [
            remote(source, target, send.at[slot, i], recv.at[slot, i], to_device)
            for i, (source, target) in enumerate(zip(parts, block_parts(plan, window, rank)))
        ]
        for copy in copies:
            copy.start()
        return copies

    flying = {}
    for step in range(1, half):
        flying[step] = send_own(plan.device_of(seq, 2 * other(chip, step, half) + core), step)
    flying[0] = send_own(partner, 0)
    for source, target in zip(parts, block_parts(plan, window, rank)):
        target[...] = source[...]
    passed = []
    for step in range(1, half):
        for copy in flying[step]:
            copy.wait_recv()
        came = 2 * other(chip, half - step, half) + core
        copies = [
            remote(place, place, pass_send.at[step, i], recv.at[half + step, i], partner)
            for i, place in enumerate(block_parts(plan, window, came))
        ]
        for copy in copies:
            copy.start()
        passed.extend(copies)
    for copy in flying[0]:
        copy.wait_recv()
    for copy in passed:
        copy.wait_recv()
    for copies in flying.values():
        for copy in copies:
            copy.wait_send()
    for copy in passed:
        copy.wait_send()


def entry_kernel(plan, tokens, grads, mod_part, *refs):
    if plan.chip_heads:
        merge, merge_out, *refs = refs[:1] + refs[4:5] + refs[1:4] + refs[5:]
        merge_send, merge_recv, *refs = refs[-2:] + refs[:-2]
    (token_window, grad_window, mods, token_own, grad_own, plane, across, chunk, edge_send, edge_recv,
     t_send, t_recv, t_pass, g_send, g_recv, g_pass, m_send, m_recv) = refs
    device = lax.axis_index("dev")
    seq, rank = plan.place_of(device)
    meet(every_device(plan, device))
    swaps = []
    if plan.chip_heads:
        core = lax.rem(rank, 2)
        partner = plan.device_of(seq, 2 * lax.div(rank, 2) + 1 - core)
        for stream in range(2):
            copy = remote(
                merge.at[2 * stream + 1 - core],
                merge_out.at[stream, core],
                merge_send.at[stream],
                merge_recv.at[stream],
                partner,
            )
            copy.start()
            swaps.append(copy)
            merge_out[stream, core] = merge[2 * stream + core]
    hops = []
    for step in range(1, plan.group):
        to = other(rank, step, plan.group)
        copy = remote(mod_part.at[to], plane.at[step], m_send.at[0, step], m_recv.at[0, step], plan.device_of(seq, to))
        copy.start()
        hops.append(copy)
    arrays = ((tokens, token_own), (grads, grad_own))
    count = len(plan.segments)
    for which, (source, own) in enumerate(arrays):
        for index, (to_rank, row, rows, step, owner, owner_row) in enumerate(plan.segments):
            @pl.when(rank == owner)
            def _():
                remote(
                    source.at[pl.ds(owner_row, rows)],
                    own.at[pl.ds(row, rows)],
                    edge_send.at[which * count + index],
                    edge_recv.at[which * count + index],
                    plan.device_of(lax.rem(seq + plan.sequences - step, plan.sequences), to_rank),
                ).start()
    for copy in hops:
        copy.wait_recv()
    total = mod_part[rank]
    for step in range(1, plan.group):
        total = total + plane[step]
    plane[0] = total
    hops_across = []
    for step in range(1, plan.sequences):
        to = other(seq, step, plan.sequences)
        copy = remote(plane.at[0, to], across.at[seq], m_send.at[1, step], m_recv.at[1, step], plan.device_of(to, rank))
        copy.start()
        hops_across.append(copy)
    across[seq] = plane[0, seq]
    for which, (source, own) in enumerate(arrays):
        for index, (to_rank, row, rows, step, owner, owner_row) in enumerate(plan.segments):
            @pl.when(rank == to_rank)
            def _():
                remote(
                    source.at[pl.ds(owner_row, rows)],
                    own.at[pl.ds(row, rows)],
                    edge_send.at[which * count + index],
                    edge_recv.at[which * count + index],
                    plan.device_of(lax.rem(seq + plan.sequences + step, plan.sequences), owner),
                ).wait_recv()
    share_rows(plan, seq, rank, (tokens, token_own), token_window, t_send, t_recv, t_pass)
    for copy in hops_across:
        copy.wait_recv()
    half = plan.sequences // 2
    for stream in range(2):
        total = across[stream * half]
        for i in range(1, half):
            total = total + across[stream * half + i]
        chunk[stream] = total
    hops_back = []
    for step in range(1, plan.group):
        to = other(rank, step, plan.group)
        copy = remote(chunk, mods.at[rank], m_send.at[2, step], m_recv.at[2, step], plan.device_of(seq, to))
        copy.start()
        hops_back.append(copy)
    mods[rank] = chunk[...]
    share_rows(plan, seq, rank, (grads, grad_own), grad_window, g_send, g_recv, g_pass)
    for copy in hops_back:
        copy.wait_recv()
    for copy in hops + hops_across + hops_back:
        copy.wait_send()
    for copy in swaps:
        copy.wait()
    for which, (source, own) in enumerate(arrays):
        for index, (to_rank, row, rows, step, owner, owner_row) in enumerate(plan.segments):
            @pl.when(rank == owner)
            def _():
                remote(
                    source.at[pl.ds(owner_row, rows)],
                    own.at[pl.ds(row, rows)],
                    edge_send.at[which * count + index],
                    edge_recv.at[which * count + index],
                    plan.device_of(lax.rem(seq + plan.sequences - step, plan.sequences), to_rank),
                ).wait_send()


def entry(plan, tokens, grads, mod_part, merge):
    lanes = mod_part.shape[1] // plan.group // 128
    pieces = mod_part.reshape(plan.sequences, plan.group, lanes, 128).transpose(1, 0, 2, 3)
    window = jax.ShapeDtypeStruct((plan.rows, plan.width), BF16)
    dma = pltpu.SemaphoreType.DMA
    most = max(plan.group, plan.sequences)
    shapes = (window, window, jax.ShapeDtypeStruct((plan.group, 2, lanes, 128), F32))
    operands = (tokens, grads, pieces)
    scratch = (
        [
            pltpu.VMEM((plan.piece, plan.width), BF16),
            pltpu.VMEM((plan.piece, plan.width), BF16),
            pltpu.VMEM((plan.group, plan.sequences, lanes, 128), F32),
            pltpu.VMEM((plan.sequences, lanes, 128), F32),
            pltpu.VMEM((2, lanes, 128), F32),
            dma((2 * len(plan.segments),)),
            dma((2 * len(plan.segments),)),
        ]
        + share_scratch(plan)
        + share_scratch(plan)
        + [dma((3, most)), dma((3, most))]
    )
    if plan.chip_heads:
        shapes += (jax.ShapeDtypeStruct((2, 2) + merge.shape[1:], BF16),)
        operands += (merge,)
        scratch += [dma((2,)), dma((2,))]
    token_window, grad_window, mods, *rest = call(
        functools.partial(entry_kernel, plan), "entry", 1, shapes, scratch, operands
    )
    merge_pair = rest[0].reshape(2, -1, plan.width) if plan.chip_heads else merge
    return token_window, grad_window, mods.transpose(1, 0, 2, 3).reshape(2, -1), merge_pair


def project_columns(plan, rank):
    share = plan.width // plan.group
    first = (rank % 2) * (plan.width // 2) + (rank // 2) * share
    return [part * plan.width + first for part in range(3)], share


def up_columns(plan, rank, cols):
    planes = plan.sequences // 2
    share = cols // planes // plan.group
    return [plane * plan.group * share + rank * share for plane in range(planes)], share


def start_swap(plan, seq, rank, source, target, send, recv):
    copies = []
    for step in range(1, plan.group):
        to = other(rank, step, plan.group)
        copy = remote(source.at[to], target.at[rank], send.at[step], recv.at[step], plan.device_of(seq, to))
        copy.start()
        copies.append(copy)
    target[rank] = source[rank]
    return copies


def swap_in_kernel(plan, project, up, project_out, up_out, project_cut, up_cut, p_send, p_recv, u_send, u_recv):
    seq, rank = here(plan)
    for to in range(plan.group):
        starts, share = project_columns(plan, to)
        project_cut[to] = fold_rows(jnp.concatenate([project[:, c : c + share] for c in starts], axis=1))
    meet(group_devices(plan, seq, rank))
    copies = start_swap(plan, seq, rank, project_cut, project_out, p_send, p_recv)
    for to in range(plan.group):
        starts, share = up_columns(plan, to, up.shape[1])
        up_cut[to] = jnp.concatenate([up[:, c : c + share] for c in starts], axis=1)
    copies += start_swap(plan, seq, rank, up_cut, up_out, u_send, u_recv)
    for copy in copies:
        copy.wait()


def swap_in(plan, project, up):
    rows = project.shape[0]
    dma = pltpu.SemaphoreType.DMA
    shapes = [
        (plan.group, rows // 2, 2 * project.shape[1] // plan.group),
        (plan.group, rows, up.shape[1] // plan.group),
    ]
    return call(
        functools.partial(swap_in_kernel, plan),
        "swap_in",
        4,
        tuple(jax.ShapeDtypeStruct(shape, BF16) for shape in shapes),
        [pltpu.VMEM(shape, BF16) for shape in shapes] + [dma((plan.group,))] * 4,
        (project, up),
    )


def place_columns(plan, got, out, columns, unfold):
    for source in range(plan.group):
        starts, share = columns(plan, source)
        piece = unfold_rows(got[source]) if unfold else got[source]
        for i, c in enumerate(starts):
            out[:, c : c + share] = piece[:, i * share : (i + 1) * share]


def line_sum(plan, seq, rank, term, out, up_in, up_out, down_in, down_out, up_send, up_recv, down_send, down_recv):
    count = plan.sequences

    def hop(source, target, send, recv, owner, to):
        return remote(source.at[owner], target.at[owner], send.at[owner], recv.at[owner], plan.device_of(to, rank))

    above, below = lax.rem(seq + 1, count), lax.rem(seq + count - 1, count)
    ways = [
        (list(range(count - 1, 0, -1)), above, below, up_in, up_out, up_send, up_recv, lambda owner: seq < owner, seq == 0),
        (list(range(count - 1)), below, above, down_in, down_out, down_send, down_recv, lambda owner: seq > owner,
         seq == count - 1),
    ]
    for turn in range(count - 1):
        for owners, to, back, came, goes, send, recv, mine, first in ways:
            owner = owners[turn]

            @pl.when(mine(owner) & first)
            def _():
                hop(term, came, send, recv, owner, to).start()

            @pl.when(mine(owner) & jnp.logical_not(first))
            def _():
                hop(goes, came, send, recv, owner, back).wait_recv()
                goes[owner] = (term[owner].astype(F32) + came[owner].astype(F32)).astype(BF16)
                hop(goes, came, send, recv, owner, to).start()

    out[...] = term[seq].astype(F32)
    for owners, to, back, came, goes, send, recv, mine, first in ways:
        for owner in owners:
            @pl.when(seq == owner)
            def _():
                hop(goes, came, send, recv, owner, back).wait_recv()
                out[...] += came[owner].astype(F32)

            @pl.when(mine(owner))
            def _():
                hop(goes, came, send, recv, owner, to).wait_send()


def finish_kernel(plan, up, project, *refs):
    if plan.chip_heads:
        term, up_out, project_out, merge_out, *refs = refs
        *refs, line = refs[:6] + [refs[6:]]
    else:
        up_out, project_out, *refs = refs
    up_got, project_got, u_send, u_recv, p_send, p_recv = refs
    seq, rank = here(plan)
    meet(group_devices(plan, seq, rank) + column_devices(plan, seq, rank))
    ups = start_swap(plan, seq, rank, up, up_got, u_send, u_recv)
    projects = start_swap(plan, seq, rank, project, project_got, p_send, p_recv)
    if plan.chip_heads:
        line_sum(plan, seq, rank, term, merge_out, *line)
    for copy in ups:
        copy.wait()
    place_columns(plan, up_got, up_out, lambda p, r: up_columns(p, r, up_out.shape[1]), False)
    for copy in projects:
        copy.wait()
    place_columns(plan, project_got, project_out, project_columns, True)


def finish(plan, up, project, term):
    dma = pltpu.SemaphoreType.DMA
    rows = up.shape[1]
    shapes = (
        jax.ShapeDtypeStruct((rows, plan.group * up.shape[2]), BF16),
        jax.ShapeDtypeStruct((rows, plan.group * project.shape[2] // 2), BF16),
    )
    operands = (up, project)
    scratch = [pltpu.VMEM(up.shape, BF16), pltpu.VMEM(project.shape, BF16)] + [dma((plan.group,))] * 4
    if plan.chip_heads:
        shapes += (jax.ShapeDtypeStruct(term.shape[1:], F32),)
        operands += (term,)
        scratch += [pltpu.VMEM(term.shape, BF16)] * 4 + [dma((plan.sequences,))] * 4
    up_grad, project_grad, *merge_grad = call(
        functools.partial(finish_kernel, plan), "finish", 6, shapes, scratch, operands
    )
    return up_grad.astype(F32), project_grad.astype(F32), merge_grad


def pick_rows(table, text):
    return jnp.where(text > 0, table[1:2, :], table[0:1, :])


def norm_rows(values):
    mean = jnp.mean(values, axis=1, keepdims=True)
    centred = values - mean
    inv = lax.rsqrt(jnp.mean(centred * centred, axis=1, keepdims=True) + EPSILON)
    return centred * inv, inv


def middle_kernel(plan, rows, pair, window_text, tokens, gate_a, scale_b, shift_b, text, merged, window, own, *scratch):
    seq, rank = here(plan)
    meet(group_devices(plan, seq, rank))
    result = scatter_start(plan, seq, rank, rows, pair, window_text, PLAIN, *scratch[:SUM_SCRATCH])

    def use(place, total):
        merged[place] = total
        mask = text[place]
        middle = tokens[place].astype(F32) + pick_rows(gate_a[...], mask) * total
        normed, _ = norm_rows(middle)
        own[place] = (normed * (1.0 + pick_rows(scale_b[...], mask)) + pick_rows(shift_b[...], mask)).astype(BF16)

    result(use)
    share_rows(plan, seq, rank, own_parts(plan, own), window, *scratch[SUM_SCRATCH:])


def own_shape(plan, dtype=F32):
    return jax.ShapeDtypeStruct((plan.own, plan.width), dtype)


def window_shape(plan):
    return jax.ShapeDtypeStruct((plan.rows, plan.width), BF16)


def middle_rows(plan, rows, pair, window_text, tokens, gate_a, scale_b, shift_b, text):
    return call(
        functools.partial(middle_kernel, plan),
        "middle",
        2,
        (own_shape(plan), window_shape(plan)),
        [pltpu.VMEM((plan.own, plan.width), BF16)] + sum_scratch(plan, F32) + share_scratch(plan),
        (rows, pair, window_text, tokens, gate_a, scale_b, shift_b, text),
    )


def back_kernel(plan, rows, pair, window_text, grad, middle, gate_a, scale_b, text, grad_hidden, grad_middle, window, own, *scratch):
    seq, rank = here(plan)
    meet(group_devices(plan, seq, rank))
    result = scatter_start(plan, seq, rank, rows, pair, window_text, CONTRACT_LAST, *scratch[:SUM_SCRATCH])

    def use(place, total):
        grad_hidden[place] = total
        mask = text[place]
        normed, inv = norm_rows(middle[place])
        inner = total * (1.0 + pick_rows(scale_b[...], mask))
        mean_grad = jnp.mean(inner, axis=1, keepdims=True)
        mean_cross = jnp.mean(inner * normed, axis=1, keepdims=True)
        back = grad[place].astype(F32) + inv * (inner - mean_grad - normed * mean_cross)
        grad_middle[place] = back
        own[place] = (pick_rows(gate_a[...], mask) * back).astype(BF16)

    result(use)
    share_rows(plan, seq, rank, own_parts(plan, own), window, *scratch[SUM_SCRATCH:])


def back_rows(plan, rows, pair, window_text, grad, middle, gate_a, scale_b, text):
    return call(
        functools.partial(back_kernel, plan),
        "back",
        3,
        (own_shape(plan), own_shape(plan), window_shape(plan)),
        [pltpu.VMEM((plan.own, plan.width), BF16)] + sum_scratch(plan) + share_scratch(plan),
        (rows, pair, window_text, grad, middle, gate_a, scale_b, text),
    )


def edge_copy(plan, seq, source, first_row, target, send, recv, index):
    from_rank, row, rows, step, owner, owner_row = plan.segments[index]
    return remote(
        source.at[pl.ds(first_row + row, rows)],
        target.at[pl.ds(owner_row, rows)],
        send.at[index],
        recv.at[index],
        plan.device_of(lax.rem(seq + plan.sequences + step, plan.sequences), owner),
    )


def start_edges(plan, seq, rank, *refs):
    for index, segment in enumerate(plan.segments):
        @pl.when(rank == segment[0])
        def _():
            edge_copy(plan, seq, *refs, index).start()


def finish_edges(plan, seq, rank, *refs):
    for index, segment in enumerate(plan.segments):
        @pl.when(rank == segment[4])
        def _():
            edge_copy(plan, seq, *refs, index).wait_recv()

        @pl.when(rank == segment[0])
        def _():
            edge_copy(plan, seq, *refs, index).wait_send()


def edge_scratch(plan):
    return [pltpu.SemaphoreType.DMA((len(plan.segments),))] * 2


def stream_sums(values, masks):
    return jnp.concatenate([jnp.sum(values * mask, axis=0, keepdims=True) for mask in masks], axis=0)


def last_kernel(plan, names, *refs):
    at = types.SimpleNamespace(**dict(zip(names, refs)))
    low_scratch = refs[len(names) : len(names) + SUM_SCRATCH]
    back_scratch = refs[len(names) + SUM_SCRATCH : len(names) + 2 * SUM_SCRATCH]
    device = lax.axis_index("dev")
    seq, rank = plan.place_of(device)
    stream = lax.div(2 * seq, plan.sequences)
    at.layer_extra[...] = jnp.zeros_like(at.layer_extra)
    at.token_extra[...] = jnp.zeros_like(at.token_extra)
    meet(every_device(plan, device))
    low_sum = scatter_start(plan, seq, rank, at.activated, at.down_pair, at.window_text, PLAIN, *low_scratch)
    back_sum = scatter_start(plan, seq, rank, at.grads, at.project_pair, at.window_text, CONTRACT_LAST, *back_scratch)
    swaps = []
    if plan.chip_heads:
        core = lax.rem(rank, 2)
        partner = plan.device_of(seq, 2 * lax.div(rank, 2) + 1 - core)
        for j in range(2):
            copy = remote(
                at.term.at[j, 1 - core], at.term_out.at[2 * j + core], at.term_send.at[j], at.term_recv.at[j], partner
            )
            copy.start()
            swaps.append(copy)
            at.term_out[2 * j + core] = at.term[j, core]
    width = plan.width
    at.local[...] = jnp.zeros_like(at.local)
    at.local[:, 2 * width : 5 * width] = at.rest[...]

    def add(first, place, values):
        masks = (at.masks[place, 0:1], at.masks[place, 1:2])
        at.local[:, first * width : (first + 1) * width] += stream_sums(values, masks)

    def use_low(place, lowered):
        at.layer_own[place] = (at.middle[place] + pick_rows(at.gate_b[...], at.text[place]) * lowered).astype(BF16)
        add(5, place, at.grad[place].astype(F32) * lowered)

    low_sum(use_low)
    layer_edges = (at.layer_own, plan.rows_dev, at.layer_extra, at.l_send, at.l_recv)
    start_edges(plan, seq, rank, *layer_edges)
    at.layer[...] = at.layer_own[pl.ds(0, plan.rows_dev)]

    def use_back(place, total):
        normed, inv = norm_rows(at.tokens[place].astype(F32))
        add(0, place, total)
        add(1, place, total * normed)
        inner = total * (1.0 + pick_rows(at.scale_a[...], at.text[place]))
        mean_grad = jnp.mean(inner, axis=1, keepdims=True)
        mean_cross = jnp.mean(inner * normed, axis=1, keepdims=True)
        at.token_own[place] = at.grad_middle[place] + inv * (inner - mean_grad - normed * mean_cross)

    back_sum(use_back)
    cols = 6 * width // plan.group

    def chunk(index):
        return pl.ds(pl.multiple_of(index * cols, 128), cols)

    hops = []
    for step in range(1, plan.group):
        to = other(rank, step, plan.group)
        copy = remote(
            at.local.at[:, chunk(to)], at.first.at[step], at.t_send.at[0, step], at.t_recv.at[0, step], plan.device_of(seq, to)
        )
        copy.start()
        hops.append(copy)
    token_edges = (at.token_own, plan.rows_dev, at.token_extra, at.e_send, at.e_recv)
    start_edges(plan, seq, rank, *token_edges)
    for copy in hops:
        copy.wait_recv()
    sums = at.local[:, chunk(rank)]
    for step in range(1, plan.group):
        sums = sums + at.first[step]
    for i in range(2):
        at.mine[i] = sums[i : i + 1]
    across = []
    for step in range(1, plan.sequences):
        to = other(seq, step, plan.sequences)
        to_stream = lax.div(2 * to, plan.sequences)
        copy = remote(
            at.mine.at[to_stream], at.second.at[seq], at.t_send.at[1, step], at.t_recv.at[1, step], plan.device_of(to, rank)
        )
        copy.start()
        across.append(copy)
    at.second[seq] = at.mine[stream]
    at.token[...] = at.token_own[pl.ds(0, plan.rows_dev)]
    for copy in across:
        copy.wait_recv()
    last = []
    for step in range(1, plan.group):
        to = other(rank, step, plan.group)
        copy = remote(at.second, at.table.at[rank], at.t_send.at[2, step], at.t_recv.at[2, step], plan.device_of(seq, to))
        copy.start()
        last.append(copy)
    at.table[rank] = at.second[...]
    for copy in last:
        copy.wait_recv()

    piece = None
    for index in range(plan.group):
        grads = jnp.concatenate([at.table[index, s] for s in range(plan.sequences)], axis=0).astype(BF16)
        part = lax.dot_general(
            grads, at.weight[:, index * cols : (index + 1) * cols], CONTRACT_LAST, preferred_element_type=F32
        )
        piece = part if piece is None else piece + part
    at.piece[...] = piece
    at.everyone[seq, rank] = piece
    spread = []
    for step in range(1, plan.group):
        to = other(rank, step, plan.group)
        copy = remote(
            at.piece, at.everyone.at[seq, rank], at.c_send.at[0, step], at.c_recv.at[0, step], plan.device_of(seq, to)
        )
        copy.start()
        spread.append(copy)
    for copy in spread:
        copy.wait_recv()
    for step in range(1, plan.sequences):
        to = other(seq, step, plan.sequences)
        copy = remote(
            at.everyone.at[seq], at.everyone.at[seq], at.c_send.at[1, step], at.c_recv.at[1, step], plan.device_of(to, rank)
        )
        copy.start()
        spread.append(copy)
    for copy in spread[plan.group - 1 :]:
        copy.wait_recv()
    for copy in hops + across + last + spread:
        copy.wait_send()
    for copy in swaps:
        copy.wait()
    finish_edges(plan, seq, rank, *layer_edges)
    finish_edges(plan, seq, rank, *token_edges)


def last_rows(plan, term, weight, **operands):
    rows, share = weight.shape[0], plan.width // plan.group // 2
    cols = 6 * plan.width // plan.group
    most = max(plan.group, plan.sequences)
    dma = pltpu.SemaphoreType.DMA

    def placed(dtype):
        return jax.ShapeDtypeStruct((plan.rows_dev, plan.width), dtype)

    operands = dict(operands, weight=weight)
    outs = dict(
        layer=placed(BF16),
        layer_extra=placed(BF16),
        token=placed(F32),
        token_extra=placed(F32),
        table=jax.ShapeDtypeStruct((plan.group, plan.sequences, 1, cols), F32),
        everyone=jax.ShapeDtypeStruct((plan.sequences, plan.group, plan.sequences, rows), F32),
    )
    edges = len(plan.segments)
    scratch = dict(
        layer_own=pltpu.VMEM((plan.own, plan.width), BF16),
        token_own=pltpu.VMEM((plan.own, plan.width), F32),
        local=pltpu.VMEM((2, 6 * plan.width), F32),
        first=pltpu.VMEM((plan.group, 2, cols), F32),
        second=pltpu.VMEM((plan.sequences, 1, cols), F32),
        mine=pltpu.VMEM((2, 1, cols), F32),
        piece=pltpu.VMEM((plan.sequences, rows), F32),
        t_send=dma((3, most)),
        t_recv=dma((3, most)),
        c_send=dma((2, most)),
        c_recv=dma((2, most)),
        l_send=dma((edges,)),
        l_recv=dma((edges,)),
        e_send=dma((edges,)),
        e_recv=dma((edges,)),
    )
    if plan.chip_heads:
        operands["term"] = term.reshape(2, 2, share, plan.width)
        outs["term_out"] = jax.ShapeDtypeStruct((plan.sequences, share, plan.width), BF16)
        scratch.update(term_send=dma((2,)), term_recv=dma((2,)))
    names = tuple(operands) + tuple(outs) + tuple(scratch)
    got = call(
        functools.partial(last_kernel, plan, names),
        "last",
        10,
        tuple(outs.values()),
        list(scratch.values()) + sum_scratch(plan) + sum_scratch(plan),
        tuple(operands.values()),
        vmem=58 << 20,
    )
    got = types.SimpleNamespace(**dict(zip(outs, got)))
    got.table = got.table[:, :, 0].transpose(1, 0, 2).reshape(plan.sequences, -1)
    got.term = got.term_out if plan.chip_heads else term
    return got


def over_sequences(plan, pieces):
    full = lax.all_gather(pieces, "dev", axis=0, axis_index_groups=plan.rank_groups())
    return full.reshape((plan.devices,) + pieces.shape[1:])


def over_sequences_sum(plan, pieces):
    return lax.psum_scatter(pieces, "dev", scatter_dimension=0, axis_index_groups=plan.rank_groups())


def merge_rows(plan, weight, rank):
    if plan.chip_heads:
        return lax.all_gather(weight, "dev", axis=0, axis_index_groups=plan.rank_groups())
    share = plan.width // plan.group
    full = lax.all_gather(weight, "dev", axis=0, tiled=True)
    full = full.reshape(2, 2, plan.group // 2, share, weight.shape[1])
    full = lax.dynamic_index_in_dim(full, lax.rem(rank, 2), 1, keepdims=False)
    return lax.dynamic_index_in_dim(full, lax.div(rank, 2), 1, keepdims=False)


def merge_sum(plan, term, rank):
    half = plan.group // 2
    _, share, cols = term.shape
    mine = [jnp.where(lax.rem(rank, 2) == k, term, jnp.zeros((), BF16)) for k in range(2)]
    full = jnp.zeros((2, 2, half, share, cols), BF16)
    full = lax.dynamic_update_slice_in_dim(full, jnp.stack(mine, axis=1)[:, :, None], lax.div(rank, 2), 2)
    return lax.psum_scatter(full.reshape(-1, cols), "dev", scatter_dimension=0, tiled=True)


def down_slices(plan, weight):
    full = lax.all_gather(weight, "dev", axis=0, axis_index_groups=plan.rank_groups())
    return full.reshape(2, -1, weight.shape[1])


def pick(table, text_rows):
    return jnp.where(text_rows[:, None], table[1][None, :], table[0][None, :])


def on_device(
    tokens,
    conditioning,
    text_lengths,
    modulation_weight,
    project_weight,
    merge_weight,
    up_weight,
    down_weight,
    cotangent,
):
    rows_dev, width = tokens.shape
    mod_rows = modulation_weight.shape[0]
    plan = Plan(lax.axis_size("dev"), conditioning.shape[0], rows_dev, width)
    device = lax.axis_index("dev")
    seq, rank = plan.place_of(device)
    feature_start = device * mod_rows % width

    ends = jnp.cumsum(IMG + text_lengths)
    starts = jnp.concatenate([jnp.zeros((1,), jnp.int32), ends[:-1]])
    positions = device * rows_dev + jnp.arange(rows_dev, dtype=jnp.int32)
    row_seq = jnp.sum((starts[None, :] <= positions[:, None]).astype(jnp.int32), axis=1) - 1
    offset = plan.span * seq - plan.edge + jnp.arange(plan.rows, dtype=jnp.int32) - starts[seq]
    valid = (offset >= 0) & (offset < IMG + text_lengths[seq])
    is_text = offset >= IMG
    bias = jnp.where(valid, 0.0, MASKED).astype(F32)[None, :]
    window_text = is_text.astype(F32)[:, None]
    own_valid = own_rows(plan, valid[:, None], rank)[:, 0]
    own_text = own_rows(plan, is_text[:, None], rank)[:, 0]

    cond_float = conditioning.astype(F32)
    silu_low = jax.nn.silu(cond_float).astype(BF16)
    silu_part = lax.dynamic_slice_in_dim(silu_low, feature_start, mod_rows, 1)
    mod_part = jnp.dot(silu_part, modulation_weight, preferred_element_type=F32)

    merge_pair = merge_rows(plan, merge_weight, rank)
    project_pieces, up_pieces = swap_in(plan, project_weight, up_weight)
    project_pieces, up_pieces, merge_pair = lax.optimization_barrier((project_pieces, up_pieces, merge_pair))
    project_pair = over_sequences(plan, project_pieces)
    share = project_pair.shape[2] // 2
    project_pair = jnp.concatenate([project_pair[:, :, :share], project_pair[:, :, share:]], axis=1)
    project_pair = lax.optimization_barrier(project_pair.reshape(2, width, share))
    up_pair = over_sequences(plan, up_pieces).reshape(2, width, -1)
    down_pair = down_slices(plan, down_weight)

    token_window, grad_window, mods, merge_pair = entry(plan, tokens, cotangent, mod_part, merge_pair)
    shift_a, scale_a, gate_a, shift_b, scale_b, gate_b = jnp.split(mods, 6, axis=1)
    grad_window = jnp.where(valid[:, None], grad_window, jnp.zeros((), BF16))

    cols = project_pair.shape[2]
    hidden_a, projected = stream_rows(
        plan, project_kernel, 128, cols, True, "project", ((width, BF16), (cols, BF16)),
        token_window, project_pair, window_text, shift_a, scale_a,
    )
    attended = attend(plan, projected, bias)

    own_tokens = own_rows(plan, token_window, rank)
    own_grad = own_rows(plan, grad_window, rank)
    text_mask = own_text.astype(F32)[:, None]
    merged, hidden_b = middle_rows(
        plan, attended, merge_pair, window_text, own_tokens, gate_a, scale_b, shift_b, text_mask
    )
    middle = own_tokens.astype(F32) + pick(gate_a, own_text) * merged
    normed_b, inv_b = layer_norm(middle)

    units = up_pair.shape[2]
    upper, activated = stream_rows(
        plan, up_kernel, 128, units, False, "up", ((units, F32), (units, BF16)), hidden_b, up_pair, window_text
    )
    grad_lowered = (pick(gate_b, is_text) * grad_window.astype(F32)).astype(BF16)
    down_term = weight_terms(plan, activated, grad_lowered, window_text, "down_terms")
    down_term = down_term.reshape(plan.sequences, -1, width)
    down_term, grad_lowered = lax.optimization_barrier((down_term, grad_lowered))
    down_sum = over_sequences_sum(plan, down_term)
    (grad_upper,) = stream_rows(
        plan, down_back_kernel, block_rows(plan.rows, 256), units, True, "down_back", ((units, BF16),),
        grad_lowered, down_pair, window_text, upper,
    )
    up_term = weight_terms(plan, hidden_b, grad_upper, window_text, "up_terms")
    up_term = up_term.reshape(plan.sequences, plan.group, mod_rows, -1)
    grad_upper, up_term = lax.optimization_barrier((grad_upper, up_term))
    up_sum = over_sequences_sum(plan, up_term)
    grad_hidden_b, grad_middle, grad_merged = back_rows(
        plan, grad_upper, up_pair, window_text, own_grad, middle, gate_a, scale_b, text_mask
    )
    merge_term = weight_terms(plan, attended, grad_merged, window_text, "merge_terms")

    grad_projected = attend_back(plan, projected, grad_merged, merge_pair, window_text, bias)
    grad_projected, down_sum = lax.optimization_barrier((grad_projected, down_sum))
    down_grad = down_sum.astype(F32)
    project_term = weight_terms(plan, hidden_a, grad_projected, window_text, "project_terms", mod_rows)
    project_term = project_term.reshape((plan.sequences, plan.group) + project_term.shape[1:])
    grad_projected, project_term = lax.optimization_barrier((grad_projected, project_term))
    project_sum = over_sequences_sum(plan, project_term)

    masks = jnp.stack([own_valid & ~own_text, own_valid & own_text], axis=1).astype(F32)
    rest = jnp.concatenate(
        [
            jnp.stack([jnp.sum(value * masks[:, j : j + 1], axis=0) for j in range(2)])
            for value in (grad_middle * merged, grad_hidden_b, grad_hidden_b * normed_b)
        ],
        axis=1,
    )
    got = last_rows(
        plan,
        merge_term,
        modulation_weight,
        activated=activated,
        down_pair=down_pair,
        grads=grad_projected,
        project_pair=project_pair,
        window_text=window_text,
        tokens=own_tokens,
        middle=middle,
        grad=own_grad,
        grad_middle=grad_middle,
        gate_b=gate_b,
        scale_a=scale_a,
        text=text_mask,
        masks=masks,
        rest=rest,
    )
    foreign = (row_seq != seq)[:, None]
    layer_out = jnp.where(foreign, got.layer_extra, got.layer)
    tokens_grad = jnp.where(foreign, got.token_extra, got.token)
    own_grads = got.table.astype(BF16)
    modulation_grad = lax.dot_general(silu_part, own_grads, CONTRACT_FIRST, preferred_element_type=F32)
    everyone = got.everyone.reshape(2, plan.devices // 2, plan.sequences, mod_rows)
    grad_silu = (everyone[0] + everyone[1]).transpose(1, 0, 2).reshape(plan.sequences, width)
    conditioning_grad = jax.vjp(jax.nn.silu, cond_float)[1](grad_silu)[0]
    modulation_grad, up_sum = lax.optimization_barrier((modulation_grad, up_sum))
    merge_out, project_sum, *done = lax.optimization_barrier(
        (got.term, project_sum, modulation_grad, down_grad, layer_out, tokens_grad, conditioning_grad)
    )
    modulation_grad, down_grad, layer_out, tokens_grad, conditioning_grad = done
    up_grad, project_grad, merge_grad = finish(plan, up_sum, project_sum, merge_out)
    merge_grad = merge_grad[0] if merge_grad else merge_sum(plan, merge_out, rank).astype(F32)
    return (
        layer_out,
        tokens_grad,
        conditioning_grad,
        modulation_grad,
        project_grad,
        merge_grad,
        up_grad,
        down_grad,
    )


def solution(mesh):
    shard, whole = P("dev", None), P()
    return jax.shard_map(
        on_device,
        mesh=mesh,
        in_specs=(shard, whole, whole, shard, shard, shard, shard, shard, shard),
        out_specs=(shard, shard, whole, shard, shard, shard, shard, shard),
        check_vma=False,
    )
```

```python
import functools
import types

import jax
import jax.numpy as jnp
import numpy as np
from jax import lax
from jax.experimental import pallas as pl
from jax.experimental.pallas import tpu as pltpu
from jax.sharding import PartitionSpec as P

HEADS = 24
HDIM = 64
IMG = 1024
TXT_MIN = 86
TXT_MAX = 154
EPSILON = 1e-06
F32 = jnp.float32
BF16 = jnp.bfloat16
CONTRACT_LAST = (((1,), (1,)), ((), ()))
PLAIN = (((1,), (0,)), ((), ()))
CONTRACT_FIRST = (((0,), (0,)), ((), ()))
MASKED = -1e30


class Plan:
    def __init__(self, devices, sequences, rows_dev, width):
        self.devices, self.sequences, self.rows_dev, self.width = devices, sequences, rows_dev, width
        self.group = devices // sequences
        self.span = self.group * rows_dev
        mean = self.span - IMG
        up, down = TXT_MAX - mean, mean - TXT_MIN
        drift = 0
        for k in range(sequences + 1):
            drift = max(drift, min(up * k, down * (sequences - k)), min(down * k, up * (sequences - k)))
        self.edge = -(-drift // 64) * 64
        self.rows = self.span + 2 * self.edge
        self.piece = 2 * self.edge // self.group
        self.own = rows_dev + self.piece
        self.image_end = -(-(self.edge + drift + IMG) // 128) * 128
        self.text_start = (self.edge - drift + IMG) // 128 * 128
        self.heads = HEADS // self.group
        self.segments = self.edge_segments()
        self.chip_heads = devices == 4 * self.group

    def device_of(self, seq, rank):
        return seq * self.group + rank

    def place_of(self, device):
        return lax.div(device, self.group), lax.rem(device, self.group)

    def seq_groups(self):
        return [[self.device_of(s, r) for r in range(self.group)] for s in range(self.sequences)]

    def rank_groups(self):
        return [[self.device_of(s, r) for s in range(self.sequences)] for r in range(self.group)]

    def edge_row(self, rank):
        half = self.group // 2
        return jnp.where(rank < half, self.piece * rank, self.edge + self.span + self.piece * (rank - half))

    def main_row(self, rank):
        return self.edge + self.rows_dev * rank

    def edge_segments(self):
        found = []
        for rank in range(self.group):
            half = self.group // 2
            first = self.piece * rank - self.edge if rank < half else self.span + self.piece * (rank - half)
            row = 0
            while row < self.piece:
                owner, owner_row = (first + row) // self.rows_dev, (first + row) % self.rows_dev
                count = min(self.piece - row, self.rows_dev - owner_row)
                found.append((rank, row, count, owner // self.group, owner % self.group, owner_row))
                row += count
        return found


def layer_norm(values):
    mean = jnp.mean(values, axis=-1, keepdims=True)
    centred = values - mean
    variance = jnp.mean(centred * centred, axis=-1, keepdims=True)
    inv_std = lax.rsqrt(variance + EPSILON)
    return (centred * inv_std, inv_std)


def norm_back(grad_normed, normed, inv_std):
    mean_grad = jnp.mean(grad_normed, axis=-1, keepdims=True)
    mean_cross = jnp.mean(grad_normed * normed, axis=-1, keepdims=True)
    return inv_std * (grad_normed - mean_grad - normed * mean_cross)


def softmax_parts(query, key, bias):
    scores = lax.dot_general(query, key, CONTRACT_LAST, preferred_element_type=F32) + bias
    top = jnp.max(scores, axis=1, keepdims=True)
    exponent = jnp.exp(scores - top)
    total = jnp.sum(exponent, axis=1, keepdims=True)
    return exponent * (1.0 / total)


def head_columns(heads, part, head):
    first = (part * heads + head) * HDIM
    return slice(first, first + HDIM)


def attend_kernel(heads, block, projected, bias_ref, out_ref):
    rows = pl.ds(pl.multiple_of(pl.program_id(0) * block, block), block)
    bias = bias_ref[...]
    outs = []
    for head in range(heads):
        query = projected[rows, head_columns(heads, 0, head)] * jnp.asarray(HDIM ** (-0.5), BF16)
        probs = softmax_parts(query, projected[:, head_columns(heads, 1, head)], bias).astype(BF16)
        outs.append(jnp.dot(probs, projected[:, head_columns(heads, 2, head)], preferred_element_type=F32))
    out_ref[...] = jnp.concatenate(outs, axis=1).astype(BF16)


def block_rows(rows, most):
    return most if rows % most == 0 else 128


def constant(shape):
    return pl.BlockSpec(shape, lambda i: (0,) * len(shape))


def attend(plan, projected, bias):
    rows, cols = projected.shape[0], projected.shape[1] // 3
    block = block_rows(rows, 128)
    return pl.pallas_call(
        functools.partial(attend_kernel, plan.heads, block),
        out_shape=jax.ShapeDtypeStruct((rows, cols), BF16),
        grid=(rows // block,),
        in_specs=[constant(projected.shape), constant(bias.shape)],
        out_specs=pl.BlockSpec((block, cols), lambda i: (i, 0)),
        compiler_params=pltpu.CompilerParams(vmem_limit_bytes=48 << 20),
        cost_estimate=pl.CostEstimate(flops=16 * rows * rows * cols, bytes_accessed=8 * rows * cols, transcendentals=0),
        name="attend",
    )(projected, bias)


def attend_back_kernel(
    heads, steps, block, projected, grad_merged, merge_pair, text, bias_ref, out, key_sum, value_sum
):
    step = pl.program_id(0)
    scale = jnp.asarray(HDIM ** (-0.5), BF16)

    @pl.when(step == 0)
    def _():
        key_sum[...] = jnp.zeros_like(key_sum)
        value_sum[...] = jnp.zeros_like(value_sum)

    rows = pl.ds(pl.multiple_of(step * block, block), block)
    bias = bias_ref[...]
    image, other_stream = [
        lax.dot_general(grad_merged[...], merge_pair[j], CONTRACT_LAST, preferred_element_type=F32) for j in range(2)
    ]
    grad_attended = jnp.where(text[...] > 0, other_stream, image).astype(BF16)
    grads = []
    for head in range(heads):
        query = projected[rows, head_columns(heads, 0, head)] * scale
        key = projected[:, head_columns(heads, 1, head)]
        grad_out = grad_attended[:, head * HDIM : (head + 1) * HDIM]
        probs = softmax_parts(query, key, bias)
        grad_probs = lax.dot_general(
            grad_out, projected[:, head_columns(heads, 2, head)], CONTRACT_LAST, preferred_element_type=F32
        )
        inner = jnp.sum(probs * grad_probs, axis=1, keepdims=True)
        grad_scores = (probs * (grad_probs - inner)).astype(BF16)
        grads.append(jnp.dot(grad_scores, key, preferred_element_type=F32) * HDIM ** (-0.5))
        key_sum[head] += lax.dot_general(query, grad_scores, CONTRACT_FIRST, preferred_element_type=F32)
        value_sum[head] += lax.dot_general(grad_out, probs.astype(BF16), CONTRACT_FIRST, preferred_element_type=F32)
    cols = heads * HDIM
    out[rows, :cols] = jnp.concatenate(grads, axis=1).astype(BF16)

    @pl.when(step == steps - 1)
    def _():
        total = out.shape[0]
        out[:, cols : 2 * cols] = key_sum[...].reshape(cols, total).T.astype(BF16)
        out[:, 2 * cols :] = value_sum[...].reshape(cols, total).T.astype(BF16)


def attend_back(plan, projected, grad_merged, merge_pair, text, bias):
    rows, cols = projected.shape[0], projected.shape[1] // 3
    block = block_rows(rows, 256)
    return pl.pallas_call(
        functools.partial(attend_back_kernel, plan.heads, rows // block, block),
        out_shape=jax.ShapeDtypeStruct(projected.shape, BF16),
        grid=(rows // block,),
        in_specs=[
            constant(projected.shape),
            pl.BlockSpec((block, plan.width), lambda i: (i, 0)),
            constant(merge_pair.shape),
            pl.BlockSpec((block, 1), lambda i: (i, 0)),
            constant(bias.shape),
        ],
        out_specs=constant(projected.shape),
        scratch_shapes=[pltpu.VMEM((plan.heads, HDIM, rows), F32)] * 2,
        compiler_params=pltpu.CompilerParams(vmem_limit_bytes=56 << 20),
        cost_estimate=pl.CostEstimate(flops=40 * rows * rows * cols, bytes_accessed=14 * rows * cols, transcendentals=0),
        name="attend_back",
    )(projected, grad_merged, merge_pair, text, bias)


def fold_rows(piece):
    half = piece.shape[0] // 2
    return jnp.concatenate([piece[:half], piece[half:]], axis=1)


def unfold_rows(piece):
    half = piece.shape[1] // 2
    return jnp.concatenate([piece[:, :half], piece[:, half:]], axis=0)


def terms_kernel(plan, fold, chunk, rows, grads, text, out, kept):
    width = rows.shape[1]
    for stream, (first, last) in enumerate(((0, plan.image_end), (plan.text_start, plan.rows))):
        count = last - first
        mask = text[pl.ds(first, count)]
        keep = (mask > 0) if stream else (mask <= 0)
        kept[pl.ds(0, count)] = jnp.where(keep, grads[pl.ds(first, count)], jnp.zeros((), BF16))

        def step(i, carry):
            start = pl.multiple_of(i * chunk, chunk)
            term = lax.dot_general(
                rows[pl.ds(first, count), pl.ds(start, chunk)],
                kept[pl.ds(0, count)],
                CONTRACT_FIRST,
                preferred_element_type=F32,
            ).astype(BF16)
            if fold:
                for j in range(chunk // fold):
                    out[(stream * width) // fold + i * (chunk // fold) + j] = fold_rows(term[j * fold : (j + 1) * fold])
            else:
                out[stream, pl.ds(start, chunk)] = term
            return carry

        if width == chunk:
            step(0, 0)
        else:
            lax.fori_loop(0, width // chunk, step, 0)


def weight_terms(plan, rows, grads, text, name, fold=0):
    width, cols = rows.shape[1], grads.shape[1]
    chunk = 384 if fold else 256 if width % 256 == 0 else width
    shape = (2 * width // fold, fold // 2, 2 * cols) if fold else (2, width, cols)
    return pl.pallas_call(
        functools.partial(terms_kernel, plan, fold, chunk),
        out_shape=jax.ShapeDtypeStruct(shape, BF16),
        in_specs=[pl.BlockSpec(memory_space=pltpu.VMEM)] * 3,
        out_specs=pl.BlockSpec(memory_space=pltpu.VMEM),
        scratch_shapes=[pltpu.VMEM((plan.image_end, cols), BF16)],
        compiler_params=pltpu.CompilerParams(vmem_limit_bytes=40 << 20),
        cost_estimate=pl.CostEstimate(flops=3 * plan.rows * width * cols, bytes_accessed=1 << 23, transcendentals=0),
        name=name,
    )(rows, grads, text)


def gelu(values):
    return jax.nn.gelu(values, approximate=True)


def in_blocks(plan, size, body):
    def step(i, carry):
        body(i, pl.ds(pl.multiple_of(i * size, size), size))
        return carry

    lax.fori_loop(0, plan.rows // size, step, 0)


def blockwise(plan, i, size, block, pair, dims, mask, out):
    @pl.when(i * size < plan.image_end)
    def _():
        out[...] = lax.dot_general(block, pair[0], dims, preferred_element_type=F32)

    @pl.when(i * size + size > plan.text_start)
    def _():
        out[...] = jnp.where(mask > 0, lax.dot_general(block, pair[1], dims, preferred_element_type=F32), out[...])


def project_kernel(plan, size, rows, pair, text, shift, scale, hidden, out, held):
    def body(i, place):
        mask = text[place]
        normed, _ = norm_rows(rows[place].astype(F32))
        block = (normed * (1.0 + pick_rows(scale[...], mask)) + pick_rows(shift[...], mask)).astype(BF16)
        hidden[place] = block
        blockwise(plan, i, size, block, pair, PLAIN, mask, held)
        out[place] = held[...].astype(BF16)

    in_blocks(plan, size, body)


def up_kernel(plan, size, rows, pair, text, upper, activated):
    def body(i, place):
        blockwise(plan, i, size, rows[place], pair, PLAIN, text[place], upper.at[place])
        activated[place] = gelu(upper[place]).astype(BF16)

    in_blocks(plan, size, body)


def down_back_kernel(plan, size, rows, pair, text, upper, out, held):
    def body(i, place):
        blockwise(plan, i, size, rows[place], pair, CONTRACT_LAST, text[place], held)
        out[place] = jax.vjp(gelu, upper[place])[1](held[...])[0].astype(BF16)

    in_blocks(plan, size, body)


def stream_rows(plan, kernel, size, cols, held, name, outs, *operands):
    spec = pl.BlockSpec(memory_space=pltpu.VMEM)
    shapes = tuple(jax.ShapeDtypeStruct((plan.rows, width), dtype) for width, dtype in outs)
    return pl.pallas_call(
        functools.partial(kernel, plan, size),
        out_shape=shapes,
        in_specs=[spec] * len(operands),
        out_specs=(spec,) * len(shapes),
        scratch_shapes=[pltpu.VMEM((size, cols), F32)] if held else [],
        compiler_params=pltpu.CompilerParams(vmem_limit_bytes=40 << 20),
        cost_estimate=pl.CostEstimate(
            flops=2 * plan.rows * plan.width * cols, bytes_accessed=1 << 24, transcendentals=0
        ),
        name=name,
    )(*operands)


VMEM = pl.BlockSpec(memory_space=pltpu.VMEM)


def own_rows(plan, window, rank):
    main = lax.dynamic_slice_in_dim(window, plan.main_row(rank), plan.rows_dev, 0)
    edge = lax.dynamic_slice_in_dim(window, plan.edge_row(rank), plan.piece, 0)
    return jnp.concatenate([main, edge], axis=0)


def remote(source, target, send_sem, recv_sem, device):
    return pltpu.make_async_remote_copy(
        src_ref=source,
        dst_ref=target,
        send_sem=send_sem,
        recv_sem=recv_sem,
        device_id=(device,),
        device_id_type=pl.DeviceIdType.MESH,
    )


def here(plan):
    return plan.place_of(lax.axis_index("dev"))


def other(rank, step, size):
    return lax.rem(rank + step, size)


def meet(devices):
    barrier = pltpu.get_barrier_semaphore()
    for device in devices:
        pl.semaphore_signal(barrier, inc=1, device_id=(device,), device_id_type=pl.DeviceIdType.MESH)
    pl.semaphore_wait(barrier, len(devices))


def group_devices(plan, seq, rank):
    return [plan.device_of(seq, other(rank, step, plan.group)) for step in range(1, plan.group)]


def column_devices(plan, seq, rank):
    return [plan.device_of(other(seq, step, plan.sequences), rank) for step in range(1, plan.sequences)]


def every_device(plan, device):
    return [other(device, step, plan.devices) for step in range(1, plan.devices)]


def call(kernel, name, ident, out_shape, scratch, operands, in_specs=None, out_specs=None, vmem=40 << 20):
    outs = out_shape if isinstance(out_shape, tuple) else (out_shape,)
    return pl.pallas_call(
        kernel,
        out_shape=out_shape,
        in_specs=in_specs or [VMEM] * len(operands),
        out_specs=out_specs or (tuple([VMEM] * len(outs)) if isinstance(out_shape, tuple) else VMEM),
        scratch_shapes=scratch,
        compiler_params=pltpu.CompilerParams(
            collective_id=ident, has_side_effects=True, vmem_limit_bytes=vmem
        ),
        name=name,
    )(*operands)


def aligned(start):
    return pl.multiple_of(start, 16)


def block_parts(plan, ref, rank):
    return (
        ref.at[pl.ds(aligned(plan.main_row(rank)), plan.rows_dev)],
        ref.at[pl.ds(aligned(plan.edge_row(rank)), plan.piece)],
    )


def own_parts(plan, ref):
    return ref.at[pl.ds(0, plan.rows_dev)], ref.at[pl.ds(plan.rows_dev, plan.piece)]


def load_block(plan, ref, rank):
    main, edge = block_parts(plan, ref, rank)
    return jnp.concatenate([main[...], edge[...]], axis=0)


def sum_scratch(plan, wire=BF16):
    half, own, width = plan.group // 2, plan.own, plan.width
    return [
        pltpu.VMEM((half + 1, own, width), F32),
        pltpu.VMEM((half, own, width), F32),
        pltpu.VMEM((half - 1, own, width), wire),
        pltpu.VMEM((half - 1, own, width), wire),
        pltpu.SemaphoreType.DMA((half,)),
        pltpu.SemaphoreType.DMA((half,)),
        pltpu.SemaphoreType.DMA((half,)),
        pltpu.SemaphoreType.DMA((half,)),
    ]


SUM_SCRATCH = 8


def product(plan, rows, pair, text, dims, rank, out):
    block = load_block(plan, rows, rank)
    text_row = load_block(plan, text, rank) > 0
    chunk = 256

    def step(i, carry):
        cols = pl.ds(pl.multiple_of(i * chunk, chunk), chunk)
        parts = []
        for stream in range(2):
            weight = pair[stream, cols, :] if dims is CONTRACT_LAST else pair[stream, :, cols]
            parts.append(lax.dot_general(block, weight, dims, preferred_element_type=F32))
        out[:, cols] = jnp.where(text_row, parts[1], parts[0])
        return carry

    lax.fori_loop(0, plan.width // chunk, step, 0)


def scatter_start(plan, seq, rank, rows, pair, text, dims, away, near, going, coming,
                  pair_send, pair_recv, far_send, far_recv):
    half = plan.group // 2
    chip, core = lax.div(rank, 2), lax.rem(rank, 2)
    partner = plan.device_of(seq, 2 * chip + 1 - core)
    order = list(range(1, half)) + [0]

    def pair_copy(step):
        return remote(away.at[step], near.at[step], pair_send.at[step], pair_recv.at[step], partner)

    def far_copy(step):
        to = plan.device_of(seq, 2 * other(chip, step, half) + core)
        return remote(going.at[step - 1], coming.at[step - 1], far_send.at[step], far_recv.at[step], to)

    def turn(i, carry):
        for_partner = (i < 2) | (lax.rem(i, 2) == 1) & (i < 2 * half - 1)
        place = jnp.where(i < 2, i, jnp.where(for_partner, lax.div(i + 1, 2), lax.div(i, 2) - 1))
        place = jnp.where(i == 2 * half - 1, half - 1, place)
        step = other(place, 1, half)
        block = 2 * other(chip, step, half) + jnp.where(for_partner, 1 - core, core)
        product(plan, rows, pair, text, dims, block, away.at[jnp.where(for_partner, step, half)])

        @pl.when(for_partner)
        def _():
            pair_copy(step).start()

        @pl.when(jnp.logical_not(for_partner))
        def _():
            pair_copy(step).wait_recv()
            away[half] = away[half] + near[step]

        @pl.when(jnp.logical_not(for_partner) & (place < half - 1))
        def _():
            going[step - 1] = away[half].astype(going.dtype)
            far_copy(step).start()

        return carry

    lax.fori_loop(0, 2 * half, turn, 0)

    def result(use):
        for step in range(1, half):
            far_copy(step).wait_recv()
        size = 32 if plan.own % 32 == 0 else 16

        def some(i, carry):
            place = pl.ds(pl.multiple_of(i * size, size), size)
            total = away[half, place]
            for step in range(1, half):
                total = total + coming[step - 1, place].astype(F32)
            use(place, total)
            return carry

        lax.fori_loop(0, plan.own // size, some, 0)
        for step in range(half):
            pair_copy(step).wait_send()
        for step in range(1, half):
            far_copy(step).wait_send()

    return result


def share_scratch(plan):
    return [pltpu.SemaphoreType.DMA((plan.group, 2))] * 2 + [pltpu.SemaphoreType.DMA((plan.group, 2))]


def share_rows(plan, seq, rank, parts, window, send, recv, pass_send):
    half = plan.group // 2
    chip, core = lax.div(rank, 2), lax.rem(rank, 2)
    partner_rank = 2 * chip + 1 - core
    partner = plan.device_of(seq, partner_rank)

    def send_own(to_device, slot):
        copies = [
            remote(source, target, send.at[slot, i], recv.at[slot, i], to_device)
            for i, (source, target) in enumerate(zip(parts, block_parts(plan, window, rank)))
        ]
        for copy in copies:
            copy.start()
        return copies

    flying = {}
    for step in range(1, half):
        flying[step] = send_own(plan.device_of(seq, 2 * other(chip, step, half) + core), step)
    flying[0] = send_own(partner, 0)
    for source, target in zip(parts, block_parts(plan, window, rank)):
        target[...] = source[...]
    passed = []
    for step in range(1, half):
        for copy in flying[step]:
            copy.wait_recv()
        came = 2 * other(chip, half - step, half) + core
        copies = [
            remote(place, place, pass_send.at[step, i], recv.at[half + step, i], partner)
            for i, place in enumerate(block_parts(plan, window, came))
        ]
        for copy in copies:
            copy.start()
        passed.extend(copies)
    for copy in flying[0]:
        copy.wait_recv()
    for copy in passed:
        copy.wait_recv()
    for copies in flying.values():
        for copy in copies:
            copy.wait_send()
    for copy in passed:
        copy.wait_send()


def entry_kernel(plan, tokens, grads, mod_part, *refs):
    if plan.chip_heads:
        merge, merge_out, *refs = refs[:1] + refs[4:5] + refs[1:4] + refs[5:]
        merge_send, merge_recv, *refs = refs[-2:] + refs[:-2]
    (token_window, grad_window, mods, token_own, grad_own, plane, across, chunk, edge_send, edge_recv,
     t_send, t_recv, t_pass, g_send, g_recv, g_pass, m_send, m_recv) = refs
    device = lax.axis_index("dev")
    seq, rank = plan.place_of(device)
    meet(every_device(plan, device))
    swaps = []
    if plan.chip_heads:
        core = lax.rem(rank, 2)
        partner = plan.device_of(seq, 2 * lax.div(rank, 2) + 1 - core)
        for stream in range(2):
            copy = remote(
                merge.at[2 * stream + 1 - core],
                merge_out.at[stream, core],
                merge_send.at[stream],
                merge_recv.at[stream],
                partner,
            )
            copy.start()
            swaps.append(copy)
            merge_out[stream, core] = merge[2 * stream + core]
    hops = []
    for step in range(1, plan.group):
        to = other(rank, step, plan.group)
        copy = remote(mod_part.at[to], plane.at[step], m_send.at[0, step], m_recv.at[0, step], plan.device_of(seq, to))
        copy.start()
        hops.append(copy)
    arrays = ((tokens, token_own), (grads, grad_own))
    count = len(plan.segments)
    for which, (source, own) in enumerate(arrays):
        for index, (to_rank, row, rows, step, owner, owner_row) in enumerate(plan.segments):
            @pl.when(rank == owner)
            def _():
                remote(
                    source.at[pl.ds(owner_row, rows)],
                    own.at[pl.ds(row, rows)],
                    edge_send.at[which * count + index],
                    edge_recv.at[which * count + index],
                    plan.device_of(lax.rem(seq + plan.sequences - step, plan.sequences), to_rank),
                ).start()
    for copy in hops:
        copy.wait_recv()
    total = mod_part[rank]
    for step in range(1, plan.group):
        total = total + plane[step]
    plane[0] = total
    hops_across = []
    for step in range(1, plan.sequences):
        to = other(seq, step, plan.sequences)
        copy = remote(plane.at[0, to], across.at[seq], m_send.at[1, step], m_recv.at[1, step], plan.device_of(to, rank))
        copy.start()
        hops_across.append(copy)
    across[seq] = plane[0, seq]
    for which, (source, own) in enumerate(arrays):
        for index, (to_rank, row, rows, step, owner, owner_row) in enumerate(plan.segments):
            @pl.when(rank == to_rank)
            def _():
                remote(
                    source.at[pl.ds(owner_row, rows)],
                    own.at[pl.ds(row, rows)],
                    edge_send.at[which * count + index],
                    edge_recv.at[which * count + index],
                    plan.device_of(lax.rem(seq + plan.sequences + step, plan.sequences), owner),
                ).wait_recv()
    share_rows(plan, seq, rank, (tokens, token_own), token_window, t_send, t_recv, t_pass)
    for copy in hops_across:
        copy.wait_recv()
    half = plan.sequences // 2
    for stream in range(2):
        total = across[stream * half]
        for i in range(1, half):
            total = total + across[stream * half + i]
        chunk[stream] = total
    hops_back = []
    for step in range(1, plan.group):
        to = other(rank, step, plan.group)
        copy = remote(chunk, mods.at[rank], m_send.at[2, step], m_recv.at[2, step], plan.device_of(seq, to))
        copy.start()
        hops_back.append(copy)
    mods[rank] = chunk[...]
    share_rows(plan, seq, rank, (grads, grad_own), grad_window, g_send, g_recv, g_pass)
    for copy in hops_back:
        copy.wait_recv()
    for copy in hops + hops_across + hops_back:
        copy.wait_send()
    for copy in swaps:
        copy.wait()
    for which, (source, own) in enumerate(arrays):
        for index, (to_rank, row, rows, step, owner, owner_row) in enumerate(plan.segments):
            @pl.when(rank == owner)
            def _():
                remote(
                    source.at[pl.ds(owner_row, rows)],
                    own.at[pl.ds(row, rows)],
                    edge_send.at[which * count + index],
                    edge_recv.at[which * count + index],
                    plan.device_of(lax.rem(seq + plan.sequences - step, plan.sequences), to_rank),
                ).wait_send()


def entry(plan, tokens, grads, mod_part, merge):
    lanes = mod_part.shape[1] // plan.group // 128
    pieces = mod_part.reshape(plan.sequences, plan.group, lanes, 128).transpose(1, 0, 2, 3)
    window = jax.ShapeDtypeStruct((plan.rows, plan.width), BF16)
    dma = pltpu.SemaphoreType.DMA
    most = max(plan.group, plan.sequences)
    shapes = (window, window, jax.ShapeDtypeStruct((plan.group, 2, lanes, 128), F32))
    operands = (tokens, grads, pieces)
    scratch = (
        [
            pltpu.VMEM((plan.piece, plan.width), BF16),
            pltpu.VMEM((plan.piece, plan.width), BF16),
            pltpu.VMEM((plan.group, plan.sequences, lanes, 128), F32),
            pltpu.VMEM((plan.sequences, lanes, 128), F32),
            pltpu.VMEM((2, lanes, 128), F32),
            dma((2 * len(plan.segments),)),
            dma((2 * len(plan.segments),)),
        ]
        + share_scratch(plan)
        + share_scratch(plan)
        + [dma((3, most)), dma((3, most))]
    )
    if plan.chip_heads:
        shapes += (jax.ShapeDtypeStruct((2, 2) + merge.shape[1:], BF16),)
        operands += (merge,)
        scratch += [dma((2,)), dma((2,))]
    token_window, grad_window, mods, *rest = call(
        functools.partial(entry_kernel, plan), "entry", 1, shapes, scratch, operands
    )
    merge_pair = rest[0].reshape(2, -1, plan.width) if plan.chip_heads else merge
    return token_window, grad_window, mods.transpose(1, 0, 2, 3).reshape(2, -1), merge_pair


def project_columns(plan, rank):
    share = plan.width // plan.group
    first = (rank % 2) * (plan.width // 2) + (rank // 2) * share
    return [part * plan.width + first for part in range(3)], share


def up_columns(plan, rank, cols):
    planes = plan.sequences // 2
    share = cols // planes // plan.group
    return [plane * plan.group * share + rank * share for plane in range(planes)], share


def start_swap(plan, seq, rank, source, target, send, recv):
    copies = []
    for step in range(1, plan.group):
        to = other(rank, step, plan.group)
        copy = remote(source.at[to], target.at[rank], send.at[step], recv.at[step], plan.device_of(seq, to))
        copy.start()
        copies.append(copy)
    target[rank] = source[rank]
    return copies


def swap_in_kernel(plan, project, up, project_out, up_out, project_cut, up_cut, p_send, p_recv, u_send, u_recv):
    seq, rank = here(plan)
    for to in range(plan.group):
        starts, share = project_columns(plan, to)
        project_cut[to] = fold_rows(jnp.concatenate([project[:, c : c + share] for c in starts], axis=1))
    meet(group_devices(plan, seq, rank))
    copies = start_swap(plan, seq, rank, project_cut, project_out, p_send, p_recv)
    for to in range(plan.group):
        starts, share = up_columns(plan, to, up.shape[1])
        up_cut[to] = jnp.concatenate([up[:, c : c + share] for c in starts], axis=1)
    copies += start_swap(plan, seq, rank, up_cut, up_out, u_send, u_recv)
    for copy in copies:
        copy.wait()


def swap_in(plan, project, up):
    rows = project.shape[0]
    dma = pltpu.SemaphoreType.DMA
    shapes = [
        (plan.group, rows // 2, 2 * project.shape[1] // plan.group),
        (plan.group, rows, up.shape[1] // plan.group),
    ]
    return call(
        functools.partial(swap_in_kernel, plan),
        "swap_in",
        4,
        tuple(jax.ShapeDtypeStruct(shape, BF16) for shape in shapes),
        [pltpu.VMEM(shape, BF16) for shape in shapes] + [dma((plan.group,))] * 4,
        (project, up),
    )


def place_columns(plan, got, out, columns, unfold):
    for source in range(plan.group):
        starts, share = columns(plan, source)
        piece = unfold_rows(got[source]) if unfold else got[source]
        for i, c in enumerate(starts):
            out[:, c : c + share] = piece[:, i * share : (i + 1) * share]


def line_sum(plan, seq, rank, term, out, up_in, up_out, down_in, down_out, up_send, up_recv, down_send, down_recv):
    count = plan.sequences

    def hop(source, target, send, recv, owner, to):
        return remote(source.at[owner], target.at[owner], send.at[owner], recv.at[owner], plan.device_of(to, rank))

    above, below = lax.rem(seq + 1, count), lax.rem(seq + count - 1, count)
    ways = [
        (list(range(count - 1, 0, -1)), above, below, up_in, up_out, up_send, up_recv, lambda owner: seq < owner, seq == 0),
        (list(range(count - 1)), below, above, down_in, down_out, down_send, down_recv, lambda owner: seq > owner,
         seq == count - 1),
    ]
    def pass_on(turn, way):
        owners, to, back, came, goes, send, recv, mine, first = way
        owner = owners[turn]

        @pl.when(mine(owner) & first)
        def _():
            hop(term, came, send, recv, owner, to).start()

        @pl.when(mine(owner) & jnp.logical_not(first))
        def _():
            hop(goes, came, send, recv, owner, back).wait_recv()
            goes[owner] = (term[owner].astype(F32) + came[owner].astype(F32)).astype(BF16)
            hop(goes, came, send, recv, owner, to).start()

    for turn in range(count - 1):
        @pl.when(seq < count // 2)
        def _():
            pass_on(turn, ways[0])
            pass_on(turn, ways[1])

        @pl.when(seq >= count // 2)
        def _():
            pass_on(turn, ways[1])
            pass_on(turn, ways[0])

    out[...] = term[seq].astype(F32)
    for owners, to, back, came, goes, send, recv, mine, first in ways:
        for owner in owners:
            @pl.when(seq == owner)
            def _():
                hop(goes, came, send, recv, owner, back).wait_recv()
                out[...] += came[owner].astype(F32)

            @pl.when(mine(owner))
            def _():
                hop(goes, came, send, recv, owner, to).wait_send()


def finish_kernel(plan, up, project, *refs):
    if plan.chip_heads:
        term, up_out, project_out, merge_out, *refs = refs
        *refs, line = refs[:6] + [refs[6:]]
    else:
        up_out, project_out, *refs = refs
    up_got, project_got, u_send, u_recv, p_send, p_recv = refs
    seq, rank = here(plan)
    meet(group_devices(plan, seq, rank) + column_devices(plan, seq, rank))
    ups = start_swap(plan, seq, rank, up, up_got, u_send, u_recv)
    projects = start_swap(plan, seq, rank, project, project_got, p_send, p_recv)
    if plan.chip_heads:
        line_sum(plan, seq, rank, term, merge_out, *line)
    for copy in ups:
        copy.wait()
    place_columns(plan, up_got, up_out, lambda p, r: up_columns(p, r, up_out.shape[1]), False)
    for copy in projects:
        copy.wait()
    place_columns(plan, project_got, project_out, project_columns, True)


def finish(plan, up, project, term):
    dma = pltpu.SemaphoreType.DMA
    rows = up.shape[1]
    shapes = (
        jax.ShapeDtypeStruct((rows, plan.group * up.shape[2]), BF16),
        jax.ShapeDtypeStruct((rows, plan.group * project.shape[2] // 2), BF16),
    )
    operands = (up, project)
    scratch = [pltpu.VMEM(up.shape, BF16), pltpu.VMEM(project.shape, BF16)] + [dma((plan.group,))] * 4
    if plan.chip_heads:
        shapes += (jax.ShapeDtypeStruct(term.shape[1:], F32),)
        operands += (term,)
        scratch += [pltpu.VMEM(term.shape, BF16)] * 4 + [dma((plan.sequences,))] * 4
    up_grad, project_grad, *merge_grad = call(
        functools.partial(finish_kernel, plan), "finish", 6, shapes, scratch, operands
    )
    return up_grad.astype(F32), project_grad.astype(F32), merge_grad


def pick_rows(table, text):
    return jnp.where(text > 0, table[1:2, :], table[0:1, :])


def norm_rows(values):
    mean = jnp.mean(values, axis=1, keepdims=True)
    centred = values - mean
    inv = lax.rsqrt(jnp.mean(centred * centred, axis=1, keepdims=True) + EPSILON)
    return centred * inv, inv


def middle_kernel(plan, rows, pair, window_text, tokens, gate_a, scale_b, shift_b, text, merged, window, own, *scratch):
    seq, rank = here(plan)
    meet(group_devices(plan, seq, rank))
    result = scatter_start(plan, seq, rank, rows, pair, window_text, PLAIN, *scratch[:SUM_SCRATCH])

    def use(place, total):
        merged[place] = total
        mask = text[place]
        middle = tokens[place].astype(F32) + pick_rows(gate_a[...], mask) * total
        normed, _ = norm_rows(middle)
        own[place] = (normed * (1.0 + pick_rows(scale_b[...], mask)) + pick_rows(shift_b[...], mask)).astype(BF16)

    result(use)
    share_rows(plan, seq, rank, own_parts(plan, own), window, *scratch[SUM_SCRATCH:])


def own_shape(plan, dtype=F32):
    return jax.ShapeDtypeStruct((plan.own, plan.width), dtype)


def window_shape(plan):
    return jax.ShapeDtypeStruct((plan.rows, plan.width), BF16)


def middle_rows(plan, rows, pair, window_text, tokens, gate_a, scale_b, shift_b, text):
    return call(
        functools.partial(middle_kernel, plan),
        "middle",
        2,
        (own_shape(plan), window_shape(plan)),
        [pltpu.VMEM((plan.own, plan.width), BF16)] + sum_scratch(plan, F32) + share_scratch(plan),
        (rows, pair, window_text, tokens, gate_a, scale_b, shift_b, text),
    )


def back_kernel(plan, rows, pair, window_text, grad, middle, gate_a, scale_b, text, grad_hidden, grad_middle, window, own, *scratch):
    seq, rank = here(plan)
    meet(group_devices(plan, seq, rank))
    result = scatter_start(plan, seq, rank, rows, pair, window_text, CONTRACT_LAST, *scratch[:SUM_SCRATCH])

    def use(place, total):
        grad_hidden[place] = total
        mask = text[place]
        normed, inv = norm_rows(middle[place])
        inner = total * (1.0 + pick_rows(scale_b[...], mask))
        mean_grad = jnp.mean(inner, axis=1, keepdims=True)
        mean_cross = jnp.mean(inner * normed, axis=1, keepdims=True)
        back = grad[place].astype(F32) + inv * (inner - mean_grad - normed * mean_cross)
        grad_middle[place] = back
        own[place] = (pick_rows(gate_a[...], mask) * back).astype(BF16)

    result(use)
    share_rows(plan, seq, rank, own_parts(plan, own), window, *scratch[SUM_SCRATCH:])


def back_rows(plan, rows, pair, window_text, grad, middle, gate_a, scale_b, text):
    return call(
        functools.partial(back_kernel, plan),
        "back",
        3,
        (own_shape(plan), own_shape(plan), window_shape(plan)),
        [pltpu.VMEM((plan.own, plan.width), BF16)] + sum_scratch(plan) + share_scratch(plan),
        (rows, pair, window_text, grad, middle, gate_a, scale_b, text),
    )


def edge_copy(plan, seq, source, first_row, target, send, recv, index):
    from_rank, row, rows, step, owner, owner_row = plan.segments[index]
    return remote(
        source.at[pl.ds(first_row + row, rows)],
        target.at[pl.ds(owner_row, rows)],
        send.at[index],
        recv.at[index],
        plan.device_of(lax.rem(seq + plan.sequences + step, plan.sequences), owner),
    )


def start_edges(plan, seq, rank, *refs):
    for index, segment in enumerate(plan.segments):
        @pl.when(rank == segment[0])
        def _():
            edge_copy(plan, seq, *refs, index).start()


def finish_edges(plan, seq, rank, *refs):
    for index, segment in enumerate(plan.segments):
        @pl.when(rank == segment[4])
        def _():
            edge_copy(plan, seq, *refs, index).wait_recv()

        @pl.when(rank == segment[0])
        def _():
            edge_copy(plan, seq, *refs, index).wait_send()


def edge_scratch(plan):
    return [pltpu.SemaphoreType.DMA((len(plan.segments),))] * 2


def stream_sums(values, masks):
    return jnp.concatenate([jnp.sum(values * mask, axis=0, keepdims=True) for mask in masks], axis=0)


def last_kernel(plan, names, *refs):
    at = types.SimpleNamespace(**dict(zip(names, refs)))
    low_scratch = refs[len(names) : len(names) + SUM_SCRATCH]
    back_scratch = refs[len(names) + SUM_SCRATCH : len(names) + 2 * SUM_SCRATCH]
    device = lax.axis_index("dev")
    seq, rank = plan.place_of(device)
    stream = lax.div(2 * seq, plan.sequences)
    at.layer_extra[...] = jnp.zeros_like(at.layer_extra)
    at.token_extra[...] = jnp.zeros_like(at.token_extra)
    meet(every_device(plan, device))
    low_sum = scatter_start(plan, seq, rank, at.activated, at.down_pair, at.window_text, PLAIN, *low_scratch)
    back_sum = scatter_start(plan, seq, rank, at.grads, at.project_pair, at.window_text, CONTRACT_LAST, *back_scratch)
    swaps = []
    if plan.chip_heads:
        core = lax.rem(rank, 2)
        partner = plan.device_of(seq, 2 * lax.div(rank, 2) + 1 - core)
        for j in range(2):
            copy = remote(
                at.term.at[j, 1 - core], at.term_out.at[2 * j + core], at.term_send.at[j], at.term_recv.at[j], partner
            )
            copy.start()
            swaps.append(copy)
            at.term_out[2 * j + core] = at.term[j, core]
    width = plan.width
    at.local[...] = jnp.zeros_like(at.local)
    at.local[:, 2 * width : 5 * width] = at.rest[...]

    def add(first, place, values):
        masks = (at.masks[place, 0:1], at.masks[place, 1:2])
        at.local[:, first * width : (first + 1) * width] += stream_sums(values, masks)

    def use_low(place, lowered):
        at.layer_own[place] = (at.middle[place] + pick_rows(at.gate_b[...], at.text[place]) * lowered).astype(BF16)
        add(5, place, at.grad[place].astype(F32) * lowered)

    low_sum(use_low)
    layer_edges = (at.layer_own, plan.rows_dev, at.layer_extra, at.l_send, at.l_recv)
    start_edges(plan, seq, rank, *layer_edges)
    at.layer[...] = at.layer_own[pl.ds(0, plan.rows_dev)]

    def use_back(place, total):
        normed, inv = norm_rows(at.tokens[place].astype(F32))
        add(0, place, total)
        add(1, place, total * normed)
        inner = total * (1.0 + pick_rows(at.scale_a[...], at.text[place]))
        mean_grad = jnp.mean(inner, axis=1, keepdims=True)
        mean_cross = jnp.mean(inner * normed, axis=1, keepdims=True)
        at.token_own[place] = at.grad_middle[place] + inv * (inner - mean_grad - normed * mean_cross)

    back_sum(use_back)
    cols = 6 * width // plan.group

    def chunk(index):
        return pl.ds(pl.multiple_of(index * cols, 128), cols)

    hops = []
    for step in range(1, plan.group):
        to = other(rank, step, plan.group)
        copy = remote(
            at.local.at[:, chunk(to)], at.first.at[step], at.t_send.at[0, step], at.t_recv.at[0, step], plan.device_of(seq, to)
        )
        copy.start()
        hops.append(copy)
    token_edges = (at.token_own, plan.rows_dev, at.token_extra, at.e_send, at.e_recv)
    start_edges(plan, seq, rank, *token_edges)
    for copy in hops:
        copy.wait_recv()
    sums = at.local[:, chunk(rank)]
    for step in range(1, plan.group):
        sums = sums + at.first[step]
    for i in range(2):
        at.mine[i] = sums[i : i + 1]
    across = []
    for step in range(1, plan.sequences):
        to = other(seq, step, plan.sequences)
        to_stream = lax.div(2 * to, plan.sequences)
        copy = remote(
            at.mine.at[to_stream], at.second.at[seq], at.t_send.at[1, step], at.t_recv.at[1, step], plan.device_of(to, rank)
        )
        copy.start()
        across.append(copy)
    at.second[seq] = at.mine[stream]
    at.token[...] = at.token_own[pl.ds(0, plan.rows_dev)]
    for copy in across:
        copy.wait_recv()
    last = []
    for step in range(1, plan.group):
        to = other(rank, step, plan.group)
        copy = remote(at.second, at.table.at[rank], at.t_send.at[2, step], at.t_recv.at[2, step], plan.device_of(seq, to))
        copy.start()
        last.append(copy)
    at.table[rank] = at.second[...]
    for copy in last:
        copy.wait_recv()

    piece = None
    for index in range(plan.group):
        grads = jnp.concatenate([at.table[index, s] for s in range(plan.sequences)], axis=0).astype(BF16)
        part = lax.dot_general(
            grads, at.weight[:, index * cols : (index + 1) * cols], CONTRACT_LAST, preferred_element_type=F32
        )
        piece = part if piece is None else piece + part
    at.piece[...] = piece
    at.everyone[seq, rank] = piece
    spread = []
    for step in range(1, plan.group):
        to = other(rank, step, plan.group)
        copy = remote(
            at.piece, at.everyone.at[seq, rank], at.c_send.at[0, step], at.c_recv.at[0, step], plan.device_of(seq, to)
        )
        copy.start()
        spread.append(copy)
    for copy in spread:
        copy.wait_recv()
    for step in range(1, plan.sequences):
        to = other(seq, step, plan.sequences)
        copy = remote(
            at.everyone.at[seq], at.everyone.at[seq], at.c_send.at[1, step], at.c_recv.at[1, step], plan.device_of(to, rank)
        )
        copy.start()
        spread.append(copy)
    for copy in spread[plan.group - 1 :]:
        copy.wait_recv()
    for copy in hops + across + last + spread:
        copy.wait_send()
    for copy in swaps:
        copy.wait()
    finish_edges(plan, seq, rank, *layer_edges)
    finish_edges(plan, seq, rank, *token_edges)


def last_rows(plan, term, weight, **operands):
    rows, share = weight.shape[0], plan.width // plan.group // 2
    cols = 6 * plan.width // plan.group
    most = max(plan.group, plan.sequences)
    dma = pltpu.SemaphoreType.DMA

    def placed(dtype):
        return jax.ShapeDtypeStruct((plan.rows_dev, plan.width), dtype)

    operands = dict(operands, weight=weight)
    outs = dict(
        layer=placed(BF16),
        layer_extra=placed(BF16),
        token=placed(F32),
        token_extra=placed(F32),
        table=jax.ShapeDtypeStruct((plan.group, plan.sequences, 1, cols), F32),
        everyone=jax.ShapeDtypeStruct((plan.sequences, plan.group, plan.sequences, rows), F32),
    )
    edges = len(plan.segments)
    scratch = dict(
        layer_own=pltpu.VMEM((plan.own, plan.width), BF16),
        token_own=pltpu.VMEM((plan.own, plan.width), F32),
        local=pltpu.VMEM((2, 6 * plan.width), F32),
        first=pltpu.VMEM((plan.group, 2, cols), F32),
        second=pltpu.VMEM((plan.sequences, 1, cols), F32),
        mine=pltpu.VMEM((2, 1, cols), F32),
        piece=pltpu.VMEM((plan.sequences, rows), F32),
        t_send=dma((3, most)),
        t_recv=dma((3, most)),
        c_send=dma((2, most)),
        c_recv=dma((2, most)),
        l_send=dma((edges,)),
        l_recv=dma((edges,)),
        e_send=dma((edges,)),
        e_recv=dma((edges,)),
    )
    if plan.chip_heads:
        operands["term"] = term.reshape(2, 2, share, plan.width)
        outs["term_out"] = jax.ShapeDtypeStruct((plan.sequences, share, plan.width), BF16)
        scratch.update(term_send=dma((2,)), term_recv=dma((2,)))
    names = tuple(operands) + tuple(outs) + tuple(scratch)
    got = call(
        functools.partial(last_kernel, plan, names),
        "last",
        10,
        tuple(outs.values()),
        list(scratch.values()) + sum_scratch(plan) + sum_scratch(plan),
        tuple(operands.values()),
        vmem=58 << 20,
    )
    got = types.SimpleNamespace(**dict(zip(outs, got)))
    got.table = got.table[:, :, 0].transpose(1, 0, 2).reshape(plan.sequences, -1)
    got.term = got.term_out if plan.chip_heads else term
    return got


def over_sequences(plan, pieces):
    full = lax.all_gather(pieces, "dev", axis=0, axis_index_groups=plan.rank_groups())
    return full.reshape((plan.devices,) + pieces.shape[1:])


def over_sequences_sum(plan, pieces):
    return lax.psum_scatter(pieces, "dev", scatter_dimension=0, axis_index_groups=plan.rank_groups())


def merge_rows(plan, weight, rank):
    if plan.chip_heads:
        return lax.all_gather(weight, "dev", axis=0, axis_index_groups=plan.rank_groups())
    share = plan.width // plan.group
    full = lax.all_gather(weight, "dev", axis=0, tiled=True)
    full = full.reshape(2, 2, plan.group // 2, share, weight.shape[1])
    full = lax.dynamic_index_in_dim(full, lax.rem(rank, 2), 1, keepdims=False)
    return lax.dynamic_index_in_dim(full, lax.div(rank, 2), 1, keepdims=False)


def merge_sum(plan, term, rank):
    half = plan.group // 2
    _, share, cols = term.shape
    mine = [jnp.where(lax.rem(rank, 2) == k, term, jnp.zeros((), BF16)) for k in range(2)]
    full = jnp.zeros((2, 2, half, share, cols), BF16)
    full = lax.dynamic_update_slice_in_dim(full, jnp.stack(mine, axis=1)[:, :, None], lax.div(rank, 2), 2)
    return lax.psum_scatter(full.reshape(-1, cols), "dev", scatter_dimension=0, tiled=True)


def down_slices(plan, weight):
    full = lax.all_gather(weight, "dev", axis=0, axis_index_groups=plan.rank_groups())
    return full.reshape(2, -1, weight.shape[1])


def pick(table, text_rows):
    return jnp.where(text_rows[:, None], table[1][None, :], table[0][None, :])


def on_device(
    tokens,
    conditioning,
    text_lengths,
    modulation_weight,
    project_weight,
    merge_weight,
    up_weight,
    down_weight,
    cotangent,
):
    rows_dev, width = tokens.shape
    mod_rows = modulation_weight.shape[0]
    plan = Plan(lax.axis_size("dev"), conditioning.shape[0], rows_dev, width)
    device = lax.axis_index("dev")
    seq, rank = plan.place_of(device)
    feature_start = device * mod_rows % width

    ends = jnp.cumsum(IMG + text_lengths)
    starts = jnp.concatenate([jnp.zeros((1,), jnp.int32), ends[:-1]])
    positions = device * rows_dev + jnp.arange(rows_dev, dtype=jnp.int32)
    row_seq = jnp.sum((starts[None, :] <= positions[:, None]).astype(jnp.int32), axis=1) - 1
    offset = plan.span * seq - plan.edge + jnp.arange(plan.rows, dtype=jnp.int32) - starts[seq]
    valid = (offset >= 0) & (offset < IMG + text_lengths[seq])
    is_text = offset >= IMG
    bias = jnp.where(valid, 0.0, MASKED).astype(F32)[None, :]
    window_text = is_text.astype(F32)[:, None]
    own_valid = own_rows(plan, valid[:, None], rank)[:, 0]
    own_text = own_rows(plan, is_text[:, None], rank)[:, 0]

    cond_float = conditioning.astype(F32)
    silu_low = jax.nn.silu(cond_float).astype(BF16)
    silu_part = lax.dynamic_slice_in_dim(silu_low, feature_start, mod_rows, 1)
    mod_part = jnp.dot(silu_part, modulation_weight, preferred_element_type=F32)

    merge_pair = merge_rows(plan, merge_weight, rank)
    project_pieces, up_pieces = swap_in(plan, project_weight, up_weight)
    project_pieces, up_pieces, merge_pair = lax.optimization_barrier((project_pieces, up_pieces, merge_pair))
    project_pair = over_sequences(plan, project_pieces)
    share = project_pair.shape[2] // 2
    project_pair = jnp.concatenate([project_pair[:, :, :share], project_pair[:, :, share:]], axis=1)
    project_pair = lax.optimization_barrier(project_pair.reshape(2, width, share))
    up_pair = over_sequences(plan, up_pieces).reshape(2, width, -1)
    down_pair = down_slices(plan, down_weight)

    token_window, grad_window, mods, merge_pair = entry(plan, tokens, cotangent, mod_part, merge_pair)
    shift_a, scale_a, gate_a, shift_b, scale_b, gate_b = jnp.split(mods, 6, axis=1)
    grad_window = jnp.where(valid[:, None], grad_window, jnp.zeros((), BF16))

    cols = project_pair.shape[2]
    hidden_a, projected = stream_rows(
        plan, project_kernel, 128, cols, True, "project", ((width, BF16), (cols, BF16)),
        token_window, project_pair, window_text, shift_a, scale_a,
    )
    attended = attend(plan, projected, bias)

    own_tokens = own_rows(plan, token_window, rank)
    own_grad = own_rows(plan, grad_window, rank)
    text_mask = own_text.astype(F32)[:, None]
    merged, hidden_b = middle_rows(
        plan, attended, merge_pair, window_text, own_tokens, gate_a, scale_b, shift_b, text_mask
    )
    middle = own_tokens.astype(F32) + pick(gate_a, own_text) * merged
    normed_b, inv_b = layer_norm(middle)

    units = up_pair.shape[2]
    upper, activated = stream_rows(
        plan, up_kernel, 128, units, False, "up", ((units, F32), (units, BF16)), hidden_b, up_pair, window_text
    )
    grad_lowered = (pick(gate_b, is_text) * grad_window.astype(F32)).astype(BF16)
    down_term = weight_terms(plan, activated, grad_lowered, window_text, "down_terms")
    down_term = down_term.reshape(plan.sequences, -1, width)
    down_term, grad_lowered = lax.optimization_barrier((down_term, grad_lowered))
    down_sum = over_sequences_sum(plan, down_term)
    (grad_upper,) = stream_rows(
        plan, down_back_kernel, block_rows(plan.rows, 256), units, True, "down_back", ((units, BF16),),
        grad_lowered, down_pair, window_text, upper,
    )
    up_term = weight_terms(plan, hidden_b, grad_upper, window_text, "up_terms")
    up_term = up_term.reshape(plan.sequences, plan.group, mod_rows, -1)
    grad_upper, up_term = lax.optimization_barrier((grad_upper, up_term))
    up_sum = over_sequences_sum(plan, up_term)
    grad_hidden_b, grad_middle, grad_merged = back_rows(
        plan, grad_upper, up_pair, window_text, own_grad, middle, gate_a, scale_b, text_mask
    )
    merge_term = weight_terms(plan, attended, grad_merged, window_text, "merge_terms")

    grad_projected = attend_back(plan, projected, grad_merged, merge_pair, window_text, bias)
    grad_projected, down_sum = lax.optimization_barrier((grad_projected, down_sum))
    down_grad = down_sum.astype(F32)
    project_term = weight_terms(plan, hidden_a, grad_projected, window_text, "project_terms", mod_rows)
    project_term = project_term.reshape((plan.sequences, plan.group) + project_term.shape[1:])
    grad_projected, project_term = lax.optimization_barrier((grad_projected, project_term))
    project_sum = over_sequences_sum(plan, project_term)

    masks = jnp.stack([own_valid & ~own_text, own_valid & own_text], axis=1).astype(F32)
    rest = jnp.concatenate(
        [
            jnp.stack([jnp.sum(value * masks[:, j : j + 1], axis=0) for j in range(2)])
            for value in (grad_middle * merged, grad_hidden_b, grad_hidden_b * normed_b)
        ],
        axis=1,
    )
    got = last_rows(
        plan,
        merge_term,
        modulation_weight,
        activated=activated,
        down_pair=down_pair,
        grads=grad_projected,
        project_pair=project_pair,
        window_text=window_text,
        tokens=own_tokens,
        middle=middle,
        grad=own_grad,
        grad_middle=grad_middle,
        gate_b=gate_b,
        scale_a=scale_a,
        text=text_mask,
        masks=masks,
        rest=rest,
    )
    foreign = (row_seq != seq)[:, None]
    layer_out = jnp.where(foreign, got.layer_extra, got.layer)
    tokens_grad = jnp.where(foreign, got.token_extra, got.token)
    own_grads = got.table.astype(BF16)
    modulation_grad = lax.dot_general(silu_part, own_grads, CONTRACT_FIRST, preferred_element_type=F32)
    everyone = got.everyone.reshape(2, plan.devices // 2, plan.sequences, mod_rows)
    grad_silu = (everyone[0] + everyone[1]).transpose(1, 0, 2).reshape(plan.sequences, width)
    conditioning_grad = jax.vjp(jax.nn.silu, cond_float)[1](grad_silu)[0]
    modulation_grad, up_sum = lax.optimization_barrier((modulation_grad, up_sum))
    merge_out, project_sum, *done = lax.optimization_barrier(
        (got.term, project_sum, modulation_grad, down_grad, layer_out, tokens_grad, conditioning_grad)
    )
    modulation_grad, down_grad, layer_out, tokens_grad, conditioning_grad = done
    up_grad, project_grad, merge_grad = finish(plan, up_sum, project_sum, merge_out)
    merge_grad = merge_grad[0] if merge_grad else merge_sum(plan, merge_out, rank).astype(F32)
    return (
        layer_out,
        tokens_grad,
        conditioning_grad,
        modulation_grad,
        project_grad,
        merge_grad,
        up_grad,
        down_grad,
    )


def solution(mesh):
    shard, whole = P("dev", None), P()
    return jax.shard_map(
        on_device,
        mesh=mesh,
        in_specs=(shard, whole, whole, shard, shard, shard, shard, shard, shard),
        out_specs=(shard, shard, whole, shard, shard, shard, shard, shard),
        check_vma=False,
    )
```

```python
import functools
import types

import jax
import jax.numpy as jnp
import numpy as np
from jax import lax
from jax.experimental import pallas as pl
from jax.experimental.pallas import tpu as pltpu
from jax.sharding import PartitionSpec as P

HEADS = 24
HDIM = 64
IMG = 1024
TXT_MIN = 86
TXT_MAX = 154
EPSILON = 1e-06
F32 = jnp.float32
BF16 = jnp.bfloat16
CONTRACT_LAST = (((1,), (1,)), ((), ()))
PLAIN = (((1,), (0,)), ((), ()))
CONTRACT_FIRST = (((0,), (0,)), ((), ()))
MASKED = -1e30


class Plan:
    def __init__(self, devices, sequences, rows_dev, width):
        self.devices, self.sequences, self.rows_dev, self.width = devices, sequences, rows_dev, width
        self.group = devices // sequences
        self.span = self.group * rows_dev
        mean = self.span - IMG
        up, down = TXT_MAX - mean, mean - TXT_MIN
        drift = 0
        for k in range(sequences + 1):
            drift = max(drift, min(up * k, down * (sequences - k)), min(down * k, up * (sequences - k)))
        self.edge = -(-drift // 64) * 64
        self.rows = self.span + 2 * self.edge
        self.piece = 2 * self.edge // self.group
        self.own = rows_dev + self.piece
        self.image_end = -(-(self.edge + drift + IMG) // 128) * 128
        self.text_start = (self.edge - drift + IMG) // 128 * 128
        self.heads = HEADS // self.group
        self.segments = self.edge_segments()
        self.chip_heads = devices == 4 * self.group

    def device_of(self, seq, rank):
        return seq * self.group + rank

    def place_of(self, device):
        return lax.div(device, self.group), lax.rem(device, self.group)

    def seq_groups(self):
        return [[self.device_of(s, r) for r in range(self.group)] for s in range(self.sequences)]

    def rank_groups(self):
        return [[self.device_of(s, r) for s in range(self.sequences)] for r in range(self.group)]

    def edge_row(self, rank):
        half = self.group // 2
        return jnp.where(rank < half, self.piece * rank, self.edge + self.span + self.piece * (rank - half))

    def main_row(self, rank):
        return self.edge + self.rows_dev * rank

    def edge_segments(self):
        found = []
        for rank in range(self.group):
            half = self.group // 2
            first = self.piece * rank - self.edge if rank < half else self.span + self.piece * (rank - half)
            row = 0
            while row < self.piece:
                owner, owner_row = (first + row) // self.rows_dev, (first + row) % self.rows_dev
                count = min(self.piece - row, self.rows_dev - owner_row)
                found.append((rank, row, count, owner // self.group, owner % self.group, owner_row))
                row += count
        return found


def layer_norm(values):
    mean = jnp.mean(values, axis=-1, keepdims=True)
    centred = values - mean
    variance = jnp.mean(centred * centred, axis=-1, keepdims=True)
    inv_std = lax.rsqrt(variance + EPSILON)
    return (centred * inv_std, inv_std)


def norm_back(grad_normed, normed, inv_std):
    mean_grad = jnp.mean(grad_normed, axis=-1, keepdims=True)
    mean_cross = jnp.mean(grad_normed * normed, axis=-1, keepdims=True)
    return inv_std * (grad_normed - mean_grad - normed * mean_cross)


def softmax_parts(query, key, bias):
    scores = lax.dot_general(query, key, CONTRACT_LAST, preferred_element_type=F32) + bias
    top = jnp.max(scores, axis=1, keepdims=True)
    exponent = jnp.exp(scores - top)
    total = jnp.sum(exponent, axis=1, keepdims=True)
    return exponent * (1.0 / total)


def head_columns(heads, part, head):
    first = (part * heads + head) * HDIM
    return slice(first, first + HDIM)


def attend_kernel(heads, block, projected, bias_ref, out_ref):
    rows = pl.ds(pl.multiple_of(pl.program_id(0) * block, block), block)
    bias = bias_ref[...]
    outs = []
    for head in range(heads):
        query = projected[rows, head_columns(heads, 0, head)] * jnp.asarray(HDIM ** (-0.5), BF16)
        probs = softmax_parts(query, projected[:, head_columns(heads, 1, head)], bias).astype(BF16)
        outs.append(jnp.dot(probs, projected[:, head_columns(heads, 2, head)], preferred_element_type=F32))
    out_ref[...] = jnp.concatenate(outs, axis=1).astype(BF16)


def block_rows(rows, most):
    return most if rows % most == 0 else 128


def constant(shape):
    return pl.BlockSpec(shape, lambda i: (0,) * len(shape))


def attend(plan, projected, bias):
    rows, cols = projected.shape[0], projected.shape[1] // 3
    block = block_rows(rows, 128)
    return pl.pallas_call(
        functools.partial(attend_kernel, plan.heads, block),
        out_shape=jax.ShapeDtypeStruct((rows, cols), BF16),
        grid=(rows // block,),
        in_specs=[constant(projected.shape), constant(bias.shape)],
        out_specs=pl.BlockSpec((block, cols), lambda i: (i, 0)),
        compiler_params=pltpu.CompilerParams(vmem_limit_bytes=48 << 20),
        cost_estimate=pl.CostEstimate(flops=16 * rows * rows * cols, bytes_accessed=8 * rows * cols, transcendentals=0),
        name="attend",
    )(projected, bias)


def attend_back_kernel(
    heads, steps, block, projected, grad_merged, merge_pair, text, bias_ref, out, key_sum, value_sum
):
    step = pl.program_id(0)
    scale = jnp.asarray(HDIM ** (-0.5), BF16)

    @pl.when(step == 0)
    def _():
        key_sum[...] = jnp.zeros_like(key_sum)
        value_sum[...] = jnp.zeros_like(value_sum)

    rows = pl.ds(pl.multiple_of(step * block, block), block)
    bias = bias_ref[...]
    image, other_stream = [
        lax.dot_general(grad_merged[...], merge_pair[j], CONTRACT_LAST, preferred_element_type=F32) for j in range(2)
    ]
    grad_attended = jnp.where(text[...] > 0, other_stream, image).astype(BF16)
    grads = []
    for head in range(heads):
        query = projected[rows, head_columns(heads, 0, head)] * scale
        key = projected[:, head_columns(heads, 1, head)]
        grad_out = grad_attended[:, head * HDIM : (head + 1) * HDIM]
        probs = softmax_parts(query, key, bias)
        grad_probs = lax.dot_general(
            grad_out, projected[:, head_columns(heads, 2, head)], CONTRACT_LAST, preferred_element_type=F32
        )
        inner = jnp.sum(probs * grad_probs, axis=1, keepdims=True)
        grad_scores = (probs * (grad_probs - inner)).astype(BF16)
        grads.append(jnp.dot(grad_scores, key, preferred_element_type=F32) * HDIM ** (-0.5))
        key_sum[head] += lax.dot_general(query, grad_scores, CONTRACT_FIRST, preferred_element_type=F32)
        value_sum[head] += lax.dot_general(grad_out, probs.astype(BF16), CONTRACT_FIRST, preferred_element_type=F32)
    cols = heads * HDIM
    out[rows, :cols] = jnp.concatenate(grads, axis=1).astype(BF16)

    @pl.when(step == steps - 1)
    def _():
        total = out.shape[0]
        out[:, cols : 2 * cols] = key_sum[...].reshape(cols, total).T.astype(BF16)
        out[:, 2 * cols :] = value_sum[...].reshape(cols, total).T.astype(BF16)


def attend_back(plan, projected, grad_merged, merge_pair, text, bias):
    rows, cols = projected.shape[0], projected.shape[1] // 3
    block = block_rows(rows, 256)
    return pl.pallas_call(
        functools.partial(attend_back_kernel, plan.heads, rows // block, block),
        out_shape=jax.ShapeDtypeStruct(projected.shape, BF16),
        grid=(rows // block,),
        in_specs=[
            constant(projected.shape),
            pl.BlockSpec((block, plan.width), lambda i: (i, 0)),
            constant(merge_pair.shape),
            pl.BlockSpec((block, 1), lambda i: (i, 0)),
            constant(bias.shape),
        ],
        out_specs=constant(projected.shape),
        scratch_shapes=[pltpu.VMEM((plan.heads, HDIM, rows), F32)] * 2,
        compiler_params=pltpu.CompilerParams(vmem_limit_bytes=56 << 20),
        cost_estimate=pl.CostEstimate(flops=40 * rows * rows * cols, bytes_accessed=14 * rows * cols, transcendentals=0),
        name="attend_back",
    )(projected, grad_merged, merge_pair, text, bias)


def fold_rows(piece):
    half = piece.shape[0] // 2
    return jnp.concatenate([piece[:half], piece[half:]], axis=1)


def unfold_rows(piece):
    half = piece.shape[1] // 2
    return jnp.concatenate([piece[:, :half], piece[:, half:]], axis=0)


def terms_kernel(plan, fold, chunk, rows, grads, text, out, kept):
    width = rows.shape[1]
    for stream, (first, last) in enumerate(((0, plan.image_end), (plan.text_start, plan.rows))):
        count = last - first
        mask = text[pl.ds(first, count)]
        keep = (mask > 0) if stream else (mask <= 0)
        kept[pl.ds(0, count)] = jnp.where(keep, grads[pl.ds(first, count)], jnp.zeros((), BF16))

        def step(i, carry):
            start = pl.multiple_of(i * chunk, chunk)
            term = lax.dot_general(
                rows[pl.ds(first, count), pl.ds(start, chunk)],
                kept[pl.ds(0, count)],
                CONTRACT_FIRST,
                preferred_element_type=F32,
            ).astype(BF16)
            if fold:
                for j in range(chunk // fold):
                    out[(stream * width) // fold + i * (chunk // fold) + j] = fold_rows(term[j * fold : (j + 1) * fold])
            else:
                out[stream, pl.ds(start, chunk)] = term
            return carry

        if width == chunk:
            step(0, 0)
        else:
            lax.fori_loop(0, width // chunk, step, 0)


def weight_terms(plan, rows, grads, text, name, fold=0):
    width, cols = rows.shape[1], grads.shape[1]
    chunk = 384 if fold else 256 if width % 256 == 0 else width
    shape = (2 * width // fold, fold // 2, 2 * cols) if fold else (2, width, cols)
    return pl.pallas_call(
        functools.partial(terms_kernel, plan, fold, chunk),
        out_shape=jax.ShapeDtypeStruct(shape, BF16),
        in_specs=[pl.BlockSpec(memory_space=pltpu.VMEM)] * 3,
        out_specs=pl.BlockSpec(memory_space=pltpu.VMEM),
        scratch_shapes=[pltpu.VMEM((plan.image_end, cols), BF16)],
        compiler_params=pltpu.CompilerParams(vmem_limit_bytes=40 << 20),
        cost_estimate=pl.CostEstimate(flops=3 * plan.rows * width * cols, bytes_accessed=1 << 23, transcendentals=0),
        name=name,
    )(rows, grads, text)


def gelu(values):
    return jax.nn.gelu(values, approximate=True)


def in_blocks(plan, size, body):
    def step(i, carry):
        body(i, pl.ds(pl.multiple_of(i * size, size), size))
        return carry

    lax.fori_loop(0, plan.rows // size, step, 0)


def blockwise(plan, i, size, block, pair, dims, mask, out):
    @pl.when(i * size < plan.image_end)
    def _():
        out[...] = lax.dot_general(block, pair[0], dims, preferred_element_type=F32)

    @pl.when(i * size + size > plan.text_start)
    def _():
        out[...] = jnp.where(mask > 0, lax.dot_general(block, pair[1], dims, preferred_element_type=F32), out[...])


def project_kernel(plan, size, rows, pair, text, shift, scale, hidden, out, held):
    def body(i, place):
        mask = text[place]
        normed, _ = norm_rows(rows[place].astype(F32))
        block = (normed * (1.0 + pick_rows(scale[...], mask)) + pick_rows(shift[...], mask)).astype(BF16)
        hidden[place] = block
        blockwise(plan, i, size, block, pair, PLAIN, mask, held)
        out[place] = held[...].astype(BF16)

    in_blocks(plan, size, body)


def up_kernel(plan, size, rows, pair, text, upper, activated):
    def body(i, place):
        blockwise(plan, i, size, rows[place], pair, PLAIN, text[place], upper.at[place])
        activated[place] = gelu(upper[place]).astype(BF16)

    in_blocks(plan, size, body)


def down_back_kernel(plan, size, rows, pair, text, upper, out, held):
    def body(i, place):
        blockwise(plan, i, size, rows[place], pair, CONTRACT_LAST, text[place], held)
        out[place] = jax.vjp(gelu, upper[place])[1](held[...])[0].astype(BF16)

    in_blocks(plan, size, body)


def stream_rows(plan, kernel, size, cols, held, name, outs, *operands):
    spec = pl.BlockSpec(memory_space=pltpu.VMEM)
    shapes = tuple(jax.ShapeDtypeStruct((plan.rows, width), dtype) for width, dtype in outs)
    return pl.pallas_call(
        functools.partial(kernel, plan, size),
        out_shape=shapes,
        in_specs=[spec] * len(operands),
        out_specs=(spec,) * len(shapes),
        scratch_shapes=[pltpu.VMEM((size, cols), F32)] if held else [],
        compiler_params=pltpu.CompilerParams(vmem_limit_bytes=40 << 20),
        cost_estimate=pl.CostEstimate(
            flops=2 * plan.rows * plan.width * cols, bytes_accessed=1 << 24, transcendentals=0
        ),
        name=name,
    )(*operands)


VMEM = pl.BlockSpec(memory_space=pltpu.VMEM)


def own_rows(plan, window, rank):
    main = lax.dynamic_slice_in_dim(window, plan.main_row(rank), plan.rows_dev, 0)
    edge = lax.dynamic_slice_in_dim(window, plan.edge_row(rank), plan.piece, 0)
    return jnp.concatenate([main, edge], axis=0)


def remote(source, target, send_sem, recv_sem, device):
    return pltpu.make_async_remote_copy(
        src_ref=source,
        dst_ref=target,
        send_sem=send_sem,
        recv_sem=recv_sem,
        device_id=(device,),
        device_id_type=pl.DeviceIdType.MESH,
    )


def here(plan):
    return plan.place_of(lax.axis_index("dev"))


def other(rank, step, size):
    return lax.rem(rank + step, size)


def meet(devices):
    barrier = pltpu.get_barrier_semaphore()
    for device in devices:
        pl.semaphore_signal(barrier, inc=1, device_id=(device,), device_id_type=pl.DeviceIdType.MESH)
    pl.semaphore_wait(barrier, len(devices))


def group_devices(plan, seq, rank):
    return [plan.device_of(seq, other(rank, step, plan.group)) for step in range(1, plan.group)]


def column_devices(plan, seq, rank):
    return [plan.device_of(other(seq, step, plan.sequences), rank) for step in range(1, plan.sequences)]


def every_device(plan, device):
    return [other(device, step, plan.devices) for step in range(1, plan.devices)]


def call(kernel, name, ident, out_shape, scratch, operands, in_specs=None, out_specs=None, vmem=40 << 20):
    outs = out_shape if isinstance(out_shape, tuple) else (out_shape,)
    return pl.pallas_call(
        kernel,
        out_shape=out_shape,
        in_specs=in_specs or [VMEM] * len(operands),
        out_specs=out_specs or (tuple([VMEM] * len(outs)) if isinstance(out_shape, tuple) else VMEM),
        scratch_shapes=scratch,
        compiler_params=pltpu.CompilerParams(
            collective_id=ident, has_side_effects=True, vmem_limit_bytes=vmem
        ),
        name=name,
    )(*operands)


def aligned(start):
    return pl.multiple_of(start, 16)


def block_parts(plan, ref, rank):
    return (
        ref.at[pl.ds(aligned(plan.main_row(rank)), plan.rows_dev)],
        ref.at[pl.ds(aligned(plan.edge_row(rank)), plan.piece)],
    )


def own_parts(plan, ref):
    return ref.at[pl.ds(0, plan.rows_dev)], ref.at[pl.ds(plan.rows_dev, plan.piece)]


def load_block(plan, ref, rank):
    main, edge = block_parts(plan, ref, rank)
    return jnp.concatenate([main[...], edge[...]], axis=0)


def sum_scratch(plan, wire=BF16):
    half, own, width = plan.group // 2, plan.own, plan.width
    return [
        pltpu.VMEM((half + 1, own, width), F32),
        pltpu.VMEM((half, own, width), F32),
        pltpu.VMEM((half - 1, own, width), wire),
        pltpu.VMEM((half - 1, own, width), wire),
        pltpu.SemaphoreType.DMA((half,)),
        pltpu.SemaphoreType.DMA((half,)),
        pltpu.SemaphoreType.DMA((half,)),
        pltpu.SemaphoreType.DMA((half,)),
    ]


SUM_SCRATCH = 8


def product(plan, rows, pair, text, dims, rank, out):
    block = load_block(plan, rows, rank)
    text_row = load_block(plan, text, rank) > 0
    chunk = 256

    def step(i, carry):
        cols = pl.ds(pl.multiple_of(i * chunk, chunk), chunk)
        parts = []
        for stream in range(2):
            weight = pair[stream, cols, :] if dims is CONTRACT_LAST else pair[stream, :, cols]
            parts.append(lax.dot_general(block, weight, dims, preferred_element_type=F32))
        out[:, cols] = jnp.where(text_row, parts[1], parts[0])
        return carry

    lax.fori_loop(0, plan.width // chunk, step, 0)


def scatter_start(plan, seq, rank, rows, pair, text, dims, away, near, going, coming,
                  pair_send, pair_recv, far_send, far_recv):
    half = plan.group // 2
    chip, core = lax.div(rank, 2), lax.rem(rank, 2)
    partner = plan.device_of(seq, 2 * chip + 1 - core)
    order = list(range(1, half)) + [0]

    def pair_copy(step):
        return remote(away.at[step], near.at[step], pair_send.at[step], pair_recv.at[step], partner)

    def far_copy(step):
        to = plan.device_of(seq, 2 * other(chip, step, half) + core)
        return remote(going.at[step - 1], coming.at[step - 1], far_send.at[step], far_recv.at[step], to)

    def turn(i, carry):
        for_partner = (i < 2) | (lax.rem(i, 2) == 1) & (i < 2 * half - 1)
        place = jnp.where(i < 2, i, jnp.where(for_partner, lax.div(i + 1, 2), lax.div(i, 2) - 1))
        place = jnp.where(i == 2 * half - 1, half - 1, place)
        step = other(place, 1, half)
        block = 2 * other(chip, step, half) + jnp.where(for_partner, 1 - core, core)
        product(plan, rows, pair, text, dims, block, away.at[jnp.where(for_partner, step, half)])

        @pl.when(for_partner)
        def _():
            pair_copy(step).start()

        @pl.when(jnp.logical_not(for_partner))
        def _():
            pair_copy(step).wait_recv()
            away[half] = away[half] + near[step]

        @pl.when(jnp.logical_not(for_partner) & (place < half - 1))
        def _():
            going[step - 1] = away[half].astype(going.dtype)
            far_copy(step).start()

        return carry

    lax.fori_loop(0, 2 * half, turn, 0)

    def result(use):
        for step in range(1, half):
            far_copy(step).wait_recv()
        size = 32 if plan.own % 32 == 0 else 16

        def some(i, carry):
            place = pl.ds(pl.multiple_of(i * size, size), size)
            total = away[half, place]
            for step in range(1, half):
                total = total + coming[step - 1, place].astype(F32)
            use(place, total)
            return carry

        lax.fori_loop(0, plan.own // size, some, 0)
        for step in range(half):
            pair_copy(step).wait_send()
        for step in range(1, half):
            far_copy(step).wait_send()

    return result


def share_scratch(plan):
    return [pltpu.SemaphoreType.DMA((plan.group, 2))] * 2 + [pltpu.SemaphoreType.DMA((plan.group, 2))]


def share_rows(plan, seq, rank, parts, window, send, recv, pass_send):
    half = plan.group // 2
    chip, core = lax.div(rank, 2), lax.rem(rank, 2)
    partner_rank = 2 * chip + 1 - core
    partner = plan.device_of(seq, partner_rank)

    def send_own(to_device, slot):
        copies = [
            remote(source, target, send.at[slot, i], recv.at[slot, i], to_device)
            for i, (source, target) in enumerate(zip(parts, block_parts(plan, window, rank)))
        ]
        for copy in copies:
            copy.start()
        return copies

    flying = {}
    for step in range(1, half):
        flying[step] = send_own(plan.device_of(seq, 2 * other(chip, step, half) + core), step)
    flying[0] = send_own(partner, 0)
    for source, target in zip(parts, block_parts(plan, window, rank)):
        target[...] = source[...]
    passed = []
    for step in range(1, half):
        for copy in flying[step]:
            copy.wait_recv()
        came = 2 * other(chip, half - step, half) + core
        copies = [
            remote(place, place, pass_send.at[step, i], recv.at[half + step, i], partner)
            for i, place in enumerate(block_parts(plan, window, came))
        ]
        for copy in copies:
            copy.start()
        passed.extend(copies)
    for copy in flying[0]:
        copy.wait_recv()
    for copy in passed:
        copy.wait_recv()
    for copies in flying.values():
        for copy in copies:
            copy.wait_send()
    for copy in passed:
        copy.wait_send()


def entry_kernel(plan, tokens, grads, mod_part, *refs):
    if plan.chip_heads:
        merge, merge_out, *refs = refs[:1] + refs[4:5] + refs[1:4] + refs[5:]
        merge_send, merge_recv, *refs = refs[-2:] + refs[:-2]
    (token_window, grad_window, mods, token_own, grad_own, plane, across, chunk, edge_send, edge_recv,
     t_send, t_recv, t_pass, g_send, g_recv, g_pass, m_send, m_recv) = refs
    device = lax.axis_index("dev")
    seq, rank = plan.place_of(device)
    meet(every_device(plan, device))
    swaps = []
    if plan.chip_heads:
        core = lax.rem(rank, 2)
        partner = plan.device_of(seq, 2 * lax.div(rank, 2) + 1 - core)
        for stream in range(2):
            copy = remote(
                merge.at[2 * stream + 1 - core],
                merge_out.at[stream, core],
                merge_send.at[stream],
                merge_recv.at[stream],
                partner,
            )
            copy.start()
            swaps.append(copy)
            merge_out[stream, core] = merge[2 * stream + core]
    hops = []
    for step in range(1, plan.group):
        to = other(rank, step, plan.group)
        copy = remote(mod_part.at[to], plane.at[step], m_send.at[0, step], m_recv.at[0, step], plan.device_of(seq, to))
        copy.start()
        hops.append(copy)
    arrays = ((tokens, token_own), (grads, grad_own))
    count = len(plan.segments)
    for which, (source, own) in enumerate(arrays):
        for index, (to_rank, row, rows, step, owner, owner_row) in enumerate(plan.segments):
            @pl.when(rank == owner)
            def _():
                remote(
                    source.at[pl.ds(owner_row, rows)],
                    own.at[pl.ds(row, rows)],
                    edge_send.at[which * count + index],
                    edge_recv.at[which * count + index],
                    plan.device_of(lax.rem(seq + plan.sequences - step, plan.sequences), to_rank),
                ).start()
    for copy in hops:
        copy.wait_recv()
    total = mod_part[rank]
    for step in range(1, plan.group):
        total = total + plane[step]
    plane[0] = total
    hops_across = []
    for step in range(1, plan.sequences):
        to = other(seq, step, plan.sequences)
        copy = remote(plane.at[0, to], across.at[seq], m_send.at[1, step], m_recv.at[1, step], plan.device_of(to, rank))
        copy.start()
        hops_across.append(copy)
    across[seq] = plane[0, seq]
    for which, (source, own) in enumerate(arrays):
        for index, (to_rank, row, rows, step, owner, owner_row) in enumerate(plan.segments):
            @pl.when(rank == to_rank)
            def _():
                remote(
                    source.at[pl.ds(owner_row, rows)],
                    own.at[pl.ds(row, rows)],
                    edge_send.at[which * count + index],
                    edge_recv.at[which * count + index],
                    plan.device_of(lax.rem(seq + plan.sequences + step, plan.sequences), owner),
                ).wait_recv()
    share_rows(plan, seq, rank, (tokens, token_own), token_window, t_send, t_recv, t_pass)
    for copy in hops_across:
        copy.wait_recv()
    half = plan.sequences // 2
    for stream in range(2):
        total = across[stream * half]
        for i in range(1, half):
            total = total + across[stream * half + i]
        chunk[stream] = total
    hops_back = []
    for step in range(1, plan.group):
        to = other(rank, step, plan.group)
        copy = remote(chunk, mods.at[rank], m_send.at[2, step], m_recv.at[2, step], plan.device_of(seq, to))
        copy.start()
        hops_back.append(copy)
    mods[rank] = chunk[...]
    share_rows(plan, seq, rank, (grads, grad_own), grad_window, g_send, g_recv, g_pass)
    for copy in hops_back:
        copy.wait_recv()
    for copy in hops + hops_across + hops_back:
        copy.wait_send()
    for copy in swaps:
        copy.wait()
    for which, (source, own) in enumerate(arrays):
        for index, (to_rank, row, rows, step, owner, owner_row) in enumerate(plan.segments):
            @pl.when(rank == owner)
            def _():
                remote(
                    source.at[pl.ds(owner_row, rows)],
                    own.at[pl.ds(row, rows)],
                    edge_send.at[which * count + index],
                    edge_recv.at[which * count + index],
                    plan.device_of(lax.rem(seq + plan.sequences - step, plan.sequences), to_rank),
                ).wait_send()


def entry(plan, tokens, grads, mod_part, merge):
    lanes = mod_part.shape[1] // plan.group // 128
    pieces = mod_part.reshape(plan.sequences, plan.group, lanes, 128).transpose(1, 0, 2, 3)
    window = jax.ShapeDtypeStruct((plan.rows, plan.width), BF16)
    dma = pltpu.SemaphoreType.DMA
    most = max(plan.group, plan.sequences)
    shapes = (window, window, jax.ShapeDtypeStruct((plan.group, 2, lanes, 128), F32))
    operands = (tokens, grads, pieces)
    scratch = (
        [
            pltpu.VMEM((plan.piece, plan.width), BF16),
            pltpu.VMEM((plan.piece, plan.width), BF16),
            pltpu.VMEM((plan.group, plan.sequences, lanes, 128), F32),
            pltpu.VMEM((plan.sequences, lanes, 128), F32),
            pltpu.VMEM((2, lanes, 128), F32),
            dma((2 * len(plan.segments),)),
            dma((2 * len(plan.segments),)),
        ]
        + share_scratch(plan)
        + share_scratch(plan)
        + [dma((3, most)), dma((3, most))]
    )
    if plan.chip_heads:
        shapes += (jax.ShapeDtypeStruct((2, 2) + merge.shape[1:], BF16),)
        operands += (merge,)
        scratch += [dma((2,)), dma((2,))]
    token_window, grad_window, mods, *rest = call(
        functools.partial(entry_kernel, plan), "entry", 1, shapes, scratch, operands
    )
    merge_pair = rest[0].reshape(2, -1, plan.width) if plan.chip_heads else merge
    return token_window, grad_window, mods.transpose(1, 0, 2, 3).reshape(2, -1), merge_pair


def project_columns(plan, rank):
    share = plan.width // plan.group
    first = (rank % 2) * (plan.width // 2) + (rank // 2) * share
    return [part * plan.width + first for part in range(3)], share


def up_columns(plan, rank, cols):
    planes = plan.sequences // 2
    share = cols // planes // plan.group
    return [plane * plan.group * share + rank * share for plane in range(planes)], share


def start_swap(plan, seq, rank, source, target, send, recv):
    copies = []
    for step in range(1, plan.group):
        to = other(rank, step, plan.group)
        copy = remote(source.at[to], target.at[rank], send.at[step], recv.at[step], plan.device_of(seq, to))
        copy.start()
        copies.append(copy)
    target[rank] = source[rank]
    return copies


def swap_in_kernel(plan, project, up, project_out, up_out, project_cut, up_cut, p_send, p_recv, u_send, u_recv):
    seq, rank = here(plan)
    for to in range(plan.group):
        starts, share = project_columns(plan, to)
        project_cut[to] = fold_rows(jnp.concatenate([project[:, c : c + share] for c in starts], axis=1))
    meet(group_devices(plan, seq, rank))
    copies = start_swap(plan, seq, rank, project_cut, project_out, p_send, p_recv)
    for to in range(plan.group):
        starts, share = up_columns(plan, to, up.shape[1])
        up_cut[to] = jnp.concatenate([up[:, c : c + share] for c in starts], axis=1)
    copies += start_swap(plan, seq, rank, up_cut, up_out, u_send, u_recv)
    for copy in copies:
        copy.wait()


def swap_in(plan, project, up):
    rows = project.shape[0]
    dma = pltpu.SemaphoreType.DMA
    shapes = [
        (plan.group, rows // 2, 2 * project.shape[1] // plan.group),
        (plan.group, rows, up.shape[1] // plan.group),
    ]
    return call(
        functools.partial(swap_in_kernel, plan),
        "swap_in",
        4,
        tuple(jax.ShapeDtypeStruct(shape, BF16) for shape in shapes),
        [pltpu.VMEM(shape, BF16) for shape in shapes] + [dma((plan.group,))] * 4,
        (project, up),
    )


def place_columns(plan, got, out, columns, unfold):
    for source in range(plan.group):
        starts, share = columns(plan, source)
        piece = unfold_rows(got[source]) if unfold else got[source]
        for i, c in enumerate(starts):
            out[:, c : c + share] = piece[:, i * share : (i + 1) * share].astype(out.dtype)


def line_sum(plan, seq, rank, term, out, up_in, up_out, down_in, down_out, up_send, up_recv, down_send, down_recv):
    count = plan.sequences

    def hop(source, target, send, recv, owner, to):
        return remote(source.at[owner], target.at[owner], send.at[owner], recv.at[owner], plan.device_of(to, rank))

    above, below = lax.rem(seq + 1, count), lax.rem(seq + count - 1, count)
    ways = [
        (list(range(count - 1, 0, -1)), above, below, up_in, up_out, up_send, up_recv, lambda owner: seq < owner, seq == 0),
        (list(range(count - 1)), below, above, down_in, down_out, down_send, down_recv, lambda owner: seq > owner,
         seq == count - 1),
    ]
    def pass_on(turn, way):
        owners, to, back, came, goes, send, recv, mine, first = way
        owner = owners[turn]

        @pl.when(mine(owner) & first)
        def _():
            hop(term, came, send, recv, owner, to).start()

        @pl.when(mine(owner) & jnp.logical_not(first))
        def _():
            hop(goes, came, send, recv, owner, back).wait_recv()
            goes[owner] = (term[owner].astype(F32) + came[owner].astype(F32)).astype(BF16)
            hop(goes, came, send, recv, owner, to).start()

    for turn in range(count - 1):
        @pl.when(seq < count // 2)
        def _():
            pass_on(turn, ways[0])
            pass_on(turn, ways[1])

        @pl.when(seq >= count // 2)
        def _():
            pass_on(turn, ways[1])
            pass_on(turn, ways[0])

    out[...] = term[seq].astype(F32)
    for owners, to, back, came, goes, send, recv, mine, first in ways:
        for owner in owners:
            @pl.when(seq == owner)
            def _():
                hop(goes, came, send, recv, owner, back).wait_recv()
                out[...] += came[owner].astype(F32)

            @pl.when(mine(owner))
            def _():
                hop(goes, came, send, recv, owner, to).wait_send()


def finish_kernel(plan, up, project, *refs):
    if plan.chip_heads:
        term, up_got, project_got, merge_out, *refs = refs
        *refs, line = refs[:4] + [refs[4:]]
    else:
        up_got, project_got, *refs = refs
    u_send, u_recv, p_send, p_recv = refs
    seq, rank = here(plan)
    meet(group_devices(plan, seq, rank) + column_devices(plan, seq, rank))
    ups = start_swap(plan, seq, rank, up, up_got, u_send, u_recv)
    projects = start_swap(plan, seq, rank, project, project_got, p_send, p_recv)
    if plan.chip_heads:
        line_sum(plan, seq, rank, term, merge_out, *line)
    for copy in ups + projects:
        copy.wait()


def place_kernel(plan, up_got, project_got, up_out, project_out):
    place_columns(plan, up_got, up_out, lambda p, r: up_columns(p, r, up_out.shape[1]), False)
    place_columns(plan, project_got, project_out, project_columns, True)


def finish(plan, up, project, term):
    dma = pltpu.SemaphoreType.DMA
    rows = up.shape[1]
    shapes = tuple(jax.ShapeDtypeStruct(pieces.shape, BF16) for pieces in (up, project))
    operands = (up, project)
    scratch = [dma((plan.group,))] * 4
    if plan.chip_heads:
        shapes += (jax.ShapeDtypeStruct(term.shape[1:], F32),)
        operands += (term,)
        scratch += [pltpu.VMEM(term.shape, BF16)] * 4 + [dma((plan.sequences,))] * 4
    up_got, project_got, *merge_grad = call(
        functools.partial(finish_kernel, plan), "finish", 6, shapes, scratch, operands
    )
    up_grad, project_grad = pl.pallas_call(
        functools.partial(place_kernel, plan),
        out_shape=(
            jax.ShapeDtypeStruct((rows, plan.group * up.shape[2]), F32),
            jax.ShapeDtypeStruct((rows, plan.group * project.shape[2] // 2), F32),
        ),
        in_specs=[VMEM, VMEM],
        out_specs=(VMEM, VMEM),
        compiler_params=pltpu.CompilerParams(vmem_limit_bytes=24 << 20),
        name="place",
    )(up_got, project_got)
    return up_grad, project_grad, merge_grad


def pick_rows(table, text):
    return jnp.where(text > 0, table[1:2, :], table[0:1, :])


def norm_rows(values):
    mean = jnp.mean(values, axis=1, keepdims=True)
    centred = values - mean
    inv = lax.rsqrt(jnp.mean(centred * centred, axis=1, keepdims=True) + EPSILON)
    return centred * inv, inv


def middle_kernel(plan, rows, pair, window_text, tokens, gate_a, scale_b, shift_b, text, merged, window, own, *scratch):
    seq, rank = here(plan)
    meet(group_devices(plan, seq, rank))
    result = scatter_start(plan, seq, rank, rows, pair, window_text, PLAIN, *scratch[:SUM_SCRATCH])

    def use(place, total):
        merged[place] = total
        mask = text[place]
        middle = tokens[place].astype(F32) + pick_rows(gate_a[...], mask) * total
        normed, _ = norm_rows(middle)
        own[place] = (normed * (1.0 + pick_rows(scale_b[...], mask)) + pick_rows(shift_b[...], mask)).astype(BF16)

    result(use)
    share_rows(plan, seq, rank, own_parts(plan, own), window, *scratch[SUM_SCRATCH:])


def own_shape(plan, dtype=F32):
    return jax.ShapeDtypeStruct((plan.own, plan.width), dtype)


def window_shape(plan):
    return jax.ShapeDtypeStruct((plan.rows, plan.width), BF16)


def middle_rows(plan, rows, pair, window_text, tokens, gate_a, scale_b, shift_b, text):
    return call(
        functools.partial(middle_kernel, plan),
        "middle",
        2,
        (own_shape(plan), window_shape(plan)),
        [pltpu.VMEM((plan.own, plan.width), BF16)] + sum_scratch(plan, F32) + share_scratch(plan),
        (rows, pair, window_text, tokens, gate_a, scale_b, shift_b, text),
    )


def back_kernel(plan, rows, pair, window_text, grad, middle, gate_a, scale_b, text, grad_hidden, grad_middle, window, own, *scratch):
    seq, rank = here(plan)
    meet(group_devices(plan, seq, rank))
    result = scatter_start(plan, seq, rank, rows, pair, window_text, CONTRACT_LAST, *scratch[:SUM_SCRATCH])

    def use(place, total):
        grad_hidden[place] = total
        mask = text[place]
        normed, inv = norm_rows(middle[place])
        inner = total * (1.0 + pick_rows(scale_b[...], mask))
        mean_grad = jnp.mean(inner, axis=1, keepdims=True)
        mean_cross = jnp.mean(inner * normed, axis=1, keepdims=True)
        back = grad[place].astype(F32) + inv * (inner - mean_grad - normed * mean_cross)
        grad_middle[place] = back
        own[place] = (pick_rows(gate_a[...], mask) * back).astype(BF16)

    result(use)
    share_rows(plan, seq, rank, own_parts(plan, own), window, *scratch[SUM_SCRATCH:])


def back_rows(plan, rows, pair, window_text, grad, middle, gate_a, scale_b, text):
    return call(
        functools.partial(back_kernel, plan),
        "back",
        3,
        (own_shape(plan), own_shape(plan), window_shape(plan)),
        [pltpu.VMEM((plan.own, plan.width), BF16)] + sum_scratch(plan) + share_scratch(plan),
        (rows, pair, window_text, grad, middle, gate_a, scale_b, text),
    )


def edge_copy(plan, seq, source, first_row, target, send, recv, index):
    from_rank, row, rows, step, owner, owner_row = plan.segments[index]
    return remote(
        source.at[pl.ds(first_row + row, rows)],
        target.at[pl.ds(owner_row, rows)],
        send.at[index],
        recv.at[index],
        plan.device_of(lax.rem(seq + plan.sequences + step, plan.sequences), owner),
    )


def start_edges(plan, seq, rank, *refs):
    for index, segment in enumerate(plan.segments):
        @pl.when(rank == segment[0])
        def _():
            edge_copy(plan, seq, *refs, index).start()


def finish_edges(plan, seq, rank, *refs):
    for index, segment in enumerate(plan.segments):
        @pl.when(rank == segment[4])
        def _():
            edge_copy(plan, seq, *refs, index).wait_recv()

        @pl.when(rank == segment[0])
        def _():
            edge_copy(plan, seq, *refs, index).wait_send()


def edge_scratch(plan):
    return [pltpu.SemaphoreType.DMA((len(plan.segments),))] * 2


def stream_sums(values, masks):
    return jnp.concatenate([jnp.sum(values * mask, axis=0, keepdims=True) for mask in masks], axis=0)


def last_kernel(plan, names, *refs):
    at = types.SimpleNamespace(**dict(zip(names, refs)))
    low_scratch = refs[len(names) : len(names) + SUM_SCRATCH]
    back_scratch = refs[len(names) + SUM_SCRATCH : len(names) + 2 * SUM_SCRATCH]
    device = lax.axis_index("dev")
    seq, rank = plan.place_of(device)
    stream = lax.div(2 * seq, plan.sequences)
    at.layer_extra[...] = jnp.zeros_like(at.layer_extra)
    at.token_extra[...] = jnp.zeros_like(at.token_extra)
    meet(every_device(plan, device))
    low_sum = scatter_start(plan, seq, rank, at.activated, at.down_pair, at.window_text, PLAIN, *low_scratch)
    back_sum = scatter_start(plan, seq, rank, at.grads, at.project_pair, at.window_text, CONTRACT_LAST, *back_scratch)
    swaps = []
    if plan.chip_heads:
        core = lax.rem(rank, 2)
        partner = plan.device_of(seq, 2 * lax.div(rank, 2) + 1 - core)
        for j in range(2):
            copy = remote(
                at.term.at[j, 1 - core], at.term_out.at[2 * j + core], at.term_send.at[j], at.term_recv.at[j], partner
            )
            copy.start()
            swaps.append(copy)
            at.term_out[2 * j + core] = at.term[j, core]
    width = plan.width
    at.local[...] = jnp.zeros_like(at.local)
    at.local[:, 2 * width : 5 * width] = at.rest[...]

    def add(first, place, values):
        masks = (at.masks[place, 0:1], at.masks[place, 1:2])
        at.local[:, first * width : (first + 1) * width] += stream_sums(values, masks)

    def use_low(place, lowered):
        at.layer_own[place] = (at.middle[place] + pick_rows(at.gate_b[...], at.text[place]) * lowered).astype(BF16)
        add(5, place, at.grad[place].astype(F32) * lowered)

    low_sum(use_low)
    layer_edges = (at.layer_own, plan.rows_dev, at.layer_extra, at.l_send, at.l_recv)
    start_edges(plan, seq, rank, *layer_edges)
    at.layer[...] = at.layer_own[pl.ds(0, plan.rows_dev)]

    def use_back(place, total):
        normed, inv = norm_rows(at.tokens[place].astype(F32))
        add(0, place, total)
        add(1, place, total * normed)
        inner = total * (1.0 + pick_rows(at.scale_a[...], at.text[place]))
        mean_grad = jnp.mean(inner, axis=1, keepdims=True)
        mean_cross = jnp.mean(inner * normed, axis=1, keepdims=True)
        at.token_own[place] = at.grad_middle[place] + inv * (inner - mean_grad - normed * mean_cross)

    back_sum(use_back)
    cols = 6 * width // plan.group

    def chunk(index):
        return pl.ds(pl.multiple_of(index * cols, 128), cols)

    hops = []
    for step in range(1, plan.group):
        to = other(rank, step, plan.group)
        copy = remote(
            at.local.at[:, chunk(to)], at.first.at[step], at.t_send.at[0, step], at.t_recv.at[0, step], plan.device_of(seq, to)
        )
        copy.start()
        hops.append(copy)
    token_edges = (at.token_own, plan.rows_dev, at.token_extra, at.e_send, at.e_recv)
    start_edges(plan, seq, rank, *token_edges)
    for copy in hops:
        copy.wait_recv()
    sums = at.local[:, chunk(rank)]
    for step in range(1, plan.group):
        sums = sums + at.first[step]
    for i in range(2):
        at.mine[i] = sums[i : i + 1]
    across = []
    for step in range(1, plan.sequences):
        to = other(seq, step, plan.sequences)
        to_stream = lax.div(2 * to, plan.sequences)
        copy = remote(
            at.mine.at[to_stream], at.second.at[seq], at.t_send.at[1, step], at.t_recv.at[1, step], plan.device_of(to, rank)
        )
        copy.start()
        across.append(copy)
    at.second[seq] = at.mine[stream]
    at.token[...] = at.token_own[pl.ds(0, plan.rows_dev)]
    for copy in across:
        copy.wait_recv()
    last = []
    for step in range(1, plan.group):
        to = other(rank, step, plan.group)
        copy = remote(at.second, at.table.at[rank], at.t_send.at[2, step], at.t_recv.at[2, step], plan.device_of(seq, to))
        copy.start()
        last.append(copy)
    at.table[rank] = at.second[...]
    for copy in last:
        copy.wait_recv()

    piece = None
    for index in range(plan.group):
        grads = jnp.concatenate([at.table[index, s] for s in range(plan.sequences)], axis=0).astype(BF16)
        part = lax.dot_general(
            grads, at.weight[:, index * cols : (index + 1) * cols], CONTRACT_LAST, preferred_element_type=F32
        )
        piece = part if piece is None else piece + part
    at.piece[...] = piece
    at.everyone[seq, rank] = piece
    spread = []
    for step in range(1, plan.group):
        to = other(rank, step, plan.group)
        copy = remote(
            at.piece, at.everyone.at[seq, rank], at.c_send.at[0, step], at.c_recv.at[0, step], plan.device_of(seq, to)
        )
        copy.start()
        spread.append(copy)
    for copy in spread:
        copy.wait_recv()
    for step in range(1, plan.sequences):
        to = other(seq, step, plan.sequences)
        copy = remote(
            at.everyone.at[seq], at.everyone.at[seq], at.c_send.at[1, step], at.c_recv.at[1, step], plan.device_of(to, rank)
        )
        copy.start()
        spread.append(copy)
    for copy in spread[plan.group - 1 :]:
        copy.wait_recv()
    for copy in hops + across + last + spread:
        copy.wait_send()
    for copy in swaps:
        copy.wait()
    finish_edges(plan, seq, rank, *layer_edges)
    finish_edges(plan, seq, rank, *token_edges)


def last_rows(plan, term, weight, **operands):
    rows, share = weight.shape[0], plan.width // plan.group // 2
    cols = 6 * plan.width // plan.group
    most = max(plan.group, plan.sequences)
    dma = pltpu.SemaphoreType.DMA

    def placed(dtype):
        return jax.ShapeDtypeStruct((plan.rows_dev, plan.width), dtype)

    operands = dict(operands, weight=weight)
    outs = dict(
        layer=placed(BF16),
        layer_extra=placed(BF16),
        token=placed(F32),
        token_extra=placed(F32),
        table=jax.ShapeDtypeStruct((plan.group, plan.sequences, 1, cols), F32),
        everyone=jax.ShapeDtypeStruct((plan.sequences, plan.group, plan.sequences, rows), F32),
    )
    edges = len(plan.segments)
    scratch = dict(
        layer_own=pltpu.VMEM((plan.own, plan.width), BF16),
        token_own=pltpu.VMEM((plan.own, plan.width), F32),
        local=pltpu.VMEM((2, 6 * plan.width), F32),
        first=pltpu.VMEM((plan.group, 2, cols), F32),
        second=pltpu.VMEM((plan.sequences, 1, cols), F32),
        mine=pltpu.VMEM((2, 1, cols), F32),
        piece=pltpu.VMEM((plan.sequences, rows), F32),
        t_send=dma((3, most)),
        t_recv=dma((3, most)),
        c_send=dma((2, most)),
        c_recv=dma((2, most)),
        l_send=dma((edges,)),
        l_recv=dma((edges,)),
        e_send=dma((edges,)),
        e_recv=dma((edges,)),
    )
    if plan.chip_heads:
        operands["term"] = term.reshape(2, 2, share, plan.width)
        outs["term_out"] = jax.ShapeDtypeStruct((plan.sequences, share, plan.width), BF16)
        scratch.update(term_send=dma((2,)), term_recv=dma((2,)))
    names = tuple(operands) + tuple(outs) + tuple(scratch)
    got = call(
        functools.partial(last_kernel, plan, names),
        "last",
        10,
        tuple(outs.values()),
        list(scratch.values()) + sum_scratch(plan) + sum_scratch(plan),
        tuple(operands.values()),
        vmem=58 << 20,
    )
    got = types.SimpleNamespace(**dict(zip(outs, got)))
    got.table = got.table[:, :, 0].transpose(1, 0, 2).reshape(plan.sequences, -1)
    got.term = got.term_out if plan.chip_heads else term
    return got


def over_sequences(plan, pieces):
    full = lax.all_gather(pieces, "dev", axis=0, axis_index_groups=plan.rank_groups())
    return full.reshape((plan.devices,) + pieces.shape[1:])


def over_sequences_sum(plan, pieces):
    return lax.psum_scatter(pieces, "dev", scatter_dimension=0, axis_index_groups=plan.rank_groups())


def merge_rows(plan, weight, rank):
    if plan.chip_heads:
        return lax.all_gather(weight, "dev", axis=0, axis_index_groups=plan.rank_groups())
    share = plan.width // plan.group
    full = lax.all_gather(weight, "dev", axis=0, tiled=True)
    full = full.reshape(2, 2, plan.group // 2, share, weight.shape[1])
    full = lax.dynamic_index_in_dim(full, lax.rem(rank, 2), 1, keepdims=False)
    return lax.dynamic_index_in_dim(full, lax.div(rank, 2), 1, keepdims=False)


def merge_sum(plan, term, rank):
    half = plan.group // 2
    _, share, cols = term.shape
    mine = [jnp.where(lax.rem(rank, 2) == k, term, jnp.zeros((), BF16)) for k in range(2)]
    full = jnp.zeros((2, 2, half, share, cols), BF16)
    full = lax.dynamic_update_slice_in_dim(full, jnp.stack(mine, axis=1)[:, :, None], lax.div(rank, 2), 2)
    return lax.psum_scatter(full.reshape(-1, cols), "dev", scatter_dimension=0, tiled=True)


def down_slices(plan, weight):
    full = lax.all_gather(weight, "dev", axis=0, axis_index_groups=plan.rank_groups())
    return full.reshape(2, -1, weight.shape[1])


def pick(table, text_rows):
    return jnp.where(text_rows[:, None], table[1][None, :], table[0][None, :])


def on_device(
    tokens,
    conditioning,
    text_lengths,
    modulation_weight,
    project_weight,
    merge_weight,
    up_weight,
    down_weight,
    cotangent,
):
    rows_dev, width = tokens.shape
    mod_rows = modulation_weight.shape[0]
    plan = Plan(lax.axis_size("dev"), conditioning.shape[0], rows_dev, width)
    device = lax.axis_index("dev")
    seq, rank = plan.place_of(device)
    feature_start = device * mod_rows % width

    ends = jnp.cumsum(IMG + text_lengths)
    starts = jnp.concatenate([jnp.zeros((1,), jnp.int32), ends[:-1]])
    positions = device * rows_dev + jnp.arange(rows_dev, dtype=jnp.int32)
    row_seq = jnp.sum((starts[None, :] <= positions[:, None]).astype(jnp.int32), axis=1) - 1
    offset = plan.span * seq - plan.edge + jnp.arange(plan.rows, dtype=jnp.int32) - starts[seq]
    valid = (offset >= 0) & (offset < IMG + text_lengths[seq])
    is_text = offset >= IMG
    bias = jnp.where(valid, 0.0, MASKED).astype(F32)[None, :]
    window_text = is_text.astype(F32)[:, None]
    own_valid = own_rows(plan, valid[:, None], rank)[:, 0]
    own_text = own_rows(plan, is_text[:, None], rank)[:, 0]

    cond_float = conditioning.astype(F32)
    silu_low = jax.nn.silu(cond_float).astype(BF16)
    silu_part = lax.dynamic_slice_in_dim(silu_low, feature_start, mod_rows, 1)
    mod_part = jnp.dot(silu_part, modulation_weight, preferred_element_type=F32)

    merge_pair = merge_rows(plan, merge_weight, rank)
    project_pieces, up_pieces = swap_in(plan, project_weight, up_weight)
    project_pieces, up_pieces, merge_pair = lax.optimization_barrier((project_pieces, up_pieces, merge_pair))
    project_pair = over_sequences(plan, project_pieces)
    share = project_pair.shape[2] // 2
    project_pair = jnp.concatenate([project_pair[:, :, :share], project_pair[:, :, share:]], axis=1)
    project_pair = lax.optimization_barrier(project_pair.reshape(2, width, share))
    up_pair = over_sequences(plan, up_pieces).reshape(2, width, -1)
    down_pair = down_slices(plan, down_weight)

    token_window, grad_window, mods, merge_pair = entry(plan, tokens, cotangent, mod_part, merge_pair)
    shift_a, scale_a, gate_a, shift_b, scale_b, gate_b = jnp.split(mods, 6, axis=1)
    grad_window = jnp.where(valid[:, None], grad_window, jnp.zeros((), BF16))

    cols = project_pair.shape[2]
    hidden_a, projected = stream_rows(
        plan, project_kernel, 128, cols, True, "project", ((width, BF16), (cols, BF16)),
        token_window, project_pair, window_text, shift_a, scale_a,
    )
    attended = attend(plan, projected, bias)

    own_tokens = own_rows(plan, token_window, rank)
    own_grad = own_rows(plan, grad_window, rank)
    text_mask = own_text.astype(F32)[:, None]
    merged, hidden_b = middle_rows(
        plan, attended, merge_pair, window_text, own_tokens, gate_a, scale_b, shift_b, text_mask
    )
    middle = own_tokens.astype(F32) + pick(gate_a, own_text) * merged
    normed_b, inv_b = layer_norm(middle)

    units = up_pair.shape[2]
    upper, activated = stream_rows(
        plan, up_kernel, 128, units, False, "up", ((units, F32), (units, BF16)), hidden_b, up_pair, window_text
    )
    grad_lowered = (pick(gate_b, is_text) * grad_window.astype(F32)).astype(BF16)
    down_term = weight_terms(plan, activated, grad_lowered, window_text, "down_terms")
    down_term = down_term.reshape(plan.sequences, -1, width)
    down_term, grad_lowered = lax.optimization_barrier((down_term, grad_lowered))
    down_sum = over_sequences_sum(plan, down_term)
    (grad_upper,) = stream_rows(
        plan, down_back_kernel, block_rows(plan.rows, 256), units, True, "down_back", ((units, BF16),),
        grad_lowered, down_pair, window_text, upper,
    )
    up_term = weight_terms(plan, hidden_b, grad_upper, window_text, "up_terms")
    up_term = up_term.reshape(plan.sequences, plan.group, mod_rows, -1)
    grad_upper, up_term = lax.optimization_barrier((grad_upper, up_term))
    up_sum = over_sequences_sum(plan, up_term)
    grad_hidden_b, grad_middle, grad_merged = back_rows(
        plan, grad_upper, up_pair, window_text, own_grad, middle, gate_a, scale_b, text_mask
    )
    merge_term = weight_terms(plan, attended, grad_merged, window_text, "merge_terms")

    grad_projected = attend_back(plan, projected, grad_merged, merge_pair, window_text, bias)
    grad_projected, down_sum = lax.optimization_barrier((grad_projected, down_sum))
    down_grad = down_sum.astype(F32)
    project_term = weight_terms(plan, hidden_a, grad_projected, window_text, "project_terms", mod_rows)
    project_term = project_term.reshape((plan.sequences, plan.group) + project_term.shape[1:])
    grad_projected, project_term = lax.optimization_barrier((grad_projected, project_term))
    project_sum = over_sequences_sum(plan, project_term)

    masks = jnp.stack([own_valid & ~own_text, own_valid & own_text], axis=1).astype(F32)
    rest = jnp.concatenate(
        [
            jnp.stack([jnp.sum(value * masks[:, j : j + 1], axis=0) for j in range(2)])
            for value in (grad_middle * merged, grad_hidden_b, grad_hidden_b * normed_b)
        ],
        axis=1,
    )
    got = last_rows(
        plan,
        merge_term,
        modulation_weight,
        activated=activated,
        down_pair=down_pair,
        grads=grad_projected,
        project_pair=project_pair,
        window_text=window_text,
        tokens=own_tokens,
        middle=middle,
        grad=own_grad,
        grad_middle=grad_middle,
        gate_b=gate_b,
        scale_a=scale_a,
        text=text_mask,
        masks=masks,
        rest=rest,
    )
    foreign = (row_seq != seq)[:, None]
    layer_out = jnp.where(foreign, got.layer_extra, got.layer)
    tokens_grad = jnp.where(foreign, got.token_extra, got.token)
    own_grads = got.table.astype(BF16)
    modulation_grad = lax.dot_general(silu_part, own_grads, CONTRACT_FIRST, preferred_element_type=F32)
    everyone = got.everyone.reshape(2, plan.devices // 2, plan.sequences, mod_rows)
    grad_silu = (everyone[0] + everyone[1]).transpose(1, 0, 2).reshape(plan.sequences, width)
    conditioning_grad = jax.vjp(jax.nn.silu, cond_float)[1](grad_silu)[0]
    modulation_grad, up_sum = lax.optimization_barrier((modulation_grad, up_sum))
    merge_out, project_sum, *done = lax.optimization_barrier(
        (got.term, project_sum, modulation_grad, down_grad, layer_out, tokens_grad, conditioning_grad)
    )
    modulation_grad, down_grad, layer_out, tokens_grad, conditioning_grad = done
    up_grad, project_grad, merge_grad = finish(plan, up_sum, project_sum, merge_out)
    merge_grad = merge_grad[0] if merge_grad else merge_sum(plan, merge_out, rank).astype(F32)
    return (
        layer_out,
        tokens_grad,
        conditioning_grad,
        modulation_grad,
        project_grad,
        merge_grad,
        up_grad,
        down_grad,
    )


def solution(mesh):
    shard, whole = P("dev", None), P()
    return jax.shard_map(
        on_device,
        mesh=mesh,
        in_specs=(shard, whole, whole, shard, shard, shard, shard, shard, shard),
        out_specs=(shard, shard, whole, shard, shard, shard, shard, shard),
        check_vma=False,
    )
```

```python
import functools
import types

import jax
import jax.numpy as jnp
import numpy as np
from jax import lax
from jax.experimental import pallas as pl
from jax.experimental.pallas import tpu as pltpu
from jax.sharding import PartitionSpec as P

HEADS = 24
HDIM = 64
IMG = 1024
TXT_MIN = 86
TXT_MAX = 154
EPSILON = 1e-06
F32 = jnp.float32
BF16 = jnp.bfloat16
CONTRACT_LAST = (((1,), (1,)), ((), ()))
PLAIN = (((1,), (0,)), ((), ()))
CONTRACT_FIRST = (((0,), (0,)), ((), ()))
MASKED = -1e30


class Plan:
    def __init__(self, devices, sequences, rows_dev, width):
        self.devices, self.sequences, self.rows_dev, self.width = devices, sequences, rows_dev, width
        self.group = devices // sequences
        self.span = self.group * rows_dev
        mean = self.span - IMG
        up, down = TXT_MAX - mean, mean - TXT_MIN
        drift = 0
        for k in range(sequences + 1):
            drift = max(drift, min(up * k, down * (sequences - k)), min(down * k, up * (sequences - k)))
        self.edge = -(-drift // 64) * 64
        self.rows = self.span + 2 * self.edge
        self.piece = 2 * self.edge // self.group
        self.own = rows_dev + self.piece
        self.image_end = -(-(self.edge + drift + IMG) // 128) * 128
        self.text_start = (self.edge - drift + IMG) // 128 * 128
        self.heads = HEADS // self.group
        self.segments = self.edge_segments()
        self.chip_heads = devices == 4 * self.group

    def device_of(self, seq, rank):
        return seq * self.group + rank

    def place_of(self, device):
        return lax.div(device, self.group), lax.rem(device, self.group)

    def seq_groups(self):
        return [[self.device_of(s, r) for r in range(self.group)] for s in range(self.sequences)]

    def rank_groups(self):
        return [[self.device_of(s, r) for s in range(self.sequences)] for r in range(self.group)]

    def edge_row(self, rank):
        half = self.group // 2
        return jnp.where(rank < half, self.piece * rank, self.edge + self.span + self.piece * (rank - half))

    def main_row(self, rank):
        return self.edge + self.rows_dev * rank

    def edge_segments(self):
        found = []
        for rank in range(self.group):
            half = self.group // 2
            first = self.piece * rank - self.edge if rank < half else self.span + self.piece * (rank - half)
            row = 0
            while row < self.piece:
                owner, owner_row = (first + row) // self.rows_dev, (first + row) % self.rows_dev
                count = min(self.piece - row, self.rows_dev - owner_row)
                found.append((rank, row, count, owner // self.group, owner % self.group, owner_row))
                row += count
        return found


def layer_norm(values):
    mean = jnp.mean(values, axis=-1, keepdims=True)
    centred = values - mean
    variance = jnp.mean(centred * centred, axis=-1, keepdims=True)
    inv_std = lax.rsqrt(variance + EPSILON)
    return (centred * inv_std, inv_std)


def norm_back(grad_normed, normed, inv_std):
    mean_grad = jnp.mean(grad_normed, axis=-1, keepdims=True)
    mean_cross = jnp.mean(grad_normed * normed, axis=-1, keepdims=True)
    return inv_std * (grad_normed - mean_grad - normed * mean_cross)


def softmax_parts(query, key, bias):
    scores = lax.dot_general(query, key, CONTRACT_LAST, preferred_element_type=F32) + bias
    top = jnp.max(scores, axis=1, keepdims=True)
    exponent = jnp.exp(scores - top)
    total = jnp.sum(exponent, axis=1, keepdims=True)
    return exponent * (1.0 / total)


def head_columns(heads, part, head):
    first = (part * heads + head) * HDIM
    return slice(first, first + HDIM)


def attend_kernel(heads, block, projected, bias_ref, out_ref):
    rows = pl.ds(pl.multiple_of(pl.program_id(0) * block, block), block)
    bias = bias_ref[...]
    outs = []
    for head in range(heads):
        query = projected[rows, head_columns(heads, 0, head)] * jnp.asarray(HDIM ** (-0.5), BF16)
        probs = softmax_parts(query, projected[:, head_columns(heads, 1, head)], bias).astype(BF16)
        outs.append(jnp.dot(probs, projected[:, head_columns(heads, 2, head)], preferred_element_type=F32))
    out_ref[...] = jnp.concatenate(outs, axis=1).astype(BF16)


def block_rows(rows, most):
    return most if rows % most == 0 else 128


def constant(shape):
    return pl.BlockSpec(shape, lambda i: (0,) * len(shape))


def attend(plan, projected, bias):
    rows, cols = projected.shape[0], projected.shape[1] // 3
    block = block_rows(rows, 128)
    return pl.pallas_call(
        functools.partial(attend_kernel, plan.heads, block),
        out_shape=jax.ShapeDtypeStruct((rows, cols), BF16),
        grid=(rows // block,),
        in_specs=[constant(projected.shape), constant(bias.shape)],
        out_specs=pl.BlockSpec((block, cols), lambda i: (i, 0)),
        compiler_params=pltpu.CompilerParams(vmem_limit_bytes=48 << 20),
        cost_estimate=pl.CostEstimate(flops=16 * rows * rows * cols, bytes_accessed=8 * rows * cols, transcendentals=0),
        name="attend",
    )(projected, bias)


def attend_back_kernel(
    heads, steps, block, projected, grad_merged, merge_pair, text, bias_ref, out, key_sum, value_sum
):
    step = pl.program_id(0)
    scale = jnp.asarray(HDIM ** (-0.5), BF16)

    @pl.when(step == 0)
    def _():
        key_sum[...] = jnp.zeros_like(key_sum)
        value_sum[...] = jnp.zeros_like(value_sum)

    rows = pl.ds(pl.multiple_of(step * block, block), block)
    bias = bias_ref[...]
    image, other_stream = [
        lax.dot_general(grad_merged[...], merge_pair[j], CONTRACT_LAST, preferred_element_type=F32) for j in range(2)
    ]
    grad_attended = jnp.where(text[...] > 0, other_stream, image).astype(BF16)
    grads = []
    for head in range(heads):
        query = projected[rows, head_columns(heads, 0, head)] * scale
        key = projected[:, head_columns(heads, 1, head)]
        grad_out = grad_attended[:, head * HDIM : (head + 1) * HDIM]
        probs = softmax_parts(query, key, bias)
        grad_probs = lax.dot_general(
            grad_out, projected[:, head_columns(heads, 2, head)], CONTRACT_LAST, preferred_element_type=F32
        )
        inner = jnp.sum(probs * grad_probs, axis=1, keepdims=True)
        grad_scores = (probs * (grad_probs - inner)).astype(BF16)
        grads.append(jnp.dot(grad_scores, key, preferred_element_type=F32) * HDIM ** (-0.5))
        key_sum[head] += lax.dot_general(query, grad_scores, CONTRACT_FIRST, preferred_element_type=F32)
        value_sum[head] += lax.dot_general(grad_out, probs.astype(BF16), CONTRACT_FIRST, preferred_element_type=F32)
    cols = heads * HDIM
    out[rows, :cols] = jnp.concatenate(grads, axis=1).astype(BF16)

    @pl.when(step == steps - 1)
    def _():
        total = out.shape[0]
        out[:, cols : 2 * cols] = key_sum[...].reshape(cols, total).T.astype(BF16)
        out[:, 2 * cols :] = value_sum[...].reshape(cols, total).T.astype(BF16)


def attend_back(plan, projected, grad_merged, merge_pair, text, bias):
    rows, cols = projected.shape[0], projected.shape[1] // 3
    block = block_rows(rows, 256)
    return pl.pallas_call(
        functools.partial(attend_back_kernel, plan.heads, rows // block, block),
        out_shape=jax.ShapeDtypeStruct(projected.shape, BF16),
        grid=(rows // block,),
        in_specs=[
            constant(projected.shape),
            pl.BlockSpec((block, plan.width), lambda i: (i, 0)),
            constant(merge_pair.shape),
            pl.BlockSpec((block, 1), lambda i: (i, 0)),
            constant(bias.shape),
        ],
        out_specs=constant(projected.shape),
        scratch_shapes=[pltpu.VMEM((plan.heads, HDIM, rows), F32)] * 2,
        compiler_params=pltpu.CompilerParams(vmem_limit_bytes=56 << 20),
        cost_estimate=pl.CostEstimate(flops=40 * rows * rows * cols, bytes_accessed=14 * rows * cols, transcendentals=0),
        name="attend_back",
    )(projected, grad_merged, merge_pair, text, bias)


def fold_rows(piece):
    half = piece.shape[0] // 2
    return jnp.concatenate([piece[:half], piece[half:]], axis=1)


def unfold_rows(piece):
    half = piece.shape[1] // 2
    return jnp.concatenate([piece[:, :half], piece[:, half:]], axis=0)


def terms_kernel(plan, fold, chunk, rows, grads, text, out, kept):
    width = rows.shape[1]
    for stream, (first, last) in enumerate(((0, plan.image_end), (plan.text_start, plan.rows))):
        count = last - first
        mask = text[pl.ds(first, count)]
        keep = (mask > 0) if stream else (mask <= 0)
        kept[pl.ds(0, count)] = jnp.where(keep, grads[pl.ds(first, count)], jnp.zeros((), BF16))

        def step(i, carry):
            start = pl.multiple_of(i * chunk, chunk)
            term = lax.dot_general(
                rows[pl.ds(first, count), pl.ds(start, chunk)],
                kept[pl.ds(0, count)],
                CONTRACT_FIRST,
                preferred_element_type=F32,
            ).astype(BF16)
            if fold:
                for j in range(chunk // fold):
                    out[(stream * width) // fold + i * (chunk // fold) + j] = fold_rows(term[j * fold : (j + 1) * fold])
            else:
                out[stream, pl.ds(start, chunk)] = term
            return carry

        if width == chunk:
            step(0, 0)
        else:
            lax.fori_loop(0, width // chunk, step, 0)


def weight_terms(plan, rows, grads, text, name, fold=0):
    width, cols = rows.shape[1], grads.shape[1]
    chunk = 384 if width % 384 == 0 else width
    shape = (2 * width // fold, fold // 2, 2 * cols) if fold else (2, width, cols)
    return pl.pallas_call(
        functools.partial(terms_kernel, plan, fold, chunk),
        out_shape=jax.ShapeDtypeStruct(shape, BF16),
        in_specs=[pl.BlockSpec(memory_space=pltpu.VMEM)] * 3,
        out_specs=pl.BlockSpec(memory_space=pltpu.VMEM),
        scratch_shapes=[pltpu.VMEM((plan.image_end, cols), BF16)],
        compiler_params=pltpu.CompilerParams(vmem_limit_bytes=40 << 20),
        cost_estimate=pl.CostEstimate(flops=3 * plan.rows * width * cols, bytes_accessed=1 << 23, transcendentals=0),
        name=name,
    )(rows, grads, text)


def gelu(values):
    return jax.nn.gelu(values, approximate=True)


def in_blocks(plan, size, body):
    def step(i, carry):
        body(i, pl.ds(pl.multiple_of(i * size, size), size))
        return carry

    lax.fori_loop(0, plan.rows // size, step, 0)


def blockwise(plan, i, size, block, pair, dims, mask, out):
    @pl.when(i * size < plan.image_end)
    def _():
        out[...] = lax.dot_general(block, pair[0], dims, preferred_element_type=F32)

    @pl.when(i * size + size > plan.text_start)
    def _():
        out[...] = jnp.where(mask > 0, lax.dot_general(block, pair[1], dims, preferred_element_type=F32), out[...])


def project_kernel(plan, size, rows, pair, text, shift, scale, hidden, out, held):
    def body(i, place):
        mask = text[place]
        normed, _ = norm_rows(rows[place].astype(F32))
        block = (normed * (1.0 + pick_rows(scale[...], mask)) + pick_rows(shift[...], mask)).astype(BF16)
        hidden[place] = block
        blockwise(plan, i, size, block, pair, PLAIN, mask, held)
        out[place] = held[...].astype(BF16)

    in_blocks(plan, size, body)


def up_kernel(plan, size, rows, pair, text, upper, activated):
    def body(i, place):
        blockwise(plan, i, size, rows[place], pair, PLAIN, text[place], upper.at[place])
        activated[place] = gelu(upper[place]).astype(BF16)

    in_blocks(plan, size, body)


def down_back_kernel(plan, size, rows, pair, text, upper, out, held):
    def body(i, place):
        blockwise(plan, i, size, rows[place], pair, CONTRACT_LAST, text[place], held)
        out[place] = jax.vjp(gelu, upper[place])[1](held[...])[0].astype(BF16)

    in_blocks(plan, size, body)


def stream_rows(plan, kernel, size, cols, held, name, outs, *operands):
    spec = pl.BlockSpec(memory_space=pltpu.VMEM)
    shapes = tuple(jax.ShapeDtypeStruct((plan.rows, width), dtype) for width, dtype in outs)
    return pl.pallas_call(
        functools.partial(kernel, plan, size),
        out_shape=shapes,
        in_specs=[spec] * len(operands),
        out_specs=(spec,) * len(shapes),
        scratch_shapes=[pltpu.VMEM((size, cols), F32)] if held else [],
        compiler_params=pltpu.CompilerParams(vmem_limit_bytes=40 << 20),
        cost_estimate=pl.CostEstimate(
            flops=2 * plan.rows * plan.width * cols, bytes_accessed=1 << 24, transcendentals=0
        ),
        name=name,
    )(*operands)


VMEM = pl.BlockSpec(memory_space=pltpu.VMEM)


def own_rows(plan, window, rank):
    main = lax.dynamic_slice_in_dim(window, plan.main_row(rank), plan.rows_dev, 0)
    edge = lax.dynamic_slice_in_dim(window, plan.edge_row(rank), plan.piece, 0)
    return jnp.concatenate([main, edge], axis=0)


def remote(source, target, send_sem, recv_sem, device):
    return pltpu.make_async_remote_copy(
        src_ref=source,
        dst_ref=target,
        send_sem=send_sem,
        recv_sem=recv_sem,
        device_id=(device,),
        device_id_type=pl.DeviceIdType.MESH,
    )


def here(plan):
    return plan.place_of(lax.axis_index("dev"))


def other(rank, step, size):
    return lax.rem(rank + step, size)


def meet(devices):
    barrier = pltpu.get_barrier_semaphore()
    for device in devices:
        pl.semaphore_signal(barrier, inc=1, device_id=(device,), device_id_type=pl.DeviceIdType.MESH)
    pl.semaphore_wait(barrier, len(devices))


def group_devices(plan, seq, rank):
    return [plan.device_of(seq, other(rank, step, plan.group)) for step in range(1, plan.group)]


def column_devices(plan, seq, rank):
    return [plan.device_of(other(seq, step, plan.sequences), rank) for step in range(1, plan.sequences)]


def every_device(plan, device):
    return [other(device, step, plan.devices) for step in range(1, plan.devices)]


def call(kernel, name, ident, out_shape, scratch, operands, in_specs=None, out_specs=None, vmem=40 << 20):
    outs = out_shape if isinstance(out_shape, tuple) else (out_shape,)
    return pl.pallas_call(
        kernel,
        out_shape=out_shape,
        in_specs=in_specs or [VMEM] * len(operands),
        out_specs=out_specs or (tuple([VMEM] * len(outs)) if isinstance(out_shape, tuple) else VMEM),
        scratch_shapes=scratch,
        compiler_params=pltpu.CompilerParams(
            collective_id=ident, has_side_effects=True, vmem_limit_bytes=vmem
        ),
        name=name,
    )(*operands)


def aligned(start):
    return pl.multiple_of(start, 16)


def block_parts(plan, ref, rank):
    return (
        ref.at[pl.ds(aligned(plan.main_row(rank)), plan.rows_dev)],
        ref.at[pl.ds(aligned(plan.edge_row(rank)), plan.piece)],
    )


def own_parts(plan, ref):
    return ref.at[pl.ds(0, plan.rows_dev)], ref.at[pl.ds(plan.rows_dev, plan.piece)]


def load_block(plan, ref, rank):
    main, edge = block_parts(plan, ref, rank)
    return jnp.concatenate([main[...], edge[...]], axis=0)


def sum_scratch(plan, wire=BF16):
    half, own, width = plan.group // 2, plan.own, plan.width
    return [
        pltpu.VMEM((half + 1, own, width), F32),
        pltpu.VMEM((half, own, width), F32),
        pltpu.VMEM((half - 1, own, width), wire),
        pltpu.VMEM((half - 1, own, width), wire),
        pltpu.SemaphoreType.DMA((half,)),
        pltpu.SemaphoreType.DMA((half,)),
        pltpu.SemaphoreType.DMA((half,)),
        pltpu.SemaphoreType.DMA((half,)),
    ]


SUM_SCRATCH = 8


def product(plan, rows, pair, text, dims, rank, out):
    block = load_block(plan, rows, rank)
    text_row = load_block(plan, text, rank) > 0
    chunk = 256

    def step(i, carry):
        cols = pl.ds(pl.multiple_of(i * chunk, chunk), chunk)
        parts = []
        for stream in range(2):
            weight = pair[stream, cols, :] if dims is CONTRACT_LAST else pair[stream, :, cols]
            parts.append(lax.dot_general(block, weight, dims, preferred_element_type=F32))
        out[:, cols] = jnp.where(text_row, parts[1], parts[0])
        return carry

    lax.fori_loop(0, plan.width // chunk, step, 0)


def scatter_start(plan, seq, rank, rows, pair, text, dims, away, near, going, coming,
                  pair_send, pair_recv, far_send, far_recv):
    half = plan.group // 2
    chip, core = lax.div(rank, 2), lax.rem(rank, 2)
    partner = plan.device_of(seq, 2 * chip + 1 - core)
    order = list(range(1, half)) + [0]

    def pair_copy(step):
        return remote(away.at[step], near.at[step], pair_send.at[step], pair_recv.at[step], partner)

    def far_copy(step):
        to = plan.device_of(seq, 2 * other(chip, step, half) + core)
        return remote(going.at[step - 1], coming.at[step - 1], far_send.at[step], far_recv.at[step], to)

    def turn(i, carry):
        for_partner = (i < 2) | (lax.rem(i, 2) == 1) & (i < 2 * half - 1)
        place = jnp.where(i < 2, i, jnp.where(for_partner, lax.div(i + 1, 2), lax.div(i, 2) - 1))
        place = jnp.where(i == 2 * half - 1, half - 1, place)
        step = other(place, 1, half)
        block = 2 * other(chip, step, half) + jnp.where(for_partner, 1 - core, core)
        product(plan, rows, pair, text, dims, block, away.at[jnp.where(for_partner, step, half)])

        @pl.when(for_partner)
        def _():
            pair_copy(step).start()

        @pl.when(jnp.logical_not(for_partner))
        def _():
            pair_copy(step).wait_recv()
            away[half] = away[half] + near[step]

        @pl.when(jnp.logical_not(for_partner) & (place < half - 1))
        def _():
            going[step - 1] = away[half].astype(going.dtype)
            far_copy(step).start()

        return carry

    lax.fori_loop(0, 2 * half, turn, 0)

    def result(use):
        for step in range(1, half):
            far_copy(step).wait_recv()
        size = 32 if plan.own % 32 == 0 else 16

        def some(i, carry):
            place = pl.ds(pl.multiple_of(i * size, size), size)
            total = away[half, place]
            for step in range(1, half):
                total = total + coming[step - 1, place].astype(F32)
            use(place, total)
            return carry

        lax.fori_loop(0, plan.own // size, some, 0)
        for step in range(half):
            pair_copy(step).wait_send()
        for step in range(1, half):
            far_copy(step).wait_send()

    return result


def share_scratch(plan):
    return [pltpu.SemaphoreType.DMA((plan.group, 2))] * 2 + [pltpu.SemaphoreType.DMA((plan.group, 2))]


def share_rows(plan, seq, rank, parts, window, send, recv, pass_send):
    half = plan.group // 2
    chip, core = lax.div(rank, 2), lax.rem(rank, 2)
    partner_rank = 2 * chip + 1 - core
    partner = plan.device_of(seq, partner_rank)

    def send_own(to_device, slot):
        copies = [
            remote(source, target, send.at[slot, i], recv.at[slot, i], to_device)
            for i, (source, target) in enumerate(zip(parts, block_parts(plan, window, rank)))
        ]
        for copy in copies:
            copy.start()
        return copies

    flying = {}
    for step in range(1, half):
        flying[step] = send_own(plan.device_of(seq, 2 * other(chip, step, half) + core), step)
    flying[0] = send_own(partner, 0)
    for source, target in zip(parts, block_parts(plan, window, rank)):
        target[...] = source[...]
    passed = []
    for step in range(1, half):
        for copy in flying[step]:
            copy.wait_recv()
        came = 2 * other(chip, half - step, half) + core
        copies = [
            remote(place, place, pass_send.at[step, i], recv.at[half + step, i], partner)
            for i, place in enumerate(block_parts(plan, window, came))
        ]
        for copy in copies:
            copy.start()
        passed.extend(copies)
    for copy in flying[0]:
        copy.wait_recv()
    for copy in passed:
        copy.wait_recv()
    for copies in flying.values():
        for copy in copies:
            copy.wait_send()
    for copy in passed:
        copy.wait_send()


def entry_kernel(plan, tokens, grads, mod_part, *refs):
    if plan.chip_heads:
        merge, merge_out, *refs = refs[:1] + refs[4:5] + refs[1:4] + refs[5:]
        merge_send, merge_recv, *refs = refs[-2:] + refs[:-2]
    (token_window, grad_window, mods, token_own, grad_own, plane, across, chunk, edge_send, edge_recv,
     t_send, t_recv, t_pass, g_send, g_recv, g_pass, m_send, m_recv) = refs
    device = lax.axis_index("dev")
    seq, rank = plan.place_of(device)
    meet(every_device(plan, device))
    swaps = []
    if plan.chip_heads:
        core = lax.rem(rank, 2)
        partner = plan.device_of(seq, 2 * lax.div(rank, 2) + 1 - core)
        for stream in range(2):
            copy = remote(
                merge.at[2 * stream + 1 - core],
                merge_out.at[stream, core],
                merge_send.at[stream],
                merge_recv.at[stream],
                partner,
            )
            copy.start()
            swaps.append(copy)
            merge_out[stream, core] = merge[2 * stream + core]
    hops = []
    for step in range(1, plan.group):
        to = other(rank, step, plan.group)
        copy = remote(mod_part.at[to], plane.at[step], m_send.at[0, step], m_recv.at[0, step], plan.device_of(seq, to))
        copy.start()
        hops.append(copy)
    arrays = ((tokens, token_own), (grads, grad_own))
    count = len(plan.segments)
    for which, (source, own) in enumerate(arrays):
        for index, (to_rank, row, rows, step, owner, owner_row) in enumerate(plan.segments):
            @pl.when(rank == owner)
            def _():
                remote(
                    source.at[pl.ds(owner_row, rows)],
                    own.at[pl.ds(row, rows)],
                    edge_send.at[which * count + index],
                    edge_recv.at[which * count + index],
                    plan.device_of(lax.rem(seq + plan.sequences - step, plan.sequences), to_rank),
                ).start()
    for copy in hops:
        copy.wait_recv()
    total = mod_part[rank]
    for step in range(1, plan.group):
        total = total + plane[step]
    plane[0] = total
    hops_across = []
    for step in range(1, plan.sequences):
        to = other(seq, step, plan.sequences)
        copy = remote(plane.at[0, to], across.at[seq], m_send.at[1, step], m_recv.at[1, step], plan.device_of(to, rank))
        copy.start()
        hops_across.append(copy)
    across[seq] = plane[0, seq]
    for which, (source, own) in enumerate(arrays):
        for index, (to_rank, row, rows, step, owner, owner_row) in enumerate(plan.segments):
            @pl.when(rank == to_rank)
            def _():
                remote(
                    source.at[pl.ds(owner_row, rows)],
                    own.at[pl.ds(row, rows)],
                    edge_send.at[which * count + index],
                    edge_recv.at[which * count + index],
                    plan.device_of(lax.rem(seq + plan.sequences + step, plan.sequences), owner),
                ).wait_recv()
    share_rows(plan, seq, rank, (tokens, token_own), token_window, t_send, t_recv, t_pass)
    for copy in hops_across:
        copy.wait_recv()
    half = plan.sequences // 2
    for stream in range(2):
        total = across[stream * half]
        for i in range(1, half):
            total = total + across[stream * half + i]
        chunk[stream] = total
    hops_back = []
    for step in range(1, plan.group):
        to = other(rank, step, plan.group)
        copy = remote(chunk, mods.at[rank], m_send.at[2, step], m_recv.at[2, step], plan.device_of(seq, to))
        copy.start()
        hops_back.append(copy)
    mods[rank] = chunk[...]
    share_rows(plan, seq, rank, (grads, grad_own), grad_window, g_send, g_recv, g_pass)
    for copy in hops_back:
        copy.wait_recv()
    for copy in hops + hops_across + hops_back:
        copy.wait_send()
    for copy in swaps:
        copy.wait()
    for which, (source, own) in enumerate(arrays):
        for index, (to_rank, row, rows, step, owner, owner_row) in enumerate(plan.segments):
            @pl.when(rank == owner)
            def _():
                remote(
                    source.at[pl.ds(owner_row, rows)],
                    own.at[pl.ds(row, rows)],
                    edge_send.at[which * count + index],
                    edge_recv.at[which * count + index],
                    plan.device_of(lax.rem(seq + plan.sequences - step, plan.sequences), to_rank),
                ).wait_send()


def entry(plan, tokens, grads, mod_part, merge):
    lanes = mod_part.shape[1] // plan.group // 128
    pieces = mod_part.reshape(plan.sequences, plan.group, lanes, 128).transpose(1, 0, 2, 3)
    window = jax.ShapeDtypeStruct((plan.rows, plan.width), BF16)
    dma = pltpu.SemaphoreType.DMA
    most = max(plan.group, plan.sequences)
    shapes = (window, window, jax.ShapeDtypeStruct((plan.group, 2, lanes, 128), F32))
    operands = (tokens, grads, pieces)
    scratch = (
        [
            pltpu.VMEM((plan.piece, plan.width), BF16),
            pltpu.VMEM((plan.piece, plan.width), BF16),
            pltpu.VMEM((plan.group, plan.sequences, lanes, 128), F32),
            pltpu.VMEM((plan.sequences, lanes, 128), F32),
            pltpu.VMEM((2, lanes, 128), F32),
            dma((2 * len(plan.segments),)),
            dma((2 * len(plan.segments),)),
        ]
        + share_scratch(plan)
        + share_scratch(plan)
        + [dma((3, most)), dma((3, most))]
    )
    if plan.chip_heads:
        shapes += (jax.ShapeDtypeStruct((2, 2) + merge.shape[1:], BF16),)
        operands += (merge,)
        scratch += [dma((2,)), dma((2,))]
    token_window, grad_window, mods, *rest = call(
        functools.partial(entry_kernel, plan), "entry", 1, shapes, scratch, operands
    )
    merge_pair = rest[0].reshape(2, -1, plan.width) if plan.chip_heads else merge
    return token_window, grad_window, mods.transpose(1, 0, 2, 3).reshape(2, -1), merge_pair


def project_columns(plan, rank):
    share = plan.width // plan.group
    first = (rank % 2) * (plan.width // 2) + (rank // 2) * share
    return [part * plan.width + first for part in range(3)], share


def up_columns(plan, rank, cols):
    planes = plan.sequences // 2
    share = cols // planes // plan.group
    return [plane * plan.group * share + rank * share for plane in range(planes)], share


def start_swap(plan, seq, rank, source, target, send, recv):
    copies = []
    for step in range(1, plan.group):
        to = other(rank, step, plan.group)
        copy = remote(source.at[to], target.at[rank], send.at[step], recv.at[step], plan.device_of(seq, to))
        copy.start()
        copies.append(copy)
    target[rank] = source[rank]
    return copies


def swap_in_kernel(plan, project, up, project_out, up_out, project_cut, up_cut, p_send, p_recv, u_send, u_recv):
    seq, rank = here(plan)
    for to in range(plan.group):
        starts, share = project_columns(plan, to)
        project_cut[to] = fold_rows(jnp.concatenate([project[:, c : c + share] for c in starts], axis=1))
    meet(group_devices(plan, seq, rank))
    copies = start_swap(plan, seq, rank, project_cut, project_out, p_send, p_recv)
    for to in range(plan.group):
        starts, share = up_columns(plan, to, up.shape[1])
        up_cut[to] = jnp.concatenate([up[:, c : c + share] for c in starts], axis=1)
    copies += start_swap(plan, seq, rank, up_cut, up_out, u_send, u_recv)
    for copy in copies:
        copy.wait()


def swap_in(plan, project, up):
    rows = project.shape[0]
    dma = pltpu.SemaphoreType.DMA
    shapes = [
        (plan.group, rows // 2, 2 * project.shape[1] // plan.group),
        (plan.group, rows, up.shape[1] // plan.group),
    ]
    return call(
        functools.partial(swap_in_kernel, plan),
        "swap_in",
        4,
        tuple(jax.ShapeDtypeStruct(shape, BF16) for shape in shapes),
        [pltpu.VMEM(shape, BF16) for shape in shapes] + [dma((plan.group,))] * 4,
        (project, up),
    )


def place_columns(plan, got, out, columns, unfold):
    for source in range(plan.group):
        starts, share = columns(plan, source)
        piece = unfold_rows(got[source]) if unfold else got[source]
        for i, c in enumerate(starts):
            out[:, c : c + share] = piece[:, i * share : (i + 1) * share]


def line_sum(plan, seq, rank, term, out, up_in, up_out, down_in, down_out, up_send, up_recv, down_send, down_recv):
    count = plan.sequences

    def hop(source, target, send, recv, owner, to):
        return remote(source.at[owner], target.at[owner], send.at[owner], recv.at[owner], plan.device_of(to, rank))

    above, below = lax.rem(seq + 1, count), lax.rem(seq + count - 1, count)
    ways = [
        (list(range(count - 1, 0, -1)), above, below, up_in, up_out, up_send, up_recv, lambda owner: seq < owner, seq == 0),
        (list(range(count - 1)), below, above, down_in, down_out, down_send, down_recv, lambda owner: seq > owner,
         seq == count - 1),
    ]
    def pass_on(turn, way):
        owners, to, back, came, goes, send, recv, mine, first = way
        owner = owners[turn]

        @pl.when(mine(owner) & first)
        def _():
            hop(term, came, send, recv, owner, to).start()

        @pl.when(mine(owner) & jnp.logical_not(first))
        def _():
            hop(goes, came, send, recv, owner, back).wait_recv()
            goes[owner] = (term[owner].astype(F32) + came[owner].astype(F32)).astype(BF16)
            hop(goes, came, send, recv, owner, to).start()

    for turn in range(count - 1):
        @pl.when(seq < count // 2)
        def _():
            pass_on(turn, ways[0])
            pass_on(turn, ways[1])

        @pl.when(seq >= count // 2)
        def _():
            pass_on(turn, ways[1])
            pass_on(turn, ways[0])

    out[...] = term[seq].astype(F32)
    for owners, to, back, came, goes, send, recv, mine, first in ways:
        for owner in owners:
            @pl.when(seq == owner)
            def _():
                hop(goes, came, send, recv, owner, back).wait_recv()
                out[...] += came[owner].astype(F32)

            @pl.when(mine(owner))
            def _():
                hop(goes, came, send, recv, owner, to).wait_send()


def finish_kernel(plan, up, project, *refs):
    if plan.chip_heads:
        term, up_out, project_out, merge_out, *refs = refs
        *refs, line = refs[:6] + [refs[6:]]
    else:
        up_out, project_out, *refs = refs
    up_got, project_got, u_send, u_recv, p_send, p_recv = refs
    seq, rank = here(plan)
    meet(group_devices(plan, seq, rank) + column_devices(plan, seq, rank))
    ups = start_swap(plan, seq, rank, up, up_got, u_send, u_recv)
    projects = start_swap(plan, seq, rank, project, project_got, p_send, p_recv)
    if plan.chip_heads:
        line_sum(plan, seq, rank, term, merge_out, *line)
    for copy in ups:
        copy.wait()
    place_columns(plan, up_got, up_out, lambda p, r: up_columns(p, r, up_out.shape[1]), False)
    for copy in projects:
        copy.wait()
    place_columns(plan, project_got, project_out, project_columns, True)


def finish(plan, up, project, term):
    dma = pltpu.SemaphoreType.DMA
    rows = up.shape[1]
    shapes = (
        jax.ShapeDtypeStruct((rows, plan.group * up.shape[2]), BF16),
        jax.ShapeDtypeStruct((rows, plan.group * project.shape[2] // 2), BF16),
    )
    operands = (up, project)
    scratch = [pltpu.VMEM(up.shape, BF16), pltpu.VMEM(project.shape, BF16)] + [dma((plan.group,))] * 4
    if plan.chip_heads:
        shapes += (jax.ShapeDtypeStruct(term.shape[1:], F32),)
        operands += (term,)
        scratch += [pltpu.VMEM(term.shape, BF16)] * 4 + [dma((plan.sequences,))] * 4
    up_grad, project_grad, *merge_grad = call(
        functools.partial(finish_kernel, plan), "finish", 6, shapes, scratch, operands
    )
    return up_grad.astype(F32), project_grad.astype(F32), merge_grad


def pick_rows(table, text):
    return jnp.where(text > 0, table[1:2, :], table[0:1, :])


def norm_rows(values):
    mean = jnp.mean(values, axis=1, keepdims=True)
    centred = values - mean
    inv = lax.rsqrt(jnp.mean(centred * centred, axis=1, keepdims=True) + EPSILON)
    return centred * inv, inv


def middle_kernel(plan, rows, pair, window_text, tokens, gate_a, scale_b, shift_b, text, merged, window, own, *scratch):
    seq, rank = here(plan)
    meet(group_devices(plan, seq, rank))
    result = scatter_start(plan, seq, rank, rows, pair, window_text, PLAIN, *scratch[:SUM_SCRATCH])

    def use(place, total):
        merged[place] = total
        mask = text[place]
        middle = tokens[place].astype(F32) + pick_rows(gate_a[...], mask) * total
        normed, _ = norm_rows(middle)
        own[place] = (normed * (1.0 + pick_rows(scale_b[...], mask)) + pick_rows(shift_b[...], mask)).astype(BF16)

    result(use)
    share_rows(plan, seq, rank, own_parts(plan, own), window, *scratch[SUM_SCRATCH:])


def own_shape(plan, dtype=F32):
    return jax.ShapeDtypeStruct((plan.own, plan.width), dtype)


def window_shape(plan):
    return jax.ShapeDtypeStruct((plan.rows, plan.width), BF16)


def middle_rows(plan, rows, pair, window_text, tokens, gate_a, scale_b, shift_b, text):
    return call(
        functools.partial(middle_kernel, plan),
        "middle",
        2,
        (own_shape(plan), window_shape(plan)),
        [pltpu.VMEM((plan.own, plan.width), BF16)] + sum_scratch(plan, F32) + share_scratch(plan),
        (rows, pair, window_text, tokens, gate_a, scale_b, shift_b, text),
    )


def back_kernel(plan, rows, pair, window_text, grad, middle, gate_a, scale_b, text, grad_hidden, grad_middle, window, own, *scratch):
    seq, rank = here(plan)
    meet(group_devices(plan, seq, rank))
    result = scatter_start(plan, seq, rank, rows, pair, window_text, CONTRACT_LAST, *scratch[:SUM_SCRATCH])

    def use(place, total):
        grad_hidden[place] = total
        mask = text[place]
        normed, inv = norm_rows(middle[place])
        inner = total * (1.0 + pick_rows(scale_b[...], mask))
        mean_grad = jnp.mean(inner, axis=1, keepdims=True)
        mean_cross = jnp.mean(inner * normed, axis=1, keepdims=True)
        back = grad[place].astype(F32) + inv * (inner - mean_grad - normed * mean_cross)
        grad_middle[place] = back
        own[place] = (pick_rows(gate_a[...], mask) * back).astype(BF16)

    result(use)
    share_rows(plan, seq, rank, own_parts(plan, own), window, *scratch[SUM_SCRATCH:])


def back_rows(plan, rows, pair, window_text, grad, middle, gate_a, scale_b, text):
    return call(
        functools.partial(back_kernel, plan),
        "back",
        3,
        (own_shape(plan), own_shape(plan), window_shape(plan)),
        [pltpu.VMEM((plan.own, plan.width), BF16)] + sum_scratch(plan) + share_scratch(plan),
        (rows, pair, window_text, grad, middle, gate_a, scale_b, text),
    )


def edge_copy(plan, seq, source, first_row, target, send, recv, index):
    from_rank, row, rows, step, owner, owner_row = plan.segments[index]
    return remote(
        source.at[pl.ds(first_row + row, rows)],
        target.at[pl.ds(owner_row, rows)],
        send.at[index],
        recv.at[index],
        plan.device_of(lax.rem(seq + plan.sequences + step, plan.sequences), owner),
    )


def start_edges(plan, seq, rank, *refs):
    for index, segment in enumerate(plan.segments):
        @pl.when(rank == segment[0])
        def _():
            edge_copy(plan, seq, *refs, index).start()


def finish_edges(plan, seq, rank, *refs):
    for index, segment in enumerate(plan.segments):
        @pl.when(rank == segment[4])
        def _():
            edge_copy(plan, seq, *refs, index).wait_recv()

        @pl.when(rank == segment[0])
        def _():
            edge_copy(plan, seq, *refs, index).wait_send()


def edge_scratch(plan):
    return [pltpu.SemaphoreType.DMA((len(plan.segments),))] * 2


def stream_sums(values, masks):
    return jnp.concatenate([jnp.sum(values * mask, axis=0, keepdims=True) for mask in masks], axis=0)


def last_kernel(plan, names, *refs):
    at = types.SimpleNamespace(**dict(zip(names, refs)))
    low_scratch = refs[len(names) : len(names) + SUM_SCRATCH]
    back_scratch = refs[len(names) + SUM_SCRATCH : len(names) + 2 * SUM_SCRATCH]
    device = lax.axis_index("dev")
    seq, rank = plan.place_of(device)
    stream = lax.div(2 * seq, plan.sequences)
    at.layer_extra[...] = jnp.zeros_like(at.layer_extra)
    at.token_extra[...] = jnp.zeros_like(at.token_extra)
    meet(every_device(plan, device))
    low_sum = scatter_start(plan, seq, rank, at.activated, at.down_pair, at.window_text, PLAIN, *low_scratch)
    back_sum = scatter_start(plan, seq, rank, at.grads, at.project_pair, at.window_text, CONTRACT_LAST, *back_scratch)
    swaps = []
    if plan.chip_heads:
        core = lax.rem(rank, 2)
        partner = plan.device_of(seq, 2 * lax.div(rank, 2) + 1 - core)
        for j in range(2):
            copy = remote(
                at.term.at[j, 1 - core], at.term_out.at[2 * j + core], at.term_send.at[j], at.term_recv.at[j], partner
            )
            copy.start()
            swaps.append(copy)
            at.term_out[2 * j + core] = at.term[j, core]
    width = plan.width
    at.local[...] = jnp.zeros_like(at.local)
    at.local[:, 2 * width : 5 * width] = at.rest[...]

    def add(first, place, values):
        masks = (at.masks[place, 0:1], at.masks[place, 1:2])
        at.local[:, first * width : (first + 1) * width] += stream_sums(values, masks)

    def use_low(place, lowered):
        at.layer_own[place] = (at.middle[place] + pick_rows(at.gate_b[...], at.text[place]) * lowered).astype(BF16)
        add(5, place, at.grad[place].astype(F32) * lowered)

    low_sum(use_low)
    layer_edges = (at.layer_own, plan.rows_dev, at.layer_extra, at.l_send, at.l_recv)
    start_edges(plan, seq, rank, *layer_edges)
    at.layer[...] = at.layer_own[pl.ds(0, plan.rows_dev)]

    def use_back(place, total):
        normed, inv = norm_rows(at.tokens[place].astype(F32))
        add(0, place, total)
        add(1, place, total * normed)
        inner = total * (1.0 + pick_rows(at.scale_a[...], at.text[place]))
        mean_grad = jnp.mean(inner, axis=1, keepdims=True)
        mean_cross = jnp.mean(inner * normed, axis=1, keepdims=True)
        at.token_own[place] = at.grad_middle[place] + inv * (inner - mean_grad - normed * mean_cross)

    back_sum(use_back)
    cols = 6 * width // plan.group

    def chunk(index):
        return pl.ds(pl.multiple_of(index * cols, 128), cols)

    hops = []
    for step in range(1, plan.group):
        to = other(rank, step, plan.group)
        copy = remote(
            at.local.at[:, chunk(to)], at.first.at[step], at.t_send.at[0, step], at.t_recv.at[0, step], plan.device_of(seq, to)
        )
        copy.start()
        hops.append(copy)
    token_edges = (at.token_own, plan.rows_dev, at.token_extra, at.e_send, at.e_recv)
    start_edges(plan, seq, rank, *token_edges)
    for copy in hops:
        copy.wait_recv()
    sums = at.local[:, chunk(rank)]
    for step in range(1, plan.group):
        sums = sums + at.first[step]
    for i in range(2):
        at.mine[i] = sums[i : i + 1]
    across = []
    for step in range(1, plan.sequences):
        to = other(seq, step, plan.sequences)
        to_stream = lax.div(2 * to, plan.sequences)
        copy = remote(
            at.mine.at[to_stream], at.second.at[seq], at.t_send.at[1, step], at.t_recv.at[1, step], plan.device_of(to, rank)
        )
        copy.start()
        across.append(copy)
    at.second[seq] = at.mine[stream]
    at.token[...] = at.token_own[pl.ds(0, plan.rows_dev)]
    for copy in across:
        copy.wait_recv()
    last = []
    for step in range(1, plan.group):
        to = other(rank, step, plan.group)
        copy = remote(at.second, at.table.at[rank], at.t_send.at[2, step], at.t_recv.at[2, step], plan.device_of(seq, to))
        copy.start()
        last.append(copy)
    at.table[rank] = at.second[...]
    for copy in last:
        copy.wait_recv()

    piece = None
    for index in range(plan.group):
        grads = jnp.concatenate([at.table[index, s] for s in range(plan.sequences)], axis=0).astype(BF16)
        part = lax.dot_general(
            grads, at.weight[:, index * cols : (index + 1) * cols], CONTRACT_LAST, preferred_element_type=F32
        )
        piece = part if piece is None else piece + part
    at.piece[...] = piece
    at.everyone[seq, rank] = piece
    spread = []
    for step in range(1, plan.group):
        to = other(rank, step, plan.group)
        copy = remote(
            at.piece, at.everyone.at[seq, rank], at.c_send.at[0, step], at.c_recv.at[0, step], plan.device_of(seq, to)
        )
        copy.start()
        spread.append(copy)
    for copy in spread:
        copy.wait_recv()
    for step in range(1, plan.sequences):
        to = other(seq, step, plan.sequences)
        copy = remote(
            at.everyone.at[seq], at.everyone.at[seq], at.c_send.at[1, step], at.c_recv.at[1, step], plan.device_of(to, rank)
        )
        copy.start()
        spread.append(copy)
    for copy in spread[plan.group - 1 :]:
        copy.wait_recv()
    for copy in hops + across + last + spread:
        copy.wait_send()
    for copy in swaps:
        copy.wait()
    finish_edges(plan, seq, rank, *layer_edges)
    finish_edges(plan, seq, rank, *token_edges)


def last_rows(plan, term, weight, **operands):
    rows, share = weight.shape[0], plan.width // plan.group // 2
    cols = 6 * plan.width // plan.group
    most = max(plan.group, plan.sequences)
    dma = pltpu.SemaphoreType.DMA

    def placed(dtype):
        return jax.ShapeDtypeStruct((plan.rows_dev, plan.width), dtype)

    operands = dict(operands, weight=weight)
    outs = dict(
        layer=placed(BF16),
        layer_extra=placed(BF16),
        token=placed(F32),
        token_extra=placed(F32),
        table=jax.ShapeDtypeStruct((plan.group, plan.sequences, 1, cols), F32),
        everyone=jax.ShapeDtypeStruct((plan.sequences, plan.group, plan.sequences, rows), F32),
    )
    edges = len(plan.segments)
    scratch = dict(
        layer_own=pltpu.VMEM((plan.own, plan.width), BF16),
        token_own=pltpu.VMEM((plan.own, plan.width), F32),
        local=pltpu.VMEM((2, 6 * plan.width), F32),
        first=pltpu.VMEM((plan.group, 2, cols), F32),
        second=pltpu.VMEM((plan.sequences, 1, cols), F32),
        mine=pltpu.VMEM((2, 1, cols), F32),
        piece=pltpu.VMEM((plan.sequences, rows), F32),
        t_send=dma((3, most)),
        t_recv=dma((3, most)),
        c_send=dma((2, most)),
        c_recv=dma((2, most)),
        l_send=dma((edges,)),
        l_recv=dma((edges,)),
        e_send=dma((edges,)),
        e_recv=dma((edges,)),
    )
    if plan.chip_heads:
        operands["term"] = term.reshape(2, 2, share, plan.width)
        outs["term_out"] = jax.ShapeDtypeStruct((plan.sequences, share, plan.width), BF16)
        scratch.update(term_send=dma((2,)), term_recv=dma((2,)))
    names = tuple(operands) + tuple(outs) + tuple(scratch)
    got = call(
        functools.partial(last_kernel, plan, names),
        "last",
        10,
        tuple(outs.values()),
        list(scratch.values()) + sum_scratch(plan) + sum_scratch(plan),
        tuple(operands.values()),
        vmem=58 << 20,
    )
    got = types.SimpleNamespace(**dict(zip(outs, got)))
    got.table = got.table[:, :, 0].transpose(1, 0, 2).reshape(plan.sequences, -1)
    got.term = got.term_out if plan.chip_heads else term
    return got


def over_sequences(plan, pieces):
    full = lax.all_gather(pieces, "dev", axis=0, axis_index_groups=plan.rank_groups())
    return full.reshape((plan.devices,) + pieces.shape[1:])


def over_sequences_sum(plan, pieces):
    return lax.psum_scatter(pieces, "dev", scatter_dimension=0, axis_index_groups=plan.rank_groups())


def merge_rows(plan, weight, rank):
    if plan.chip_heads:
        return lax.all_gather(weight, "dev", axis=0, axis_index_groups=plan.rank_groups())
    share = plan.width // plan.group
    full = lax.all_gather(weight, "dev", axis=0, tiled=True)
    full = full.reshape(2, 2, plan.group // 2, share, weight.shape[1])
    full = lax.dynamic_index_in_dim(full, lax.rem(rank, 2), 1, keepdims=False)
    return lax.dynamic_index_in_dim(full, lax.div(rank, 2), 1, keepdims=False)


def merge_sum(plan, term, rank):
    half = plan.group // 2
    _, share, cols = term.shape
    mine = [jnp.where(lax.rem(rank, 2) == k, term, jnp.zeros((), BF16)) for k in range(2)]
    full = jnp.zeros((2, 2, half, share, cols), BF16)
    full = lax.dynamic_update_slice_in_dim(full, jnp.stack(mine, axis=1)[:, :, None], lax.div(rank, 2), 2)
    return lax.psum_scatter(full.reshape(-1, cols), "dev", scatter_dimension=0, tiled=True)


def down_slices(plan, weight):
    full = lax.all_gather(weight, "dev", axis=0, axis_index_groups=plan.rank_groups())
    return full.reshape(2, -1, weight.shape[1])


def pick(table, text_rows):
    return jnp.where(text_rows[:, None], table[1][None, :], table[0][None, :])


def on_device(
    tokens,
    conditioning,
    text_lengths,
    modulation_weight,
    project_weight,
    merge_weight,
    up_weight,
    down_weight,
    cotangent,
):
    rows_dev, width = tokens.shape
    mod_rows = modulation_weight.shape[0]
    plan = Plan(lax.axis_size("dev"), conditioning.shape[0], rows_dev, width)
    device = lax.axis_index("dev")
    seq, rank = plan.place_of(device)
    feature_start = device * mod_rows % width

    ends = jnp.cumsum(IMG + text_lengths)
    starts = jnp.concatenate([jnp.zeros((1,), jnp.int32), ends[:-1]])
    positions = device * rows_dev + jnp.arange(rows_dev, dtype=jnp.int32)
    row_seq = jnp.sum((starts[None, :] <= positions[:, None]).astype(jnp.int32), axis=1) - 1
    offset = plan.span * seq - plan.edge + jnp.arange(plan.rows, dtype=jnp.int32) - starts[seq]
    valid = (offset >= 0) & (offset < IMG + text_lengths[seq])
    is_text = offset >= IMG
    bias = jnp.where(valid, 0.0, MASKED).astype(F32)[None, :]
    window_text = is_text.astype(F32)[:, None]
    own_valid = own_rows(plan, valid[:, None], rank)[:, 0]
    own_text = own_rows(plan, is_text[:, None], rank)[:, 0]

    cond_float = conditioning.astype(F32)
    silu_low = jax.nn.silu(cond_float).astype(BF16)
    silu_part = lax.dynamic_slice_in_dim(silu_low, feature_start, mod_rows, 1)
    mod_part = jnp.dot(silu_part, modulation_weight, preferred_element_type=F32)

    merge_pair = merge_rows(plan, merge_weight, rank)
    project_pieces, up_pieces = swap_in(plan, project_weight, up_weight)
    project_pieces, up_pieces, merge_pair = lax.optimization_barrier((project_pieces, up_pieces, merge_pair))
    project_pair = over_sequences(plan, project_pieces)
    share = project_pair.shape[2] // 2
    project_pair = jnp.concatenate([project_pair[:, :, :share], project_pair[:, :, share:]], axis=1)
    project_pair = lax.optimization_barrier(project_pair.reshape(2, width, share))
    up_pair = over_sequences(plan, up_pieces).reshape(2, width, -1)
    down_pair = down_slices(plan, down_weight)

    token_window, grad_window, mods, merge_pair = entry(plan, tokens, cotangent, mod_part, merge_pair)
    shift_a, scale_a, gate_a, shift_b, scale_b, gate_b = jnp.split(mods, 6, axis=1)
    grad_window = jnp.where(valid[:, None], grad_window, jnp.zeros((), BF16))

    cols = project_pair.shape[2]
    hidden_a, projected = stream_rows(
        plan, project_kernel, 128, cols, True, "project", ((width, BF16), (cols, BF16)),
        token_window, project_pair, window_text, shift_a, scale_a,
    )
    attended = attend(plan, projected, bias)

    own_tokens = own_rows(plan, token_window, rank)
    own_grad = own_rows(plan, grad_window, rank)
    text_mask = own_text.astype(F32)[:, None]
    merged, hidden_b = middle_rows(
        plan, attended, merge_pair, window_text, own_tokens, gate_a, scale_b, shift_b, text_mask
    )
    middle = own_tokens.astype(F32) + pick(gate_a, own_text) * merged
    normed_b, inv_b = layer_norm(middle)

    units = up_pair.shape[2]
    upper, activated = stream_rows(
        plan, up_kernel, 128, units, False, "up", ((units, F32), (units, BF16)), hidden_b, up_pair, window_text
    )
    grad_lowered = (pick(gate_b, is_text) * grad_window.astype(F32)).astype(BF16)
    down_term = weight_terms(plan, activated, grad_lowered, window_text, "down_terms")
    down_term = down_term.reshape(plan.sequences, -1, width)
    down_term, grad_lowered = lax.optimization_barrier((down_term, grad_lowered))
    down_sum = over_sequences_sum(plan, down_term)
    (grad_upper,) = stream_rows(
        plan, down_back_kernel, block_rows(plan.rows, 256), units, True, "down_back", ((units, BF16),),
        grad_lowered, down_pair, window_text, upper,
    )
    up_term = weight_terms(plan, hidden_b, grad_upper, window_text, "up_terms")
    up_term = up_term.reshape(plan.sequences, plan.group, mod_rows, -1)
    grad_upper, up_term = lax.optimization_barrier((grad_upper, up_term))
    up_sum = over_sequences_sum(plan, up_term)
    grad_hidden_b, grad_middle, grad_merged = back_rows(
        plan, grad_upper, up_pair, window_text, own_grad, middle, gate_a, scale_b, text_mask
    )
    merge_term = weight_terms(plan, attended, grad_merged, window_text, "merge_terms")

    grad_projected = attend_back(plan, projected, grad_merged, merge_pair, window_text, bias)
    grad_projected, down_sum = lax.optimization_barrier((grad_projected, down_sum))
    down_grad = down_sum.astype(F32)
    project_term = weight_terms(plan, hidden_a, grad_projected, window_text, "project_terms", mod_rows)
    project_term = project_term.reshape((plan.sequences, plan.group) + project_term.shape[1:])
    grad_projected, project_term = lax.optimization_barrier((grad_projected, project_term))
    project_sum = over_sequences_sum(plan, project_term)

    masks = jnp.stack([own_valid & ~own_text, own_valid & own_text], axis=1).astype(F32)
    rest = jnp.concatenate(
        [
            jnp.stack([jnp.sum(value * masks[:, j : j + 1], axis=0) for j in range(2)])
            for value in (grad_middle * merged, grad_hidden_b, grad_hidden_b * normed_b)
        ],
        axis=1,
    )
    got = last_rows(
        plan,
        merge_term,
        modulation_weight,
        activated=activated,
        down_pair=down_pair,
        grads=grad_projected,
        project_pair=project_pair,
        window_text=window_text,
        tokens=own_tokens,
        middle=middle,
        grad=own_grad,
        grad_middle=grad_middle,
        gate_b=gate_b,
        scale_a=scale_a,
        text=text_mask,
        masks=masks,
        rest=rest,
    )
    foreign = (row_seq != seq)[:, None]
    layer_out = jnp.where(foreign, got.layer_extra, got.layer)
    tokens_grad = jnp.where(foreign, got.token_extra, got.token)
    own_grads = got.table.astype(BF16)
    modulation_grad = lax.dot_general(silu_part, own_grads, CONTRACT_FIRST, preferred_element_type=F32)
    everyone = got.everyone.reshape(2, plan.devices // 2, plan.sequences, mod_rows)
    grad_silu = (everyone[0] + everyone[1]).transpose(1, 0, 2).reshape(plan.sequences, width)
    conditioning_grad = jax.vjp(jax.nn.silu, cond_float)[1](grad_silu)[0]
    modulation_grad, up_sum = lax.optimization_barrier((modulation_grad, up_sum))
    merge_out, project_sum, *done = lax.optimization_barrier(
        (got.term, project_sum, modulation_grad, down_grad, layer_out, tokens_grad, conditioning_grad)
    )
    modulation_grad, down_grad, layer_out, tokens_grad, conditioning_grad = done
    up_grad, project_grad, merge_grad = finish(plan, up_sum, project_sum, merge_out)
    merge_grad = merge_grad[0] if merge_grad else merge_sum(plan, merge_out, rank).astype(F32)
    return (
        layer_out,
        tokens_grad,
        conditioning_grad,
        modulation_grad,
        project_grad,
        merge_grad,
        up_grad,
        down_grad,
    )


def solution(mesh):
    shard, whole = P("dev", None), P()
    return jax.shard_map(
        on_device,
        mesh=mesh,
        in_specs=(shard, whole, whole, shard, shard, shard, shard, shard, shard),
        out_specs=(shard, shard, whole, shard, shard, shard, shard, shard),
        check_vma=False,
    )
```
